32 devices in a mesh: section: 2 (over core), dp: 16 (over z, y, x).
Axes of the slice: x: 2, y: 2, z: 4, core: 2. Of those that a mesh axis runs over, the one named last changes fastest.
Arguments:
- pixels: bfloat16 [32, 1024, 192], P('dp'), may hold values from -6 to 6
- visible: int32 [32, 256], P('dp'), may hold values from 0 to 1023, as said below
- masked: int32 [32, 768], P('dp'), may hold values from 0 to 1023
- loss_mask: int32 [32, 768], P('dp'), may hold values 0 or 1
- master: float32 [2, 7225344], P('section', 'dp')
- momentum: float32 [2, 7225344], P('section', 'dp'), may hold values from -5.9604645e-07 to 5.9604645e-07
- vectors: float32 [2, 11520], P('section')
- vec_moment: float32 [2, 11520], P('section'), may hold values from -1.9073486e-06 to 1.9073486e-06
- factors: float32 [2, 8, 7680], P('section'), may hold values from -6 to 6
- errors: bfloat16 [2, 16, 7225344], P('section', 'dp'), may hold values from -0.005859375 to 0.005859375
Outputs:
- new_master: float32 [2, 7225344], P('section', 'dp')
- new_low: bfloat16 [2, 7225344], P('section', 'dp')
- new_moment: float32 [2, 7225344], P('section', 'dp')
- new_vectors: float32 [2, 11520], P('section')
- new_vec_moment: float32 [2, 11520], P('section')
- new_factors: float32 [2, 8, 7680], P('section')
- new_errors: float32 [2, 16, 7225344], P('section', 'dp')
- loss: float32 [1], replicated
- grad_norm: float32 [1], replicated
The draws below stay inside these ranges and needn't reach their ends.
Inputs may be any that keep to these rules, and one draw needn't show every extreme that they name: Per sample, visible and masked together hold each token index below 1024 exactly once.
All inputs are finite; a program needn't handle non-finite values. No bound on the sum of `loss_mask` on one device may be relied on, other than what follows from the above.
Results may differ from the reference program's by a relative error of at most 0.0083.
The reference program's roundings to bfloat16 on the way count: a program that leaves them out, or rounds other values in their place, can miss the bound.
Values may be sent and summed in bfloat16 or wider, within the bound.
A program may use at most 512 MiB of HBM per device.

```python
import math
import jax
import jax.numpy as jnp
from jax import lax

DE = 768
FFE = 3072
HEADS_ENC = 12
DD = 512
FFD = 2048
HEADS_DEC = 16
PATCH = 192
RANK = 8
SEQ = 1024
VIS = 256
SAMP_DEV = 2
SAMPLES = 32
MASKED = 768
FLAT = 7225344
VLEN = 11520
QL = 7680
N_DP = 16


def mask_order(key):
    sample_keys = jax.random.split(jax.random.fold_in(key, 17), SAMPLES)
    return jax.vmap(lambda one_key: jax.random.permutation(one_key, SEQ))(sample_keys).astype(jnp.int32)


def draw_visible(key, part):
    return mask_order(key)[:, :VIS]


def draw_masked(key, part):
    return mask_order(key)[:, VIS:]


def section_scales(section):
    if section == 0:
        segments = [(3 * DE * DE, 1.3 * DE ** (-0.5)), (DE * DE, 4.0 * DE ** (-0.5)), (DE * FFE, DE ** (-0.5)), (FFE * DE, FFE ** (-0.5)), (PATCH * DE, PATCH ** (-0.5))]
    else:
        segments = [(3 * DD * DD, 1.3 * DD ** (-0.5)), (DD * DD, 4.0 * DD ** (-0.5)), (DD * FFD, DD ** (-0.5)), (FFD * DD, FFD ** (-0.5)), (PATCH * DD, DD ** (-0.5)), (DE * DD, DE ** (-0.5))]
    where_at = jnp.arange(FLAT)
    scaling = jnp.full((FLAT,), 0.02, jnp.float32)
    start = 0
    for length, value in segments:
        scaling = jnp.where((where_at >= start) & (where_at < start + length), value, scaling)
        start += length
    return scaling


def draw_master(key, part):
    normal_part = jax.random.normal(key, (2, FLAT), jnp.float32)
    return normal_part * jnp.stack([section_scales(0), section_scales(1)])


def vector_row(key, width):
    normal_part = jax.random.normal(key, (VLEN,), jnp.float32)
    uniform_part = jax.random.uniform(jax.random.fold_in(key, 3), (VLEN,), jnp.float32, -1.0, 1.0)
    where_at = jnp.arange(VLEN)
    row_ids = where_at // width
    inside = where_at < 11 * width
    gain_rows = inside & ((row_ids == 0) | (row_ids == 2) | (row_ids == 4))
    token_row = inside & (row_ids == 10)
    return jnp.where(gain_rows, 1.0 + 0.3 * uniform_part, jnp.where(token_row, normal_part, 0.5 * normal_part))


def draw_vectors(key, part):
    return jnp.stack([vector_row(jax.random.fold_in(key, 5), DE), vector_row(jax.random.fold_in(key, 6), DD)])


def with_ends(values, own_key, least, top_value):
    dims = values.shape
    index_at = [jax.random.randint(jax.random.fold_in(own_key, axis), (), 0, dims[axis]) for axis in range(len(dims))]
    values = values.at[tuple(index_at)].set(least)
    longest = dims.index(max(dims))
    index_at[longest] = (index_at[longest] + 1) % dims[longest]
    return values.at[tuple(index_at)].set(top_value)


def shard_levels(own_key, extent, shards, least, high):
    def one(position, blocks):
        heights = jax.random.uniform(jax.random.fold_in(jax.random.fold_in(own_key, 6), position), (blocks,), jnp.float32, least / len(shards), high / len(shards))
        return jnp.repeat(jnp.exp(heights), extent[position] // blocks).reshape((-1,) + (1,) * (len(extent) - position - 1))

    factor_of = one(*shards[0])
    for cut in shards[1:]:
        factor_of = factor_of * one(*cut)
    return factor_of


def gaussian(rng, dims, scale, most, cuts=(), kind=jnp.bfloat16):
    array = scale * jax.random.normal(rng, dims, jnp.float32)
    if cuts:
        array = array * shard_levels(rng, dims, cuts, -0.22, 0.18)
    return jnp.clip(array, -most, most).astype(kind)


def setup_inputs(seed: int = 0) -> dict:
    key_of = jax.random.split(jax.random.key(seed), 11)
    return {
        "pixels": gaussian(key_of[0], (SAMPLES, SEQ, PATCH), 1.0, 6.0, ((0, 16),)),
        "visible": draw_visible(jax.random.fold_in(key_of[10], 71), 0),
        "masked": draw_masked(jax.random.fold_in(key_of[10], 71), 0),
        "loss_mask": with_ends((jax.random.randint(key_of[3], (SAMPLES, MASKED), 0, 4) < 3).astype(jnp.int32), jax.random.fold_in(key_of[3], 1), 0, 1),
        "master": draw_master(jax.random.fold_in(key_of[10], 71), 0),
        "momentum": gaussian(key_of[5], (2, FLAT), (0.00015 * (2 * FLAT) ** -0.5), 5.960464477539062e-07, ((0, 2), (1, 16)), jnp.float32),
        "vectors": draw_vectors(jax.random.fold_in(key_of[10], 71), 0),
        "vec_moment": gaussian(key_of[7], (2, VLEN), (0.0005 * (2 * FLAT) ** -0.5), 1.9073486328125e-06, ((0, 2),), jnp.float32),
        "factors": gaussian(key_of[8], (2, RANK, QL), 1.0, 6.0, ((0, 2),), jnp.float32),
        "errors": gaussian(key_of[9], (2, N_DP, FLAT), (0.015 * (N_DP / (SAMPLES * MASKED)) ** 0.5), 0.005859375, ((0, 2), (1, 16))),
    }


@jax.custom_vjp
def low(v):
    return lax.optimization_barrier(v.astype(jnp.bfloat16)).astype(jnp.float32)

@jax.custom_vjp
def low_back(v):
    return v

def low_keep(v):
    return (low(v), None)

def low_pass(kept, grad):
    return (grad,)

def back_keep(v):
    return (v, None)

def back_low(kept, grad):
    return (low(grad),)
low.defvjp(low_keep, low_pass)
low_back.defvjp(back_keep, back_low)
highest = lax.Precision.HIGHEST
clip_limit = 0.0001
moment_decay = 0.9
rate_base = 0.5

def product(left, right):
    return jnp.dot(left, right, precision=highest)

def layer_norm(tokens, gain, shift):
    centred = tokens - lax.optimization_barrier(jnp.mean(tokens, axis=-1, keepdims=True))
    spread = lax.optimization_barrier(jnp.mean(centred * centred, axis=-1, keepdims=True))
    return centred * lax.rsqrt(spread + 1e-06) * gain + shift

def positions(width):
    places = jnp.arange(SEQ, dtype=jnp.float32)[:, None]
    column = jnp.arange(width)
    freqs = jnp.exp(-(column // 2 * 2).astype(jnp.float32) / width * math.log(10000.0))
    return jnp.sin(places * freqs + (column % 2).astype(jnp.float32) * (math.pi / 2))

def section_shapes(section):
    if section == 0:
        return [(DE, 3 * DE), (DE, DE), (DE, FFE), (FFE, DE), (PATCH, DE)]
    return [(DD, 3 * DD), (DD, DD), (DD, FFD), (FFD, DD), (PATCH, DD), (DE, DD)]

def unpack_mats(flat, shapes):
    pieces = []
    offset = 0
    for rows_n, cols_n in shapes:
        piece = lax.slice_in_dim(flat, offset, offset + rows_n * cols_n, axis=flat.ndim - 1)
        pieces.append(piece.reshape(flat.shape[:-1] + (rows_n, cols_n)))
        offset += rows_n * cols_n
    return pieces

def unpack_vecs(flat, width, hidden):
    return (flat[:11 * width].reshape(11, width), flat[11 * width:11 * width + hidden], flat[11 * width + hidden:12 * width + hidden])

def learning_rate():
    return rate_base * math.sqrt(2.0 * (FLAT + VLEN) / DD) / clip_limit

def orthonormal(left):
    columns = []
    for column in range(RANK):
        vector_now = left[:, column]
        for basis in columns:
            vector_now = vector_now - jnp.sum(basis * vector_now) * basis
        columns.append(vector_now * lax.rsqrt(jnp.sum(vector_now * vector_now) + 1e-12))
    return jnp.stack(columns, axis=1)

def block(tokens, mats, vector_rows, bias_up, head_count):
    width = tokens.shape[1]
    head_size = width // head_count
    normed = low(layer_norm(tokens, vector_rows[0], vector_rows[1]))
    qkv_bias = jnp.concatenate([vector_rows[6], jnp.zeros_like(vector_rows[6]), vector_rows[7]])
    joined = low(low_back(product(normed, mats[0]) + qkv_bias))
    heads_view = joined.reshape(-1, 3, head_count, head_size).transpose(1, 2, 0, 3)
    scores = jnp.einsum('hqd,hkd->hqk', heads_view[0], heads_view[1], precision=highest) * head_size ** (-0.5)
    scores = low_back(scores)
    weights = low(jax.nn.softmax(scores, axis=-1))
    attended = jnp.einsum('hqk,hkd->hqd', weights, heads_view[2], precision=highest)
    attended = low(low_back(attended.transpose(1, 0, 2).reshape(-1, width)))
    middle = tokens + low_back(product(attended, mats[1]) + vector_rows[8])
    second = low(layer_norm(middle, vector_rows[2], vector_rows[3]))
    hidden = low_back(product(second, mats[2]) + bias_up)
    active = low(jax.nn.gelu(hidden, approximate=False))
    return middle + low_back(product(active, mats[3]) + vector_rows[9])

def sample_loss(low_weights, vector_set, sample_pixels, visible_rows, masked_rows, sample_mask, count):
    encoder = unpack_mats(low_weights[0], section_shapes(0))
    decoder = unpack_mats(low_weights[1], section_shapes(1))
    enc_rows, enc_bias, unused = unpack_vecs(vector_set[0], DE, FFE)
    dec_rows, dec_bias, dec_extra = unpack_vecs(vector_set[1], DD, FFD)
    pixel_vals = sample_pixels.astype(jnp.float32)
    embedded = low_back(product(pixel_vals[visible_rows], encoder[4]) + enc_rows[10] + positions(DE)[visible_rows])
    encoded = block(embedded, encoder, enc_rows, enc_bias, HEADS_ENC)
    sent_rows = low(low_back(layer_norm(encoded, enc_rows[4], enc_rows[5])))
    projected = low_back(product(sent_rows, decoder[5]) + dec_extra)
    filled = jnp.zeros((SEQ, DD), jnp.float32).at[visible_rows].set(projected)
    filled = filled.at[masked_rows].set(jnp.broadcast_to(dec_rows[10], (SEQ - VIS, DD))) + positions(DD)
    decoded = block(filled, decoder, dec_rows, dec_bias, HEADS_DEC)
    final_norm = low(layer_norm(decoded[masked_rows], dec_rows[4], dec_rows[5]))
    predicted = low_back(product(final_norm, decoder[4].T))
    errors_sq = lax.optimization_barrier(jnp.mean((predicted - pixel_vals[masked_rows]) ** 2, axis=1))
    return jnp.sum(sample_mask.astype(jnp.float32) * errors_sq) / count

def reference(pixels, visible, masked, loss_mask, master, momentum, vectors, vec_moment, factors, errors):
    count = jnp.sum(loss_mask).astype(jnp.float32)
    low_weights = low(master)

    def replica_grads(replica):

        def replica_loss(weights_in, vectors_in):

            def one_sample(running, sample):
                term = jax.checkpoint(sample_loss)(weights_in, vectors_in, pixels[sample], visible[sample], masked[sample], loss_mask[sample], count)
                return (running + term, None)
            samples_at = replica * SAMP_DEV + jnp.arange(SAMP_DEV, dtype=jnp.int32)
            running, unused = lax.scan(one_sample, jnp.zeros((), jnp.float32), samples_at)
            return running
        value, pullback = jax.vjp(replica_loss, low_weights, vectors)
        grad_w, grad_v = pullback(jnp.ones((), jnp.float32))
        return (value, grad_w, grad_v)
    losses, grad_w, grad_v = lax.map(replica_grads, jnp.arange(N_DP, dtype=jnp.int32))
    merged = N_DP * jnp.swapaxes(grad_w, 0, 1) + errors.astype(jnp.float32)
    vec_grad = lax.optimization_barrier(jnp.sum(grad_v, axis=0))
    squares = jnp.sum(vec_grad * vec_grad)
    approx_rows = []
    factor_rows = []
    for section in range(2):
        shapes = section_shapes(section)
        matrices = unpack_mats(merged[section], shapes)
        col_at = 0
        approx_parts = []
        right_parts = []
        for matrix, (rows_n, cols_n) in zip(matrices, shapes):
            part = factors[section][:, col_at:col_at + cols_n]
            col_at += cols_n
            left = jnp.einsum('nab,kb->ak', matrix, part, precision=highest) / N_DP
            ortho = orthonormal(left)
            right = jnp.einsum('nab,ak->kb', matrix, ortho, precision=highest) / N_DP
            approx = jnp.dot(ortho, right, precision=highest)
            squares = squares + jnp.sum(approx * approx)
            approx_parts.append(approx.reshape(-1))
            right_parts.append(right)
        flat = jnp.concatenate(approx_parts)
        approx_rows.append(jnp.pad(flat, (0, FLAT - flat.shape[0])))
        rights = jnp.concatenate(right_parts, axis=1)
        factor_rows.append(jnp.pad(rights, ((0, 0), (0, QL - rights.shape[1]))))
    flat_approx = jnp.stack(approx_rows)
    norm = jnp.sqrt(squares)
    scale = jnp.minimum(1.0, clip_limit / (norm + 1e-06))
    rate = learning_rate()
    new_moment = moment_decay * momentum + scale * flat_approx
    new_master = master - rate * new_moment
    new_vm = moment_decay * vec_moment + scale * vec_grad
    new_vectors = vectors - rate * new_vm
    new_factors = jnp.stack(factor_rows)
    new_errors = merged - flat_approx[:, None, :]
    total_loss = jnp.sum(losses)
    return (new_master, new_master.astype(jnp.bfloat16), new_moment, new_vectors, new_vm, new_factors, new_errors, total_loss.reshape(1), norm.reshape(1))
```

```python
import functools
import math

import jax
import jax.numpy as jnp
from jax import lax
from jax.experimental import pallas as pl
from jax.experimental.pallas import tpu as pltpu
from jax.sharding import PartitionSpec as P

DE = 768
FFE = 3072
HEADS_ENC = 12
DD = 512
FFD = 2048
HEADS_DEC = 16
PATCH = 192
RANK = 8
SEQ = 1024
VIS = 256
FLAT = 7225344
VLEN = 11520

f32 = jnp.float32
bf16 = jnp.bfloat16
clip_limit = 0.0001
moment_decay = 0.9
rate_base = 0.5
LANES = 128
BIG = 66000000


def nn(left, right):
    return lax.dot_general(left, right, (((1,), (0,)), ((), ())), preferred_element_type=f32)


def nt(left, right):
    return lax.dot_general(left, right, (((1,), (1,)), ((), ())), preferred_element_type=f32)


def tn(left, right):
    return lax.dot_general(left, right, (((0,), (0,)), ((), ())), preferred_element_type=f32)


def split3(value):
    high = value.astype(bf16)
    rest = value - high.astype(f32)
    middle = rest.astype(bf16)
    return jnp.concatenate([high, middle, (rest - middle.astype(f32)).astype(bf16)], axis=0)


def join3(value):
    return value[:RANK] + value[RANK : 2 * RANK] + value[2 * RANK :]


def layer_norm(tokens, gain, shift):
    centred = tokens - jnp.mean(tokens, axis=-1, keepdims=True)
    spread = jnp.mean(centred * centred, axis=-1, keepdims=True)
    return centred * lax.rsqrt(spread + 1e-06) * gain + shift


def positions_at(places, width):
    column = jnp.arange(width)
    freqs = jnp.exp(-(column // 2 * 2).astype(f32) / width * math.log(10000.0))
    return jnp.sin(places.astype(f32)[:, None] * freqs + (column % 2).astype(f32) * (math.pi / 2))


def section_shapes(section):
    if section == 0:
        return [(DE, 3 * DE), (DE, DE), (DE, FFE), (FFE, DE), (PATCH, DE)]
    return [(DD, 3 * DD), (DD, DD), (DD, FFD), (FFD, DD), (PATCH, DD), (DE, DD)]


ROWS_L = [sum(rows for rows, cols in section_shapes(s)) for s in range(2)]
COLS_R = [sum(cols for rows, cols in section_shapes(s)) for s in range(2)]


def unpack_vecs(flat, width, hidden):
    return (
        flat[: 11 * width].reshape(11, width),
        flat[11 * width : 11 * width + hidden],
        flat[11 * width + hidden : 12 * width + hidden],
    )


def learning_rate():
    return rate_base * math.sqrt(2.0 * (FLAT + VLEN) / DD) / clip_limit


def unflat_body(src_ref, out_ref, wide_ref, *, blocks, rows, stacked):
    wide_ref[...] = src_ref[...].astype(f32)
    for block in range(blocks):
        part = wide_ref[pl.ds(block, rows, stride=blocks), :].astype(bf16)
        if stacked:
            out_ref[block] = part
        else:
            out_ref[:, block * LANES : (block + 1) * LANES] = part


def unflat(flat, start, rows_n, cols_n, stacked=False):
    blocks = cols_n // LANES
    rows = 192 if rows_n == PATCH else 128 if blocks > 8 else 256
    if stacked:
        out_shape = jax.ShapeDtypeStruct((blocks, rows_n, LANES), bf16)
        out_spec = pl.BlockSpec((blocks, rows, LANES), lambda i: (0, i, 0))
    else:
        out_shape = jax.ShapeDtypeStruct((rows_n, cols_n), bf16)
        out_spec = pl.BlockSpec((rows, cols_n), lambda i: (i, 0))
    step = rows * blocks
    return pl.pallas_call(
        functools.partial(unflat_body, blocks=blocks, rows=rows, stacked=stacked),
        grid=(rows_n // rows,),
        in_specs=[pl.BlockSpec((pl.Element(step), pl.Element(LANES)), lambda i: (pl.multiple_of(start // LANES + i * step, 16), 0))],
        out_specs=out_spec,
        out_shape=out_shape,
        scratch_shapes=[pltpu.VMEM((step, LANES), f32)],
        name="unflat",
    )(flat)


def unflat_all(flat, start, section, stacked=False):
    mats = []
    for rows_n, cols_n in section_shapes(section):
        mats.append(unflat(flat, start, rows_n, cols_n, stacked))
        start += rows_n * cols_n
    return mats


def head_mask(head, size):
    lane = lax.broadcasted_iota(jnp.int32, (1, LANES), 1)
    return (lane // size == head).astype(bf16)


def attend_body(q_ref, k_ref, v_ref, o_ref, lse_ref, *, size, rows_q):
    seq = k_ref.shape[0]
    scale = size ** (-0.5)
    fold = scale * math.log2(math.e)

    def one(step, carry):
        at = pl.ds(pl.multiple_of(step * rows_q, rows_q), rows_q)
        queries = q_ref[at, :]
        total = jnp.zeros((rows_q, LANES), f32)
        for head in range(LANES // size):
            mask = head_mask(head, size)
            scores = nt(k_ref[...], queries * mask)
            peak = jnp.max(scores, axis=0, keepdims=True) * fold
            power = jnp.exp2(scores * fold - peak)
            mass = jnp.sum(power, axis=0, keepdims=True)
            probs = (power * (1.0 / mass)).astype(bf16)
            total = total + tn(probs, v_ref[...] * mask)
            lse_ref[0, head : head + 1, at] = peak + jnp.log2(mass)
        o_ref[at, :] = total
        return carry

    lax.fori_loop(0, seq // rows_q, one, 0)


def attend(joined, heads):
    seq, width = joined.shape[0], joined.shape[1] // 3
    size = width // heads
    groups = width // LANES
    per = LANES // size
    rows_q = min(512, seq)
    return pl.pallas_call(
        functools.partial(attend_body, size=size, rows_q=rows_q),
        grid=(groups,),
        in_specs=[
            pl.BlockSpec((seq, LANES), lambda g: (0, g)),
            pl.BlockSpec((seq, LANES), lambda g: (0, groups + g)),
            pl.BlockSpec((seq, LANES), lambda g: (0, 2 * groups + g)),
        ],
        out_specs=[
            pl.BlockSpec((seq, LANES), lambda g: (0, g)),
            pl.BlockSpec((1, per, seq), lambda g: (g, 0, 0)),
        ],
        out_shape=[
            jax.ShapeDtypeStruct((seq, width), f32),
            jax.ShapeDtypeStruct((groups, per, seq), f32),
        ],
        name="attend",
    )(joined, joined, joined)


def attend_back_body(q_ref, k_ref, v_ref, do_ref, o_ref, lse_ref, dq_ref, dk_ref, dv_ref, dk_sum, dv_sum, *, size, rows_q):
    seq = k_ref.shape[0]
    scale = size ** (-0.5)
    fold = scale * math.log2(math.e)
    dk_sum[...] = jnp.zeros_like(dk_sum)
    dv_sum[...] = jnp.zeros_like(dv_sum)

    def one(step, carry):
        at = pl.ds(pl.multiple_of(step * rows_q, rows_q), rows_q)
        queries = q_ref[at, :]
        grads = do_ref[at, :]
        prod = grads.astype(f32) * o_ref[at, :]
        total = jnp.zeros((rows_q, LANES), f32)
        high = prod.astype(bf16)
        rest = prod - high.astype(f32)
        middle = rest.astype(bf16)
        for head in range(LANES // size):
            mask = head_mask(head, size)
            wide = jnp.broadcast_to(mask, (16, LANES))
            delta = (nt(wide, high) + nt(wide, middle))[0:1]
            q_one = queries * mask
            g_one = grads * mask
            scores = nt(k_ref[...], q_one)
            probs = jnp.exp2(scores * fold - lse_ref[0, head : head + 1, at])
            slope = nt(v_ref[...], g_one)
            grad_s = (probs * (slope - delta)).astype(bf16)
            dv_sum[...] += nn(probs.astype(bf16), g_one)
            dk_sum[...] += nn(grad_s, q_one)
            total = total + tn(grad_s, k_ref[...] * mask)
        dq_ref[at, :] = (total * scale).astype(bf16)
        return carry

    lax.fori_loop(0, seq // rows_q, one, 0)
    dk_ref[...] = (dk_sum[...] * scale).astype(bf16)
    dv_ref[...] = dv_sum[...].astype(bf16)


def attend_back(joined, grad_out, out, lse, heads):
    seq, width = joined.shape[0], joined.shape[1] // 3
    size = width // heads
    groups = width // LANES
    per = LANES // size
    rows_q = min(512, seq)
    col = pl.BlockSpec((seq, LANES), lambda g: (0, g))
    return pl.pallas_call(
        functools.partial(attend_back_body, size=size, rows_q=rows_q),
        grid=(groups,),
        in_specs=[
            col,
            pl.BlockSpec((seq, LANES), lambda g: (0, groups + g)),
            pl.BlockSpec((seq, LANES), lambda g: (0, 2 * groups + g)),
            col,
            col,
            pl.BlockSpec((1, per, seq), lambda g: (g, 0, 0)),
        ],
        out_specs=[col, col, col],
        out_shape=[jax.ShapeDtypeStruct((seq, width), bf16)] * 3,
        scratch_shapes=[pltpu.VMEM((seq, LANES), f32)] * 2,
        name="attend_back",
    )(joined, joined, joined, grad_out, out, lse)


def block_forward(tokens, mats, rows, bias_up, heads):
    normed = layer_norm(tokens, rows[0], rows[1]).astype(bf16)
    qkv_bias = jnp.concatenate([rows[6], jnp.zeros_like(rows[6]), rows[7]])
    joined = (nn(normed, mats[0]) + qkv_bias).astype(bf16)
    out, lse = attend(joined, heads)
    attended = out.astype(bf16)
    middle = tokens + nn(attended, mats[1]) + rows[8]
    second = layer_norm(middle, rows[2], rows[3]).astype(bf16)
    hidden = nn(second, mats[2]) + bias_up
    active = jax.nn.gelu(hidden, approximate=False).astype(bf16)
    result = middle + nn(active, mats[3]) + rows[9]
    return result, (tokens, normed, joined, out, lse, attended, middle, second, hidden, active)


def block_backward(kept, grad_result, mats, rows, heads):
    tokens, normed, joined, out, lse, attended, middle, second, hidden, active = kept
    width = tokens.shape[1]
    b_down = grad_result.astype(bf16)
    v_down = jnp.sum(b_down.astype(f32), axis=0)
    grad_active = nt(b_down, mats[3])
    unused, pull = jax.vjp(lambda v: jax.nn.gelu(v, approximate=False), hidden)
    b_up = pull(grad_active)[0].astype(bf16)
    v_up = jnp.sum(b_up.astype(f32), axis=0)
    grad_second = nt(b_up, mats[2])
    unused, pull = jax.vjp(layer_norm, middle, rows[2], rows[3])
    grad_norm, v_gain2, v_shift2 = pull(grad_second)
    grad_middle = grad_result + grad_norm
    b_proj = grad_middle.astype(bf16)
    v_proj = jnp.sum(b_proj.astype(f32), axis=0)
    grad_att = nt(b_proj, mats[1]).astype(bf16)
    dq, dk, dv = attend_back(joined, grad_att, out, lse, heads)
    b_qkv = jnp.concatenate([dq, dk, dv], axis=1)
    v_q = jnp.sum(dq.astype(f32), axis=0)
    v_v = jnp.sum(dv.astype(f32), axis=0)
    grad_normed = nt(b_qkv, mats[0])
    unused, pull = jax.vjp(layer_norm, tokens, rows[0], rows[1])
    grad_norm, v_gain1, v_shift1 = pull(grad_normed)
    grad_tokens = grad_middle + grad_norm
    pairs = [(normed, b_qkv), (attended, b_proj), (second, b_up), (active, b_down)]
    return grad_tokens, pairs, [v_gain1, v_shift1, v_gain2, v_shift2, None, None, v_q, v_v, v_proj, v_down, None], v_up


def skinny_body(*refs, counts):
    n = counts
    x_refs, u_refs, v_refs, outs = refs[:n], refs[n : 2 * n], refs[2 * n : 3 * n], refs[3 * n :]
    for x_ref, u_ref, v_ref, o_ref in zip(x_refs, u_refs, v_refs, outs):
        part = join3(nt(split3(x_ref[...]), u_ref[...]))
        o_ref[...] = join3(nn(split3(part), v_ref[...]))


def skinny(xs, us, vs):
    n = len(xs)
    full = pl.BlockSpec(memory_space=pltpu.VMEM)
    return pl.pallas_call(
        functools.partial(skinny_body, counts=n),
        in_specs=[full] * (3 * n),
        out_specs=[full] * n,
        out_shape=[jax.ShapeDtypeStruct((RANK, v.shape[1]), f32) for v in vs],
        compiler_params=pltpu.CompilerParams(vmem_limit_bytes=BIG),
        name="skinny",
    )(*xs, *us, *vs)


def ortho_body(left_ref, out_ref, *, widths, scale):
    at = 0
    rank_id = lax.broadcasted_iota(jnp.int32, (RANK, 1), 0)
    for width in widths:
        basis = left_ref[:, at : at + width] * scale
        for column in range(RANK):
            current = basis[column : column + 1]
            current = current * lax.rsqrt(jnp.sum(current * current, axis=1, keepdims=True) + 1e-12)
            dots = jnp.sum(basis * current, axis=1, keepdims=True)
            basis = jnp.where(
                rank_id > column, basis - dots * current, jnp.where(rank_id == column, current, basis)
            )
        out_ref[:, at : at + width] = basis
        at += width


def orthonormal(left, widths, scale):
    full = pl.BlockSpec(memory_space=pltpu.VMEM)
    return pl.pallas_call(
        functools.partial(ortho_body, widths=widths, scale=scale),
        in_specs=[full],
        out_specs=full,
        out_shape=jax.ShapeDtypeStruct(left.shape, f32),
        name="orthonormal",
    )(left)


def err_left_body(x_ref, e_ref, o_ref):
    total = jnp.zeros((e_ref.shape[1], 3 * RANK), f32)
    pieces = split3(x_ref[...])
    for block in range(e_ref.shape[0]):
        total = total + nt(e_ref[block], pieces[:, block * LANES : (block + 1) * LANES])
    o_ref[...] = join3(total.T)


def err_left(factor, err):
    full = pl.BlockSpec(memory_space=pltpu.VMEM)
    return pl.pallas_call(
        err_left_body,
        in_specs=[full] * 2,
        out_specs=full,
        out_shape=jax.ShapeDtypeStruct((RANK, err.shape[1]), f32),
        compiler_params=pltpu.CompilerParams(vmem_limit_bytes=BIG),
        name="err_left",
    )(factor, err)


def err_right_body(x_ref, e_ref, o_ref, *, offset):
    pieces = split3(x_ref[...])
    rows = pieces.shape[1]
    blocks = o_ref.shape[1] // LANES

    for block in range(blocks):
        o_ref[:, block * LANES : (block + 1) * LANES] = join3(nn(pieces, e_ref[block * rows : (block + 1) * rows]))


def err_right(ortho, err, start, cols_n):
    rows = ortho.shape[1]
    full = pl.BlockSpec(memory_space=pltpu.VMEM)
    step = rows * cols_n // LANES
    return pl.pallas_call(
        functools.partial(err_right_body, offset=0),
        grid=(1,),
        in_specs=[
            pl.BlockSpec((RANK, rows), lambda i: (0, 0)),
            pl.BlockSpec((pl.Element(step), pl.Element(LANES)), lambda i: (start // LANES, 0)),
        ],
        out_specs=pl.BlockSpec((RANK, cols_n), lambda i: (0, 0)),
        out_shape=jax.ShapeDtypeStruct((RANK, cols_n), f32),
        compiler_params=pltpu.CompilerParams(vmem_limit_bytes=BIG),
        name="err_right",
    )(ortho, err)


def finish_body(a0, a1, b0, b1, e_ref, o_ref, r_ref, *rest, rows, blocks, gain):
    err_out, app_out = rest[-2:]
    o_high = o_ref[...].astype(bf16)
    o_low = (o_ref[...] - o_high.astype(f32)).astype(bf16)
    left = jnp.concatenate([o_high, o_low, o_high], axis=0)
    lhs0 = a0[...].T
    lhs1 = a1[...].T
    left_t = left.T
    for block in range(blocks):
        cols = slice(block * LANES, (block + 1) * LANES)
        r_part = r_ref[:, cols]
        r_high = r_part.astype(bf16)
        r_low = (r_part - r_high.astype(f32)).astype(bf16)
        approx = nn(left_t, jnp.concatenate([r_high, r_high, r_low], axis=0))
        grad = nn(lhs0, b0[:, cols]) + nn(lhs1, b1[:, cols])
        at = pl.ds(block, rows, stride=blocks)
        app_out[at, :] = approx
        err_out[at, :] = (gain * grad + e_ref[block].astype(f32)) - approx


def finish(pair0, pair1, err3, ortho, right, start, gain, bufs):
    a0, b0 = pair0
    a1, b1 = pair1
    rows_n, cols_n = a0.shape[1], b0.shape[1]
    seq = a0.shape[0]
    blocks = cols_n // LANES
    rows = 128 if rows_n % 128 == 0 else rows_n
    step = rows * blocks
    flat_rows = FLAT // LANES
    whole = lambda i: (0, 0)
    flat_spec = pl.BlockSpec((pl.Element(step), pl.Element(LANES)), lambda i: (pl.multiple_of(start // LANES + i * step, 16), 0))
    in_specs = [
        pl.BlockSpec((seq, rows), lambda i: (0, i)),
        pl.BlockSpec((seq, rows), lambda i: (0, i)),
        pl.BlockSpec((seq, cols_n), whole, pipeline_mode=pl.Buffered(1)),
        pl.BlockSpec((seq, cols_n), whole, pipeline_mode=pl.Buffered(1)),
        pl.BlockSpec((blocks, rows, LANES), lambda i: (0, i, 0)),
        pl.BlockSpec((RANK, rows), lambda i: (0, i)),
        pl.BlockSpec((RANK, cols_n), whole, pipeline_mode=pl.Buffered(1)),
    ]
    args = [a0, a1, b0, b1, err3, ortho, right]
    aliases = {}
    if bufs is not None:
        in_specs += [pl.BlockSpec(memory_space=pl.ANY)] * 2
        args += list(bufs)
        aliases = {7: 0, 8: 1}
    return pl.pallas_call(
        functools.partial(finish_body, rows=rows, blocks=blocks, gain=gain),
        grid=(rows_n // rows,),
        in_specs=in_specs,
        out_specs=[flat_spec, flat_spec],
        out_shape=[jax.ShapeDtypeStruct((flat_rows, LANES), f32)] * 2,
        input_output_aliases=aliases,
        compiler_params=pltpu.CompilerParams(vmem_limit_bytes=BIG),
        name="finish",
    )(*args)


def tail_body(e_ref, buf0, buf1, err_out, app_out):
    err_out[...] = e_ref[...].astype(f32)
    app_out[...] = jnp.zeros_like(app_out)


def finish_tail(err_flat, start, bufs):
    flat_rows = FLAT // LANES
    count = flat_rows - start // LANES
    steps = 12
    step = count // steps
    assert step * steps == count and step % 16 == 0
    spec = pl.BlockSpec((pl.Element(step), pl.Element(LANES)), lambda i: (pl.multiple_of(start // LANES + i * step, 16), 0))
    return pl.pallas_call(
        tail_body,
        grid=(steps,),
        in_specs=[spec] + [pl.BlockSpec(memory_space=pl.ANY)] * 2,
        out_specs=[spec, spec],
        out_shape=[jax.ShapeDtypeStruct((flat_rows, LANES), f32)] * 2,
        input_output_aliases={1: 0, 2: 1},
        compiler_params=pltpu.CompilerParams(vmem_limit_bytes=BIG),
        name="finish_tail",
    )(err_flat, *bufs)


def swap_body(*refs, n_enc, n_dec):
    n = n_enc + n_dec
    src, dst = refs[:n], refs[n : 2 * n]
    send, recv = refs[2 * n :]
    me = lax.axis_index("section")
    other = 1 - me
    barrier = pltpu.get_barrier_semaphore()
    pl.semaphore_signal(barrier, inc=1, device_id={"section": other}, device_id_type=pl.DeviceIdType.MESH)
    pl.semaphore_wait(barrier, 1)

    def copy(i):
        return pltpu.make_async_remote_copy(
            src_ref=src[i],
            dst_ref=dst[i],
            send_sem=send.at[i],
            recv_sem=recv.at[i],
            device_id={"section": other},
            device_id_type=pl.DeviceIdType.MESH,
        )

    enc, dec = range(n_enc), range(n_enc, n)

    @pl.when(me == 0)
    def _():
        for i in dec:
            copy(i).start()
        for i in dec:
            copy(i).wait_send()
        for i in enc:
            copy(i).wait_recv()

    @pl.when(me == 1)
    def _():
        for i in enc:
            copy(i).start()
        for i in enc:
            copy(i).wait_send()
        for i in dec:
            copy(i).wait_recv()


def swap(enc, dec):
    arrays = list(enc) + list(dec)
    n = len(arrays)
    outs = pl.pallas_call(
        functools.partial(swap_body, n_enc=len(enc), n_dec=len(dec)),
        in_specs=[pl.BlockSpec(memory_space=pl.ANY)] * n,
        out_specs=[pl.BlockSpec(memory_space=pl.ANY)] * n,
        out_shape=[jax.ShapeDtypeStruct(a.shape, a.dtype) for a in arrays],
        scratch_shapes=[pltpu.SemaphoreType.DMA((n,)), pltpu.SemaphoreType.DMA((n,))],
        compiler_params=pltpu.CompilerParams(collective_id=1, has_side_effects=True),
        name="swap",
    )(*arrays)
    return outs[: len(enc)], outs[len(enc) :]


def pack_rows(rows, pieces, width, length):
    empty = jnp.zeros((width,), f32)
    parts = [empty if row is None else row for row in rows] + pieces
    used = sum(part.shape[0] for part in parts)
    return jnp.concatenate(parts + [jnp.zeros((length - used,), f32)])


def local(pixels, visible, masked, loss_mask, master, momentum, vectors, vec_moment, factors, errors):
    sec = lax.axis_index("section")
    replicas = lax.axis_size("dp")
    replica_id = lax.axis_index("dp")

    low_own = lax.all_gather(master[0].astype(bf16), "dp", axis=0, tiled=True)
    low_both = lax.all_gather(low_own, "section", axis=0, tiled=True).reshape(-1, LANES)
    vec_both = lax.all_gather(vectors[0], "section", axis=0)
    fac_both = lax.all_gather(factors[0], "section", axis=0)
    count = lax.psum(jnp.sum(loss_mask).astype(f32), "dp")

    vis = lax.dynamic_index_in_dim(visible, sec, 0, keepdims=False)
    mas = lax.dynamic_index_in_dim(masked, sec, 0, keepdims=False)
    mask_row = lax.dynamic_index_in_dim(loss_mask, sec, 0, keepdims=False).astype(f32)
    order = jnp.concatenate([vis, mas])
    pix = lax.dynamic_index_in_dim(pixels, sec, 0, keepdims=False)
    pick = (order[:, None] == jnp.arange(SEQ, dtype=jnp.int32)[None, :]).astype(bf16)
    pix_order = nn(pick, pix).astype(bf16)
    pix_vis = pix_order[:VIS]
    target = pix_order[VIS:].astype(f32)
    table_dec = positions_at(order, DD)
    table_enc = positions_at(vis, DE)
    err_flat = errors.reshape(FLAT // LANES, LANES)

    def errs_for(section):
        def run():
            stacks = unflat_all(err_flat, 0, section, stacked=True)
            lefts = []
            col_at = 0
            for stack, (rows_n, cols_n) in zip(stacks, section_shapes(section)):
                lefts.append(err_left(factors[0][:, col_at : col_at + cols_n], stack))
                col_at += cols_n
            flat = jnp.concatenate([stack.reshape(-1, LANES) for stack in stacks])
            pad = FLAT // LANES - flat.shape[0]
            flat = jnp.concatenate([flat, jnp.zeros((pad, LANES), bf16)]) if pad else flat
            zero = [jnp.zeros((RANK, n), f32) for n in ROWS_L]
            zero[section] = jnp.concatenate(lefts, axis=1)
            return flat, jnp.concatenate(zero, axis=1)

        return run

    err_stack, err_lefts = lax.cond(sec == 0, errs_for(0), errs_for(1))

    enc = unflat_all(low_both, 0, 0)
    dec = unflat_all(low_both, FLAT, 1)
    rows_e, bias_e, unused = unpack_vecs(vec_both[0], DE, FFE)
    rows_d, bias_d, extra_d = unpack_vecs(vec_both[1], DD, FFD)

    embedded = nn(pix_vis, enc[4]) + rows_e[10] + table_enc
    coded, kept_e = block_forward(embedded, enc, rows_e, bias_e, HEADS_ENC)
    sent_full, sent_pull = jax.vjp(layer_norm, coded, rows_e[4], rows_e[5])
    sent = sent_full.astype(bf16)
    projected = nn(sent, dec[5]) + extra_d
    filled = jnp.concatenate([projected, jnp.broadcast_to(rows_d[10], (SEQ - VIS, DD))]) + table_dec
    result, kept_d = block_forward(filled, dec, rows_d, bias_d, HEADS_DEC)
    final_full, final_pull = jax.vjp(layer_norm, result[VIS:], rows_d[4], rows_d[5])
    final = final_full.astype(bf16)
    residual = nt(final, dec[4]) - target
    loss_part = jnp.sum(mask_row * jnp.mean(residual * residual, axis=1)) / count
    grad_pred = (mask_row[:, None] * (2.0 * residual / PATCH) / count).astype(bf16)
    grad_picked, v_gain3, v_shift3 = final_pull(nn(grad_pred, dec[4]))
    grad_result = jnp.concatenate([jnp.zeros((VIS, DD), f32), grad_picked])
    grad_filled, pairs_d, vrows_d, v_up_d = block_backward(kept_d, grad_result, dec, rows_d, HEADS_DEC)
    b_proj = grad_filled[:VIS].astype(bf16)
    pairs_d = pairs_d + [(grad_pred, final), (sent, b_proj)]
    vrows_d[4], vrows_d[5], vrows_d[10] = v_gain3, v_shift3, jnp.sum(grad_filled[VIS:], axis=0)
    vec_d = pack_rows(vrows_d, [v_up_d, jnp.sum(b_proj.astype(f32), axis=0)], DD, VLEN)
    grad_sent = nt(b_proj, dec[5]).astype(bf16)
    grad_coded, v_gain3, v_shift3 = sent_pull(grad_sent.astype(f32))
    grad_start, pairs_e, vrows_e, v_up_e = block_backward(kept_e, grad_coded, enc, rows_e, HEADS_ENC)
    b_start = grad_start.astype(bf16)
    pairs_e = pairs_e + [(pix_vis, b_start)]
    vrows_e[4], vrows_e[5], vrows_e[10] = v_gain3, v_shift3, jnp.sum(b_start.astype(f32), axis=0)
    vec_e = pack_rows(vrows_e, [v_up_e], DE, VLEN)

    pairs = pairs_e + pairs_d
    gain = float(replicas)
    xs = []
    for section in range(2):
        col_at = 0
        for rows_n, cols_n in section_shapes(section):
            xs.append(fac_both[section][:, col_at : col_at + cols_n])
            col_at += cols_n
    lefts = skinny(xs, [b for a, b in pairs], [a for a, b in pairs])
    left_part = gain * jnp.concatenate(lefts, axis=1) + err_lefts
    left_sum, vec_sum, loss_sum = lax.psum((left_part, jnp.stack([vec_e, vec_d]), loss_part), ("section", "dp"))

    n_enc = len(pairs_e)
    flat_e = [x for pair in pairs_e for x in pair]
    flat_d = [x for pair in pairs_d for x in pair]
    other_e, other_d = swap(flat_e, flat_d)

    widths = [rows_n for s in range(2) for rows_n, cols_n in section_shapes(s)]
    ortho = orthonormal(left_sum, widths, 1.0 / replicas)
    orthos = []
    at = 0
    for width in widths:
        orthos.append(ortho[:, at : at + width])
        at += width
    rights = skinny(orthos, [a for a, b in pairs], [b for a, b in pairs])

    def err_rights_for(section):
        def run():
            start = 0
            outs = []
            base = 0 if section == 0 else n_enc
            for i, (rows_n, cols_n) in enumerate(section_shapes(section)):
                outs.append(err_right(orthos[base + i], err_stack, start, cols_n))
                start += rows_n * cols_n
            zero = [jnp.zeros((RANK, n), f32) for n in COLS_R]
            zero[section] = jnp.concatenate(outs, axis=1)
            return jnp.concatenate(zero, axis=1)

        return run

    right_part = gain * jnp.concatenate(rights, axis=1) + lax.cond(sec == 0, err_rights_for(0), err_rights_for(1))
    right_sum = lax.psum(right_part, ("section", "dp")) / replicas

    squares = jnp.sum(vec_sum * vec_sum)
    row_at = col_at = 0
    for section in range(2):
        for rows_n, cols_n in section_shapes(section):
            o_part = ortho[:, row_at : row_at + rows_n]
            r_part = right_sum[:, col_at : col_at + cols_n]
            gram_o = jnp.sum(o_part[:, None, :] * o_part[None, :, :], axis=-1)
            gram_r = jnp.sum(r_part[:, None, :] * r_part[None, :, :], axis=-1)
            squares = squares + jnp.sum(gram_o * gram_r)
            row_at += rows_n
            col_at += cols_n
    norm = jnp.sqrt(squares)
    scale = jnp.minimum(1.0, clip_limit / (norm + 1e-06))

    def finish_for(section):
        def run():
            mine = pairs_e if section == 0 else pairs_d
            flat = other_e if section == 0 else other_d
            theirs = [(flat[2 * i], flat[2 * i + 1]) for i in range(len(mine))]
            bufs = None
            start = 0
            base = 0 if section == 0 else n_enc
            col_at = 0 if section == 0 else COLS_R[0]
            for i, (rows_n, cols_n) in enumerate(section_shapes(section)):
                blocks = cols_n // LANES
                stack = lax.slice_in_dim(err_stack, start // LANES, (start + rows_n * cols_n) // LANES, axis=0)
                stack = stack.reshape(blocks, rows_n, LANES)
                bufs = finish(
                    mine[i], theirs[i], stack, orthos[base + i],
                    right_sum[:, col_at : col_at + cols_n], start, gain, bufs,
                )
                start += rows_n * cols_n
                col_at += cols_n
            if start < FLAT:
                bufs = finish_tail(err_flat, start, bufs)
            return bufs

        return run

    new_errors, approx = lax.cond(sec == 0, finish_for(0), finish_for(1))
    shard_len = master.shape[1]
    own_part = lax.dynamic_slice_in_dim(approx.reshape(-1), replica_id * shard_len, shard_len)
    rate = learning_rate()
    new_moment = moment_decay * momentum[0] + scale * own_part
    new_master = master[0] - rate * new_moment
    vec_own = lax.dynamic_index_in_dim(vec_sum, sec, 0, keepdims=False)
    new_vm = moment_decay * vec_moment[0] + scale * vec_own
    new_vectors = vectors[0] - rate * new_vm
    right_e, right_d = right_sum[:, : COLS_R[0]], right_sum[:, COLS_R[0] :]
    cols_total = factors.shape[2]
    right_d = jnp.pad(right_d, ((0, 0), (0, cols_total - COLS_R[1])))
    right_e = jnp.pad(right_e, ((0, 0), (0, cols_total - COLS_R[0])))
    new_factors = jnp.where(sec == 0, right_e, right_d)
    return (
        new_master[None],
        new_master.astype(bf16)[None],
        new_moment[None],
        new_vectors[None],
        new_vm[None],
        new_factors[None],
        new_errors.reshape(1, 1, -1),
        loss_sum.reshape(1),
        norm.reshape(1),
    )


def solution(mesh):
    return jax.shard_map(
        local,
        mesh=mesh,
        in_specs=(
            P("dp", None, None),
            P("dp", None),
            P("dp", None),
            P("dp", None),
            P("section", "dp"),
            P("section", "dp"),
            P("section", None),
            P("section", None),
            P("section", None, None),
            P("section", "dp", None),
        ),
        out_specs=(
            P("section", "dp"),
            P("section", "dp"),
            P("section", "dp"),
            P("section", None),
            P("section", None),
            P("section", None, None),
            P("section", "dp", None),
            P(),
            P(),
        ),
        check_vma=False,
    )
```

```python
import functools
import math

import jax
import jax.numpy as jnp
from jax import lax
from jax.experimental import pallas as pl
from jax.experimental.pallas import tpu as pltpu
from jax.sharding import PartitionSpec as P

DE = 768
FFE = 3072
HEADS_ENC = 12
DD = 512
FFD = 2048
HEADS_DEC = 16
PATCH = 192
RANK = 8
SEQ = 1024
VIS = 256
FLAT = 7225344
VLEN = 11520

f32 = jnp.float32
bf16 = jnp.bfloat16
clip_limit = 0.0001
moment_decay = 0.9
rate_base = 0.5
LANES = 128
BIG = 66000000


def nn(left, right):
    return lax.dot_general(left, right, (((1,), (0,)), ((), ())), preferred_element_type=f32)


def nt(left, right):
    return lax.dot_general(left, right, (((1,), (1,)), ((), ())), preferred_element_type=f32)


def tn(left, right):
    return lax.dot_general(left, right, (((0,), (0,)), ((), ())), preferred_element_type=f32)


def split3(value):
    high = value.astype(bf16)
    rest = value - high.astype(f32)
    middle = rest.astype(bf16)
    return jnp.concatenate([high, middle, (rest - middle.astype(f32)).astype(bf16)], axis=0)


def join3(value):
    return value[:RANK] + value[RANK : 2 * RANK] + value[2 * RANK :]


def layer_norm(tokens, gain, shift):
    centred = tokens - jnp.mean(tokens, axis=-1, keepdims=True)
    spread = jnp.mean(centred * centred, axis=-1, keepdims=True)
    return centred * lax.rsqrt(spread + 1e-06) * gain + shift


def positions_at(places, width):
    column = jnp.arange(width)
    freqs = jnp.exp(-(column // 2 * 2).astype(f32) / width * math.log(10000.0))
    return jnp.sin(places.astype(f32)[:, None] * freqs + (column % 2).astype(f32) * (math.pi / 2))


def section_shapes(section):
    if section == 0:
        return [(DE, 3 * DE), (DE, DE), (DE, FFE), (FFE, DE), (PATCH, DE)]
    return [(DD, 3 * DD), (DD, DD), (DD, FFD), (FFD, DD), (PATCH, DD), (DE, DD)]


def unpack_vecs(flat, width, hidden):
    return (
        flat[: 11 * width].reshape(11, width),
        flat[11 * width : 11 * width + hidden],
        flat[11 * width + hidden : 12 * width + hidden],
    )


def learning_rate():
    return rate_base * math.sqrt(2.0 * (FLAT + VLEN) / DD) / clip_limit


def unflat_body(src_ref, out_ref, wide_ref, *, blocks, rows, stacked):
    wide_ref[...] = src_ref[...].astype(f32)
    for block in range(blocks):
        part = wide_ref[pl.ds(block, rows, stride=blocks), :].astype(bf16)
        if stacked:
            out_ref[block] = part
        else:
            out_ref[:, block * LANES : (block + 1) * LANES] = part


def unflat(flat, start, rows_n, cols_n, stacked=False):
    blocks = cols_n // LANES
    rows = 192 if rows_n == PATCH else 128 if blocks > 8 else 256
    if stacked:
        out_shape = jax.ShapeDtypeStruct((blocks, rows_n, LANES), bf16)
        out_spec = pl.BlockSpec((blocks, rows, LANES), lambda i: (0, i, 0))
    else:
        out_shape = jax.ShapeDtypeStruct((rows_n, cols_n), bf16)
        out_spec = pl.BlockSpec((rows, cols_n), lambda i: (i, 0))
    step = rows * blocks
    return pl.pallas_call(
        functools.partial(unflat_body, blocks=blocks, rows=rows, stacked=stacked),
        grid=(rows_n // rows,),
        in_specs=[pl.BlockSpec((pl.Element(step), pl.Element(LANES)), lambda i: (pl.multiple_of(start // LANES + i * step, 16), 0))],
        out_specs=out_spec,
        out_shape=out_shape,
        scratch_shapes=[pltpu.VMEM((step, LANES), f32)],
        name="unflat",
    )(flat)


def unflat_all(flat, start, section, stacked=False):
    mats = []
    for rows_n, cols_n in section_shapes(section):
        mats.append(unflat(flat, start, rows_n, cols_n, stacked))
        start += rows_n * cols_n
    return mats


def head_mask(head, size):
    lane = lax.broadcasted_iota(jnp.int32, (1, LANES), 1)
    return (lane // size == head).astype(bf16)


def attend_body(q_ref, k_ref, v_ref, o_ref, lse_ref, *, size, rows_q):
    seq = k_ref.shape[0]
    scale = size ** (-0.5)
    fold = scale * math.log2(math.e)

    def one(step, carry):
        at = pl.ds(pl.multiple_of(step * rows_q, rows_q), rows_q)
        queries = q_ref[at, :]
        total = jnp.zeros((rows_q, LANES), f32)
        for head in range(LANES // size):
            mask = head_mask(head, size)
            scores = nt(k_ref[...], queries * mask)
            peak = jnp.max(scores, axis=0, keepdims=True) * fold
            power = jnp.exp2(scores * fold - peak)
            mass = jnp.sum(power, axis=0, keepdims=True)
            probs = (power * (1.0 / mass)).astype(bf16)
            total = total + tn(probs, v_ref[...] * mask)
            lse_ref[0, head : head + 1, at] = peak + jnp.log2(mass)
        o_ref[at, :] = total
        return carry

    lax.fori_loop(0, seq // rows_q, one, 0)


def attend(joined, heads):
    seq, width = joined.shape[0], joined.shape[1] // 3
    size = width // heads
    groups = width // LANES
    per = LANES // size
    rows_q = min(512, seq)
    return pl.pallas_call(
        functools.partial(attend_body, size=size, rows_q=rows_q),
        grid=(groups,),
        in_specs=[
            pl.BlockSpec((seq, LANES), lambda g: (0, g)),
            pl.BlockSpec((seq, LANES), lambda g: (0, groups + g)),
            pl.BlockSpec((seq, LANES), lambda g: (0, 2 * groups + g)),
        ],
        out_specs=[
            pl.BlockSpec((seq, LANES), lambda g: (0, g)),
            pl.BlockSpec((1, per, seq), lambda g: (g, 0, 0)),
        ],
        out_shape=[
            jax.ShapeDtypeStruct((seq, width), f32),
            jax.ShapeDtypeStruct((groups, per, seq), f32),
        ],
        name="attend",
    )(joined, joined, joined)


def attend_back_body(q_ref, k_ref, v_ref, do_ref, o_ref, lse_ref, dq_ref, dk_ref, dv_ref, dk_sum, dv_sum, *, size, rows_q):
    seq = k_ref.shape[0]
    scale = size ** (-0.5)
    fold = scale * math.log2(math.e)
    dk_sum[...] = jnp.zeros_like(dk_sum)
    dv_sum[...] = jnp.zeros_like(dv_sum)

    def one(step, carry):
        at = pl.ds(pl.multiple_of(step * rows_q, rows_q), rows_q)
        queries = q_ref[at, :]
        grads = do_ref[at, :]
        prod = grads.astype(f32) * o_ref[at, :]
        total = jnp.zeros((rows_q, LANES), f32)
        high = prod.astype(bf16)
        rest = prod - high.astype(f32)
        middle = rest.astype(bf16)
        for head in range(LANES // size):
            mask = head_mask(head, size)
            wide = jnp.broadcast_to(mask, (16, LANES))
            delta = (nt(wide, high) + nt(wide, middle))[0:1]
            q_one = queries * mask
            g_one = grads * mask
            scores = nt(k_ref[...], q_one)
            probs = jnp.exp2(scores * fold - lse_ref[0, head : head + 1, at])
            slope = nt(v_ref[...], g_one)
            grad_s = (probs * (slope - delta)).astype(bf16)
            dv_sum[...] += nn(probs.astype(bf16), g_one)
            dk_sum[...] += nn(grad_s, q_one)
            total = total + tn(grad_s, k_ref[...] * mask)
        dq_ref[at, :] = (total * scale).astype(bf16)
        return carry

    lax.fori_loop(0, seq // rows_q, one, 0)
    dk_ref[...] = (dk_sum[...] * scale).astype(bf16)
    dv_ref[...] = dv_sum[...].astype(bf16)


def attend_back(joined, grad_out, out, lse, heads):
    seq, width = joined.shape[0], joined.shape[1] // 3
    size = width // heads
    groups = width // LANES
    per = LANES // size
    rows_q = min(512, seq)
    col = pl.BlockSpec((seq, LANES), lambda g: (0, g))
    return pl.pallas_call(
        functools.partial(attend_back_body, size=size, rows_q=rows_q),
        grid=(groups,),
        in_specs=[
            col,
            pl.BlockSpec((seq, LANES), lambda g: (0, groups + g)),
            pl.BlockSpec((seq, LANES), lambda g: (0, 2 * groups + g)),
            col,
            col,
            pl.BlockSpec((1, per, seq), lambda g: (g, 0, 0)),
        ],
        out_specs=[col, col, col],
        out_shape=[jax.ShapeDtypeStruct((seq, width), bf16)] * 3,
        scratch_shapes=[pltpu.VMEM((seq, LANES), f32)] * 2,
        name="attend_back",
    )(joined, joined, joined, grad_out, out, lse)


def block_forward(tokens, mats, rows, bias_up, heads):
    normed = layer_norm(tokens, rows[0], rows[1]).astype(bf16)
    qkv_bias = jnp.concatenate([rows[6], jnp.zeros_like(rows[6]), rows[7]])
    joined = (nn(normed, mats[0]) + qkv_bias).astype(bf16)
    out, lse = attend(joined, heads)
    attended = out.astype(bf16)
    middle = tokens + nn(attended, mats[1]) + rows[8]
    second = layer_norm(middle, rows[2], rows[3]).astype(bf16)
    hidden = nn(second, mats[2]) + bias_up
    active = jax.nn.gelu(hidden, approximate=False).astype(bf16)
    result = middle + nn(active, mats[3]) + rows[9]
    return result, (tokens, normed, joined, out, lse, attended, middle, second, hidden, active)


def block_backward(kept, grad_result, mats, rows, heads):
    tokens, normed, joined, out, lse, attended, middle, second, hidden, active = kept
    width = tokens.shape[1]
    b_down = grad_result.astype(bf16)
    v_down = jnp.sum(b_down.astype(f32), axis=0)
    grad_active = nt(b_down, mats[3])
    unused, pull = jax.vjp(lambda v: jax.nn.gelu(v, approximate=False), hidden)
    b_up = pull(grad_active)[0].astype(bf16)
    v_up = jnp.sum(b_up.astype(f32), axis=0)
    grad_second = nt(b_up, mats[2])
    unused, pull = jax.vjp(layer_norm, middle, rows[2], rows[3])
    grad_norm, v_gain2, v_shift2 = pull(grad_second)
    grad_middle = grad_result + grad_norm
    b_proj = grad_middle.astype(bf16)
    v_proj = jnp.sum(b_proj.astype(f32), axis=0)
    grad_att = nt(b_proj, mats[1]).astype(bf16)
    dq, dk, dv = attend_back(joined, grad_att, out, lse, heads)
    b_qkv = jnp.concatenate([dq, dk, dv], axis=1)
    v_q = jnp.sum(dq.astype(f32), axis=0)
    v_v = jnp.sum(dv.astype(f32), axis=0)
    grad_normed = nt(b_qkv, mats[0])
    unused, pull = jax.vjp(layer_norm, tokens, rows[0], rows[1])
    grad_norm, v_gain1, v_shift1 = pull(grad_normed)
    grad_tokens = grad_middle + grad_norm
    pairs = [(normed, b_qkv), (attended, b_proj), (second, b_up), (active, b_down)]
    return grad_tokens, pairs, [v_gain1, v_shift1, v_gain2, v_shift2, None, None, v_q, v_v, v_proj, v_down, None], v_up


def tiles_of(width):
    return -(-width // LANES)


def spans(which):
    at, found = [], []
    for section in range(2):
        start = 0
        for shape in section_shapes(section):
            found.append((section, start, shape[which]))
            start += tiles_of(shape[which]) * LANES
        at.append(start)
    return found, at


ROW_SPANS, ROW_WIDTHS = spans(0)
COL_SPANS, COL_WIDTHS = spans(1)
ROW_PAD = max(ROW_WIDTHS)
VEC_TILES = -(-VLEN // (RANK * LANES))


def sum_rows(replicas, tiles):
    return -(-tiles // replicas) * replicas * RANK


def put_tiles(out_ref, section, start, value):
    width = value.shape[1]
    for tile in range(tiles_of(width)):
        here = min(LANES, width - tile * LANES)
        row = (start // LANES + tile) * RANK
        out_ref[section, row : row + RANK, :here] = value[:, tile * LANES : tile * LANES + here]


def skinny_body(*refs, n, x_spans, y_spans, extra_row):
    x_ref, u_refs, v_refs, tail_ref, out_ref = refs[0], refs[1 : 1 + n], refs[1 + n : 1 + 2 * n], refs[-2], refs[-1]
    out_ref[...] = jnp.zeros_like(out_ref)
    gain_ref = None
    for u_ref, v_ref, (section, start, width), (out_section, out_start, unused) in zip(u_refs, v_refs, x_spans, y_spans):
        part = join3(nt(split3(x_ref[section, :, start : start + width]), u_ref[...]))
        put_tiles(out_ref, out_section, out_start, extra_row[1] * join3(nn(split3(part), v_ref[...])))
    if extra_row[0]:
        out_ref[:, extra_row[0] : extra_row[0] + tail_ref.shape[1]] = tail_ref[...]


def skinny(x, us, vs, x_spans, y_spans, tail, tail_row, gain, rows):
    n = len(us)
    full = pl.BlockSpec(memory_space=pltpu.VMEM)
    return pl.pallas_call(
        functools.partial(skinny_body, n=n, x_spans=x_spans, y_spans=y_spans, extra_row=(tail_row, gain)),
        in_specs=[full] * (2 * n + 2),
        out_specs=full,
        out_shape=jax.ShapeDtypeStruct((2, rows, LANES), f32),
        compiler_params=pltpu.CompilerParams(vmem_limit_bytes=BIG),
        name="skinny",
    )(x, *us, *vs, tail)


def ortho_body(sum_ref, out_ref, wide, *, scale):
    rank_id = lax.broadcasted_iota(jnp.int32, (RANK, 1), 0)
    for section, start, width in ROW_SPANS:
        padded = tiles_of(width) * LANES
        for tile in range(padded // LANES):
            row = (start // LANES + tile) * RANK
            wide[:, tile * LANES : (tile + 1) * LANES] = sum_ref[section, row : row + RANK] * scale
        basis = wide[:, :padded]
        for column in range(RANK):
            current = basis[column : column + 1]
            current = current * lax.rsqrt(jnp.sum(current * current, axis=1, keepdims=True) + 1e-12)
            dots = jnp.sum(basis * current, axis=1, keepdims=True)
            basis = jnp.where(
                rank_id > column, basis - dots * current, jnp.where(rank_id == column, current, basis)
            )
        out_ref[section, :, start : start + padded] = basis


def orthonormal(sums, scale):
    full = pl.BlockSpec(memory_space=pltpu.VMEM)
    return pl.pallas_call(
        functools.partial(ortho_body, scale=scale),
        in_specs=[full],
        out_specs=full,
        out_shape=jax.ShapeDtypeStruct((2, RANK, ROW_PAD), f32),
        scratch_shapes=[pltpu.VMEM((RANK, FFE), f32)],
        name="orthonormal",
    )(sums)


def chunk_rows(rows_n, cols_n):
    if rows_n == PATCH:
        return PATCH
    return 128 if cols_n > 8 * LANES else 256


def err_prep_body(e_ref, x_ref, *rest, blocks, rows):
    out_ref, left_ref, wide = rest[-3:]
    wide[...] = e_ref[0].reshape(rows * blocks, LANES).astype(f32)
    pieces = split3(x_ref[...])
    total = jnp.zeros((rows, 3 * RANK), f32)
    for block in range(blocks):
        part = wide[pl.ds(block, rows, stride=blocks), :].astype(bf16)
        out_ref[block * rows : (block + 1) * rows, :] = part
        total = total + nt(part, pieces[:, block * LANES : (block + 1) * LANES])
    value = join3(total.T)
    left_ref[...] = jnp.zeros_like(left_ref)
    for tile in range(tiles_of(rows)):
        here = min(LANES, rows - tile * LANES)
        left_ref[tile * RANK : (tile + 1) * RANK, :here] = value[:, tile * LANES : tile * LANES + here]


def err_prep(errors, factor, start, rows_n, cols_n, buf):
    blocks = cols_n // LANES
    rows = chunk_rows(rows_n, cols_n)
    step = rows * blocks
    steps = rows_n // rows
    tiles = tiles_of(rows)
    in_specs = [
        pl.BlockSpec((pl.Element(1), pl.Element(1), pl.Element(step * LANES)), lambda i: (0, 0, pl.multiple_of(start + i * step * LANES, 1024))),
        pl.BlockSpec((RANK, cols_n), lambda i: (0, 0)),
    ]
    args = [errors, factor]
    aliases = {}
    if buf is not None:
        in_specs.append(pl.BlockSpec(memory_space=pl.ANY))
        args.append(buf)
        aliases = {2: 0}
    return pl.pallas_call(
        functools.partial(err_prep_body, blocks=blocks, rows=rows),
        grid=(steps,),
        in_specs=in_specs,
        out_specs=[
            pl.BlockSpec((pl.Element(step), pl.Element(LANES)), lambda i: (pl.multiple_of(start // LANES + i * step, 16), 0)),
            pl.BlockSpec((tiles * RANK, LANES), lambda i: (i, 0)),
        ],
        out_shape=[
            jax.ShapeDtypeStruct((FLAT // LANES, LANES), bf16),
            jax.ShapeDtypeStruct((steps * tiles * RANK, LANES), f32),
        ],
        input_output_aliases=aliases,
        scratch_shapes=[pltpu.VMEM((step, LANES), f32)],
        name="err_prep",
    )(*args)


def err_right_body(x_ref, e_ref, o_ref, bufs, sems, *, section, scale):
    plan = []
    start = 0
    for (rows_n, cols_n), row_span, col_span in zip(
        section_shapes(section),
        [span for span in ROW_SPANS if span[0] == section],
        [span for span in COL_SPANS if span[0] == section],
    ):
        rows = chunk_rows(rows_n, cols_n)
        blocks = cols_n // LANES
        for chunk in range(rows_n // rows):
            plan.append((start // LANES + chunk * rows * blocks, rows, blocks, row_span[1] + chunk * rows, col_span[1], chunk))
        start += rows_n * cols_n
    depth = bufs.shape[0]

    def fetch(index):
        at, rows, blocks = plan[index][:3]
        slot = index % depth
        return pltpu.make_async_copy(
            e_ref.at[pl.ds(at, rows * blocks)], bufs.at[slot, pl.ds(0, rows * blocks)], sems.at[slot]
        )

    o_ref[...] = jnp.zeros_like(o_ref)
    for index in range(min(depth - 1, len(plan))):
        fetch(index).start()
    for index, (at, rows, blocks, row_at, col_at, chunk) in enumerate(plan):
        if index + depth - 1 < len(plan):
            fetch(index + depth - 1).start()
        fetch(index).wait()
        pieces = split3(x_ref[section, :, row_at : row_at + rows])
        for block in range(blocks):
            part = join3(nn(pieces, bufs[index % depth, block * rows : (block + 1) * rows]))
            row = (col_at // LANES + block) * RANK
            if chunk == 0:
                o_ref[row : row + RANK] = part
            else:
                o_ref[row : row + RANK] += part


def err_right(ortho, err, section, rows):
    full = pl.BlockSpec(memory_space=pltpu.VMEM)
    most = max(chunk_rows(*shape) * shape[1] // LANES for shape in section_shapes(section))
    return pl.pallas_call(
        functools.partial(err_right_body, section=section, scale=1.0),
        in_specs=[full, pl.BlockSpec(memory_space=pl.ANY)],
        out_specs=full,
        out_shape=jax.ShapeDtypeStruct((rows, LANES), f32),
        scratch_shapes=[pltpu.VMEM((4, most, LANES), bf16), pltpu.SemaphoreType.DMA((4,))],
        compiler_params=pltpu.CompilerParams(vmem_limit_bytes=BIG),
        name="err_right",
    )(ortho, err)


def final_right_body(sum_ref, ortho_ref, vec_ref, right_ref, norm_ref, *, scale):
    squares = jnp.sum(vec_ref[...] * vec_ref[...], keepdims=True)[0]
    for (section, start, width), (unused, row_at, row_width) in zip(COL_SPANS, ROW_SPANS):
        for tile in range(width // LANES):
            row = (start // LANES + tile) * RANK
            right_ref[section, :, start + tile * LANES : start + (tile + 1) * LANES] = sum_ref[section, row : row + RANK] * scale
        o_part = ortho_ref[section, :, row_at : row_at + tiles_of(row_width) * LANES]
        r_part = right_ref[section, :, start : start + width]
        for line in range(RANK):
            gram_o = jnp.sum(o_part * o_part[line : line + 1], axis=1, keepdims=True)
            gram_r = jnp.sum(r_part * r_part[line : line + 1], axis=1, keepdims=True)
            squares = squares + jnp.sum(gram_o * gram_r, keepdims=True)
    for section in range(2):
        used = COL_WIDTHS[section]
        if used < right_ref.shape[2]:
            right_ref[section, :, used:] = jnp.zeros((RANK, right_ref.shape[2] - used), f32)
    norm_ref[...] = jnp.broadcast_to(jnp.sqrt(squares), norm_ref.shape)


def final_right(sums, ortho, vecs, cols, scale):
    full = pl.BlockSpec(memory_space=pltpu.VMEM)
    return pl.pallas_call(
        functools.partial(final_right_body, scale=scale),
        in_specs=[full] * 3,
        out_specs=[full] * 2,
        out_shape=[jax.ShapeDtypeStruct((2, RANK, cols), f32), jax.ShapeDtypeStruct((1, LANES), f32)],
        name="final_right",
    )(sums, ortho, vecs)


def finish_body(a0, a1, b0, b1, e_ref, o_ref, r_ref, *rest, rows, blocks, gain):
    err_out, app_out = rest[-2:]
    o_part = o_ref[0]
    o_high = o_part.astype(bf16)
    o_low = (o_part - o_high.astype(f32)).astype(bf16)
    left_t = jnp.concatenate([o_high, o_low, o_high], axis=0).T[:rows]
    lhs0 = a0[...].T
    lhs1 = a1[...].T
    for block in range(blocks):
        cols = slice(block * LANES, (block + 1) * LANES)
        r_part = r_ref[0, :, cols]
        r_high = r_part.astype(bf16)
        r_low = (r_part - r_high.astype(f32)).astype(bf16)
        approx = nn(left_t, jnp.concatenate([r_high, r_high, r_low], axis=0))
        grad = nn(lhs0, b0[:, cols]) + nn(lhs1, b1[:, cols])
        at = pl.ds(block, rows, stride=blocks)
        app_out[at, :] = approx
        err_out[at, :] = (gain * grad + e_ref[block * rows : (block + 1) * rows].astype(f32)) - approx


def finish(pair0, pair1, err, ortho, right, section, row_at, col_at, start, gain, bufs):
    a0, b0 = pair0
    a1, b1 = pair1
    rows_n, cols_n = a0.shape[1], b0.shape[1]
    seq = a0.shape[0]
    blocks = cols_n // LANES
    rows = chunk_rows(rows_n, cols_n)
    step = rows * blocks
    flat_rows = FLAT // LANES
    whole = lambda i: (0, 0)
    flat_spec = pl.BlockSpec((pl.Element(step), pl.Element(LANES)), lambda i: (pl.multiple_of(start // LANES + i * step, 16), 0))
    wide_rows = tiles_of(rows) * LANES
    in_specs = [
        pl.BlockSpec((seq, rows), lambda i: (0, i)),
        pl.BlockSpec((seq, rows), lambda i: (0, i)),
        pl.BlockSpec((seq, cols_n), whole, pipeline_mode=pl.Buffered(1)),
        pl.BlockSpec((seq, cols_n), whole, pipeline_mode=pl.Buffered(1)),
        flat_spec,
        pl.BlockSpec((1, RANK, wide_rows), lambda i: (section, 0, row_at // wide_rows + i)),
        pl.BlockSpec((pl.Element(1), pl.Element(RANK), pl.Element(cols_n)), lambda i: (section, 0, col_at), pipeline_mode=pl.Buffered(1)),
    ]
    assert row_at % wide_rows == 0
    args = [a0, a1, b0, b1, err, ortho, right]
    aliases = {}
    if bufs is not None:
        in_specs += [pl.BlockSpec(memory_space=pl.ANY)] * 2
        args += list(bufs)
        aliases = {7: 0, 8: 1}
    return pl.pallas_call(
        functools.partial(finish_body, rows=rows, blocks=blocks, gain=gain),
        grid=(rows_n // rows,),
        in_specs=in_specs,
        out_specs=[flat_spec, flat_spec],
        out_shape=[jax.ShapeDtypeStruct((flat_rows, LANES), f32)] * 2,
        input_output_aliases=aliases,
        compiler_params=pltpu.CompilerParams(vmem_limit_bytes=BIG),
        name="finish",
    )(*args)


def tail_body(e_ref, buf0, buf1, err_out, app_out):
    err_out[...] = e_ref[0].reshape(err_out.shape).astype(f32)
    app_out[...] = jnp.zeros_like(app_out)


def finish_tail(errors, start, bufs):
    flat_rows = FLAT // LANES
    count = flat_rows - start // LANES
    steps = 12
    step = count // steps
    assert step * steps == count and step % 16 == 0
    spec = pl.BlockSpec((pl.Element(step), pl.Element(LANES)), lambda i: (pl.multiple_of(start // LANES + i * step, 16), 0))
    return pl.pallas_call(
        tail_body,
        grid=(steps,),
        in_specs=[pl.BlockSpec((pl.Element(1), pl.Element(1), pl.Element(step * LANES)), lambda i: (0, 0, pl.multiple_of(start + i * step * LANES, 1024)))]
        + [pl.BlockSpec(memory_space=pl.ANY)] * 2,
        out_specs=[spec, spec],
        out_shape=[jax.ShapeDtypeStruct((flat_rows, LANES), f32)] * 2,
        input_output_aliases={1: 0, 2: 1},
        compiler_params=pltpu.CompilerParams(vmem_limit_bytes=BIG),
        name="finish_tail",
    )(errors, *bufs)


MESH = pl.DeviceIdType.MESH


def grid_of(replicas):
    side = 2 if replicas < 64 else 4
    return replicas // (side * side), side, side


def used_rows(section):
    counts = [sum(rows * cols for rows, cols in section_shapes(s)) // LANES for s in range(2)]
    return jnp.where(section == 0, counts[0], counts[1])


def meet(replicas):
    section, me = lax.axis_index("section"), lax.axis_index("dp")
    barrier = pltpu.get_barrier_semaphore()
    pl.semaphore_signal(barrier, inc=1, device_id={"section": 1 - section}, device_id_type=MESH)
    for step in range(1, replicas):
        pl.semaphore_signal(
            barrier, inc=1, device_id={"dp": lax.rem(me + step, replicas)}, device_id_type=MESH
        )
    pl.semaphore_wait(barrier, replicas)


def gather_body(
    low_ref, cnt_ref, vec_ref, fac_ref, flat_ref, cnts_ref, vec2_ref, fac2_ref,
    send_sem, recv_sem, swap_sem, cnt_send, cnt_recv, side_send, side_recv, own_sem, *, replicas, size,
):
    section, me = lax.axis_index("section"), lax.axis_index("dp")
    other = 1 - section
    nz, ny, nx = grid_of(replicas)
    x, y, z = lax.rem(me, nx), lax.rem(me // nx, ny), me // (nx * ny)
    cut = size // 2 // 8 * 8 if size % 8 == 0 else size
    halves = [(0, cut), (cut, size - cut)] if cut < size else [(0, cut)]
    used = used_rows(section)
    used_other = used_rows(other)

    def block_id(at_z, at_y, at_x):
        return (at_z * ny + at_y) * nx + at_x

    meet(replicas)

    def side(src, dst, slot):
        return pltpu.make_async_remote_copy(
            src_ref=src, dst_ref=dst.at[section], send_sem=side_send.at[slot], recv_sem=side_recv.at[slot],
            device_id={"section": other}, device_id_type=MESH,
        )

    def count_copy(step):
        return pltpu.make_async_remote_copy(
            src_ref=cnt_ref, dst_ref=cnts_ref.at[me], send_sem=cnt_send.at[step],
            recv_sem=cnt_recv.at[step], device_id={"dp": lax.rem(me + step, replicas)}, device_id_type=MESH,
        )

    for step in range(1, replicas):
        count_copy(step).start()
    side(vec_ref, vec2_ref, 0).start()
    side(fac_ref, fac2_ref, 1).start()
    own = pltpu.make_async_copy(low_ref, flat_ref.at[section * replicas + me], own_sem)
    own.start()

    def copy(block, half, target, way, mine=False, swap=False):
        start, rows = halves[half]
        at = flat_ref.at[section * replicas + block, pl.ds(start, rows)]
        src = low_ref.at[pl.ds(start, rows)] if mine else at
        return pltpu.make_async_remote_copy(
            src_ref=src, dst_ref=at, send_sem=send_sem.at[block, half, way],
            recv_sem=(swap_sem if swap else recv_sem).at[block, half], device_id=target, device_id_type=MESH,
        )

    def needed(block, half, limit):
        return block * size + halves[half][0] < limit

    def at_z(value):
        return {"dp": block_id(value, y, x)}

    def along_x(block, half, mine=False):
        for step in range(1, nx):
            copy(block, half, {"dp": block_id(z, y, lax.rem(x + step, nx))}, 1 + step, mine).start()

    def along_y(block, half, mine=False):
        for step in range(1, ny):
            copy(block, half, {"dp": block_id(z, lax.rem(y + step, ny), x)}, nx + step, mine).start()

    def across(block, half, mine=False):
        copy(block, half, {"section": other}, nx + ny, mine, True).start()

    def arrived(block, half):
        copy(block, half, {"section": other}, 0).wait_recv()

    def layers(k):
        return [z] if k == 0 else [z - k, z + k]

    def valid(at):
        return (at >= 0) & (at < nz)

    def first(k):
        for which, layer in enumerate(layers(k)):
            block = block_id(layer, y, x)
            for half in range(len(halves)):

                @pl.when(valid(layer) & needed(block, half, used))
                def _():
                    if k > 0:
                        arrived(block, half)
                    mine = k == 0
                    if k == 0 or which == 0:

                        @pl.when(z + 1 < nz)
                        def _():
                            copy(block, half, at_z(z + 1), 0, mine).start()

                    if k == 0 or which == 1:

                        @pl.when(z > 0)
                        def _():
                            copy(block, half, at_z(z - 1), 1, mine).start()

                    if half == 0:
                        along_x(block, half, mine)
                        along_y(block, half, mine)
                    else:
                        along_y(block, half, mine)
                        along_x(block, half, mine)
                    across(block, half, mine)

    def second(k):
        for layer in layers(k):
            for half in range(len(halves)):
                for step in range(1, nx if half == 0 else ny):
                    if half == 0:
                        block = block_id(layer, y, lax.rem(x + step, nx))
                    else:
                        block = block_id(layer, lax.rem(y + step, ny), x)

                    @pl.when(valid(layer) & needed(block, half, used))
                    def _():
                        arrived(block, half)
                        if half == 0:
                            along_y(block, half)
                        else:
                            along_x(block, half)
                        across(block, half)

    def third(k):
        for layer in layers(k):
            for half in range(len(halves)):
                for far in range(1, ny if half == 0 else nx):
                    for near in range(nx if half == 0 else ny):
                        if half == 0:
                            block = block_id(layer, lax.rem(y + far, ny), lax.rem(x + near, nx))
                        else:
                            block = block_id(layer, lax.rem(y + near, ny), lax.rem(x + far, nx))

                        @pl.when(valid(layer) & needed(block, half, used))
                        def _():
                            arrived(block, half)
                            across(block, half)

    for k in range(nz + 2):
        if k < nz:
            first(k)
        if 0 <= k - 1 < nz:
            second(k - 1)
        if 0 <= k - 2 < nz:
            third(k - 2)

    def drain(block, carry):
        at_x_, at_y_, at_z_ = lax.rem(block, nx), lax.rem(block // nx, ny), block // (nx * ny)
        for half in range(len(halves)):
            column = (at_x_ == x) & (at_y_ == y)

            @pl.when(needed(block, half, used))
            def _():
                @pl.when(column & (at_z_ <= z) & (z + 1 < nz))
                def _():
                    copy(block, half, {"section": other}, 0).wait_send()

                @pl.when(column & (at_z_ >= z) & (z > 0))
                def _():
                    copy(block, half, {"section": other}, 1).wait_send()

                single = len(halves) == 1
                sent_x = (column if half == 0 else at_x_ == x)
                sent_y = (at_y_ == y) if half == 0 else column

                @pl.when(sent_x)
                def _():
                    for step in range(1, nx):
                        copy(block, half, {"section": other}, 1 + step).wait_send()

                @pl.when(sent_y)
                def _():
                    for step in range(1, ny):
                        copy(block, half, {"section": other}, nx + step).wait_send()

                copy(block, half, {"section": other}, nx + ny).wait_send()

            @pl.when(needed(block, half, used_other))
            def _():
                copy(block, half, {"section": other}, 0, False, True).wait_recv()

        return carry

    lax.fori_loop(0, replicas, drain, 0)
    own.wait()
    for step in range(1, replicas):
        count_copy(step).wait()
    cnts_ref[me] = cnt_ref[...]
    vec2_ref[section] = vec_ref[...]
    fac2_ref[section] = fac_ref[...]
    side(vec_ref, vec2_ref, 0).wait()
    side(fac_ref, fac2_ref, 1).wait()


def gather(low, cnt, vec, fac, replicas):
    size = low.shape[0]
    vmem = pl.BlockSpec(memory_space=pltpu.VMEM)
    nz, ny, nx = grid_of(replicas)
    dma = pltpu.SemaphoreType.DMA
    return pl.pallas_call(
        functools.partial(gather_body, replicas=replicas, size=size),
        in_specs=[vmem] * 4,
        out_specs=[pl.BlockSpec(memory_space=pl.ANY), vmem, vmem, vmem],
        out_shape=[
            jax.ShapeDtypeStruct((2 * replicas, size, LANES), bf16),
            jax.ShapeDtypeStruct((replicas,) + cnt.shape, f32),
            jax.ShapeDtypeStruct((2,) + vec.shape, f32),
            jax.ShapeDtypeStruct((2,) + fac.shape, f32),
        ],
        scratch_shapes=[
            dma((replicas, 2, nx + ny + 1)), dma((replicas, 2)), dma((replicas, 2)),
            dma((replicas,)), dma((replicas,)), dma((2,)), dma((2,)), dma(()),
        ],
        compiler_params=pltpu.CompilerParams(collective_id=2, has_side_effects=True),
        name="gather",
    )(low, cnt, vec, fac)


def sum_body(
    part_ref, extra_ref, total_ref, mine, came, slots, seg, swap_send, swap_recv, send_a, recv_a, send_b, recv_b,
    *, replicas,
):
    section, me = lax.axis_index("section"), lax.axis_index("dp")
    other = 1 - section
    rows = part_ref.shape[1]
    size = rows // replicas
    meet(replicas)

    def rows_of(index):
        return pl.ds(pl.multiple_of(index * size, 8), size)

    swap = pltpu.make_async_remote_copy(
        src_ref=part_ref.at[other], dst_ref=came, send_sem=swap_send.at[0], recv_sem=swap_recv.at[0],
        device_id={"section": other}, device_id_type=MESH,
    )
    swap.start()
    mine[...] = part_ref[section] + extra_ref[...]
    swap.wait()
    mine[...] = mine[...] + came[...]

    def scatter(step):
        peer = lax.rem(me + step, replicas)
        return pltpu.make_async_remote_copy(
            src_ref=mine.at[rows_of(peer)], dst_ref=slots.at[step], send_sem=send_a.at[step],
            recv_sem=recv_a.at[step], device_id={"dp": peer}, device_id_type=MESH,
        )

    def spread(step):
        peer = lax.rem(me + step, replicas)
        return pltpu.make_async_remote_copy(
            src_ref=seg, dst_ref=total_ref.at[section, rows_of(me)], send_sem=send_b.at[step],
            recv_sem=recv_b.at[step], device_id={"dp": peer}, device_id_type=MESH,
        )

    for step in range(1, replicas):
        scatter(step).start()
    total = mine[rows_of(me), :]
    for step in range(1, replicas):
        scatter(step).wait_recv()
        total = total + slots[step]
    seg[...] = total
    for step in range(1, replicas):
        spread(step).start()
    total_ref[section, rows_of(me)] = total
    for step in range(1, replicas):
        scatter(step).wait_send()
        spread(step).wait()
    back = pltpu.make_async_remote_copy(
        src_ref=total_ref.at[section], dst_ref=total_ref.at[section], send_sem=swap_send.at[1],
        recv_sem=swap_recv.at[1], device_id={"section": other}, device_id_type=MESH,
    )
    back.start()
    back.wait()


def all_sum(part, extra, replicas, collective_id):
    rows = part.shape[1]
    vmem = pl.BlockSpec(memory_space=pltpu.VMEM)
    dma = pltpu.SemaphoreType.DMA
    size = rows // replicas
    return pl.pallas_call(
        functools.partial(sum_body, replicas=replicas),
        in_specs=[vmem, vmem],
        out_specs=vmem,
        out_shape=jax.ShapeDtypeStruct(part.shape, f32),
        scratch_shapes=[
            pltpu.VMEM((rows, LANES), f32), pltpu.VMEM((rows, LANES), f32),
            pltpu.VMEM((replicas, size, LANES), f32), pltpu.VMEM((size, LANES), f32),
            dma((2,)), dma((2,)), dma((replicas,)), dma((replicas,)), dma((replicas,)), dma((replicas,)),
        ],
        compiler_params=pltpu.CompilerParams(collective_id=collective_id, has_side_effects=True),
        name="all_sum",
    )(part, extra)


def swap_body(*refs, n_enc, n_dec):
    n = n_enc + n_dec
    src, dst = refs[:n], refs[n : 2 * n]
    send, recv = refs[2 * n :]
    me = lax.axis_index("section")
    other = 1 - me
    barrier = pltpu.get_barrier_semaphore()
    pl.semaphore_signal(barrier, inc=1, device_id={"section": other}, device_id_type=pl.DeviceIdType.MESH)
    pl.semaphore_wait(barrier, 1)

    def copy(i):
        return pltpu.make_async_remote_copy(
            src_ref=src[i],
            dst_ref=dst[i],
            send_sem=send.at[i],
            recv_sem=recv.at[i],
            device_id={"section": other},
            device_id_type=pl.DeviceIdType.MESH,
        )

    enc, dec = range(n_enc), range(n_enc, n)

    @pl.when(me == 0)
    def _():
        for i in dec:
            copy(i).start()
        for i in dec:
            copy(i).wait_send()
        for i in enc:
            copy(i).wait_recv()

    @pl.when(me == 1)
    def _():
        for i in enc:
            copy(i).start()
        for i in enc:
            copy(i).wait_send()
        for i in dec:
            copy(i).wait_recv()


def swap(enc, dec):
    arrays = list(enc) + list(dec)
    n = len(arrays)
    outs = pl.pallas_call(
        functools.partial(swap_body, n_enc=len(enc), n_dec=len(dec)),
        in_specs=[pl.BlockSpec(memory_space=pl.ANY)] * n,
        out_specs=[pl.BlockSpec(memory_space=pl.ANY)] * n,
        out_shape=[jax.ShapeDtypeStruct(a.shape, a.dtype) for a in arrays],
        scratch_shapes=[pltpu.SemaphoreType.DMA((n,)), pltpu.SemaphoreType.DMA((n,))],
        compiler_params=pltpu.CompilerParams(collective_id=1, has_side_effects=True),
        name="swap",
    )(*arrays)
    return outs[: len(enc)], outs[len(enc) :]


def pack_rows(rows, pieces, width, length):
    empty = jnp.zeros((width,), f32)
    parts = [empty if row is None else row for row in rows] + pieces
    used = sum(part.shape[0] for part in parts)
    return jnp.concatenate(parts + [jnp.zeros((length - used,), f32)])


def local(pixels, visible, masked, loss_mask, master, momentum, vectors, vec_moment, factors, errors):
    sec = lax.axis_index("section")
    replicas = lax.axis_size("dp")
    replica_id = lax.axis_index("dp")

    replicas_n = replicas
    shard_len = master.shape[1]
    size = shard_len // LANES
    gain = float(replicas)

    count_tile = jnp.full((RANK, LANES), jnp.sum(loss_mask).astype(f32))
    vec_tile = jnp.pad(vectors[0], (0, VEC_TILES * RANK * LANES - VLEN)).reshape(-1, LANES)
    flat_both, counts, vec_both, fac_both = gather(
        master[0].astype(bf16).reshape(size, LANES), count_tile, vec_tile, factors[0], replicas
    )
    low_both = flat_both.reshape(-1, LANES)
    vec_both = vec_both.reshape(2, -1)
    count = jnp.sum(counts[:, 0, 0])

    vis = lax.dynamic_index_in_dim(visible, sec, 0, keepdims=False)
    mas = lax.dynamic_index_in_dim(masked, sec, 0, keepdims=False)
    mask_row = lax.dynamic_index_in_dim(loss_mask, sec, 0, keepdims=False).astype(f32)
    order = jnp.concatenate([vis, mas])
    pix = lax.dynamic_index_in_dim(pixels, sec, 0, keepdims=False)
    pick = (order[:, None] == jnp.arange(SEQ, dtype=jnp.int32)[None, :]).astype(bf16)
    pix_order = nn(pick, pix).astype(bf16)
    pix_vis = pix_order[:VIS]
    target = pix_order[VIS:].astype(f32)
    table_dec = positions_at(order, DD)
    table_enc = positions_at(vis, DE)
    tail_row = ROW_PAD // LANES * RANK
    tail_rows = (VEC_TILES + 1) * RANK
    left_rows = sum_rows(replicas, ROW_PAD // LANES + VEC_TILES + 1)
    right_rows = sum_rows(replicas, max(COL_WIDTHS) // LANES)

    def errs_for(section):
        def run():
            buf = None
            lefts = []
            start = 0
            col_at = 0
            for rows_n, cols_n in section_shapes(section):
                buf, left = err_prep(errors, factors[0][:, col_at : col_at + cols_n], start, rows_n, cols_n, buf)
                lefts.append(left)
                start += rows_n * cols_n
                col_at += cols_n
            done = sum(left.shape[0] for left in lefts)
            lefts.append(jnp.zeros((left_rows - done, LANES), f32))
            return buf, jnp.concatenate(lefts)

        return run

    err_stack, err_lefts = lax.cond(sec == 0, errs_for(0), errs_for(1))

    enc = unflat_all(low_both, 0, 0)
    dec = unflat_all(low_both, FLAT, 1)
    rows_e, bias_e, unused = unpack_vecs(vec_both[0], DE, FFE)
    rows_d, bias_d, extra_d = unpack_vecs(vec_both[1], DD, FFD)

    embedded = nn(pix_vis, enc[4]) + rows_e[10] + table_enc
    coded, kept_e = block_forward(embedded, enc, rows_e, bias_e, HEADS_ENC)
    sent_full, sent_pull = jax.vjp(layer_norm, coded, rows_e[4], rows_e[5])
    sent = sent_full.astype(bf16)
    projected = nn(sent, dec[5]) + extra_d
    filled = jnp.concatenate([projected, jnp.broadcast_to(rows_d[10], (SEQ - VIS, DD))]) + table_dec
    result, kept_d = block_forward(filled, dec, rows_d, bias_d, HEADS_DEC)
    final_full, final_pull = jax.vjp(layer_norm, result[VIS:], rows_d[4], rows_d[5])
    final = final_full.astype(bf16)
    residual = nt(final, dec[4]) - target
    loss_part = jnp.sum(mask_row * jnp.mean(residual * residual, axis=1)) / count
    grad_pred = (mask_row[:, None] * (2.0 * residual / PATCH) / count).astype(bf16)
    grad_picked, v_gain3, v_shift3 = final_pull(nn(grad_pred, dec[4]))
    grad_result = jnp.concatenate([jnp.zeros((VIS, DD), f32), grad_picked])
    grad_filled, pairs_d, vrows_d, v_up_d = block_backward(kept_d, grad_result, dec, rows_d, HEADS_DEC)
    b_proj = grad_filled[:VIS].astype(bf16)
    pairs_d = pairs_d + [(grad_pred, final), (sent, b_proj)]
    vrows_d[4], vrows_d[5], vrows_d[10] = v_gain3, v_shift3, jnp.sum(grad_filled[VIS:], axis=0)
    vec_d = pack_rows(vrows_d, [v_up_d, jnp.sum(b_proj.astype(f32), axis=0)], DD, VLEN)
    grad_sent = nt(b_proj, dec[5]).astype(bf16)
    grad_coded, v_gain3, v_shift3 = sent_pull(grad_sent.astype(f32))
    grad_start, pairs_e, vrows_e, v_up_e = block_backward(kept_e, grad_coded, enc, rows_e, HEADS_ENC)
    b_start = grad_start.astype(bf16)
    pairs_e = pairs_e + [(pix_vis, b_start)]
    vrows_e[4], vrows_e[5], vrows_e[10] = v_gain3, v_shift3, jnp.sum(b_start.astype(f32), axis=0)
    vec_e = pack_rows(vrows_e, [v_up_e], DE, VLEN)

    pairs = pairs_e + pairs_d
    n_enc = len(pairs_e)
    flat_e = [x for pair in pairs_e for x in pair]
    flat_d = [x for pair in pairs_d for x in pair]
    vec_tiles = jnp.pad(jnp.stack([vec_e, vec_d]), ((0, 0), (0, VEC_TILES * RANK * LANES - VLEN))).reshape(2, -1, LANES)
    loss_tile = jnp.stack([jnp.full((RANK, LANES), loss_part), jnp.zeros((RANK, LANES), f32)])
    tail = jnp.concatenate([vec_tiles, loss_tile], axis=1)
    left_part = skinny(
        fac_both, [b for a, b in pairs], [a for a, b in pairs], COL_SPANS, ROW_SPANS, tail, tail_row, gain, left_rows
    )
    other_e, other_d = swap(flat_e, flat_d)
    left_sum = all_sum(left_part, err_lefts, replicas, 3)
    vec_sum = left_sum[:, tail_row : tail_row + VEC_TILES * RANK]
    loss_sum = left_sum[0, tail_row + VEC_TILES * RANK, 0]

    ortho = orthonormal(left_sum, 1.0 / replicas)
    right_part = skinny(
        ortho, [a for a, b in pairs], [b for a, b in pairs], ROW_SPANS, COL_SPANS, tail, 0, gain, right_rows
    )
    err_rights = lax.cond(
        sec == 0,
        lambda: err_right(ortho, err_stack, 0, right_rows),
        lambda: err_right(ortho, err_stack, 1, right_rows),
    )
    sums = all_sum(right_part, err_rights, replicas, 4)
    right_both, norm_row = final_right(sums, ortho, vec_sum, factors.shape[2], 1.0 / replicas)
    norm = norm_row[0, 0]
    scale = jnp.minimum(1.0, clip_limit / (norm + 1e-06))

    def finish_for(section):
        def run():
            mine = pairs_e if section == 0 else pairs_d
            flat = other_e if section == 0 else other_d
            theirs = [(flat[2 * i], flat[2 * i + 1]) for i in range(len(mine))]
            bufs = None
            start = 0
            base = 0 if section == 0 else n_enc
            for i, (rows_n, cols_n) in enumerate(section_shapes(section)):
                bufs = finish(
                    mine[i], theirs[i], err_stack, ortho, right_both, section,
                    ROW_SPANS[base + i][1], COL_SPANS[base + i][1], start, gain, bufs,
                )
                start += rows_n * cols_n
            if start < FLAT:
                bufs = finish_tail(errors, start, bufs)
            return bufs

        return run

    new_errors, approx = lax.cond(sec == 0, finish_for(0), finish_for(1))
    own_part = lax.dynamic_slice_in_dim(approx.reshape(-1), replica_id * shard_len, shard_len)
    rate = learning_rate()
    new_moment = moment_decay * momentum[0] + scale * own_part
    new_master = master[0] - rate * new_moment
    vec_own = lax.dynamic_index_in_dim(vec_sum, sec, 0, keepdims=False).reshape(-1)[:VLEN]
    new_vm = moment_decay * vec_moment[0] + scale * vec_own
    new_vectors = vectors[0] - rate * new_vm
    new_factors = lax.dynamic_index_in_dim(right_both, sec, 0, keepdims=False)
    return (
        new_master[None],
        new_master.astype(bf16)[None],
        new_moment[None],
        new_vectors[None],
        new_vm[None],
        new_factors[None],
        new_errors.reshape(1, 1, -1),
        loss_sum.reshape(1),
        norm.reshape(1),
    )


def solution(mesh):
    return jax.shard_map(
        local,
        mesh=mesh,
        in_specs=(
            P("dp", None, None),
            P("dp", None),
            P("dp", None),
            P("dp", None),
            P("section", "dp"),
            P("section", "dp"),
            P("section", None),
            P("section", None),
            P("section", None, None),
            P("section", "dp", None),
        ),
        out_specs=(
            P("section", "dp"),
            P("section", "dp"),
            P("section", "dp"),
            P("section", None),
            P("section", None),
            P("section", None, None),
            P("section", "dp", None),
            P(),
            P(),
        ),
        check_vma=False,
    )
```

```python
import functools
import math

import jax
import jax.numpy as jnp
import numpy as np
from jax import lax
from jax.experimental import pallas as pl
from jax.experimental.pallas import tpu as pltpu
from jax.sharding import PartitionSpec as P

DE = 768
FFE = 3072
HEADS_ENC = 12
DD = 512
FFD = 2048
HEADS_DEC = 16
PATCH = 192
RANK = 8
SEQ = 1024
VIS = 256
FLAT = 7225344
VLEN = 11520

f32 = jnp.float32
bf16 = jnp.bfloat16
clip_limit = 0.0001
moment_decay = 0.9
rate_base = 0.5
LANES = 128
STEP = 32
BLOCK = 256
CHUNK = 256
SPARE = 6144
BIG = 66000000


def nn(left, right):
    return lax.dot_general(left, right, (((1,), (0,)), ((), ())), preferred_element_type=f32)


def nt(left, right):
    return lax.dot_general(left, right, (((1,), (1,)), ((), ())), preferred_element_type=f32)


def tn(left, right):
    return lax.dot_general(left, right, (((0,), (0,)), ((), ())), preferred_element_type=f32)


def split3(value):
    high = value.astype(bf16)
    rest = value - high.astype(f32)
    middle = rest.astype(bf16)
    return jnp.concatenate([high, middle, (rest - middle.astype(f32)).astype(bf16)], axis=0)


def join3(value):
    return value[:RANK] + value[RANK : 2 * RANK] + value[2 * RANK :]


def norm_parts(tokens):
    centred = tokens - jnp.mean(tokens, axis=-1, keepdims=True)
    spread = lax.rsqrt(jnp.mean(centred * centred, axis=-1, keepdims=True) + 1e-06)
    return centred * spread, spread


def norm_back(grad, hat, spread, gain):
    inner = grad * gain
    return spread * (
        inner - jnp.mean(inner, axis=-1, keepdims=True) - hat * jnp.mean(inner * hat, axis=-1, keepdims=True)
    )


def column_sum(value):
    return jnp.sum(value.astype(f32), axis=0, keepdims=True)


def angle_tables(width):
    column = np.arange(width)
    freqs = np.exp(-(column // 2 * 2) / width * math.log(10000.0))
    coarse = (np.arange(0, SEQ, STEP)[:, None] * freqs).astype(np.float64)
    fine = np.arange(STEP)[:, None] * freqs + (column % 2) * (math.pi / 2)
    return jnp.asarray(np.stack([np.sin(coarse), np.cos(coarse), np.cos(fine), np.sin(fine)]), f32)


def positions_of(place, tables):
    column = lax.broadcasted_iota(jnp.int32, (1, STEP), 1)
    coarse = (place // STEP == column).astype(bf16)
    fine = (place % STEP == column).astype(bf16)

    def take(pick, table):
        high = table.astype(bf16)
        rest = table - high.astype(f32)
        middle = rest.astype(bf16)
        low = (rest - middle.astype(f32)).astype(bf16)
        return nn(pick, high) + nn(pick, middle) + nn(pick, low)

    return take(coarse, tables[0]) * take(fine, tables[2]) + take(coarse, tables[1]) * take(fine, tables[3])


def section_shapes(section):
    if section == 0:
        return [(DE, 3 * DE), (DE, DE), (DE, FFE), (FFE, DE), (PATCH, DE)]
    return [(DD, 3 * DD), (DD, DD), (DD, FFD), (FFD, DD), (PATCH, DD), (DE, DD)]


def unpack_vecs(flat, width, hidden):
    return (
        flat[: 11 * width].reshape(11, width),
        flat[11 * width : 11 * width + hidden],
        flat[11 * width + hidden : 12 * width + hidden],
    )


def learning_rate():
    return rate_base * math.sqrt(2.0 * (FLAT + VLEN) / DD) / clip_limit


def unflat_body(src_ref, out_ref, wide_ref, *, blocks, rows, stacked):
    wide_ref[...] = src_ref[...].astype(f32)
    for block in range(blocks):
        part = wide_ref[pl.ds(block, rows, stride=blocks), :].astype(bf16)
        if stacked:
            out_ref[block] = part
        else:
            out_ref[:, block * LANES : (block + 1) * LANES] = part


def unflat(flat, start, rows_n, cols_n, stacked=False):
    blocks = cols_n // LANES
    rows = 192 if rows_n == PATCH else 128 if blocks > 8 else 256
    if stacked:
        out_shape = jax.ShapeDtypeStruct((blocks, rows_n, LANES), bf16)
        out_spec = pl.BlockSpec((blocks, rows, LANES), lambda i: (0, i, 0))
    else:
        out_shape = jax.ShapeDtypeStruct((rows_n, cols_n), bf16)
        out_spec = pl.BlockSpec((rows, cols_n), lambda i: (i, 0))
    step = rows * blocks
    return pl.pallas_call(
        functools.partial(unflat_body, blocks=blocks, rows=rows, stacked=stacked),
        grid=(rows_n // rows,),
        in_specs=[pl.BlockSpec((pl.Element(step), pl.Element(LANES)), lambda i: (pl.multiple_of(start // LANES + i * step, 16), 0))],
        out_specs=out_spec,
        out_shape=out_shape,
        scratch_shapes=[pltpu.VMEM((step, LANES), f32)],
        name="unflat",
    )(flat)


def unflat_all(flat, start, section, stacked=False):
    mats = []
    for rows_n, cols_n in section_shapes(section):
        mats.append(unflat(flat, start, rows_n, cols_n, stacked))
        start += rows_n * cols_n
    return mats


def head_mask(head, size):
    lane = lax.broadcasted_iota(jnp.int32, (1, LANES), 1)
    return (lane // size == head).astype(bf16)


def attend_body(q_ref, k_ref, v_ref, o_ref, lse_ref, *, size, rows_q):
    seq = k_ref.shape[0]
    scale = size ** (-0.5)
    fold = scale * math.log2(math.e)

    def one(step, carry):
        at = pl.ds(pl.multiple_of(step * rows_q, rows_q), rows_q)
        queries = q_ref[at, :]
        total = jnp.zeros((rows_q, LANES), f32)
        for head in range(LANES // size):
            mask = head_mask(head, size)
            scores = nt(k_ref[...], queries * mask)
            peak = jnp.max(scores, axis=0, keepdims=True) * fold
            power = jnp.exp2(scores * fold - peak)
            mass = jnp.sum(power, axis=0, keepdims=True)
            probs = (power * (1.0 / mass)).astype(bf16)
            total = total + tn(probs, v_ref[...] * mask)
            lse_ref[0, head : head + 1, at] = peak + jnp.log2(mass)
        o_ref[at, :] = total
        return carry

    lax.fori_loop(0, seq // rows_q, one, 0)


def attend(joined, heads):
    seq, width = joined.shape[0], joined.shape[1] // 3
    size = width // heads
    groups = width // LANES
    per = LANES // size
    rows_q = min(512, seq)
    return pl.pallas_call(
        functools.partial(attend_body, size=size, rows_q=rows_q),
        grid=(groups,),
        in_specs=[
            pl.BlockSpec((seq, LANES), lambda g: (0, g)),
            pl.BlockSpec((seq, LANES), lambda g: (0, groups + g)),
            pl.BlockSpec((seq, LANES), lambda g: (0, 2 * groups + g)),
        ],
        out_specs=[
            pl.BlockSpec((seq, LANES), lambda g: (0, g)),
            pl.BlockSpec((1, per, seq), lambda g: (g, 0, 0)),
        ],
        out_shape=[
            jax.ShapeDtypeStruct((seq, width), f32),
            jax.ShapeDtypeStruct((groups, per, seq), f32),
        ],
        name="attend",
    )(joined, joined, joined)


def attend_back_body(q_ref, k_ref, v_ref, do_ref, o_ref, lse_ref, dq_ref, dk_ref, dv_ref, dk_sum, dv_sum, *, size, rows_q):
    seq = k_ref.shape[0]
    scale = size ** (-0.5)
    fold = scale * math.log2(math.e)
    dk_sum[...] = jnp.zeros_like(dk_sum)
    dv_sum[...] = jnp.zeros_like(dv_sum)

    def one(step, carry):
        at = pl.ds(pl.multiple_of(step * rows_q, rows_q), rows_q)
        queries = q_ref[at, :]
        grads = do_ref[at, :]
        prod = grads.astype(f32) * o_ref[at, :]
        total = jnp.zeros((rows_q, LANES), f32)
        high = prod.astype(bf16)
        rest = prod - high.astype(f32)
        middle = rest.astype(bf16)
        for head in range(LANES // size):
            mask = head_mask(head, size)
            wide = jnp.broadcast_to(mask, (16, LANES))
            delta = (nt(wide, high) + nt(wide, middle))[0:1]
            q_one = queries * mask
            g_one = grads * mask
            scores = nt(k_ref[...], q_one)
            probs = jnp.exp2(scores * fold - lse_ref[0, head : head + 1, at])
            slope = nt(v_ref[...], g_one)
            grad_s = (probs * (slope - delta)).astype(bf16)
            dv_sum[...] += nn(probs.astype(bf16), g_one)
            dk_sum[...] += nn(grad_s, q_one)
            total = total + tn(grad_s, k_ref[...] * mask)
        dq_ref[at, :] = (total * scale).astype(bf16)
        return carry

    lax.fori_loop(0, seq // rows_q, one, 0)
    dk_ref[...] = (dk_sum[...] * scale).astype(bf16)
    dv_ref[...] = dv_sum[...].astype(bf16)


def attend_back(joined, grad_out, out, lse, heads):
    seq, width = joined.shape[0], joined.shape[1] // 3
    size = width // heads
    groups = width // LANES
    per = LANES // size
    rows_q = min(512, seq)
    col = pl.BlockSpec((seq, LANES), lambda g: (0, g))
    return pl.pallas_call(
        functools.partial(attend_back_body, size=size, rows_q=rows_q),
        grid=(groups,),
        in_specs=[
            col,
            pl.BlockSpec((seq, LANES), lambda g: (0, groups + g)),
            pl.BlockSpec((seq, LANES), lambda g: (0, 2 * groups + g)),
            col,
            col,
            pl.BlockSpec((1, per, seq), lambda g: (g, 0, 0)),
        ],
        out_specs=[col, col, col],
        out_shape=[jax.ShapeDtypeStruct((seq, width), bf16)] * 3,
        scratch_shapes=[pltpu.VMEM((seq, LANES), f32)] * 2,
        name="attend_back",
    )(joined, joined, joined, grad_out, out, lse)


GRID = pltpu.CompilerParams(vmem_limit_bytes=BIG, dimension_semantics=("arbitrary",))


def tokens_spec(width, rows=BLOCK):
    return pl.BlockSpec((rows, width), lambda i: (i, 0))


def fixed(array):
    rank = len(array.shape)
    return pl.BlockSpec(array.shape, lambda i: (0,) * rank, pipeline_mode=pl.Buffered(1))


def kept_spec(shape):
    return pl.BlockSpec(shape, lambda i: (0,) * len(shape))


def shape_of(rows, cols, dtype=f32):
    return jax.ShapeDtypeStruct((rows, cols), dtype)


def embed_body(pix_ref, e_ref, vec_ref, place_ref, table_ref, out_ref):
    out_ref[...] = nn(pix_ref[...], e_ref[...]) + vec_ref[10:11] + positions_of(place_ref[...], table_ref)


def embed(pix, weight, vecs, place, tables):
    args = [pix, weight, vecs, place, tables]
    return pl.pallas_call(
        embed_body,
        grid=(1,),
        in_specs=[fixed(x) for x in args],
        out_specs=tokens_spec(weight.shape[1]),
        out_shape=shape_of(pix.shape[0], weight.shape[1]),
        compiler_params=GRID,
        name="embed",
    )(*args)


def relay_body(coded_ref, vec_e_ref, w_ref, extra_ref, vec_d_ref, place_ref, table_ref, sent_ref, out_ref):
    step = pl.program_id(0)
    place = positions_of(place_ref[...], table_ref)

    @pl.when(step == 0)
    def _():
        hat, unused = norm_parts(coded_ref[...])
        sent = (hat * vec_e_ref[4:5] + vec_e_ref[5:6]).astype(bf16)
        sent_ref[...] = sent
        out_ref[...] = nn(sent, w_ref[...]) + extra_ref[...] + place

    @pl.when(step > 0)
    def _():
        out_ref[...] = vec_d_ref[10:11] + place


def relay(coded, vec_e, weight, extra, vec_d, place, tables):
    args = [coded, vec_e, weight, extra, vec_d]
    return pl.pallas_call(
        relay_body,
        grid=(SEQ // VIS,),
        in_specs=[fixed(x) for x in args] + [pl.BlockSpec((VIS, 1), lambda i: (i, 0)), fixed(tables)],
        out_specs=[kept_spec((VIS, DE)), tokens_spec(DD, VIS)],
        out_shape=[shape_of(VIS, DE, bf16), shape_of(SEQ, DD)],
        compiler_params=GRID,
        name="relay",
    )(*args, place, tables)


def relay_back_body(b_ref, w_ref, coded_ref, vec_ref, out_ref, sums_ref):
    grad = nt(b_ref[...], w_ref[...]).astype(bf16).astype(f32)
    hat, spread = norm_parts(coded_ref[...])
    out_ref[...] = norm_back(grad, hat, spread, vec_ref[4:5])
    sums_ref[...] = jnp.zeros_like(sums_ref)
    sums_ref[0:1] = column_sum(grad * hat)
    sums_ref[1:2] = column_sum(grad)


def relay_back(b_proj, weight, coded, vecs):
    args = [b_proj, weight, coded, vecs]
    return pl.pallas_call(
        relay_back_body,
        grid=(1,),
        in_specs=[fixed(x) for x in args],
        out_specs=[tokens_spec(DE), kept_spec((8, DE))],
        out_shape=[shape_of(VIS, DE), shape_of(8, DE)],
        compiler_params=GRID,
        name="relay_back",
    )(*args)


def open_body(tok_ref, vec_ref, w_ref, normed_ref, joined_ref):
    width = tok_ref.shape[1]
    hat, unused = norm_parts(tok_ref[...])
    normed = (hat * vec_ref[0:1] + vec_ref[1:2]).astype(bf16)
    normed_ref[...] = normed
    for part, bias in ((0, vec_ref[6:7]), (1, None), (2, vec_ref[7:8])):
        cols = slice(part * width, (part + 1) * width)
        value = nn(normed, w_ref[:, cols])
        joined_ref[:, cols] = (value if bias is None else value + bias).astype(bf16)


def open_block(tokens, vecs, weight):
    seq, width = tokens.shape
    return pl.pallas_call(
        open_body,
        grid=(seq // BLOCK,),
        in_specs=[tokens_spec(width), fixed(vecs), fixed(weight)],
        out_specs=[tokens_spec(width), tokens_spec(3 * width)],
        out_shape=[shape_of(seq, width, bf16), shape_of(seq, 3 * width, bf16)],
        compiler_params=GRID,
        name="open_block",
    )(tokens, vecs, weight)


def erf(value):
    return lax.erf(value)


def close_body(tok_ref, o_ref, vec_ref, bias_ref, wo_ref, w1_ref, w2_ref, att_ref, mid_ref, sec_ref, act_ref, slope_ref, out_ref):
    attended = o_ref[...].astype(bf16)
    att_ref[...] = attended
    middle = tok_ref[...] + nn(attended, wo_ref[...]) + vec_ref[8:9]
    mid_ref[...] = middle
    hat, unused = norm_parts(middle)
    sec_ref[...] = (hat * vec_ref[2:3] + vec_ref[3:4]).astype(bf16)
    out_ref[...] = middle + vec_ref[9:10]

    def one(step, carry):
        cols = pl.ds(pl.multiple_of(step * CHUNK, CHUNK), CHUNK)
        hidden = nn(sec_ref[...], w1_ref[:, cols]) + bias_ref[:, cols]
        share = 0.5 * (1.0 + erf(hidden * math.sqrt(0.5)))
        active = (hidden * share).astype(bf16)
        act_ref[:, cols] = active
        slope_ref[:, cols] = share + hidden * (jnp.exp(-0.5 * hidden * hidden) * (1.0 / math.sqrt(2.0 * math.pi)))
        out_ref[...] += nn(active, w2_ref[cols, :])
        return carry

    lax.fori_loop(0, w1_ref.shape[1] // CHUNK, one, 0)


def close_block(tokens, out, vecs, bias_up, wo, w1, w2):
    seq, width = tokens.shape
    hidden = w1.shape[1]
    return pl.pallas_call(
        close_body,
        grid=(seq // BLOCK,),
        in_specs=[tokens_spec(width), tokens_spec(width)] + [fixed(x) for x in (vecs, bias_up, wo, w1, w2)],
        out_specs=[tokens_spec(width)] * 3 + [tokens_spec(hidden)] * 2 + [tokens_spec(width)],
        out_shape=[
            shape_of(seq, width, bf16), shape_of(seq, width), shape_of(seq, width, bf16),
            shape_of(seq, hidden, bf16), shape_of(seq, hidden), shape_of(seq, width),
        ],
        compiler_params=GRID,
        name="close_block",
    )(tokens, out, vecs, bias_up, wo, w1, w2)


def head_body(res_ref, vec_ref, w_ref, target_ref, mask_ref, count_ref, fin_ref, pred_ref, grad_ref, sums_ref, loss_ref):
    step = pl.program_id(0)

    @pl.when(step == 0)
    def _():
        grad_ref[...] = jnp.zeros_like(grad_ref)
        sums_ref[...] = jnp.zeros_like(sums_ref)
        loss_ref[...] = jnp.zeros_like(loss_ref)

    @pl.when(step > 0)
    def _():
        count = count_ref[0, 0]
        hat, spread = norm_parts(res_ref[...])
        final = (hat * vec_ref[4:5] + vec_ref[5:6]).astype(bf16)
        fin_ref[...] = final
        residual = nt(final, w_ref[...]) - target_ref[...].astype(f32)
        weight = mask_ref[...]
        rows = weight * jnp.mean(residual * residual, axis=1, keepdims=True)
        loss_ref[...] += jnp.broadcast_to(jnp.sum(rows, axis=0, keepdims=True) / count, loss_ref.shape)
        grad_pred = (weight * (2.0 * residual / PATCH) / count).astype(bf16)
        pred_ref[...] = grad_pred
        grad = nn(grad_pred, w_ref[...])
        grad_ref[...] = norm_back(grad, hat, spread, vec_ref[4:5])
        sums_ref[0:1] += column_sum(grad * hat)
        sums_ref[1:2] += column_sum(grad)


def head(result, vecs, weight, target, mask, count):
    late = lambda i: (jnp.maximum(i - 1, 0), 0)
    return pl.pallas_call(
        head_body,
        grid=(SEQ // VIS,),
        in_specs=[
            tokens_spec(DD, VIS), fixed(vecs), fixed(weight), pl.BlockSpec((VIS, PATCH), late),
            pl.BlockSpec((VIS, 1), late), fixed(count),
        ],
        out_specs=[
            pl.BlockSpec((VIS, DD), late), pl.BlockSpec((VIS, PATCH), late), tokens_spec(DD, VIS),
            kept_spec((8, DD)), kept_spec((8, LANES)),
        ],
        out_shape=[
            shape_of(SEQ - VIS, DD, bf16), shape_of(SEQ - VIS, PATCH, bf16), shape_of(SEQ, DD),
            shape_of(8, DD), shape_of(8, LANES),
        ],
        compiler_params=GRID,
        name="head",
    )(result, vecs, weight, target, mask, count)


def back_up_body(
    grad_ref, slope_ref, mid_ref, vec_ref, wo_ref, w1_ref, w2_ref,
    down_ref, up_ref, proj_ref, att_ref, out_ref, sums_ref, bias_ref, total,
):
    @pl.when(pl.program_id(0) == 0)
    def _():
        sums_ref[...] = jnp.zeros_like(sums_ref)
        bias_ref[...] = jnp.zeros_like(bias_ref)

    down = grad_ref[...].astype(bf16)
    down_ref[...] = down
    total[...] = jnp.zeros_like(total)

    def one(step, carry):
        cols = pl.ds(pl.multiple_of(step * CHUNK, CHUNK), CHUNK)
        part = (nt(down_ref[...], w2_ref[cols, :]) * slope_ref[:, cols]).astype(bf16)
        up_ref[:, cols] = part
        bias_ref[:, cols] += column_sum(part)
        total[...] += nt(part, w1_ref[:, cols])
        return carry

    lax.fori_loop(0, w1_ref.shape[1] // CHUNK, one, 0)
    grad = total[...]
    hat, spread = norm_parts(mid_ref[...])
    middle = grad_ref[...] + norm_back(grad, hat, spread, vec_ref[2:3])
    out_ref[...] = middle
    proj = middle.astype(bf16)
    proj_ref[...] = proj
    att_ref[...] = nt(proj, wo_ref[...]).astype(bf16)
    sums_ref[0:1] += column_sum(grad * hat)
    sums_ref[1:2] += column_sum(grad)
    sums_ref[2:3] += column_sum(proj)
    sums_ref[3:4] += column_sum(down)


def back_up(grad_result, slope, middle, vecs, wo, w1, w2):
    seq, width = middle.shape
    hidden = w1.shape[1]
    return pl.pallas_call(
        back_up_body,
        grid=(seq // BLOCK,),
        in_specs=[tokens_spec(width), tokens_spec(hidden), tokens_spec(width)] + [fixed(x) for x in (vecs, wo, w1, w2)],
        out_specs=[
            tokens_spec(width), tokens_spec(hidden), tokens_spec(width), tokens_spec(width), tokens_spec(width),
            kept_spec((8, width)), kept_spec((1, hidden)),
        ],
        out_shape=[
            shape_of(seq, width, bf16), shape_of(seq, hidden, bf16), shape_of(seq, width, bf16),
            shape_of(seq, width, bf16), shape_of(seq, width), shape_of(8, width), shape_of(1, hidden),
        ],
        scratch_shapes=[pltpu.VMEM((BLOCK, width), f32)],
        compiler_params=GRID,
        name="back_up",
    )(grad_result, slope, middle, vecs, wo, w1, w2)


def back_in_body(dq_ref, dk_ref, dv_ref, mid_ref, tok_ref, vec_ref, w_ref, join_ref, first_ref, sums_ref):
    step = pl.program_id(0)
    width = tok_ref.shape[1]

    @pl.when(step == 0)
    def _():
        sums_ref[...] = jnp.zeros_like(sums_ref)

    grad = jnp.zeros(tok_ref.shape, f32)
    for part, ref in enumerate((dq_ref, dk_ref, dv_ref)):
        cols = slice(part * width, (part + 1) * width)
        value = ref[...]
        join_ref[:, cols] = value
        grad = grad + nt(value, w_ref[:, cols])
        if part != 1:
            sums_ref[2 + part // 2 : 3 + part // 2] += column_sum(value)
    hat, spread = norm_parts(tok_ref[...])
    tokens = mid_ref[...] + norm_back(grad, hat, spread, vec_ref[0:1])
    sums_ref[0:1] += column_sum(grad * hat)
    sums_ref[1:2] += column_sum(grad)

    @pl.when(step == 0)
    def _():
        first = tokens.astype(bf16)
        first_ref[...] = first
        sums_ref[4:5] = column_sum(first)

    @pl.when(step > 0)
    def _():
        sums_ref[5:6] += column_sum(tokens)


def back_in(dq, dk, dv, middle, tokens, vecs, weight):
    seq, width = tokens.shape
    return pl.pallas_call(
        back_in_body,
        grid=(seq // BLOCK,),
        in_specs=[tokens_spec(width)] * 5 + [fixed(vecs), fixed(weight)],
        out_specs=[tokens_spec(3 * width), kept_spec((BLOCK, width)), kept_spec((8, width))],
        out_shape=[shape_of(seq, 3 * width, bf16), shape_of(BLOCK, width, bf16), shape_of(8, width)],
        compiler_params=GRID,
        name="back_in",
    )(dq, dk, dv, middle, tokens, vecs, weight)


def block_forward(tokens, mats, vecs, bias_up, heads):
    normed, joined = open_block(tokens, vecs, mats[0])
    out, lse = attend(joined, heads)
    attended, middle, second, active, slope, result = close_block(
        tokens, out, vecs, bias_up, mats[1], mats[2], mats[3]
    )
    return result, (tokens, normed, joined, out, lse, attended, middle, second, active, slope)


def block_backward(kept, grad_result, mats, vecs, heads):
    tokens, normed, joined, out, lse, attended, middle, second, active, slope = kept
    b_down, b_up, b_proj, grad_att, grad_middle, sums_up, bias_up = back_up(
        grad_result, slope, middle, vecs, mats[1], mats[2], mats[3]
    )
    dq, dk, dv = attend_back(joined, grad_att, out, lse, heads)
    b_qkv, first, sums_in = back_in(dq, dk, dv, grad_middle, tokens, vecs, mats[0])
    pairs = [(normed, b_qkv), (attended, b_proj), (second, b_up), (active, b_down)]
    rows = [sums_in[0], sums_in[1], sums_up[0], sums_up[1], None, None, sums_in[2], sums_in[3], sums_up[2], sums_up[3], None]
    return first, pairs, rows, bias_up[0], sums_in


def tiles_of(width):
    return -(-width // LANES)


def spans(which):
    at, found = [], []
    for section in range(2):
        start = 0
        for shape in section_shapes(section):
            found.append((section, start, shape[which]))
            start += tiles_of(shape[which]) * LANES
        at.append(start)
    return found, at


ROW_SPANS, ROW_WIDTHS = spans(0)
COL_SPANS, COL_WIDTHS = spans(1)
ROW_PAD = max(ROW_WIDTHS)
VEC_TILES = -(-VLEN // (RANK * LANES))


def sum_rows(replicas, tiles):
    return -(-tiles // replicas) * replicas * RANK


def put_tiles(out_ref, section, start, value):
    width = value.shape[1]
    for tile in range(tiles_of(width)):
        here = min(LANES, width - tile * LANES)
        row = (start // LANES + tile) * RANK
        out_ref[section, row : row + RANK, :here] = value[:, tile * LANES : tile * LANES + here]


def skinny_body(*refs, n, x_spans, y_spans, extra_row):
    x_ref, u_refs, v_refs, tail_ref, out_ref = refs[0], refs[1 : 1 + n], refs[1 + n : 1 + 2 * n], refs[-2], refs[-1]
    out_ref[...] = jnp.zeros_like(out_ref)
    gain_ref = None
    for u_ref, v_ref, (section, start, width), (out_section, out_start, unused) in zip(u_refs, v_refs, x_spans, y_spans):
        part = join3(nt(split3(x_ref[section, :, start : start + width]), u_ref[...]))
        put_tiles(out_ref, out_section, out_start, extra_row[1] * join3(nn(split3(part), v_ref[...])))
    if extra_row[0]:
        out_ref[:, extra_row[0] : extra_row[0] + tail_ref.shape[1]] = tail_ref[...]


def skinny(x, us, vs, x_spans, y_spans, tail, tail_row, gain, rows):
    n = len(us)
    full = pl.BlockSpec(memory_space=pltpu.VMEM)
    return pl.pallas_call(
        functools.partial(skinny_body, n=n, x_spans=x_spans, y_spans=y_spans, extra_row=(tail_row, gain)),
        in_specs=[full] * (2 * n + 2),
        out_specs=full,
        out_shape=jax.ShapeDtypeStruct((2, rows, LANES), f32),
        compiler_params=pltpu.CompilerParams(vmem_limit_bytes=BIG),
        name="skinny",
    )(x, *us, *vs, tail)


def ortho_body(sum_ref, out_ref, wide, *, scale):
    rank_id = lax.broadcasted_iota(jnp.int32, (RANK, 1), 0)
    for section, start, width in ROW_SPANS:
        padded = tiles_of(width) * LANES
        for tile in range(padded // LANES):
            row = (start // LANES + tile) * RANK
            wide[:, tile * LANES : (tile + 1) * LANES] = sum_ref[section, row : row + RANK] * scale
        basis = wide[:, :padded]
        for column in range(RANK):
            current = basis[column : column + 1]
            current = current * lax.rsqrt(jnp.sum(current * current, axis=1, keepdims=True) + 1e-12)
            dots = jnp.sum(basis * current, axis=1, keepdims=True)
            basis = jnp.where(
                rank_id > column, basis - dots * current, jnp.where(rank_id == column, current, basis)
            )
        out_ref[section, :, start : start + padded] = basis


def orthonormal(sums, scale):
    full = pl.BlockSpec(memory_space=pltpu.VMEM)
    return pl.pallas_call(
        functools.partial(ortho_body, scale=scale),
        in_specs=[full],
        out_specs=full,
        out_shape=jax.ShapeDtypeStruct((2, RANK, ROW_PAD), f32),
        scratch_shapes=[pltpu.VMEM((RANK, FFE), f32)],
        name="orthonormal",
    )(sums)


def chunk_rows(rows_n, cols_n):
    if rows_n == PATCH:
        return PATCH
    return 256


def err_prep_body(e_ref, x_ref, *rest, blocks, rows):
    out_ref, left_ref, wide = rest[-3:]
    wide[...] = e_ref[0].reshape(rows * blocks, LANES).astype(f32)
    pieces = split3(x_ref[...])
    total = jnp.zeros((rows, 3 * RANK), f32)
    for block in range(blocks):
        part = wide[pl.ds(block, rows, stride=blocks), :].astype(bf16)
        out_ref[block * rows : (block + 1) * rows, :] = part
        total = total + nt(part, pieces[:, block * LANES : (block + 1) * LANES])
    value = join3(total.T)
    left_ref[...] = jnp.zeros_like(left_ref)
    for tile in range(tiles_of(rows)):
        here = min(LANES, rows - tile * LANES)
        left_ref[tile * RANK : (tile + 1) * RANK, :here] = value[:, tile * LANES : tile * LANES + here]


def err_prep(errors, factor, start, rows_n, cols_n, buf):
    blocks = cols_n // LANES
    rows = chunk_rows(rows_n, cols_n)
    step = rows * blocks
    steps = rows_n // rows
    tiles = tiles_of(rows)
    in_specs = [
        pl.BlockSpec((pl.Element(1), pl.Element(1), pl.Element(step * LANES)), lambda i: (0, 0, pl.multiple_of(start + i * step * LANES, 1024))),
        pl.BlockSpec((RANK, cols_n), lambda i: (0, 0)),
    ]
    args = [errors, factor]
    aliases = {}
    if buf is not None:
        in_specs.append(pl.BlockSpec(memory_space=pl.ANY))
        args.append(buf)
        aliases = {2: 0}
    return pl.pallas_call(
        functools.partial(err_prep_body, blocks=blocks, rows=rows),
        grid=(steps,),
        in_specs=in_specs,
        out_specs=[
            pl.BlockSpec((pl.Element(step), pl.Element(LANES)), lambda i: (pl.multiple_of(start // LANES + i * step, 16), 0)),
            pl.BlockSpec((tiles * RANK, LANES), lambda i: (i, 0)),
        ],
        out_shape=[
            jax.ShapeDtypeStruct((FLAT // LANES, LANES), bf16),
            jax.ShapeDtypeStruct((steps * tiles * RANK, LANES), f32),
        ],
        input_output_aliases=aliases,
        scratch_shapes=[pltpu.VMEM((step, LANES), f32)],
        name="err_prep",
    )(*args)


def err_right_body(x_ref, e_ref, o_ref, bufs, sems, *, section, scale):
    plan = []
    start = 0
    for (rows_n, cols_n), row_span, col_span in zip(
        section_shapes(section),
        [span for span in ROW_SPANS if span[0] == section],
        [span for span in COL_SPANS if span[0] == section],
    ):
        rows = chunk_rows(rows_n, cols_n)
        blocks = cols_n // LANES
        for chunk in range(rows_n // rows):
            plan.append((start // LANES + chunk * rows * blocks, rows, blocks, row_span[1] + chunk * rows, col_span[1], chunk))
        start += rows_n * cols_n
    depth = bufs.shape[0]

    def fetch(index):
        at, rows, blocks = plan[index][:3]
        slot = index % depth
        return pltpu.make_async_copy(
            e_ref.at[pl.ds(at, rows * blocks)], bufs.at[slot, pl.ds(0, rows * blocks)], sems.at[slot]
        )

    o_ref[...] = jnp.zeros_like(o_ref)
    for index in range(min(depth - 1, len(plan))):
        fetch(index).start()
    for index, (at, rows, blocks, row_at, col_at, chunk) in enumerate(plan):
        if index + depth - 1 < len(plan):
            fetch(index + depth - 1).start()
        fetch(index).wait()
        pieces = split3(x_ref[section, :, row_at : row_at + rows])
        for block in range(blocks):
            part = join3(nn(pieces, bufs[index % depth, block * rows : (block + 1) * rows]))
            row = (col_at // LANES + block) * RANK
            if chunk == 0:
                o_ref[row : row + RANK] = part
            else:
                o_ref[row : row + RANK] += part


def err_right(ortho, err, section, rows):
    full = pl.BlockSpec(memory_space=pltpu.VMEM)
    most = max(chunk_rows(*shape) * shape[1] // LANES for shape in section_shapes(section))
    return pl.pallas_call(
        functools.partial(err_right_body, section=section, scale=1.0),
        in_specs=[full, pl.BlockSpec(memory_space=pl.ANY)],
        out_specs=full,
        out_shape=jax.ShapeDtypeStruct((rows, LANES), f32),
        scratch_shapes=[pltpu.VMEM((4, most, LANES), bf16), pltpu.SemaphoreType.DMA((4,))],
        compiler_params=pltpu.CompilerParams(vmem_limit_bytes=BIG),
        name="err_right",
    )(ortho, err)


def final_right_body(sum_ref, ortho_ref, vec_ref, right_ref, norm_ref, *, scale):
    squares = jnp.sum(vec_ref[...] * vec_ref[...], keepdims=True)[0]
    for (section, start, width), (unused, row_at, row_width) in zip(COL_SPANS, ROW_SPANS):
        for tile in range(width // LANES):
            row = (start // LANES + tile) * RANK
            right_ref[section, :, start + tile * LANES : start + (tile + 1) * LANES] = sum_ref[section, row : row + RANK] * scale
        o_part = ortho_ref[section, :, row_at : row_at + tiles_of(row_width) * LANES]
        r_part = right_ref[section, :, start : start + width]
        for line in range(RANK):
            gram_o = jnp.sum(o_part * o_part[line : line + 1], axis=1, keepdims=True)
            gram_r = jnp.sum(r_part * r_part[line : line + 1], axis=1, keepdims=True)
            squares = squares + jnp.sum(gram_o * gram_r, keepdims=True)
    for section in range(2):
        used = COL_WIDTHS[section]
        if used < right_ref.shape[2]:
            right_ref[section, :, used:] = jnp.zeros((RANK, right_ref.shape[2] - used), f32)
    norm_ref[...] = jnp.broadcast_to(jnp.sqrt(squares), norm_ref.shape)


def final_right(sums, ortho, vecs, cols, scale):
    full = pl.BlockSpec(memory_space=pltpu.VMEM)
    return pl.pallas_call(
        functools.partial(final_right_body, scale=scale),
        in_specs=[full] * 3,
        out_specs=[full] * 2,
        out_shape=[jax.ShapeDtypeStruct((2, RANK, cols), f32), jax.ShapeDtypeStruct((1, LANES), f32)],
        name="final_right",
    )(sums, ortho, vecs)


def finish_body(me_ref, a0, a1, b0, b1, e_ref, o_ref, r_ref, *rest, rows, blocks, gain, start, shard):
    err_out, app_out = rest[-2:]
    o_part = o_ref[0]
    o_high = o_part.astype(bf16)
    o_low = (o_part - o_high.astype(f32)).astype(bf16)
    left_t = jnp.concatenate([o_high, o_low, o_high], axis=0).T[:rows]
    lhs0 = a0[...].T
    lhs1 = a1[...].T
    err_rows = err_out.at[0].reshape(rows * blocks, LANES)
    keep = overlaps(pl.program_id(0), me_ref[0], start, rows * blocks, shard)
    for pair in range(blocks // 2):
        cols = slice(pair * 2 * LANES, (pair + 1) * 2 * LANES)
        r_part = r_ref[0, :, cols]
        r_high = r_part.astype(bf16)
        r_low = (r_part - r_high.astype(f32)).astype(bf16)
        approx = nn(left_t, jnp.concatenate([r_high, r_high, r_low], axis=0))
        grad = nn(lhs0, b0[:, cols]) + nn(lhs1, b1[:, cols])
        for side in range(2):
            block = pair * 2 + side
            half = slice(side * LANES, (side + 1) * LANES)
            err_rows[pl.ds(block, rows, stride=blocks), :] = (
                gain * grad[:, half] + e_ref[block * rows : (block + 1) * rows].astype(f32)
            ) - approx[:, half]

            @pl.when(keep)
            def _():
                app_out[pl.ds(block, rows, stride=blocks), :] = approx[:, half]


def overlaps(i, me, start, step, shard):
    first = start + i * step * LANES
    return (first < (me + 1) * shard) & (first + step * LANES > me * shard)


def finish(me, pair0, pair1, err, ortho, right, section, row_at, col_at, start, gain, shard, bufs):
    a0, b0 = pair0
    a1, b1 = pair1
    rows_n, cols_n = a0.shape[1], b0.shape[1]
    seq = a0.shape[0]
    blocks = cols_n // LANES
    rows = chunk_rows(rows_n, cols_n)
    step = rows * blocks
    flat_rows = FLAT // LANES
    whole = lambda i, me: (0, 0)
    flat_at = lambda i: pl.multiple_of(start // LANES + i * step, 16)
    wide_rows = tiles_of(rows) * LANES

    def shard_at(i, me):
        return pl.multiple_of(jnp.where(overlaps(i, me[0], start, step, shard), start // LANES + i * step, flat_rows), 8), 0

    in_specs = [
        pl.BlockSpec((seq, rows), lambda i, me: (0, i)),
        pl.BlockSpec((seq, rows), lambda i, me: (0, i)),
        pl.BlockSpec((seq, cols_n), whole, pipeline_mode=pl.Buffered(1)),
        pl.BlockSpec((seq, cols_n), whole, pipeline_mode=pl.Buffered(1)),
        pl.BlockSpec((pl.Element(step), pl.Element(LANES)), lambda i, me: (flat_at(i), 0)),
        pl.BlockSpec((1, RANK, wide_rows), lambda i, me: (section, 0, row_at // wide_rows + i)),
        pl.BlockSpec(
            (pl.Element(1), pl.Element(RANK), pl.Element(cols_n)), lambda i, me: (section, 0, col_at), pipeline_mode=pl.Buffered(1)
        ),
    ]
    assert row_at % wide_rows == 0
    args = [a0, a1, b0, b1, err, ortho, right]
    aliases = {}
    if bufs is not None:
        in_specs += [pl.BlockSpec(memory_space=pl.ANY)] * 2
        args += list(bufs)
        aliases = {8: 0, 9: 1}
    return pl.pallas_call(
        functools.partial(finish_body, rows=rows, blocks=blocks, gain=gain, start=start, shard=shard),
        grid_spec=pltpu.PrefetchScalarGridSpec(
            num_scalar_prefetch=1,
            grid=(rows_n // rows,),
            in_specs=in_specs,
            out_specs=[
                pl.BlockSpec(
                    (pl.Element(1), pl.Element(1), pl.Element(step * LANES)),
                    lambda i, me: (0, 0, pl.multiple_of(start + i * step * LANES, 1024)),
                ),
                pl.BlockSpec((pl.Element(step), pl.Element(LANES)), shard_at),
            ],
        ),
        out_shape=[
            jax.ShapeDtypeStruct((1, 1, FLAT), f32),
            jax.ShapeDtypeStruct((flat_rows + SPARE, LANES), f32),
        ],
        input_output_aliases=aliases,
        compiler_params=pltpu.CompilerParams(vmem_limit_bytes=BIG),
        name="finish",
    )(me, *args)


def tail_body(e_ref, buf0, err_out):
    err_out[...] = e_ref[...].astype(f32)


def finish_tail(errors, start, buf):
    count = FLAT - start
    steps = 6
    step = count // steps
    assert step * steps == count and step % 1024 == 0
    spec = pl.BlockSpec((pl.Element(1), pl.Element(1), pl.Element(step)), lambda i: (0, 0, pl.multiple_of(start + i * step, 1024)))
    return pl.pallas_call(
        tail_body,
        grid=(steps,),
        in_specs=[spec, pl.BlockSpec(memory_space=pl.ANY)],
        out_specs=spec,
        out_shape=jax.ShapeDtypeStruct((1, 1, FLAT), f32),
        input_output_aliases={1: 0},
        compiler_params=pltpu.CompilerParams(vmem_limit_bytes=BIG),
        name="finish_tail",
    )(errors, buf)


MESH = pl.DeviceIdType.MESH


def grid_of(replicas):
    side = 2 if replicas < 64 else 4
    return replicas // (side * side), side, side


def used_rows(section):
    counts = [sum(rows * cols for rows, cols in section_shapes(s)) // LANES for s in range(2)]
    return jnp.where(section == 0, counts[0], counts[1])


def meet(replicas):
    section, me = lax.axis_index("section"), lax.axis_index("dp")
    barrier = pltpu.get_barrier_semaphore()
    pl.semaphore_signal(barrier, inc=1, device_id={"section": 1 - section}, device_id_type=MESH)
    for step in range(1, replicas):
        pl.semaphore_signal(
            barrier, inc=1, device_id={"dp": lax.rem(me + step, replicas)}, device_id_type=MESH
        )
    pl.semaphore_wait(barrier, replicas)


def gather_body(
    low_ref, cnt_ref, vec_ref, fac_ref, flat_ref, cnts_ref, vec2_ref, fac2_ref,
    send_sem, recv_sem, swap_sem, cnt_send, cnt_recv, side_send, side_recv, own_sem, *, replicas, size,
):
    section, me = lax.axis_index("section"), lax.axis_index("dp")
    other = 1 - section
    nz, ny, nx = grid_of(replicas)
    x, y, z = lax.rem(me, nx), lax.rem(me // nx, ny), me // (nx * ny)
    cut = size // 2 // 8 * 8 if size % 8 == 0 else size
    halves = [(0, cut), (cut, size - cut)] if cut < size else [(0, cut)]
    used = used_rows(section)
    used_other = used_rows(other)

    def block_id(at_z, at_y, at_x):
        return (at_z * ny + at_y) * nx + at_x

    meet(replicas)

    def side(src, dst, slot):
        return pltpu.make_async_remote_copy(
            src_ref=src, dst_ref=dst.at[section], send_sem=side_send.at[slot], recv_sem=side_recv.at[slot],
            device_id={"section": other}, device_id_type=MESH,
        )

    def count_copy(step):
        return pltpu.make_async_remote_copy(
            src_ref=cnt_ref, dst_ref=cnts_ref.at[me], send_sem=cnt_send.at[step],
            recv_sem=cnt_recv.at[step], device_id={"dp": lax.rem(me + step, replicas)}, device_id_type=MESH,
        )

    for step in range(1, replicas):
        count_copy(step).start()
    side(vec_ref, vec2_ref, 0).start()
    side(fac_ref, fac2_ref, 1).start()
    own = pltpu.make_async_copy(low_ref, flat_ref.at[section * replicas + me], own_sem)
    own.start()

    def copy(block, half, target, way, mine=False, swap=False):
        start, rows = halves[half]
        at = flat_ref.at[section * replicas + block, pl.ds(start, rows)]
        src = low_ref.at[pl.ds(start, rows)] if mine else at
        return pltpu.make_async_remote_copy(
            src_ref=src, dst_ref=at, send_sem=send_sem.at[block, half, way],
            recv_sem=(swap_sem if swap else recv_sem).at[block, half], device_id=target, device_id_type=MESH,
        )

    def needed(block, half, limit):
        return block * size + halves[half][0] < limit

    def at_z(value):
        return {"dp": block_id(value, y, x)}

    def along_x(block, half, mine=False):
        for step in range(1, nx):
            copy(block, half, {"dp": block_id(z, y, lax.rem(x + step, nx))}, 1 + step, mine).start()

    def along_y(block, half, mine=False):
        for step in range(1, ny):
            copy(block, half, {"dp": block_id(z, lax.rem(y + step, ny), x)}, nx + step, mine).start()

    def across(block, half, mine=False):
        copy(block, half, {"section": other}, nx + ny, mine, True).start()

    def arrived(block, half):
        copy(block, half, {"section": other}, 0).wait_recv()

    def layers(k):
        return [z] if k == 0 else [z - k, z + k]

    def valid(at):
        return (at >= 0) & (at < nz)

    def first(k):
        for which, layer in enumerate(layers(k)):
            block = block_id(layer, y, x)
            for half in range(len(halves)):

                @pl.when(valid(layer) & needed(block, half, used))
                def _():
                    if k > 0:
                        arrived(block, half)
                    mine = k == 0
                    if k == 0 or which == 0:

                        @pl.when(z + 1 < nz)
                        def _():
                            copy(block, half, at_z(z + 1), 0, mine).start()

                    if k == 0 or which == 1:

                        @pl.when(z > 0)
                        def _():
                            copy(block, half, at_z(z - 1), 1, mine).start()

                    if half == 0:
                        along_x(block, half, mine)
                        along_y(block, half, mine)
                    else:
                        along_y(block, half, mine)
                        along_x(block, half, mine)
                    across(block, half, mine)

    def second(k):
        for layer in layers(k):
            for half in range(len(halves)):
                for step in range(1, nx if half == 0 else ny):
                    if half == 0:
                        block = block_id(layer, y, lax.rem(x + step, nx))
                    else:
                        block = block_id(layer, lax.rem(y + step, ny), x)

                    @pl.when(valid(layer) & needed(block, half, used))
                    def _():
                        arrived(block, half)
                        if half == 0:
                            along_y(block, half)
                        else:
                            along_x(block, half)
                        across(block, half)

    def third(k):
        for layer in layers(k):
            for half in range(len(halves)):
                for far in range(1, ny if half == 0 else nx):
                    for near in range(nx if half == 0 else ny):
                        if half == 0:
                            block = block_id(layer, lax.rem(y + far, ny), lax.rem(x + near, nx))
                        else:
                            block = block_id(layer, lax.rem(y + near, ny), lax.rem(x + far, nx))

                        @pl.when(valid(layer) & needed(block, half, used))
                        def _():
                            arrived(block, half)
                            across(block, half)

    for k in range(nz + 2):
        if k < nz:
            first(k)
        if 0 <= k - 1 < nz:
            second(k - 1)
        if 0 <= k - 2 < nz:
            third(k - 2)

    def drain(block, carry):
        at_x_, at_y_, at_z_ = lax.rem(block, nx), lax.rem(block // nx, ny), block // (nx * ny)
        for half in range(len(halves)):
            column = (at_x_ == x) & (at_y_ == y)

            @pl.when(needed(block, half, used))
            def _():
                @pl.when(column & (at_z_ <= z) & (z + 1 < nz))
                def _():
                    copy(block, half, {"section": other}, 0).wait_send()

                @pl.when(column & (at_z_ >= z) & (z > 0))
                def _():
                    copy(block, half, {"section": other}, 1).wait_send()

                single = len(halves) == 1
                sent_x = (column if half == 0 else at_x_ == x)
                sent_y = (at_y_ == y) if half == 0 else column

                @pl.when(sent_x)
                def _():
                    for step in range(1, nx):
                        copy(block, half, {"section": other}, 1 + step).wait_send()

                @pl.when(sent_y)
                def _():
                    for step in range(1, ny):
                        copy(block, half, {"section": other}, nx + step).wait_send()

                copy(block, half, {"section": other}, nx + ny).wait_send()

            @pl.when(needed(block, half, used_other))
            def _():
                copy(block, half, {"section": other}, 0, False, True).wait_recv()

        return carry

    lax.fori_loop(0, replicas, drain, 0)
    own.wait()
    for step in range(1, replicas):
        count_copy(step).wait()
    cnts_ref[me] = cnt_ref[...]
    vec2_ref[section] = vec_ref[...]
    fac2_ref[section] = fac_ref[...]
    side(vec_ref, vec2_ref, 0).wait()
    side(fac_ref, fac2_ref, 1).wait()


def cast_body(src_ref, out_ref):
    out_ref[...] = src_ref[...].reshape(out_ref.shape).astype(bf16)


def cast_shard(master, size):
    full = pl.BlockSpec(memory_space=pltpu.VMEM)
    return pl.pallas_call(
        cast_body, in_specs=[full], out_specs=full, out_shape=jax.ShapeDtypeStruct((size, LANES), bf16), name="cast"
    )(master)


def gather(low, cnt, vec, fac, replicas):
    size = low.shape[0]
    vmem = pl.BlockSpec(memory_space=pltpu.VMEM)
    nz, ny, nx = grid_of(replicas)
    dma = pltpu.SemaphoreType.DMA
    return pl.pallas_call(
        functools.partial(gather_body, replicas=replicas, size=size),
        in_specs=[vmem] * 4,
        out_specs=[pl.BlockSpec(memory_space=pl.ANY), vmem, vmem, vmem],
        out_shape=[
            jax.ShapeDtypeStruct((2 * replicas, size, LANES), bf16),
            jax.ShapeDtypeStruct((replicas,) + cnt.shape, f32),
            jax.ShapeDtypeStruct((2,) + vec.shape, f32),
            jax.ShapeDtypeStruct((2,) + fac.shape, f32),
        ],
        scratch_shapes=[
            dma((replicas, 2, nx + ny + 1)), dma((replicas, 2)), dma((replicas, 2)),
            dma((replicas,)), dma((replicas,)), dma((2,)), dma((2,)), dma(()),
        ],
        compiler_params=pltpu.CompilerParams(collective_id=2, has_side_effects=True),
        name="gather",
    )(low, cnt, vec, fac)


def sum_body(*refs, replicas, n_enc, n_dec):
    n = n_enc + n_dec
    sum_run(*refs[:2], refs[2 : 2 + n], refs[2 + n], refs[3 + n : 3 + 2 * n], *refs[3 + 2 * n :], replicas=replicas, n_enc=n_enc)


def sum_run(
    part_ref, extra_ref, given, total_ref, taken, mine, came, slots, seg, swap_send, swap_recv, send_a, recv_a, send_b, recv_b,
    give_sem, take_sem, *, replicas, n_enc,
):
    section, me = lax.axis_index("section"), lax.axis_index("dp")
    other = 1 - section
    rows = part_ref.shape[1]
    size = rows // replicas
    meet(replicas)

    def rows_of(index):
        return pl.ds(pl.multiple_of(index * size, 8), size)

    swap = pltpu.make_async_remote_copy(
        src_ref=part_ref.at[other], dst_ref=came, send_sem=swap_send.at[0], recv_sem=swap_recv.at[0],
        device_id={"section": other}, device_id_type=MESH,
    )
    swap.start()
    mine[...] = part_ref[section] + extra_ref[...]
    swap.wait()

    def give(i):
        return pltpu.make_async_remote_copy(
            src_ref=given[i], dst_ref=taken[i], send_sem=give_sem.at[i], recv_sem=take_sem.at[i],
            device_id={"section": other}, device_id_type=MESH,
        )

    n = len(given)
    for i in range(n):

        @pl.when(section == (1 if i < n_enc else 0))
        def _():
            give(i).start()

    mine[...] = mine[...] + came[...]

    def scatter(step):
        peer = lax.rem(me + step, replicas)
        return pltpu.make_async_remote_copy(
            src_ref=mine.at[rows_of(peer)], dst_ref=slots.at[step], send_sem=send_a.at[step],
            recv_sem=recv_a.at[step], device_id={"dp": peer}, device_id_type=MESH,
        )

    def spread(step):
        peer = lax.rem(me + step, replicas)
        return pltpu.make_async_remote_copy(
            src_ref=seg, dst_ref=total_ref.at[section, rows_of(me)], send_sem=send_b.at[step],
            recv_sem=recv_b.at[step], device_id={"dp": peer}, device_id_type=MESH,
        )

    for step in range(1, replicas):
        scatter(step).start()
    total = mine[rows_of(me), :]
    for step in range(1, replicas):
        scatter(step).wait_recv()
        total = total + slots[step]
    seg[...] = total
    for step in range(1, replicas):
        spread(step).start()
    total_ref[section, rows_of(me)] = total
    for step in range(1, replicas):
        scatter(step).wait_send()
        spread(step).wait()
    back = pltpu.make_async_remote_copy(
        src_ref=total_ref.at[section], dst_ref=total_ref.at[section], send_sem=swap_send.at[1],
        recv_sem=swap_recv.at[1], device_id={"section": other}, device_id_type=MESH,
    )
    back.start()
    back.wait()
    for i in range(n):

        @pl.when(section == (1 if i < n_enc else 0))
        def _():
            give(i).wait_send()

        @pl.when(section == (0 if i < n_enc else 1))
        def _():
            give(i).wait_recv()


def all_sum(part, extra, replicas, collective_id, enc=(), dec=()):
    rows = part.shape[1]
    vmem = pl.BlockSpec(memory_space=pltpu.VMEM)
    dma = pltpu.SemaphoreType.DMA
    size = rows // replicas
    given = list(enc) + list(dec)
    n = len(given)
    anywhere = pl.BlockSpec(memory_space=pl.ANY)
    outs = pl.pallas_call(
        functools.partial(sum_body, replicas=replicas, n_enc=len(enc), n_dec=len(dec)),
        in_specs=[vmem, vmem] + [anywhere] * n,
        out_specs=[vmem] + [anywhere] * n,
        out_shape=[jax.ShapeDtypeStruct(part.shape, f32)] + [jax.ShapeDtypeStruct(x.shape, x.dtype) for x in given],
        scratch_shapes=[
            pltpu.VMEM((rows, LANES), f32), pltpu.VMEM((rows, LANES), f32),
            pltpu.VMEM((replicas, size, LANES), f32), pltpu.VMEM((size, LANES), f32),
            dma((2,)), dma((2,)), dma((replicas,)), dma((replicas,)), dma((replicas,)), dma((replicas,)),
            dma((max(n, 1),)), dma((max(n, 1),)),
        ],
        compiler_params=pltpu.CompilerParams(collective_id=collective_id, has_side_effects=True),
        name="all_sum",
    )(part, extra, *given)
    return outs[0], outs[1 : 1 + len(enc)], outs[1 + len(enc) :]


def pack_rows(rows, pieces, width, length):
    empty = jnp.zeros((width,), f32)
    parts = [empty if row is None else row for row in rows] + pieces
    used = sum(part.shape[0] for part in parts)
    return jnp.concatenate(parts + [jnp.zeros((length - used,), f32)])


def local(pixels, visible, masked, loss_mask, master, momentum, vectors, vec_moment, factors, errors):
    sec = lax.axis_index("section")
    replicas = lax.axis_size("dp")
    replica_id = lax.axis_index("dp")

    replicas_n = replicas
    shard_len = master.shape[1]
    size = shard_len // LANES
    gain = float(replicas)

    count_tile = jnp.full((RANK, LANES), jnp.sum(loss_mask).astype(f32))
    vec_tile = jnp.pad(vectors[0], (0, VEC_TILES * RANK * LANES - VLEN)).reshape(-1, LANES)
    flat_both, counts, vec_both, fac_both = gather(
        cast_shard(master, size), count_tile, vec_tile, factors[0], replicas
    )
    low_both = flat_both.reshape(-1, LANES)
    vec_both = vec_both.reshape(2, -1)
    count = jnp.sum(counts[:, 0, 0])

    vis = lax.dynamic_index_in_dim(visible, sec, 0, keepdims=False)
    mas = lax.dynamic_index_in_dim(masked, sec, 0, keepdims=False)
    mask_row = lax.dynamic_index_in_dim(loss_mask, sec, 0, keepdims=False).astype(f32)
    order = jnp.concatenate([vis, mas])
    pix = lax.dynamic_index_in_dim(pixels, sec, 0, keepdims=False)
    pick = (order[:, None] == jnp.arange(SEQ, dtype=jnp.int32)[None, :]).astype(bf16)
    pix_order = nn(pick, pix).astype(bf16)
    pix_vis = pix_order[:VIS]
    target = pix_order[VIS:]
    place = order[:, None]
    mask_col = mask_row[:, None]
    tail_row = ROW_PAD // LANES * RANK
    tail_rows = (VEC_TILES + 1) * RANK
    left_rows = sum_rows(replicas, ROW_PAD // LANES + VEC_TILES + 1)
    right_rows = sum_rows(replicas, max(COL_WIDTHS) // LANES)

    def errs_for(section):
        def run():
            buf = None
            lefts = []
            start = 0
            col_at = 0
            for rows_n, cols_n in section_shapes(section):
                buf, left = err_prep(errors, factors[0][:, col_at : col_at + cols_n], start, rows_n, cols_n, buf)
                lefts.append(left)
                start += rows_n * cols_n
                col_at += cols_n
            done = sum(left.shape[0] for left in lefts)
            lefts.append(jnp.zeros((left_rows - done, LANES), f32))
            return buf, jnp.concatenate(lefts)

        return run

    err_stack, err_lefts = lax.cond(sec == 0, errs_for(0), errs_for(1))

    enc = unflat_all(low_both, 0, 0)
    dec = unflat_all(low_both, FLAT, 1)
    rows_e, bias_e, unused = unpack_vecs(vec_both[0], DE, FFE)
    rows_d, bias_d, extra_d = unpack_vecs(vec_both[1], DD, FFD)

    tokens_e = embed(pix_vis, enc[4], rows_e, place[:VIS], angle_tables(DE))
    coded, kept_e = block_forward(tokens_e, enc, rows_e, bias_e[None], HEADS_ENC)
    sent, filled = relay(coded, rows_e, dec[5], extra_d[None], rows_d, place, angle_tables(DD))
    result, kept_d = block_forward(filled, dec, rows_d, bias_d[None], HEADS_DEC)
    final, grad_pred, grad_result, sums_h, loss_row = head(
        result, rows_d, dec[4], target, mask_col, count.reshape(1, 1)
    )
    loss_part = loss_row[0, 0]
    b_first, pairs_d, vrows_d, v_up_d, sums_d = block_backward(kept_d, grad_result, dec, rows_d, HEADS_DEC)
    pairs_d = pairs_d + [(grad_pred, final), (sent, b_first)]
    vrows_d[4], vrows_d[5], vrows_d[10] = sums_h[0], sums_h[1], sums_d[5]
    vec_d = pack_rows(vrows_d, [v_up_d, sums_d[4]], DD, VLEN)
    grad_coded, sums_r = relay_back(b_first, dec[5], coded, rows_e)
    b_start, pairs_e, vrows_e, v_up_e, sums_e = block_backward(kept_e, grad_coded, enc, rows_e, HEADS_ENC)
    pairs_e = pairs_e + [(pix_vis, b_start)]
    vrows_e[4], vrows_e[5], vrows_e[10] = sums_r[0], sums_r[1], sums_e[4]
    vec_e = pack_rows(vrows_e, [v_up_e], DE, VLEN)

    pairs = pairs_e + pairs_d
    n_enc = len(pairs_e)
    flat_e = [x for pair in pairs_e for x in pair]
    flat_d = [x for pair in pairs_d for x in pair]
    vec_tiles = jnp.pad(jnp.stack([vec_e, vec_d]), ((0, 0), (0, VEC_TILES * RANK * LANES - VLEN))).reshape(2, -1, LANES)
    loss_tile = jnp.stack([jnp.full((RANK, LANES), loss_part), jnp.zeros((RANK, LANES), f32)])
    tail = jnp.concatenate([vec_tiles, loss_tile], axis=1)
    left_part = skinny(
        fac_both, [b for a, b in pairs], [a for a, b in pairs], COL_SPANS, ROW_SPANS, tail, tail_row, gain, left_rows
    )
    left_sum, other_e, other_d = all_sum(left_part, err_lefts, replicas, 3, flat_e, flat_d)
    vec_sum = left_sum[:, tail_row : tail_row + VEC_TILES * RANK]
    loss_sum = left_sum[0, tail_row + VEC_TILES * RANK, 0]

    ortho = orthonormal(left_sum, 1.0 / replicas)
    right_part = skinny(
        ortho, [a for a, b in pairs], [b for a, b in pairs], ROW_SPANS, COL_SPANS, tail, 0, gain, right_rows
    )
    err_rights = lax.cond(
        sec == 0,
        lambda: err_right(ortho, err_stack, 0, right_rows),
        lambda: err_right(ortho, err_stack, 1, right_rows),
    )
    sums, unused, unused = all_sum(right_part, err_rights, replicas, 4)
    right_both, norm_row = final_right(sums, ortho, vec_sum, factors.shape[2], 1.0 / replicas)
    norm = norm_row[0, 0]
    scale = jnp.minimum(1.0, clip_limit / (norm + 1e-06))

    def finish_for(section):
        def run():
            mine = pairs_e if section == 0 else pairs_d
            flat = other_e if section == 0 else other_d
            theirs = [(flat[2 * i], flat[2 * i + 1]) for i in range(len(mine))]
            bufs = None
            start = 0
            base = 0 if section == 0 else n_enc
            for i, (rows_n, cols_n) in enumerate(section_shapes(section)):
                bufs = finish(
                    me_row, mine[i], theirs[i], err_stack, ortho, right_both, section,
                    ROW_SPANS[base + i][1], COL_SPANS[base + i][1], start, gain, shard_len, bufs,
                )
                start += rows_n * cols_n
            if start < FLAT:
                bufs = [finish_tail(errors, start, bufs[0]), bufs[1]]
            return bufs[0], bufs[1]

        return run

    me_row = replica_id.astype(jnp.int32).reshape(1)
    new_errors, approx = lax.cond(sec == 0, finish_for(0), finish_for(1))
    own_part = lax.dynamic_slice_in_dim(approx.reshape(-1), replica_id * shard_len, shard_len)
    used = jnp.where(sec == 0, *[sum(rows_n * cols_n for rows_n, cols_n in section_shapes(s)) for s in range(2)])
    inside = replica_id * shard_len + lax.iota(jnp.int32, shard_len) < used
    own_part = jnp.where(inside, own_part, 0.0)
    rate = learning_rate()
    new_moment = moment_decay * momentum[0] + scale * own_part
    new_master = master[0] - rate * new_moment
    vec_own = lax.dynamic_index_in_dim(vec_sum, sec, 0, keepdims=False).reshape(-1)[:VLEN]
    new_vm = moment_decay * vec_moment[0] + scale * vec_own
    new_vectors = vectors[0] - rate * new_vm
    new_factors = lax.dynamic_index_in_dim(right_both, sec, 0, keepdims=False)
    return (
        new_master[None],
        new_master.astype(bf16)[None],
        new_moment[None],
        new_vectors[None],
        new_vm[None],
        new_factors[None],
        new_errors,
        loss_sum.reshape(1),
        norm.reshape(1),
    )


def solution(mesh):
    return jax.shard_map(
        local,
        mesh=mesh,
        in_specs=(
            P("dp", None, None),
            P("dp", None),
            P("dp", None),
            P("dp", None),
            P("section", "dp"),
            P("section", "dp"),
            P("section", None),
            P("section", None),
            P("section", None, None),
            P("section", "dp", None),
        ),
        out_specs=(
            P("section", "dp"),
            P("section", "dp"),
            P("section", "dp"),
            P("section", None),
            P("section", None),
            P("section", None, None),
            P("section", "dp", None),
            P(),
            P(),
        ),
        check_vma=False,
    )
```

```python
import functools
import math

import jax
import jax.numpy as jnp
import numpy as np
from jax import lax
from jax.experimental import pallas as pl
from jax.experimental.pallas import tpu as pltpu
from jax.sharding import PartitionSpec as P

DE = 768
FFE = 3072
HEADS_ENC = 12
DD = 512
FFD = 2048
HEADS_DEC = 16
PATCH = 192
RANK = 8
SEQ = 1024
VIS = 256
FLAT = 7225344
VLEN = 11520

(K_TOKENS, K_NORMED, K_JOINED, K_OUT, K_LSE, K_ATTENDED, K_MIDDLE, K_SECOND, K_ACTIVE, K_SLOPE, K_CODED, K_B_QKV, K_B_PROJ, K_B_UP, K_B_DOWN, K_B_PRED, K_FINAL, K_SENT, K_FIRST, K_GRAD, K_ATT, K_DK, K_DV, K_SUMS, K_BIAS, K_START) = range(26)

f32 = jnp.float32
bf16 = jnp.bfloat16
clip_limit = 0.0001
moment_decay = 0.9
rate_base = 0.5
LANES = 128
SEC, DP = "section", "dp"
STEP = 32
DEC_ROWS = 512
CHUNK = 256
SPARE = 6144
BIG = 66000000


def nn(left, right):
    return lax.dot_general(left, right, (((1,), (0,)), ((), ())), preferred_element_type=f32)


def nt(left, right):
    return lax.dot_general(left, right, (((1,), (1,)), ((), ())), preferred_element_type=f32)


def tn(left, right):
    return lax.dot_general(left, right, (((0,), (0,)), ((), ())), preferred_element_type=f32)


def split3(value):
    high = value.astype(bf16)
    rest = value - high.astype(f32)
    middle = rest.astype(bf16)
    return jnp.concatenate([high, middle, (rest - middle.astype(f32)).astype(bf16)], axis=0)


def join3(value):
    return value[:RANK] + value[RANK : 2 * RANK] + value[2 * RANK :]


def norm_parts(tokens):
    centred = tokens - jnp.mean(tokens, axis=-1, keepdims=True)
    spread = lax.rsqrt(jnp.mean(centred * centred, axis=-1, keepdims=True) + 1e-06)
    return centred * spread, spread


def norm_back(grad, hat, spread, gain):
    inner = grad * gain
    return spread * (
        inner - jnp.mean(inner, axis=-1, keepdims=True) - hat * jnp.mean(inner * hat, axis=-1, keepdims=True)
    )


def column_sum(value):
    return jnp.sum(value.astype(f32), axis=0, keepdims=True)


def angle_tables(width):
    column = np.arange(width)
    freqs = np.exp(-(column // 2 * 2) / width * math.log(10000.0))
    coarse = (np.arange(0, SEQ, STEP)[:, None] * freqs).astype(np.float64)
    fine = np.arange(STEP)[:, None] * freqs + (column % 2) * (math.pi / 2)
    return jnp.asarray(np.stack([np.sin(coarse), np.cos(coarse), np.cos(fine), np.sin(fine)]), f32)


def positions_of(place, tables):
    column = lax.broadcasted_iota(jnp.int32, (1, STEP), 1)
    coarse = (place // STEP == column).astype(bf16)
    fine = (place % STEP == column).astype(bf16)

    def take(pick, table):
        high = table.astype(bf16)
        rest = table - high.astype(f32)
        middle = rest.astype(bf16)
        low = (rest - middle.astype(f32)).astype(bf16)
        return nn(pick, high) + nn(pick, middle) + nn(pick, low)

    return take(coarse, tables[0]) * take(fine, tables[2]) + take(coarse, tables[1]) * take(fine, tables[3])


def section_shapes(section):
    if section == 0:
        return [(DE, 3 * DE), (DE, DE), (DE, FFE), (FFE, DE), (PATCH, DE)]
    return [(DD, 3 * DD), (DD, DD), (DD, FFD), (FFD, DD), (PATCH, DD), (DE, DD)]


def learning_rate():
    return rate_base * math.sqrt(2.0 * (FLAT + VLEN) / DD) / clip_limit


def head_mask(head, size):
    lane = lax.broadcasted_iota(jnp.int32, (1, LANES), 1)
    return (lane // size == head).astype(bf16)


def attend_body(q_ref, k_ref, v_ref, o_ref, lse_ref, *, size, rows_q):
    seq = k_ref.shape[0]
    scale = size ** (-0.5)
    fold = scale * math.log2(math.e)

    def one(step, carry):
        at = pl.ds(pl.multiple_of(step * rows_q, rows_q), rows_q)
        queries = q_ref[at, :]
        total = jnp.zeros((rows_q, LANES), f32)
        for head in range(LANES // size):
            mask = head_mask(head, size)
            scores = nt(k_ref[...], queries * mask)
            peak = jnp.max(scores, axis=0, keepdims=True) * fold
            power = jnp.exp2(scores * fold - peak)
            mass = jnp.sum(power, axis=0, keepdims=True)
            share = jnp.transpose(jnp.broadcast_to(1.0 / mass, (8, rows_q)))[:, :1]
            total = total + tn(power.astype(bf16), v_ref[...] * mask) * share
            lse_ref[0, head : head + 1, at] = peak + jnp.log2(mass)
        o_ref[at, :] = total
        return carry

    lax.fori_loop(0, seq // rows_q, one, 0)


def attend_back_body(q_ref, k_ref, v_ref, do_ref, o_ref, lse_ref, dq_ref, dk_ref, dv_ref, dk_sum, dv_sum, *, size, rows_q):
    seq = k_ref.shape[0]
    scale = size ** (-0.5)
    fold = scale * math.log2(math.e)
    dk_sum[...] = jnp.zeros_like(dk_sum)
    dv_sum[...] = jnp.zeros_like(dv_sum)

    def one(step, carry):
        at = pl.ds(pl.multiple_of(step * rows_q, rows_q), rows_q)
        queries = q_ref[at, :]
        grads = do_ref[at, :]
        prod = grads.astype(f32) * o_ref[at, :]
        total = jnp.zeros((rows_q, LANES), f32)
        high = prod.astype(bf16)
        rest = prod - high.astype(f32)
        middle = rest.astype(bf16)
        for head in range(LANES // size):
            mask = head_mask(head, size)
            wide = jnp.broadcast_to(mask, (16, LANES))
            delta = (nt(wide, high) + nt(wide, middle))[0:1]
            q_one = queries * mask
            g_one = grads * mask
            scores = nt(k_ref[...], q_one)
            probs = jnp.exp2(scores * fold - lse_ref[0, head : head + 1, at])
            slope = nt(v_ref[...], g_one)
            grad_s = (probs * (slope - delta)).astype(bf16)
            dv_sum[...] += nn(probs.astype(bf16), g_one)
            dk_sum[...] += nn(grad_s, q_one)
            total = total + tn(grad_s, k_ref[...] * mask)
        dq_ref[at, :] = (total * scale).astype(bf16)
        return carry

    lax.fori_loop(0, seq // rows_q, one, 0)
    dk_ref[...] = (dk_sum[...] * scale).astype(bf16)
    dv_ref[...] = dv_sum[...].astype(bf16)


def rows_at(step, count):
    return pl.ds(pl.multiple_of(step * count, count), count)


def cols_at(step, count=LANES):
    return pl.ds(pl.multiple_of(step * count, count), count)


def shape_of(rows, cols, dtype=f32):
    return jax.ShapeDtypeStruct((rows, cols), dtype)


def loop(count, body):
    def one(step, carry):
        body(step)
        return carry

    lax.fori_loop(0, count, one, 0)


def over_blocks(seq, rows, body, *refs):
    loop(seq // rows, lambda step: body(*[ref.at[rows_at(step, rows)] for ref in refs]))


def open_stage(tok_ref, normed_ref, joined_ref, vec_ref, w_ref):
    width = tok_ref.shape[1]
    hat, unused = norm_parts(tok_ref[...])
    normed = (hat * vec_ref[0:1] + vec_ref[1:2]).astype(bf16)
    normed_ref[...] = normed
    for part, bias in ((0, vec_ref[6:7]), (1, None), (2, vec_ref[7:8])):
        cols = slice(part * width, (part + 1) * width)
        value = nn(normed, w_ref[:, cols])
        joined_ref[:, cols] = (value if bias is None else value + bias).astype(bf16)


def attend_stage(joined, out, lse, size):
    seq, width = out.shape
    groups = width // LANES

    def one(group):
        attend_body(
            joined.at[:, cols_at(group)], joined.at[:, cols_at(groups + group)],
            joined.at[:, cols_at(2 * groups + group)], out.at[:, cols_at(group)], lse.at[pl.ds(group, 1)],
            size=size, rows_q=min(512, seq),
        )

    loop(groups, one)


def attend_back_stage(joined, grad_att, out, lse, b_qkv, dk_sum, dv_sum, size):
    seq, width = out.shape
    groups = width // LANES

    def one(group):
        here = [cols_at(part * groups + group) for part in range(3)]
        attend_back_body(
            *[joined.at[:, cols] for cols in here], grad_att.at[:, here[0]], out.at[:, here[0]],
            lse.at[pl.ds(group, 1)], *[b_qkv.at[:, cols] for cols in here], dk_sum, dv_sum,
            size=size, rows_q=min(512, seq),
        )

    loop(groups, one)


def close_stage(
    tok_ref, o_ref, att_ref, mid_ref, sec_ref, act_ref, slope_ref, out_ref, vec_ref, bias_ref, wo_ref, w1_ref, w2_ref
):
    attended = o_ref[...].astype(bf16)
    att_ref[...] = attended
    middle = tok_ref[...] + nn(attended, wo_ref[...]) + vec_ref[8:9]
    mid_ref[...] = middle
    hat, unused = norm_parts(middle)
    sec_ref[...] = (hat * vec_ref[2:3] + vec_ref[3:4]).astype(bf16)
    out_ref[...] = middle + vec_ref[9:10]

    def one(step):
        cols = cols_at(step, CHUNK)
        hidden = nn(sec_ref[...], w1_ref[:, cols]) + bias_ref[:, cols]
        share = 0.5 * (1.0 + lax.erf(hidden * math.sqrt(0.5)))
        active = (hidden * share).astype(bf16)
        act_ref[:, cols] = active
        slope_ref[:, cols] = share + hidden * (jnp.exp(-0.5 * hidden * hidden) * (1.0 / math.sqrt(2.0 * math.pi)))
        out_ref[...] += nn(active, w2_ref[cols, :])

    loop(w1_ref.shape[1] // CHUNK, one)


def back_up_stage(
    grad_ref, slope_ref, mid_ref, down_ref, up_ref, proj_ref, att_ref, total, vec_ref, wo_ref, w1_ref, w2_ref, sums_ref, bias_ref
):
    down = grad_ref[...].astype(bf16)
    down_ref[...] = down
    total[...] = jnp.zeros_like(total)

    def one(step):
        cols = cols_at(step, CHUNK)
        part = (nt(down_ref[...], w2_ref[cols, :]) * slope_ref[:, cols]).astype(bf16)
        up_ref[:, cols] = part
        bias_ref[:, cols] += column_sum(part)
        total[...] += nt(part, w1_ref[:, cols])

    loop(w1_ref.shape[1] // CHUNK, one)
    grad = total[...]
    hat, spread = norm_parts(mid_ref[...])
    middle = grad_ref[...] + norm_back(grad, hat, spread, vec_ref[2:3])
    grad_ref[...] = middle
    proj = middle.astype(bf16)
    proj_ref[...] = proj
    att_ref[...] = nt(proj, wo_ref[...]).astype(bf16)
    sums_ref[2:3] += column_sum(grad * hat)
    sums_ref[3:4] += column_sum(grad)
    sums_ref[8:9] += column_sum(proj)
    sums_ref[9:10] += column_sum(down)


def back_in_stage(join_ref, grad_ref, tok_ref, vec_ref, w_ref, sums_ref):
    width = tok_ref.shape[1]
    grad = nt(join_ref[...], w_ref[...])
    sums_ref[6:7] += column_sum(join_ref[:, :width])
    sums_ref[7:8] += column_sum(join_ref[:, 2 * width :])
    hat, spread = norm_parts(tok_ref[...])
    grad_ref[...] += norm_back(grad, hat, spread, vec_ref[0:1])
    sums_ref[0:1] += column_sum(grad * hat)
    sums_ref[1:2] += column_sum(grad)


def widen(flat_ref, wide, w_ref):
    rows_n, cols_n = w_ref.shape
    blocks = cols_n // LANES
    count = 64 * blocks

    def one(step):
        wide[:count] = flat_ref[rows_at(step, count), :].astype(f32)
        for block in range(blocks):
            w_ref[rows_at(step, 64), block * LANES : (block + 1) * LANES] = wide[
                pl.ds(block, 64, stride=blocks), :
            ].astype(bf16)

    loop(rows_n // 64, one)


class Weights:
    def __init__(self, flat, section, order, slots, wide, mats, sems):
        self.flat, self.slots, self.wide, self.mats, self.sems = flat, slots, wide, mats, sems
        self.order, self.shapes, self.next = order, section_shapes(section), 0
        self.base = section * (FLAT // LANES)
        for position in range(2):
            self.fetch(position).start()

    def fetch(self, position):
        index = self.order[position]
        start = self.base + sum(rows * cols for rows, cols in self.shapes[:index]) // LANES
        count = self.shapes[index][0] * self.shapes[index][1] // LANES
        return pltpu.make_async_copy(
            self.flat.at[pl.ds(start, count)], self.slots.at[position % 2, pl.ds(0, count)], self.sems.at[position]
        )

    def take(self):
        position = self.next
        self.fetch(position).wait()
        mat = self.mats[self.order[position]]
        widen(self.slots.at[position % 2], self.wide, mat)
        if position + 2 < len(self.order):
            self.fetch(position + 2).start()
        self.next += 1
        return mat


def take_rows(vec_ref, section, width, rows_ref, bias_ref, extra_ref=None):
    places = [(rows_ref, line, line * width, width) for line in range(11)]
    places.append((bias_ref, 0, 11 * width, bias_ref.shape[1]))
    if extra_ref is not None:
        places.append((extra_ref, 0, 11 * width + bias_ref.shape[1], width))
    for ref, line, offset, count in places:
        for tile in range(count // LANES):
            row = offset // LANES + tile
            ref[line : line + 1, tile * LANES : (tile + 1) * LANES] = vec_ref[section, row : row + 1]


class Copies:
    def __init__(self, sems):
        self.sems, self.made = sems, []

    def start(self, src, dst):
        copy = pltpu.make_async_copy(src, dst, self.sems.at[len(self.made)])
        copy.start()
        self.made.append(copy)
        return copy


def flat_count(section):
    return max(rows * cols for rows, cols in section_shapes(section)) // LANES


ANYWHERE = pl.BlockSpec(memory_space=pl.ANY)
WHOLE = pl.BlockSpec(memory_space=pltpu.VMEM)
ENC_KEPT = [
    (K_TOKENS, (VIS, DE), f32), (K_NORMED, (VIS, DE), bf16), (K_JOINED, (VIS, 3 * DE), bf16), (K_OUT, (VIS, DE), f32),
    (K_LSE, (DE // LANES, 2, VIS), f32), (K_ATTENDED, (VIS, DE), bf16), (K_MIDDLE, (VIS, DE), f32),
    (K_SECOND, (VIS, DE), bf16), (K_ACTIVE, (VIS, FFE), bf16), (K_SLOPE, (VIS, FFE), f32), (K_CODED, (VIS, DE), f32),
]


def encode_body(flat, pix, place, table, vec_ref, *rest):
    kept_n, mats_n = len(ENC_KEPT), len(section_shapes(0))
    kept_out, mats_out = rest[:kept_n], rest[kept_n : kept_n + mats_n]
    rest = rest[kept_n + mats_n :]
    kept = dict(zip([name for name, shape, kind in ENC_KEPT], rest[:kept_n]))
    mats = rest[kept_n : kept_n + mats_n]
    slots, wide, vecs, bias, in_sems, out_sems = rest[kept_n + mats_n :]
    take_rows(vec_ref, 0, DE, vecs, bias)
    weights = Weights(flat, 0, [4, 0, 1, 2, 3], slots, wide, mats, in_sems)
    copies = Copies(out_sems)

    def give(*names):
        for name in names:
            which = [entry[0] for entry in ENC_KEPT].index(name)
            copies.start(kept[name], kept_out[which])

    def take(index):
        mat = weights.take()
        copies.start(mat, mats_out[index])
        return mat

    kept[K_TOKENS][...] = positions_of(place[...], table) + vecs[10:11] + nn(pix[...], take(4)[...])
    open_stage(kept[K_TOKENS], kept[K_NORMED], kept[K_JOINED], vecs, take(0))
    give(K_TOKENS, K_NORMED, K_JOINED)
    attend_stage(kept[K_JOINED], kept[K_OUT], kept[K_LSE], DE // HEADS_ENC)
    give(K_OUT, K_LSE)
    wo, w1, w2 = take(1), take(2), take(3)
    keys = [K_TOKENS, K_OUT, K_ATTENDED, K_MIDDLE, K_SECOND, K_ACTIVE, K_SLOPE, K_CODED]
    close_stage(*[kept[name] for name in keys], vecs, bias, wo, w1, w2)
    give(K_ATTENDED, K_MIDDLE, K_SECOND, K_ACTIVE, K_SLOPE, K_CODED)
    for copy in copies.made:
        copy.wait()


def encode(flat, pix, place, table, vecs):
    mats = section_shapes(0)
    dma = pltpu.SemaphoreType.DMA
    outs = pl.pallas_call(
        encode_body,
        in_specs=[ANYWHERE] + [WHOLE] * 4,
        out_specs=[ANYWHERE] * (len(ENC_KEPT) + len(mats)),
        out_shape=[jax.ShapeDtypeStruct(shape, kind) for name, shape, kind in ENC_KEPT] + [shape_of(*shape, bf16) for shape in mats],
        scratch_shapes=[pltpu.VMEM(shape, kind) for name, shape, kind in ENC_KEPT]
        + [pltpu.VMEM(shape, bf16) for shape in mats]
        + [
            pltpu.VMEM((2, flat_count(0), LANES), bf16), pltpu.VMEM((64 * FFE // LANES, LANES), f32),
            pltpu.VMEM((16, DE), f32), pltpu.VMEM((1, FFE), f32), dma((len(mats),)), dma((len(ENC_KEPT) + len(mats),)),
        ],
        compiler_params=pltpu.CompilerParams(vmem_limit_bytes=BIG),
        name="encode",
    )(flat, pix, place, table, vecs)
    return dict(zip([name for name, shape, kind in ENC_KEPT], outs)), outs[len(ENC_KEPT) :]


def put_vec(part_ref, tail_row, offset, value):
    for tile in range(value.shape[1] // LANES):
        row = tail_row + offset // LANES + tile
        part_ref[row : row + 1] = value[:, tile * LANES : (tile + 1) * LANES]


def put_left(part_ref, section, index, factor_ref, u_ref, v_ref, gain):
    base = len(section_shapes(0)) * section + index
    unused, start, width = COL_SPANS[base]
    part = join3(nt(split3(factor_ref[section, :, start : start + width]), u_ref[...]))
    value = gain * join3(nn(split3(part), v_ref[...]))
    unused, start, width = ROW_SPANS[base]
    for tile in range(tiles_of(width)):
        here = min(LANES, width - tile * LANES)
        row = (start // LANES + tile) * RANK
        part_ref[row : row + RANK, :here] = value[:, tile * LANES : tile * LANES + here]


DEC_GIVEN = [
    (K_NORMED, (SEQ, DD), bf16), (K_B_QKV, (SEQ, 3 * DD), bf16), (K_ATTENDED, (SEQ, DD), bf16), (K_B_PROJ, (SEQ, DD), bf16),
    (K_SECOND, (SEQ, DD), bf16), (K_B_UP, (SEQ, FFD), bf16), (K_ACTIVE, (SEQ, FFD), bf16), (K_B_DOWN, (SEQ, DD), bf16),
    (K_B_PRED, (SEQ - VIS, PATCH), bf16), (K_FINAL, (SEQ - VIS, DD), bf16), (K_SENT, (VIS, DE), bf16), (K_FIRST, (VIS, DD), bf16),
]
DEC_HELD = [
    (K_TOKENS, (SEQ, DD), f32), (K_JOINED, (SEQ, 3 * DD), bf16), (K_OUT, (SEQ, DD), f32), (K_LSE, (DD // LANES, 4, SEQ), f32),
    (K_MIDDLE, (SEQ, DD), f32), (K_SLOPE, (SEQ, FFD), f32), (K_GRAD, (SEQ, DD), f32), (K_ATT, (SEQ, DD), bf16),
    (K_DK, (SEQ, LANES), f32), (K_DV, (SEQ, LANES), f32), (K_SUMS, (16, DD), f32), (K_BIAS, (1, FFD), f32),
]


def decode_body(
    flat, coded, place, table, vec_ref, target, mask, count_ref, factor, *rest, tail_row, gain
):
    given_n, held_n, mats_n = len(DEC_GIVEN), len(DEC_HELD), len(section_shapes(1))
    given_out, grad_coded, sums_e, part_ref = rest[:given_n], rest[given_n], rest[given_n + 1], rest[given_n + 2]
    rest = rest[given_n + 3 :]
    have = dict(zip([name for name, shape, kind in DEC_GIVEN + DEC_HELD], rest[: given_n + held_n]))
    mats = rest[given_n + held_n : given_n + held_n + mats_n]
    slots, wide, total, vec_e, bias_e, vec_d, bias, extra, in_sems, out_sems = rest[given_n + held_n + mats_n :]
    take_rows(vec_ref, 0, DE, vec_e, bias_e)
    take_rows(vec_ref, 1, DD, vec_d, bias, extra)
    weights = Weights(flat, 1, [5, 0, 1, 2, 3, 4], slots, wide, mats, in_sems)
    copies = Copies(out_sems)
    blk = total.shape[0]
    sums, bias_sum = have[K_SUMS], have[K_BIAS]

    def give(*names):
        for name in names:
            which = [entry[0] for entry in DEC_GIVEN].index(name)
            copies.start(have[name], given_out[which])

    part_ref[...] = jnp.zeros_like(part_ref)
    sums[...] = jnp.zeros_like(sums)
    bias_sum[...] = jnp.zeros_like(bias_sum)

    w_emb = weights.take()
    hat_e, spread_e = norm_parts(coded[...])
    have[K_SENT][...] = (hat_e * vec_e[4:5] + vec_e[5:6]).astype(bf16)
    give(K_SENT)
    have[K_TOKENS][:VIS] = nn(have[K_SENT][...], w_emb[...]) + extra[...] + positions_of(place[:VIS], table)

    def fill(step):
        rows = pl.ds(pl.multiple_of(VIS + step * VIS, VIS), VIS)
        have[K_TOKENS][rows] = vec_d[10:11] + positions_of(place[rows], table)

    loop(SEQ // VIS - 1, fill)
    w_qkv = weights.take()
    over_blocks(
        SEQ, blk, lambda *refs: open_stage(*refs, vec_d, w_qkv), *[have[name] for name in (K_TOKENS, K_NORMED, K_JOINED)]
    )
    give(K_NORMED)
    attend_stage(have[K_JOINED], have[K_OUT], have[K_LSE], DD // HEADS_DEC)
    wo, w1, w2 = weights.take(), weights.take(), weights.take()
    keys = [K_TOKENS, K_OUT, K_ATTENDED, K_MIDDLE, K_SECOND, K_ACTIVE, K_SLOPE, K_GRAD]
    over_blocks(SEQ, blk, lambda *refs: close_stage(*refs, vec_d, bias, wo, w1, w2), *[have[name] for name in keys])
    give(K_ATTENDED, K_SECOND, K_ACTIVE)

    w_head = weights.take()
    count = count_ref[...]

    def head(step):
        rows = pl.ds(pl.multiple_of(VIS + step * VIS, VIS), VIS)
        late = rows_at(step, VIS)
        hat, spread = norm_parts(have[K_GRAD][rows])
        final = (hat * vec_d[4:5] + vec_d[5:6]).astype(bf16)
        have[K_FINAL][late] = final
        residual = nt(final, w_head[...]) - target[late].astype(f32)
        weight = mask[late]
        loss = jnp.sum(weight * jnp.mean(residual * residual, axis=1, keepdims=True), axis=0, keepdims=True) / count
        row = tail_row + VEC_TILES * RANK
        part_ref[row : row + RANK] += jnp.broadcast_to(loss, (RANK, LANES))
        b_pred = (weight * (2.0 * residual / PATCH) / count).astype(bf16)
        have[K_B_PRED][late] = b_pred
        grad = nn(b_pred, w_head[...])
        have[K_GRAD][rows] = norm_back(grad, hat, spread, vec_d[4:5])
        sums[4:5] += column_sum(grad * hat)
        sums[5:6] += column_sum(grad)

    loop(SEQ // VIS - 1, head)
    have[K_GRAD][:VIS] = jnp.zeros((VIS, DD), f32)
    give(K_FINAL, K_B_PRED)

    keys = [K_GRAD, K_SLOPE, K_MIDDLE, K_B_DOWN, K_B_UP, K_B_PROJ, K_ATT]
    over_blocks(
        SEQ, blk, lambda *refs: back_up_stage(*refs, total, vec_d, wo, w1, w2, sums, bias_sum), *[have[name] for name in keys]
    )
    give(K_B_DOWN, K_B_UP, K_B_PROJ)
    attend_back_stage(
        have[K_JOINED], have[K_ATT], have[K_OUT], have[K_LSE], have[K_B_QKV], have[K_DK], have[K_DV], DD // HEADS_DEC
    )
    give(K_B_QKV)
    over_blocks(
        SEQ, blk, lambda *refs: back_in_stage(*refs, vec_d, w_qkv, sums), *[have[name] for name in (K_B_QKV, K_GRAD, K_TOKENS)]
    )
    first = have[K_GRAD][:VIS].astype(bf16)
    have[K_FIRST][...] = first
    give(K_FIRST)
    sums[10:11] = column_sum(have[K_GRAD][VIS:])
    back = nt(first, w_emb[...]).astype(bf16).astype(f32)
    grad_coded[...] = norm_back(back, hat_e, spread_e, vec_e[4:5])
    sums_e[...] = jnp.zeros_like(sums_e)
    sums_e[0:1] = column_sum(back * hat_e)
    sums_e[1:2] = column_sum(back)
    for line in range(11):
        put_vec(part_ref, tail_row, line * DD, sums[line : line + 1])
    put_vec(part_ref, tail_row, 11 * DD, bias_sum[...])
    put_vec(part_ref, tail_row, 11 * DD + FFD, column_sum(first))
    pairs = [(K_NORMED, K_B_QKV), (K_ATTENDED, K_B_PROJ), (K_SECOND, K_B_UP), (K_ACTIVE, K_B_DOWN), (K_B_PRED, K_FINAL), (K_SENT, K_FIRST)]
    for index, (a, b) in enumerate(pairs):
        put_left(part_ref, 1, index, factor, have[b], have[a], gain)
    for copy in copies.made:
        copy.wait()


def decode(flat, coded, place, table, vecs, target, mask, count, factor, tail_row, gain, rows):
    mats = section_shapes(1)
    dma = pltpu.SemaphoreType.DMA
    outs = pl.pallas_call(
        functools.partial(decode_body, tail_row=tail_row, gain=gain),
        in_specs=[ANYWHERE] + [WHOLE] * 8,
        out_specs=[ANYWHERE] * len(DEC_GIVEN) + [WHOLE] * 3,
        out_shape=[jax.ShapeDtypeStruct(shape, kind) for name, shape, kind in DEC_GIVEN]
        + [shape_of(VIS, DE), shape_of(8, DE), shape_of(rows, LANES)],
        scratch_shapes=[pltpu.VMEM(shape, kind) for name, shape, kind in DEC_GIVEN + DEC_HELD]
        + [pltpu.VMEM(shape, bf16) for shape in mats]
        + [
            pltpu.VMEM((2, flat_count(1), LANES), bf16), pltpu.VMEM((64 * FFD // LANES, LANES), f32),
            pltpu.VMEM((DEC_ROWS, DD), f32), pltpu.VMEM((16, DE), f32), pltpu.VMEM((1, FFE), f32), pltpu.VMEM((16, DD), f32),
            pltpu.VMEM((1, FFD), f32), pltpu.VMEM((1, DD), f32), dma((len(mats),)), dma((len(DEC_GIVEN),)),
        ],
        compiler_params=pltpu.CompilerParams(vmem_limit_bytes=BIG),
        name="decode",
    )(flat, coded, place, table, vecs, target, mask, count, factor)
    given = dict(zip([name for name, shape, kind in DEC_GIVEN], outs))
    return given, outs[-3], outs[-2], outs[-1]


ENC_GIVEN = [
    (K_B_QKV, (VIS, 3 * DE), bf16), (K_B_PROJ, (VIS, DE), bf16), (K_B_UP, (VIS, FFE), bf16), (K_B_DOWN, (VIS, DE), bf16),
    (K_START, (VIS, DE), bf16),
]
ENC_HELD = [
    (K_ATT, (VIS, DE), bf16), (K_DK, (VIS, LANES), f32), (K_DV, (VIS, LANES), f32), (K_SUMS, (16, DE), f32), (K_BIAS, (1, FFE), f32),
]
ENC_USED = [K_SLOPE, K_MIDDLE, K_JOINED, K_OUT, K_LSE, K_TOKENS, K_SECOND, K_ACTIVE, K_ATTENDED, K_NORMED]


def encode_back_body(*refs, tail_row, gain):
    used_n, given_n, held_n = len(ENC_USED), len(ENC_GIVEN), len(ENC_HELD)
    kept_in, mats_in, refs = refs[:used_n], refs[used_n : used_n + 4], refs[used_n + 4 :]
    grad_in, sums_e, vec_ref, pix, factor = refs[:5]
    given_out, part_ref, refs = refs[5 : 5 + given_n], refs[5 + given_n], refs[6 + given_n :]
    have = dict(zip(ENC_USED, refs[:used_n]))
    refs = refs[used_n:]
    have.update(zip([name for name, shape, kind in ENC_GIVEN + ENC_HELD], refs[: given_n + held_n]))
    mats = refs[given_n + held_n : given_n + held_n + 4]
    grad, total, vecs, bias_e, in_sems, out_sems = refs[given_n + held_n + 4 :]
    reads, copies = Copies(in_sems), Copies(out_sems)
    w2 = reads.start(mats_in[3], mats[3])
    take_rows(vec_ref, 0, DE, vecs, bias_e)
    waits = {name: reads.start(src, have[name]) for name, src in list(zip(ENC_USED, kept_in))[:2]}
    w1 = reads.start(mats_in[2], mats[2])
    wo = reads.start(mats_in[1], mats[1])
    waits.update({name: reads.start(src, have[name]) for name, src in list(zip(ENC_USED, kept_in))[2:]})
    w_qkv = reads.start(mats_in[0], mats[0])
    sums, bias_sum = have[K_SUMS], have[K_BIAS]

    def give(*names):
        for name in names:
            which = [entry[0] for entry in ENC_GIVEN].index(name)
            copies.start(have[name], given_out[which])

    part_ref[...] = jnp.zeros_like(part_ref)
    sums[...] = jnp.zeros_like(sums)
    bias_sum[...] = jnp.zeros_like(bias_sum)
    sums[4:5] = sums_e[0:1]
    sums[5:6] = sums_e[1:2]
    grad[...] = grad_in[...]
    for wait in (w2, waits[K_SLOPE], waits[K_MIDDLE], w1, wo):
        wait.wait()
    back_up_stage(
        grad, have[K_SLOPE], have[K_MIDDLE], have[K_B_DOWN], have[K_B_UP], have[K_B_PROJ], have[K_ATT], total,
        vecs, mats[1], mats[2], mats[3], sums, bias_sum,
    )
    give(K_B_DOWN, K_B_UP, K_B_PROJ)
    for name in (K_JOINED, K_OUT, K_LSE, K_TOKENS):
        waits[name].wait()
    attend_back_stage(
        have[K_JOINED], have[K_ATT], have[K_OUT], have[K_LSE], have[K_B_QKV], have[K_DK], have[K_DV], DE // HEADS_ENC
    )
    give(K_B_QKV)
    w_qkv.wait()
    back_in_stage(have[K_B_QKV], grad, have[K_TOKENS], vecs, mats[0], sums)
    start = grad[...].astype(bf16)
    have[K_START][...] = start
    give(K_START)
    sums[10:11] = column_sum(start)
    for line in range(11):
        put_vec(part_ref, tail_row, line * DE, sums[line : line + 1])
    put_vec(part_ref, tail_row, 11 * DE, bias_sum[...])
    for name in (K_SECOND, K_ACTIVE, K_ATTENDED, K_NORMED):
        waits[name].wait()
    pairs = [(K_NORMED, K_B_QKV), (K_ATTENDED, K_B_PROJ), (K_SECOND, K_B_UP), (K_ACTIVE, K_B_DOWN)]
    for index, (a, b) in enumerate(pairs):
        put_left(part_ref, 0, index, factor, have[b], have[a], gain)
    put_left(part_ref, 0, 4, factor, have[K_START], pix, gain)
    for copy in copies.made:
        copy.wait()


def encode_back(kept, mats, grad_coded, sums_e, vecs, pix, factor, tail_row, gain, rows):
    shapes = {name: (shape, kind) for name, shape, kind in ENC_KEPT}
    dma = pltpu.SemaphoreType.DMA
    outs = pl.pallas_call(
        functools.partial(encode_back_body, tail_row=tail_row, gain=gain),
        in_specs=[ANYWHERE] * (len(ENC_USED) + 4) + [WHOLE] * 5,
        out_specs=[ANYWHERE] * len(ENC_GIVEN) + [WHOLE],
        out_shape=[jax.ShapeDtypeStruct(shape, kind) for name, shape, kind in ENC_GIVEN] + [shape_of(rows, LANES)],
        scratch_shapes=[pltpu.VMEM(*shapes[name]) for name in ENC_USED]
        + [pltpu.VMEM(shape, kind) for name, shape, kind in ENC_GIVEN + ENC_HELD]
        + [pltpu.VMEM(shape, bf16) for shape in section_shapes(0)[:4]]
        + [
            pltpu.VMEM((VIS, DE), f32), pltpu.VMEM((VIS, DE), f32), pltpu.VMEM((16, DE), f32), pltpu.VMEM((1, FFE), f32),
            dma((len(ENC_USED) + 4,)), dma((len(ENC_GIVEN),)),
        ],
        compiler_params=pltpu.CompilerParams(vmem_limit_bytes=BIG),
        name="encode_back",
    )(*[kept[name] for name in ENC_USED], *mats[:4], grad_coded, sums_e, vecs, pix, factor)
    return dict(zip([name for name, shape, kind in ENC_GIVEN], outs)), outs[-1]


def tiles_of(width):
    return -(-width // LANES)


def spans(which):
    at, found = [], []
    for section in range(2):
        start = 0
        for shape in section_shapes(section):
            found.append((section, start, shape[which]))
            start += tiles_of(shape[which]) * LANES
        at.append(start)
    return found, at


ROW_SPANS, ROW_WIDTHS = spans(0)
COL_SPANS, COL_WIDTHS = spans(1)
ROW_PAD = max(ROW_WIDTHS)
VEC_TILES = -(-VLEN // (RANK * LANES))


def sum_rows(replicas, tiles):
    return -(-tiles // replicas) * replicas * RANK


def put_tiles(out_ref, section, start, value):
    width = value.shape[1]
    for tile in range(tiles_of(width)):
        here = min(LANES, width - tile * LANES)
        row = (start // LANES + tile) * RANK
        out_ref[section, row : row + RANK, :here] = value[:, tile * LANES : tile * LANES + here]


def chunk_rows(rows_n, cols_n):
    if rows_n == PATCH:
        return PATCH
    return 256


def err_prep_body(e_ref, x_ref, *rest, blocks, rows):
    out_ref, left_ref, wide = rest[-3:]
    wide[...] = e_ref[0].reshape(rows * blocks, LANES).astype(f32)
    pieces = split3(x_ref[...])
    total = jnp.zeros((rows, 3 * RANK), f32)
    for block in range(blocks):
        part = wide[pl.ds(block, rows, stride=blocks), :].astype(bf16)
        out_ref[block * rows : (block + 1) * rows, :] = part
        total = total + nt(part, pieces[:, block * LANES : (block + 1) * LANES])
    value = join3(total.T)
    left_ref[...] = jnp.zeros_like(left_ref)
    for tile in range(tiles_of(rows)):
        here = min(LANES, rows - tile * LANES)
        left_ref[tile * RANK : (tile + 1) * RANK, :here] = value[:, tile * LANES : tile * LANES + here]


def err_prep(errors, factor, start, rows_n, cols_n, buf):
    blocks = cols_n // LANES
    rows = chunk_rows(rows_n, cols_n)
    step = rows * blocks
    steps = rows_n // rows
    tiles = tiles_of(rows)
    in_specs = [
        pl.BlockSpec((pl.Element(1), pl.Element(1), pl.Element(step * LANES)), lambda i: (0, 0, pl.multiple_of(start + i * step * LANES, 1024))),
        pl.BlockSpec((RANK, cols_n), lambda i: (0, 0)),
    ]
    args = [errors, factor]
    aliases = {}
    if buf is not None:
        in_specs.append(pl.BlockSpec(memory_space=pl.ANY))
        args.append(buf)
        aliases = {2: 0}
    return pl.pallas_call(
        functools.partial(err_prep_body, blocks=blocks, rows=rows),
        grid=(steps,),
        in_specs=in_specs,
        out_specs=[
            pl.BlockSpec((pl.Element(step), pl.Element(LANES)), lambda i: (pl.multiple_of(start // LANES + i * step, 16), 0)),
            pl.BlockSpec((tiles * RANK, LANES), lambda i: (i, 0)),
        ],
        out_shape=[
            jax.ShapeDtypeStruct((FLAT // LANES, LANES), bf16),
            jax.ShapeDtypeStruct((steps * tiles * RANK, LANES), f32),
        ],
        input_output_aliases=aliases,
        scratch_shapes=[pltpu.VMEM((step, LANES), f32)],
        name="err_prep",
    )(*args)


def ortho_stage(sum_ref, out_ref, wide, scale):
    rank_id = lax.broadcasted_iota(jnp.int32, (RANK, 1), 0)
    for section, start, width in ROW_SPANS:
        padded = tiles_of(width) * LANES
        for tile in range(padded // LANES):
            row = (start // LANES + tile) * RANK
            wide[:, tile * LANES : (tile + 1) * LANES] = sum_ref[section, row : row + RANK] * scale
        basis = wide[:, :padded]
        for column in range(RANK):
            current = basis[column : column + 1]
            current = current * lax.rsqrt(jnp.sum(current * current, axis=1, keepdims=True) + 1e-12)
            dots = jnp.sum(basis * current, axis=1, keepdims=True)
            basis = jnp.where(
                rank_id > column, basis - dots * current, jnp.where(rank_id == column, current, basis)
            )
        out_ref[section, :, start : start + padded] = basis


def err_plan(section):
    plan = []
    start = 0
    spans = [(row, col) for row, col in zip(ROW_SPANS, COL_SPANS) if row[0] == section]
    for (rows_n, cols_n), (row_span, col_span) in zip(section_shapes(section), spans):
        rows = chunk_rows(rows_n, cols_n)
        blocks = cols_n // LANES
        for chunk in range(rows_n // rows):
            plan.append((start // LANES + chunk * rows * blocks, rows, blocks, row_span[1] + chunk * rows, col_span[1], chunk))
        start += rows_n * cols_n
    return plan


def put_tiles(out_ref, row, value):
    for tile in range(value.shape[1] // LANES):
        out_ref[row + tile * RANK : row + (tile + 1) * RANK] = value[:, tile * LANES : (tile + 1) * LANES]


def rights_body(*refs, n, scale, gain):
    sum_ref, err_ref, u_in, v_in = refs[0], refs[1], refs[2 : 2 + n], refs[2 + n : 2 + 2 * n]
    ortho_ref, part_ref, extra_ref = refs[2 + 2 * n : 5 + 2 * n]
    refs = refs[5 + 2 * n :]
    u_refs, v_refs = refs[:n], refs[n : 2 * n]
    wide, ring, ring_sems, in_sems = refs[2 * n :]
    section = lax.axis_index(SEC)
    depth = ring.shape[0]
    plans = [err_plan(which) for which in range(2)]

    def fetch(plan, index):
        at, rows, blocks = plan[index][:3]
        slot = index % depth
        return pltpu.make_async_copy(
            err_ref.at[pl.ds(at, rows * blocks)], ring.at[slot, pl.ds(0, rows * blocks)], ring_sems.at[slot]
        )

    for which, plan in enumerate(plans):

        @pl.when(section == which)
        def _():
            for index in range(depth - 1):
                fetch(plan, index).start()

    reads = Copies(in_sems)
    waits = [(reads.start(u_in[i], u_refs[i]), reads.start(v_in[i], v_refs[i])) for i in range(n)]
    ortho_stage(sum_ref, ortho_ref, wide, scale)
    extra_ref[...] = jnp.zeros_like(extra_ref)
    part_ref[...] = jnp.zeros_like(part_ref)
    for which, plan in enumerate(plans):

        @pl.when(section == which)
        def _():
            for index, (at, rows, blocks, row_at, col_at, chunk) in enumerate(plan):
                if index + depth - 1 < len(plan):
                    fetch(plan, index + depth - 1).start()
                fetch(plan, index).wait()
                pieces = split3(ortho_ref[which, :, row_at : row_at + rows])
                for block in range(0, blocks, 2):
                    pair = [ring[index % depth, (block + side) * rows : (block + side + 1) * rows] for side in range(2)]
                    part = join3(nn(pieces, jnp.concatenate(pair, axis=1)))
                    row = (col_at // LANES + block) * RANK
                    if chunk == 0:
                        put_tiles(extra_ref, row, part)
                    else:
                        for side in range(2):
                            extra_ref[row + side * RANK : row + (side + 1) * RANK] += part[:, side * LANES : (side + 1) * LANES]

    for (wait_u, wait_v), u_ref, v_ref, (which, row_at, rows), (unused, col_at, cols) in zip(waits, u_refs, v_refs, ROW_SPANS, COL_SPANS):
        wait_u.wait()
        wait_v.wait()
        part = join3(nt(split3(ortho_ref[which, :, row_at : row_at + rows]), u_ref[...]))
        put_tiles(part_ref.at[which], col_at // LANES * RANK, gain * join3(nn(split3(part), v_ref[...])))


def rights(sums, err, us, vs, scale, gain, rows):
    n = len(us)
    most = max(chunk_rows(*shape) * shape[1] // LANES for which in range(2) for shape in section_shapes(which))
    dma = pltpu.SemaphoreType.DMA
    return pl.pallas_call(
        functools.partial(rights_body, n=n, scale=scale, gain=gain),
        in_specs=[WHOLE] + [ANYWHERE] * (2 * n + 1),
        out_specs=[WHOLE] * 3,
        out_shape=[
            jax.ShapeDtypeStruct((2, RANK, ROW_PAD), f32), jax.ShapeDtypeStruct((2, rows, LANES), f32), shape_of(rows, LANES)
        ],
        scratch_shapes=[pltpu.VMEM(x.shape, bf16) for x in [*us, *vs]]
        + [pltpu.VMEM((RANK, FFE), f32), pltpu.VMEM((4, most, LANES), bf16), dma((4,)), dma((2 * n,))],
        compiler_params=pltpu.CompilerParams(vmem_limit_bytes=BIG),
        name="rights",
    )(sums, err, *us, *vs)


def final_right_body(sum_ref, ortho_ref, vec_ref, right_ref, norm_ref, *, scale):
    squares = jnp.sum(vec_ref[...] * vec_ref[...], keepdims=True)[0]
    for (section, start, width), (unused, row_at, row_width) in zip(COL_SPANS, ROW_SPANS):
        for tile in range(width // LANES):
            row = (start // LANES + tile) * RANK
            right_ref[section, :, start + tile * LANES : start + (tile + 1) * LANES] = sum_ref[section, row : row + RANK] * scale
        o_part = ortho_ref[section, :, row_at : row_at + tiles_of(row_width) * LANES]
        r_part = right_ref[section, :, start : start + width]
        for line in range(RANK):
            gram_o = jnp.sum(o_part * o_part[line : line + 1], axis=1, keepdims=True)
            gram_r = jnp.sum(r_part * r_part[line : line + 1], axis=1, keepdims=True)
            squares = squares + jnp.sum(gram_o * gram_r, keepdims=True)
    for section in range(2):
        used = COL_WIDTHS[section]
        if used < right_ref.shape[2]:
            right_ref[section, :, used:] = jnp.zeros((RANK, right_ref.shape[2] - used), f32)
    norm_ref[...] = jnp.broadcast_to(jnp.sqrt(squares), norm_ref.shape)


def final_right(sums, ortho, vecs, cols, scale):
    full = pl.BlockSpec(memory_space=pltpu.VMEM)
    return pl.pallas_call(
        functools.partial(final_right_body, scale=scale),
        in_specs=[full] * 3,
        out_specs=[full] * 2,
        out_shape=[jax.ShapeDtypeStruct((2, RANK, cols), f32), jax.ShapeDtypeStruct((1, LANES), f32)],
        name="final_right",
    )(sums, ortho, vecs)


def finish_body(me_ref, a0, a1, b0, b1, e_ref, o_ref, r_ref, *rest, rows, blocks, gain, start, shard):
    err_out, app_out = rest[-2:]
    o_part = o_ref[0]
    o_high = o_part.astype(bf16)
    o_low = (o_part - o_high.astype(f32)).astype(bf16)
    left_t = jnp.concatenate([o_high, o_low, o_high], axis=0).T[:rows]
    lhs0 = a0[...].T
    lhs1 = a1[...].T
    err_rows = err_out.at[0].reshape(rows * blocks, LANES)
    keep = overlaps(pl.program_id(0), me_ref[0], start, rows * blocks, shard)
    for pair in range(blocks // 2):
        cols = slice(pair * 2 * LANES, (pair + 1) * 2 * LANES)
        r_part = r_ref[0, :, cols]
        r_high = r_part.astype(bf16)
        r_low = (r_part - r_high.astype(f32)).astype(bf16)
        approx = nn(left_t, jnp.concatenate([r_high, r_high, r_low], axis=0))
        grad = nn(lhs0, b0[:, cols]) + nn(lhs1, b1[:, cols])
        for side in range(2):
            block = pair * 2 + side
            half = slice(side * LANES, (side + 1) * LANES)
            err_rows[pl.ds(block, rows, stride=blocks), :] = (
                gain * grad[:, half] + e_ref[block * rows : (block + 1) * rows].astype(f32)
            ) - approx[:, half]

            @pl.when(keep)
            def _():
                app_out[pl.ds(block, rows, stride=blocks), :] = approx[:, half]


def overlaps(i, me, start, step, shard):
    first = start + i * step * LANES
    return (first < (me + 1) * shard) & (first + step * LANES > me * shard)


def finish(me, pair0, pair1, err, ortho, right, section, row_at, col_at, start, gain, shard, bufs):
    a0, b0 = pair0
    a1, b1 = pair1
    rows_n, cols_n = a0.shape[1], b0.shape[1]
    seq = a0.shape[0]
    blocks = cols_n // LANES
    rows = chunk_rows(rows_n, cols_n)
    step = rows * blocks
    flat_rows = FLAT // LANES
    whole = lambda i, me: (0, 0)
    flat_at = lambda i: pl.multiple_of(start // LANES + i * step, 16)
    wide_rows = tiles_of(rows) * LANES

    def shard_at(i, me):
        return pl.multiple_of(jnp.where(overlaps(i, me[0], start, step, shard), start // LANES + i * step, flat_rows), 8), 0

    in_specs = [
        pl.BlockSpec((seq, rows), lambda i, me: (0, i)),
        pl.BlockSpec((seq, rows), lambda i, me: (0, i)),
        pl.BlockSpec((seq, cols_n), whole, pipeline_mode=pl.Buffered(1)),
        pl.BlockSpec((seq, cols_n), whole, pipeline_mode=pl.Buffered(1)),
        pl.BlockSpec((pl.Element(step), pl.Element(LANES)), lambda i, me: (flat_at(i), 0)),
        pl.BlockSpec((1, RANK, wide_rows), lambda i, me: (section, 0, row_at // wide_rows + i)),
        pl.BlockSpec(
            (pl.Element(1), pl.Element(RANK), pl.Element(cols_n)), lambda i, me: (section, 0, col_at), pipeline_mode=pl.Buffered(1)
        ),
    ]
    assert row_at % wide_rows == 0
    args = [a0, a1, b0, b1, err, ortho, right]
    aliases = {}
    if bufs is not None:
        in_specs += [pl.BlockSpec(memory_space=pl.ANY)] * 2
        args += list(bufs)
        aliases = {8: 0, 9: 1}
    return pl.pallas_call(
        functools.partial(finish_body, rows=rows, blocks=blocks, gain=gain, start=start, shard=shard),
        grid_spec=pltpu.PrefetchScalarGridSpec(
            num_scalar_prefetch=1,
            grid=(rows_n // rows,),
            in_specs=in_specs,
            out_specs=[
                pl.BlockSpec(
                    (pl.Element(1), pl.Element(1), pl.Element(step * LANES)),
                    lambda i, me: (0, 0, pl.multiple_of(start + i * step * LANES, 1024)),
                ),
                pl.BlockSpec((pl.Element(step), pl.Element(LANES)), shard_at),
            ],
        ),
        out_shape=[
            jax.ShapeDtypeStruct((1, 1, FLAT), f32),
            jax.ShapeDtypeStruct((flat_rows + SPARE, LANES), f32),
        ],
        input_output_aliases=aliases,
        compiler_params=pltpu.CompilerParams(vmem_limit_bytes=BIG),
        name="finish",
    )(me, *args)


def tail_body(e_ref, buf0, err_out):
    err_out[...] = e_ref[...].astype(f32)


def finish_tail(errors, start, buf):
    count = FLAT - start
    steps = 6
    step = count // steps
    assert step * steps == count and step % 1024 == 0
    spec = pl.BlockSpec((pl.Element(1), pl.Element(1), pl.Element(step)), lambda i: (0, 0, pl.multiple_of(start + i * step, 1024)))
    return pl.pallas_call(
        tail_body,
        grid=(steps,),
        in_specs=[spec, pl.BlockSpec(memory_space=pl.ANY)],
        out_specs=spec,
        out_shape=jax.ShapeDtypeStruct((1, 1, FLAT), f32),
        input_output_aliases={1: 0},
        compiler_params=pltpu.CompilerParams(vmem_limit_bytes=BIG),
        name="finish_tail",
    )(errors, buf)


MESH = pl.DeviceIdType.MESH


def grid_of(replicas):
    side = 2 if replicas < 64 else 4
    return replicas // (side * side), side, side


def used_rows(section):
    counts = [sum(rows * cols for rows, cols in section_shapes(s)) // LANES for s in range(2)]
    return jnp.where(section == 0, counts[0], counts[1])


def meet(replicas):
    section, me = lax.axis_index(SEC), lax.axis_index(DP)
    barrier = pltpu.get_barrier_semaphore()
    pl.semaphore_signal(barrier, inc=1, device_id={SEC: 1 - section}, device_id_type=MESH)
    for step in range(1, replicas):
        pl.semaphore_signal(
            barrier, inc=1, device_id={DP: lax.rem(me + step, replicas)}, device_id_type=MESH
        )
    pl.semaphore_wait(barrier, replicas)


def gather_body(
    low_ref, cnt_ref, vec_ref, fac_ref, flat_ref, cnts_ref, vec2_ref, fac2_ref,
    send_sem, recv_sem, swap_sem, cnt_send, cnt_recv, side_send, side_recv, own_sem, *, replicas, size,
):
    section, me = lax.axis_index(SEC), lax.axis_index(DP)
    other = 1 - section
    nz, ny, nx = grid_of(replicas)
    x, y, z = lax.rem(me, nx), lax.rem(me // nx, ny), me // (nx * ny)
    cut = size // 2 // 8 * 8 if size % 8 == 0 else size
    halves = [(0, cut), (cut, size - cut)] if cut < size else [(0, cut)]
    used = used_rows(section)
    used_other = used_rows(other)

    def block_id(at_z, at_y, at_x):
        return (at_z * ny + at_y) * nx + at_x

    meet(replicas)

    def side(src, dst, slot):
        return pltpu.make_async_remote_copy(
            src_ref=src, dst_ref=dst.at[section], send_sem=side_send.at[slot], recv_sem=side_recv.at[slot],
            device_id={SEC: other}, device_id_type=MESH,
        )

    def count_copy(step):
        return pltpu.make_async_remote_copy(
            src_ref=cnt_ref, dst_ref=cnts_ref.at[me], send_sem=cnt_send.at[step],
            recv_sem=cnt_recv.at[step], device_id={DP: lax.rem(me + step, replicas)}, device_id_type=MESH,
        )

    for step in range(1, replicas):
        count_copy(step).start()
    side(vec_ref, vec2_ref, 0).start()
    side(fac_ref, fac2_ref, 1).start()
    own = pltpu.make_async_copy(low_ref, flat_ref.at[section * replicas + me], own_sem)
    own.start()

    def copy(block, half, target, way, mine=False, swap=False):
        start, rows = halves[half]
        at = flat_ref.at[section * replicas + block, pl.ds(start, rows)]
        src = low_ref.at[pl.ds(start, rows)] if mine else at
        return pltpu.make_async_remote_copy(
            src_ref=src, dst_ref=at, send_sem=send_sem.at[block, half, way],
            recv_sem=(swap_sem if swap else recv_sem).at[block, half], device_id=target, device_id_type=MESH,
        )

    def needed(block, half, limit):
        return block * size + halves[half][0] < limit

    def at_z(value):
        return {DP: block_id(value, y, x)}

    def along_x(block, half, mine=False):
        for step in range(1, nx):
            copy(block, half, {DP: block_id(z, y, lax.rem(x + step, nx))}, 1 + step, mine).start()

    def along_y(block, half, mine=False):
        for step in range(1, ny):
            copy(block, half, {DP: block_id(z, lax.rem(y + step, ny), x)}, nx + step, mine).start()

    def across(block, half, mine=False):
        copy(block, half, {SEC: other}, nx + ny, mine, True).start()

    def arrived(block, half):
        copy(block, half, {SEC: other}, 0).wait_recv()

    def layers(k):
        return [z] if k == 0 else [z - k, z + k]

    def valid(at):
        return (at >= 0) & (at < nz)

    def first(k):
        for which, layer in enumerate(layers(k)):
            block = block_id(layer, y, x)
            for half in range(len(halves)):

                @pl.when(valid(layer) & needed(block, half, used))
                def _():
                    if k > 0:
                        arrived(block, half)
                    mine = k == 0
                    if k == 0 or which == 0:

                        @pl.when(z + 1 < nz)
                        def _():
                            copy(block, half, at_z(z + 1), 0, mine).start()

                    if k == 0 or which == 1:

                        @pl.when(z > 0)
                        def _():
                            copy(block, half, at_z(z - 1), 1, mine).start()

                    if half == 0:
                        along_x(block, half, mine)
                        along_y(block, half, mine)
                    else:
                        along_y(block, half, mine)
                        along_x(block, half, mine)
                    across(block, half, mine)

    def second(k):
        for layer in layers(k):
            for half in range(len(halves)):
                for step in range(1, nx if half == 0 else ny):
                    if half == 0:
                        block = block_id(layer, y, lax.rem(x + step, nx))
                    else:
                        block = block_id(layer, lax.rem(y + step, ny), x)

                    @pl.when(valid(layer) & needed(block, half, used))
                    def _():
                        arrived(block, half)
                        if half == 0:
                            along_y(block, half)
                        else:
                            along_x(block, half)
                        across(block, half)

    def third(k):
        for layer in layers(k):
            for half in range(len(halves)):
                for far in range(1, ny if half == 0 else nx):
                    for near in range(nx if half == 0 else ny):
                        if half == 0:
                            block = block_id(layer, lax.rem(y + far, ny), lax.rem(x + near, nx))
                        else:
                            block = block_id(layer, lax.rem(y + near, ny), lax.rem(x + far, nx))

                        @pl.when(valid(layer) & needed(block, half, used))
                        def _():
                            arrived(block, half)
                            across(block, half)

    for k in range(nz + 2):
        if k < nz:
            first(k)
        if 0 <= k - 1 < nz:
            second(k - 1)
        if 0 <= k - 2 < nz:
            third(k - 2)

    def drain(block, carry):
        at_x_, at_y_, at_z_ = lax.rem(block, nx), lax.rem(block // nx, ny), block // (nx * ny)
        for half in range(len(halves)):
            column = (at_x_ == x) & (at_y_ == y)

            @pl.when(needed(block, half, used))
            def _():
                @pl.when(column & (at_z_ <= z) & (z + 1 < nz))
                def _():
                    copy(block, half, {SEC: other}, 0).wait_send()

                @pl.when(column & (at_z_ >= z) & (z > 0))
                def _():
                    copy(block, half, {SEC: other}, 1).wait_send()

                single = len(halves) == 1
                sent_x = (column if half == 0 else at_x_ == x)
                sent_y = (at_y_ == y) if half == 0 else column

                @pl.when(sent_x)
                def _():
                    for step in range(1, nx):
                        copy(block, half, {SEC: other}, 1 + step).wait_send()

                @pl.when(sent_y)
                def _():
                    for step in range(1, ny):
                        copy(block, half, {SEC: other}, nx + step).wait_send()

                copy(block, half, {SEC: other}, nx + ny).wait_send()

            @pl.when(needed(block, half, used_other))
            def _():
                copy(block, half, {SEC: other}, 0, False, True).wait_recv()

        return carry

    lax.fori_loop(0, replicas, drain, 0)
    own.wait()
    for step in range(1, replicas):
        count_copy(step).wait()
    cnts_ref[me] = cnt_ref[...]
    vec2_ref[section] = vec_ref[...]
    fac2_ref[section] = fac_ref[...]
    side(vec_ref, vec2_ref, 0).wait()
    side(fac_ref, fac2_ref, 1).wait()


def update_body(master_ref, moment_ref, approx_ref, scale_ref, master_out, low_out, moment_out):
    moment = moment_decay * moment_ref[...] + scale_ref[...] * approx_ref[...].reshape(moment_ref.shape)
    moment_out[...] = moment
    master = master_ref[...] - learning_rate() * moment
    master_out[...] = master
    low_out[...] = master.astype(bf16)


def update(master, moment, approx, scale):
    full = pl.BlockSpec(memory_space=pltpu.VMEM)
    return pl.pallas_call(
        update_body,
        in_specs=[full] * 4,
        out_specs=[full] * 3,
        out_shape=[
            jax.ShapeDtypeStruct(master.shape, f32), jax.ShapeDtypeStruct(master.shape, bf16),
            jax.ShapeDtypeStruct(master.shape, f32),
        ],
        name="update",
    )(master, moment, approx, scale)


def cast_body(src_ref, out_ref):
    out_ref[...] = src_ref[...].reshape(out_ref.shape).astype(bf16)


def cast_shard(master, size):
    full = pl.BlockSpec(memory_space=pltpu.VMEM)
    return pl.pallas_call(
        cast_body, in_specs=[full], out_specs=full, out_shape=jax.ShapeDtypeStruct((size, LANES), bf16), name="cast"
    )(master)


def gather(low, cnt, vec, fac, replicas):
    size = low.shape[0]
    vmem = pl.BlockSpec(memory_space=pltpu.VMEM)
    nz, ny, nx = grid_of(replicas)
    dma = pltpu.SemaphoreType.DMA
    return pl.pallas_call(
        functools.partial(gather_body, replicas=replicas, size=size),
        in_specs=[vmem] * 4,
        out_specs=[pl.BlockSpec(memory_space=pl.ANY), vmem, vmem, vmem],
        out_shape=[
            jax.ShapeDtypeStruct((2 * replicas, size, LANES), bf16),
            jax.ShapeDtypeStruct((replicas,) + cnt.shape, f32),
            jax.ShapeDtypeStruct((2,) + vec.shape, f32),
            jax.ShapeDtypeStruct((2,) + fac.shape, f32),
        ],
        scratch_shapes=[
            dma((replicas, 2, nx + ny + 1)), dma((replicas, 2)), dma((replicas, 2)),
            dma((replicas,)), dma((replicas,)), dma((2,)), dma((2,)), dma(()),
        ],
        compiler_params=pltpu.CompilerParams(collective_id=2, has_side_effects=True),
        name="gather",
    )(low, cnt, vec, fac)


def sum_body(*refs, replicas, n_enc, n_dec):
    n = n_enc + n_dec
    sum_run(*refs[:2], refs[2 : 2 + n], refs[2 + n], refs[3 + n : 3 + 2 * n], *refs[3 + 2 * n :], replicas=replicas, n_enc=n_enc)


def sum_run(
    part_ref, extra_ref, given, total_ref, taken, mine, came, slots, seg, swap_send, swap_recv, send_a, recv_a, send_b, recv_b,
    give_sem, take_sem, *, replicas, n_enc,
):
    section, me = lax.axis_index(SEC), lax.axis_index(DP)
    other = 1 - section
    rows = part_ref.shape[1]
    size = rows // replicas
    meet(replicas)

    def rows_of(index):
        return pl.ds(pl.multiple_of(index * size, 8), size)

    swap = pltpu.make_async_remote_copy(
        src_ref=part_ref.at[other], dst_ref=came, send_sem=swap_send.at[0], recv_sem=swap_recv.at[0],
        device_id={SEC: other}, device_id_type=MESH,
    )
    swap.start()
    mine[...] = part_ref[section] + extra_ref[...]
    swap.wait()

    def give(i):
        return pltpu.make_async_remote_copy(
            src_ref=given[i], dst_ref=taken[i], send_sem=give_sem.at[i], recv_sem=take_sem.at[i],
            device_id={SEC: other}, device_id_type=MESH,
        )

    n = len(given)
    for i in range(n):

        @pl.when(section == (1 if i < n_enc else 0))
        def _():
            give(i).start()

    mine[...] = mine[...] + came[...]

    def scatter(step):
        peer = lax.rem(me + step, replicas)
        return pltpu.make_async_remote_copy(
            src_ref=mine.at[rows_of(peer)], dst_ref=slots.at[step], send_sem=send_a.at[step],
            recv_sem=recv_a.at[step], device_id={DP: peer}, device_id_type=MESH,
        )

    def spread(step):
        peer = lax.rem(me + step, replicas)
        return pltpu.make_async_remote_copy(
            src_ref=seg, dst_ref=total_ref.at[section, rows_of(me)], send_sem=send_b.at[step],
            recv_sem=recv_b.at[step], device_id={DP: peer}, device_id_type=MESH,
        )

    for step in range(1, replicas):
        scatter(step).start()
    total = mine[rows_of(me), :]
    for step in range(1, replicas):
        scatter(step).wait_recv()
        total = total + slots[step]
    seg[...] = total
    for step in range(1, replicas):
        spread(step).start()
    total_ref[section, rows_of(me)] = total
    for step in range(1, replicas):
        scatter(step).wait_send()
        spread(step).wait()
    back = pltpu.make_async_remote_copy(
        src_ref=total_ref.at[section], dst_ref=total_ref.at[section], send_sem=swap_send.at[1],
        recv_sem=swap_recv.at[1], device_id={SEC: other}, device_id_type=MESH,
    )
    back.start()
    back.wait()
    for i in range(n):

        @pl.when(section == (1 if i < n_enc else 0))
        def _():
            give(i).wait_send()

        @pl.when(section == (0 if i < n_enc else 1))
        def _():
            give(i).wait_recv()


def all_sum(part, extra, replicas, collective_id, enc=(), dec=()):
    rows = part.shape[1]
    vmem = pl.BlockSpec(memory_space=pltpu.VMEM)
    dma = pltpu.SemaphoreType.DMA
    size = rows // replicas
    given = list(enc) + list(dec)
    n = len(given)
    anywhere = pl.BlockSpec(memory_space=pl.ANY)
    outs = pl.pallas_call(
        functools.partial(sum_body, replicas=replicas, n_enc=len(enc), n_dec=len(dec)),
        in_specs=[vmem, vmem] + [anywhere] * n,
        out_specs=[vmem] + [anywhere] * n,
        out_shape=[jax.ShapeDtypeStruct(part.shape, f32)] + [jax.ShapeDtypeStruct(x.shape, x.dtype) for x in given],
        scratch_shapes=[
            pltpu.VMEM((rows, LANES), f32), pltpu.VMEM((rows, LANES), f32),
            pltpu.VMEM((replicas, size, LANES), f32), pltpu.VMEM((size, LANES), f32),
            dma((2,)), dma((2,)), dma((replicas,)), dma((replicas,)), dma((replicas,)), dma((replicas,)),
            dma((max(n, 1),)), dma((max(n, 1),)),
        ],
        compiler_params=pltpu.CompilerParams(collective_id=collective_id, has_side_effects=True),
        name="all_sum",
    )(part, extra, *given)
    return outs[0], outs[1 : 1 + len(enc)], outs[1 + len(enc) :]


def local(pixels, visible, masked, loss_mask, master, momentum, vectors, vec_moment, factors, errors):
    sec = lax.axis_index(SEC)
    replicas = lax.axis_size(DP)
    replica_id = lax.axis_index(DP)

    replicas_n = replicas
    shard_len = master.shape[1]
    size = shard_len // LANES
    gain = float(replicas)

    count_tile = jnp.full((RANK, LANES), jnp.sum(loss_mask).astype(f32))
    vec_tile = jnp.pad(vectors[0], (0, VEC_TILES * RANK * LANES - VLEN)).reshape(-1, LANES)
    flat_both, counts, vec_both, fac_both = gather(
        cast_shard(master, size), count_tile, vec_tile, factors[0], replicas
    )
    low_both = flat_both.reshape(-1, LANES)
    count = jnp.sum(counts[:, 0, 0])

    vis = lax.dynamic_index_in_dim(visible, sec, 0, keepdims=False)
    mas = lax.dynamic_index_in_dim(masked, sec, 0, keepdims=False)
    mask_row = lax.dynamic_index_in_dim(loss_mask, sec, 0, keepdims=False).astype(f32)
    order = jnp.concatenate([vis, mas])
    pix = lax.dynamic_index_in_dim(pixels, sec, 0, keepdims=False)
    pick = (order[:, None] == jnp.arange(SEQ, dtype=jnp.int32)[None, :]).astype(bf16)
    pix_order = nn(pick, pix).astype(bf16)
    pix_vis = pix_order[:VIS]
    target = pix_order[VIS:]
    place = order[:, None]
    mask_col = mask_row[:, None]
    tail_row = ROW_PAD // LANES * RANK
    tail_rows = (VEC_TILES + 1) * RANK
    left_rows = sum_rows(replicas, ROW_PAD // LANES + VEC_TILES + 1)
    right_rows = sum_rows(replicas, max(COL_WIDTHS) // LANES)

    def errs_for(section):
        def run():
            buf = None
            lefts = []
            start = 0
            col_at = 0
            for rows_n, cols_n in section_shapes(section):
                buf, left = err_prep(errors, factors[0][:, col_at : col_at + cols_n], start, rows_n, cols_n, buf)
                lefts.append(left)
                start += rows_n * cols_n
                col_at += cols_n
            done = sum(left.shape[0] for left in lefts)
            lefts.append(jnp.zeros((left_rows - done, LANES), f32))
            return buf, jnp.concatenate(lefts)

        return run

    err_stack, err_lefts = lax.cond(sec == 0, errs_for(0), errs_for(1))

    kept, enc = encode(low_both, pix_vis, place[:VIS], angle_tables(DE), vec_both)
    given, grad_coded, sums_e, part_d = decode(
        low_both, kept[K_CODED], place, angle_tables(DD), vec_both, target, mask_col, count.reshape(1, 1), fac_both, tail_row, gain, left_rows,
    )
    back, part_e = encode_back(kept, enc, grad_coded, sums_e, vec_both, pix_vis, fac_both, tail_row, gain, left_rows)
    pairs_e = [
        (kept[K_NORMED], back[K_B_QKV]), (kept[K_ATTENDED], back[K_B_PROJ]), (kept[K_SECOND], back[K_B_UP]),
        (kept[K_ACTIVE], back[K_B_DOWN]), (pix_vis, back[K_START]),
    ]
    pairs_d = [
        (given[K_NORMED], given[K_B_QKV]), (given[K_ATTENDED], given[K_B_PROJ]), (given[K_SECOND], given[K_B_UP]),
        (given[K_ACTIVE], given[K_B_DOWN]), (given[K_B_PRED], given[K_FINAL]), (given[K_SENT], given[K_FIRST]),
    ]
    pairs = pairs_e + pairs_d
    n_enc = len(pairs_e)
    flat_e = [x for pair in pairs_e for x in pair]
    flat_d = [x for pair in pairs_d for x in pair]
    left_part = jnp.stack([part_e, part_d])
    early_e = [5, 6]
    late_e = [i for i in range(len(flat_e)) if i not in early_e]
    early_d = [5, 6]
    late_d = [i for i in range(len(flat_d)) if i not in early_d]
    left_sum, first_e, first_d = all_sum(
        left_part, err_lefts, replicas, 3, [flat_e[i] for i in early_e], [flat_d[i] for i in early_d]
    )
    vec_sum = left_sum[:, tail_row : tail_row + VEC_TILES * RANK]
    loss_sum = left_sum[1, tail_row + VEC_TILES * RANK, 0]

    ortho, right_part, err_rights = rights(
        left_sum, err_stack, [a for a, b in pairs], [b for a, b in pairs], 1.0 / replicas, gain, right_rows
    )
    sums, second_e, second_d = all_sum(
        right_part, err_rights, replicas, 4, [flat_e[i] for i in late_e], [flat_d[i] for i in late_d]
    )
    other_e = [x for i, x in sorted([*zip(early_e, first_e), *zip(late_e, second_e)], key=lambda entry: entry[0])]
    other_d = [x for i, x in sorted([*zip(early_d, first_d), *zip(late_d, second_d)], key=lambda entry: entry[0])]
    right_both, norm_row = final_right(sums, ortho, vec_sum, factors.shape[2], 1.0 / replicas)
    norm = norm_row[0, 0]
    scale = jnp.minimum(1.0, clip_limit / (norm + 1e-06))

    def finish_for(section):
        def run():
            mine = pairs_e if section == 0 else pairs_d
            flat = other_e if section == 0 else other_d
            theirs = [(flat[2 * i], flat[2 * i + 1]) for i in range(len(mine))]
            bufs = None
            start = 0
            base = 0 if section == 0 else n_enc
            for i, (rows_n, cols_n) in enumerate(section_shapes(section)):
                bufs = finish(
                    me_row, mine[i], theirs[i], err_stack, ortho, right_both, section,
                    ROW_SPANS[base + i][1], COL_SPANS[base + i][1], start, gain, shard_len, bufs,
                )
                start += rows_n * cols_n
            if start < FLAT:
                bufs = [finish_tail(errors, start, bufs[0]), bufs[1]]
            return bufs[0], bufs[1]

        return run

    me_row = replica_id.astype(jnp.int32).reshape(1)
    new_errors, approx = lax.cond(sec == 0, finish_for(0), finish_for(1))
    own_part = lax.dynamic_slice_in_dim(approx, replica_id * size, size)
    used = jnp.where(sec == 0, *[sum(rows_n * cols_n for rows_n, cols_n in section_shapes(s)) // LANES for s in range(2)])
    inside = replica_id * size + lax.broadcasted_iota(jnp.int32, (size, 1), 0) < used
    own_part = jnp.where(inside, own_part, 0.0)
    rate = learning_rate()
    new_master, new_low, new_moment = update(master, momentum, own_part, scale.reshape(1, 1))
    vec_own = lax.dynamic_index_in_dim(vec_sum, sec, 0, keepdims=False).reshape(-1)[:VLEN]
    new_vm = moment_decay * vec_moment[0] + scale * vec_own
    new_vectors = vectors[0] - rate * new_vm
    new_factors = lax.dynamic_index_in_dim(right_both, sec, 0, keepdims=False)
    return (
        new_master,
        new_low,
        new_moment,
        new_vectors[None],
        new_vm[None],
        new_factors[None],
        new_errors,
        loss_sum.reshape(1),
        norm.reshape(1),
    )


def solution(mesh):
    return jax.shard_map(
        local,
        mesh=mesh,
        in_specs=(
            P(DP, None, None),
            P(DP, None),
            P(DP, None),
            P(DP, None),
            P(SEC, DP),
            P(SEC, DP),
            P(SEC, None),
            P(SEC, None),
            P(SEC, None, None),
            P(SEC, DP, None),
        ),
        out_specs=(
            P(SEC, DP),
            P(SEC, DP),
            P(SEC, DP),
            P(SEC, None),
            P(SEC, None),
            P(SEC, None, None),
            P(SEC, DP, None),
            P(),
            P(),
        ),
        check_vma=False,
    )
```

```python
import functools
import math

import jax
import jax.numpy as jnp
import numpy as np
from jax import lax
from jax.experimental import pallas as pl
from jax.experimental.pallas import tpu as pltpu
from jax.sharding import PartitionSpec as P

DE = 768
FFE = 3072
HEADS_ENC = 12
DD = 512
FFD = 2048
HEADS_DEC = 16
PATCH = 192
PATCH_PAD = 256
RANK = 8
SEQ = 1024
VIS = 256
FLAT = 7225344
VLEN = 11520

(K_TOKENS, K_NORMED, K_JOINED, K_OUT, K_LSE, K_ATTENDED, K_MIDDLE, K_SECOND, K_ACTIVE, K_SLOPE, K_CODED, K_B_QKV, K_B_PROJ, K_B_UP, K_B_DOWN, K_B_PRED, K_FINAL, K_SENT, K_FIRST, K_GRAD, K_ATT, K_DK, K_DV, K_SUMS, K_BIAS, K_START) = range(26)

f32 = jnp.float32
bf16 = jnp.bfloat16
clip_limit = 0.0001
moment_decay = 0.9
rate_base = 0.5
LANES = 128
SEC, DP = "section", "dp"
STEP = 32
DEC_ROWS = 512
CHUNK = 256
BIG = 66000000


def nn(left, right):
    return lax.dot_general(left, right, (((1,), (0,)), ((), ())), preferred_element_type=f32)


def nt(left, right):
    return lax.dot_general(left, right, (((1,), (1,)), ((), ())), preferred_element_type=f32)


def tn(left, right):
    return lax.dot_general(left, right, (((0,), (0,)), ((), ())), preferred_element_type=f32)


def split3(value):
    high = value.astype(bf16)
    rest = value - high.astype(f32)
    middle = rest.astype(bf16)
    return jnp.concatenate([high, middle, (rest - middle.astype(f32)).astype(bf16)], axis=0)


def join3(value):
    return value[:RANK] + value[RANK : 2 * RANK] + value[2 * RANK :]


def norm_parts(tokens):
    centred = tokens - jnp.mean(tokens, axis=-1, keepdims=True)
    spread = lax.rsqrt(jnp.mean(centred * centred, axis=-1, keepdims=True) + 1e-06)
    return centred * spread, spread


def norm_back(grad, hat, spread, gain):
    inner = grad * gain
    return spread * (
        inner - jnp.mean(inner, axis=-1, keepdims=True) - hat * jnp.mean(inner * hat, axis=-1, keepdims=True)
    )


def column_sum(value):
    return jnp.sum(value.astype(f32), axis=0, keepdims=True)


def angle_tables(width):
    column = np.arange(width)
    freqs = np.exp(-(column // 2 * 2) / width * math.log(10000.0))
    coarse = (np.arange(0, SEQ, STEP)[:, None] * freqs).astype(np.float64)
    fine = np.arange(STEP)[:, None] * freqs + (column % 2) * (math.pi / 2)
    return jnp.asarray(np.stack([np.sin(coarse), np.cos(coarse), np.cos(fine), np.sin(fine)]), f32)


def positions_of(place, tables):
    column = lax.broadcasted_iota(jnp.int32, (1, STEP), 1)
    coarse = (place // STEP == column).astype(bf16)
    fine = (place % STEP == column).astype(bf16)

    def take(pick, table):
        high = table.astype(bf16)
        rest = table - high.astype(f32)
        middle = rest.astype(bf16)
        low = (rest - middle.astype(f32)).astype(bf16)
        return nn(pick, high) + nn(pick, middle) + nn(pick, low)

    return take(coarse, tables[0]) * take(fine, tables[2]) + take(coarse, tables[1]) * take(fine, tables[3])


def section_shapes(section):
    if section == 0:
        return [(DE, 3 * DE), (DE, DE), (DE, FFE), (FFE, DE), (PATCH, DE)]
    return [(DD, 3 * DD), (DD, DD), (DD, FFD), (FFD, DD), (PATCH, DD), (DE, DD)]


def learning_rate():
    return rate_base * math.sqrt(2.0 * (FLAT + VLEN) / DD) / clip_limit


def head_mask(head, size):
    lane = lax.broadcasted_iota(jnp.int32, (1, LANES), 1)
    return (lane // size == head).astype(bf16)


def attend_body(q_ref, k_ref, v_ref, o_ref, lse_ref, *, size, rows_q):
    seq = k_ref.shape[0]
    scale = size ** (-0.5)
    fold = scale * math.log2(math.e)

    def one(step, carry):
        at = pl.ds(pl.multiple_of(step * rows_q, rows_q), rows_q)
        queries = q_ref[at, :]
        total = jnp.zeros((rows_q, LANES), f32)
        for head in range(LANES // size):
            mask = head_mask(head, size)
            scores = nt(k_ref[...], queries * mask)
            peak = jnp.max(scores, axis=0, keepdims=True) * fold
            power = jnp.exp2(scores * fold - peak)
            mass = jnp.sum(power, axis=0, keepdims=True)
            share = jnp.transpose(jnp.broadcast_to(1.0 / mass, (8, rows_q)))[:, :1]
            total = total + tn(power.astype(bf16), v_ref[...] * mask) * share
            lse_ref[0, head : head + 1, at] = peak + jnp.log2(mass)
        o_ref[at, :] = total
        return carry

    lax.fori_loop(0, seq // rows_q, one, 0)


def attend_back_body(q_ref, k_ref, v_ref, do_ref, o_ref, lse_ref, dq_ref, dk_ref, dv_ref, dk_sum, dv_sum, *, size, rows_q):
    seq = k_ref.shape[0]
    scale = size ** (-0.5)
    fold = scale * math.log2(math.e)
    dk_sum[...] = jnp.zeros_like(dk_sum)
    dv_sum[...] = jnp.zeros_like(dv_sum)

    def one(step, carry):
        at = pl.ds(pl.multiple_of(step * rows_q, rows_q), rows_q)
        queries = q_ref[at, :]
        grads = do_ref[at, :]
        prod = grads.astype(f32) * o_ref[at, :]
        total = jnp.zeros((rows_q, LANES), f32)
        high = prod.astype(bf16)
        rest = prod - high.astype(f32)
        middle = rest.astype(bf16)
        for head in range(LANES // size):
            mask = head_mask(head, size)
            wide = jnp.broadcast_to(mask, (16, LANES))
            delta = (nt(wide, high) + nt(wide, middle))[0:1]
            q_one = queries * mask
            g_one = grads * mask
            scores = nt(k_ref[...], q_one)
            probs = jnp.exp2(scores * fold - lse_ref[0, head : head + 1, at])
            slope = nt(v_ref[...], g_one)
            grad_s = (probs * (slope - delta)).astype(bf16)
            dv_sum[...] += nn(probs.astype(bf16), g_one)
            dk_sum[...] += nn(grad_s, q_one)
            total = total + tn(grad_s, k_ref[...] * mask)
        dq_ref[at, :] = (total * scale).astype(bf16)
        return carry

    lax.fori_loop(0, seq // rows_q, one, 0)
    dk_ref[...] = (dk_sum[...] * scale).astype(bf16)
    dv_ref[...] = dv_sum[...].astype(bf16)


def rows_at(step, count):
    return pl.ds(pl.multiple_of(step * count, count), count)


def cols_at(step, count=LANES):
    return pl.ds(pl.multiple_of(step * count, count), count)


def shape_of(rows, cols, dtype=f32):
    return jax.ShapeDtypeStruct((rows, cols), dtype)


def loop(count, body):
    def one(step, carry):
        body(step)
        return carry

    lax.fori_loop(0, count, one, 0)


def over_blocks(seq, rows, body, *refs):
    loop(seq // rows, lambda step: body(*[ref.at[rows_at(step, rows)] for ref in refs]))


def open_stage(tok_ref, normed_ref, joined_ref, vec_ref, w_ref):
    width = tok_ref.shape[1]
    hat, unused = norm_parts(tok_ref[...])
    normed = (hat * vec_ref[0:1] + vec_ref[1:2]).astype(bf16)
    normed_ref[...] = normed
    for part, bias in ((0, vec_ref[6:7]), (1, None), (2, vec_ref[7:8])):
        cols = slice(part * width, (part + 1) * width)
        value = nn(normed, w_ref[:, cols])
        joined_ref[:, cols] = (value if bias is None else value + bias).astype(bf16)


def attend_stage(joined, out, lse, size):
    seq, width = out.shape
    groups = width // LANES

    def one(group):
        attend_body(
            joined.at[:, cols_at(group)], joined.at[:, cols_at(groups + group)],
            joined.at[:, cols_at(2 * groups + group)], out.at[:, cols_at(group)], lse.at[pl.ds(group, 1)],
            size=size, rows_q=min(512, seq),
        )

    loop(groups, one)


def attend_back_stage(joined, grad_att, out, lse, b_qkv, dk_sum, dv_sum, size):
    seq, width = out.shape
    groups = width // LANES

    def one(group):
        here = [cols_at(part * groups + group) for part in range(3)]
        attend_back_body(
            *[joined.at[:, cols] for cols in here], grad_att.at[:, here[0]], out.at[:, here[0]],
            lse.at[pl.ds(group, 1)], *[b_qkv.at[:, cols] for cols in here], dk_sum, dv_sum,
            size=size, rows_q=min(512, seq),
        )

    loop(groups, one)


def close_stage(
    tok_ref, o_ref, att_ref, mid_ref, sec_ref, act_ref, slope_ref, out_ref, vec_ref, bias_ref, wo_ref, w1_ref, w2_ref
):
    attended = o_ref[...].astype(bf16)
    att_ref[...] = attended
    middle = tok_ref[...] + nn(attended, wo_ref[...]) + vec_ref[8:9]
    mid_ref[...] = middle
    hat, unused = norm_parts(middle)
    sec_ref[...] = (hat * vec_ref[2:3] + vec_ref[3:4]).astype(bf16)
    out_ref[...] = middle + vec_ref[9:10]

    def one(step):
        cols = cols_at(step, CHUNK)
        hidden = nn(sec_ref[...], w1_ref[:, cols]) + bias_ref[:, cols]
        share = 0.5 * (1.0 + lax.erf(hidden * math.sqrt(0.5)))
        active = (hidden * share).astype(bf16)
        act_ref[:, cols] = active
        slope_ref[:, cols] = share + hidden * (jnp.exp(-0.5 * hidden * hidden) * (1.0 / math.sqrt(2.0 * math.pi)))
        out_ref[...] += nn(active, w2_ref[cols, :])

    loop(w1_ref.shape[1] // CHUNK, one)


def back_up_stage(
    grad_ref, slope_ref, mid_ref, down_ref, up_ref, proj_ref, att_ref, total, vec_ref, wo_ref, w1_ref, w2_ref, sums_ref, bias_ref
):
    down = grad_ref[...].astype(bf16)
    down_ref[...] = down
    total[...] = jnp.zeros_like(total)

    def one(step):
        cols = cols_at(step, CHUNK)
        part = (nt(down_ref[...], w2_ref[cols, :]) * slope_ref[:, cols]).astype(bf16)
        up_ref[:, cols] = part
        bias_ref[:, cols] += column_sum(part)
        total[...] += nt(part, w1_ref[:, cols])

    loop(w1_ref.shape[1] // CHUNK, one)
    grad = total[...]
    hat, spread = norm_parts(mid_ref[...])
    middle = grad_ref[...] + norm_back(grad, hat, spread, vec_ref[2:3])
    grad_ref[...] = middle
    proj = middle.astype(bf16)
    proj_ref[...] = proj
    att_ref[...] = nt(proj, wo_ref[...]).astype(bf16)
    sums_ref[2:3] += column_sum(grad * hat)
    sums_ref[3:4] += column_sum(grad)
    sums_ref[8:9] += column_sum(proj)
    sums_ref[9:10] += column_sum(down)


def back_in_stage(join_ref, grad_ref, tok_ref, vec_ref, w_ref, sums_ref):
    width = tok_ref.shape[1]
    grad = nt(join_ref[...], w_ref[...])
    sums_ref[6:7] += column_sum(join_ref[:, :width])
    sums_ref[7:8] += column_sum(join_ref[:, 2 * width :])
    hat, spread = norm_parts(tok_ref[...])
    grad_ref[...] += norm_back(grad, hat, spread, vec_ref[0:1])
    sums_ref[0:1] += column_sum(grad * hat)
    sums_ref[1:2] += column_sum(grad)


def widen(flat_ref, wide, w_ref):
    rows_n, cols_n = w_ref.shape
    blocks = cols_n // LANES
    count = 64 * blocks

    def one(step):
        wide[:count] = flat_ref[rows_at(step, count), :].astype(f32)
        for block in range(blocks):
            w_ref[rows_at(step, 64), block * LANES : (block + 1) * LANES] = wide[
                pl.ds(block, 64, stride=blocks), :
            ].astype(bf16)

    loop(rows_n // 64, one)


class Weights:
    def __init__(self, flat, section, order, slots, wide, mats, sems):
        self.flat, self.slots, self.wide, self.mats, self.sems = flat, slots, wide, mats, sems
        self.order, self.shapes, self.next = order, section_shapes(section), 0
        self.base = section * (FLAT // LANES)
        for position in range(2):
            self.fetch(position).start()

    def fetch(self, position):
        index = self.order[position]
        start = self.base + sum(rows * cols for rows, cols in self.shapes[:index]) // LANES
        count = self.shapes[index][0] * self.shapes[index][1] // LANES
        return pltpu.make_async_copy(
            self.flat.at[pl.ds(start, count)], self.slots.at[position % 2, pl.ds(0, count)], self.sems.at[position]
        )

    def take(self):
        position = self.next
        self.fetch(position).wait()
        mat = self.mats[self.order[position]]
        widen(self.slots.at[position % 2], self.wide, mat)
        if position + 2 < len(self.order):
            self.fetch(position + 2).start()
        self.next += 1
        return mat


def take_rows(vec_ref, section, width, rows_ref, bias_ref, extra_ref=None):
    places = [(rows_ref, line, line * width, width) for line in range(11)]
    places.append((bias_ref, 0, 11 * width, bias_ref.shape[1]))
    if extra_ref is not None:
        places.append((extra_ref, 0, 11 * width + bias_ref.shape[1], width))
    for ref, line, offset, count in places:
        for tile in range(count // LANES):
            row = offset // LANES + tile
            ref[line : line + 1, tile * LANES : (tile + 1) * LANES] = vec_ref[section, row : row + 1]


class Copies:
    def __init__(self, sems):
        self.sems, self.made = sems, []

    def start(self, src, dst):
        copy = pltpu.make_async_copy(src, dst, self.sems.at[len(self.made)])
        copy.start()
        self.made.append(copy)
        return copy


def flat_count(section):
    return max(rows * cols for rows, cols in section_shapes(section)) // LANES


ANYWHERE = pl.BlockSpec(memory_space=pl.ANY)
WHOLE = pl.BlockSpec(memory_space=pltpu.VMEM)
ENC_KEPT = [
    (K_TOKENS, (VIS, DE), f32), (K_NORMED, (VIS, DE), bf16), (K_JOINED, (VIS, 3 * DE), bf16), (K_OUT, (VIS, DE), f32),
    (K_LSE, (DE // LANES, 2, VIS), f32), (K_ATTENDED, (VIS, DE), bf16), (K_MIDDLE, (VIS, DE), f32),
    (K_SECOND, (VIS, DE), bf16), (K_ACTIVE, (VIS, FFE), bf16), (K_SLOPE, (VIS, FFE), f32), (K_CODED, (VIS, DE), f32),
]


def encode_body(flat, pix, place, table, vec_ref, *rest):
    kept_n, mats_n = len(ENC_KEPT), len(section_shapes(0))
    kept_out, mats_out = rest[:kept_n], rest[kept_n : kept_n + mats_n]
    rest = rest[kept_n + mats_n :]
    kept = dict(zip([name for name, shape, kind in ENC_KEPT], rest[:kept_n]))
    mats = rest[kept_n : kept_n + mats_n]
    slots, wide, vecs, bias, in_sems, out_sems = rest[kept_n + mats_n :]
    take_rows(vec_ref, 0, DE, vecs, bias)
    weights = Weights(flat, 0, [4, 0, 1, 2, 3], slots, wide, mats, in_sems)
    copies = Copies(out_sems)

    def give(*names):
        for name in names:
            which = [entry[0] for entry in ENC_KEPT].index(name)
            copies.start(kept[name], kept_out[which])

    def take(index):
        mat = weights.take()
        copies.start(mat, mats_out[index])
        return mat

    kept[K_TOKENS][...] = positions_of(place[...], table) + vecs[10:11] + nn(pix[:, :PATCH], take(4)[...])
    open_stage(kept[K_TOKENS], kept[K_NORMED], kept[K_JOINED], vecs, take(0))
    give(K_TOKENS, K_NORMED, K_JOINED)
    attend_stage(kept[K_JOINED], kept[K_OUT], kept[K_LSE], DE // HEADS_ENC)
    give(K_OUT, K_LSE)
    wo, w1, w2 = take(1), take(2), take(3)
    keys = [K_TOKENS, K_OUT, K_ATTENDED, K_MIDDLE, K_SECOND, K_ACTIVE, K_SLOPE, K_CODED]
    close_stage(*[kept[name] for name in keys], vecs, bias, wo, w1, w2)
    give(K_ATTENDED, K_MIDDLE, K_SECOND, K_ACTIVE, K_SLOPE, K_CODED)
    for copy in copies.made:
        copy.wait()


def encode(flat, pix, place, table, vecs):
    mats = section_shapes(0)
    dma = pltpu.SemaphoreType.DMA
    outs = pl.pallas_call(
        encode_body,
        in_specs=[ANYWHERE] + [WHOLE] * 4,
        out_specs=[ANYWHERE] * (len(ENC_KEPT) + len(mats)),
        out_shape=[jax.ShapeDtypeStruct(shape, kind) for name, shape, kind in ENC_KEPT] + [shape_of(*shape, bf16) for shape in mats],
        scratch_shapes=[pltpu.VMEM(shape, kind) for name, shape, kind in ENC_KEPT]
        + [pltpu.VMEM(shape, bf16) for shape in mats]
        + [
            pltpu.VMEM((2, flat_count(0), LANES), bf16), pltpu.VMEM((64 * FFE // LANES, LANES), f32),
            pltpu.VMEM((16, DE), f32), pltpu.VMEM((1, FFE), f32), dma((len(mats),)), dma((len(ENC_KEPT) + len(mats),)),
        ],
        compiler_params=pltpu.CompilerParams(vmem_limit_bytes=BIG),
        name="encode",
    )(flat, pix, place, table, vecs)
    return dict(zip([name for name, shape, kind in ENC_KEPT], outs)), outs[len(ENC_KEPT) :]


def put_vec(part_ref, tail_row, offset, value):
    for tile in range(value.shape[1] // LANES):
        row = tail_row + offset // LANES + tile
        part_ref[row : row + 1] = value[:, tile * LANES : (tile + 1) * LANES]


def put_left(part_ref, section, index, factor_ref, u_ref, v_ref, gain):
    base = len(section_shapes(0)) * section + index
    unused, start, width = COL_SPANS[base]
    part = join3(nt(split3(factor_ref[section, :, start : start + width]), u_ref[...]))
    value = gain * join3(nn(split3(part), v_ref[...]))
    unused, start, width = ROW_SPANS[base]
    for tile in range(tiles_of(width)):
        here = min(LANES, width - tile * LANES)
        row = (start // LANES + tile) * RANK
        part_ref[row : row + RANK, :here] = value[:, tile * LANES : tile * LANES + here]


DEC_GIVEN = [
    (K_NORMED, (SEQ, DD), bf16), (K_B_QKV, (SEQ, 3 * DD), bf16), (K_ATTENDED, (SEQ, DD), bf16), (K_B_PROJ, (SEQ, DD), bf16),
    (K_SECOND, (SEQ, DD), bf16), (K_B_UP, (SEQ, FFD), bf16), (K_ACTIVE, (SEQ, FFD), bf16), (K_B_DOWN, (SEQ, DD), bf16),
    (K_B_PRED, (SEQ - VIS, PATCH_PAD), bf16), (K_FINAL, (SEQ - VIS, DD), bf16), (K_SENT, (VIS, DE), bf16), (K_FIRST, (VIS, DD), bf16),
]
DEC_HELD = [
    (K_TOKENS, (SEQ, DD), f32), (K_JOINED, (SEQ, 3 * DD), bf16), (K_OUT, (SEQ, DD), f32), (K_LSE, (DD // LANES, 4, SEQ), f32),
    (K_MIDDLE, (SEQ, DD), f32), (K_SLOPE, (SEQ, FFD), f32), (K_GRAD, (SEQ, DD), f32), (K_ATT, (SEQ, DD), bf16),
    (K_DK, (SEQ, LANES), f32), (K_DV, (SEQ, LANES), f32), (K_SUMS, (16, DD), f32), (K_BIAS, (1, FFD), f32),
]


def decode_body(
    flat, coded, place, table, vec_ref, target, mask, count_ref, factor, *rest, tail_row, gain
):
    given_n, held_n, mats_n = len(DEC_GIVEN), len(DEC_HELD), len(section_shapes(1))
    given_out, grad_coded, sums_e, part_ref = rest[:given_n], rest[given_n], rest[given_n + 1], rest[given_n + 2]
    rest = rest[given_n + 3 :]
    have = dict(zip([name for name, shape, kind in DEC_GIVEN + DEC_HELD], rest[: given_n + held_n]))
    mats = rest[given_n + held_n : given_n + held_n + mats_n]
    slots, wide, total, vec_e, bias_e, vec_d, bias, extra, in_sems, out_sems = rest[given_n + held_n + mats_n :]
    take_rows(vec_ref, 0, DE, vec_e, bias_e)
    take_rows(vec_ref, 1, DD, vec_d, bias, extra)
    weights = Weights(flat, 1, [5, 0, 1, 2, 3, 4], slots, wide, mats, in_sems)
    copies = Copies(out_sems)
    blk = total.shape[0]
    sums, bias_sum = have[K_SUMS], have[K_BIAS]

    def give(*names):
        for name in names:
            which = [entry[0] for entry in DEC_GIVEN].index(name)
            copies.start(have[name], given_out[which])

    part_ref[...] = jnp.zeros_like(part_ref)
    sums[...] = jnp.zeros_like(sums)
    bias_sum[...] = jnp.zeros_like(bias_sum)

    w_emb = weights.take()
    hat_e, spread_e = norm_parts(coded[...])
    have[K_SENT][...] = (hat_e * vec_e[4:5] + vec_e[5:6]).astype(bf16)
    give(K_SENT)
    have[K_TOKENS][:VIS] = nn(have[K_SENT][...], w_emb[...]) + extra[...] + positions_of(place[:VIS], table)

    def fill(step):
        rows = pl.ds(pl.multiple_of(VIS + step * VIS, VIS), VIS)
        have[K_TOKENS][rows] = vec_d[10:11] + positions_of(place[rows], table)

    loop(SEQ // VIS - 1, fill)
    w_qkv = weights.take()
    over_blocks(
        SEQ, blk, lambda *refs: open_stage(*refs, vec_d, w_qkv), *[have[name] for name in (K_TOKENS, K_NORMED, K_JOINED)]
    )
    give(K_NORMED)
    attend_stage(have[K_JOINED], have[K_OUT], have[K_LSE], DD // HEADS_DEC)
    wo, w1, w2 = weights.take(), weights.take(), weights.take()
    keys = [K_TOKENS, K_OUT, K_ATTENDED, K_MIDDLE, K_SECOND, K_ACTIVE, K_SLOPE, K_GRAD]
    over_blocks(SEQ, blk, lambda *refs: close_stage(*refs, vec_d, bias, wo, w1, w2), *[have[name] for name in keys])
    give(K_ATTENDED, K_SECOND, K_ACTIVE)

    w_head = weights.take()
    count = count_ref[...]

    def head(step):
        rows = pl.ds(pl.multiple_of(VIS + step * VIS, VIS), VIS)
        late = rows_at(step, VIS)
        hat, spread = norm_parts(have[K_GRAD][rows])
        final = (hat * vec_d[4:5] + vec_d[5:6]).astype(bf16)
        have[K_FINAL][late] = final
        residual = nt(final, w_head[...]) - target[late].astype(f32)
        weight = mask[late]
        loss = jnp.sum(weight * jnp.mean(residual * residual, axis=1, keepdims=True), axis=0, keepdims=True) / count
        row = tail_row + VEC_TILES * RANK
        part_ref[row : row + RANK] += jnp.broadcast_to(loss, (RANK, LANES))
        b_pred = (weight * (2.0 * residual / PATCH) / count).astype(bf16)
        have[K_B_PRED][late, :PATCH] = b_pred
        have[K_B_PRED][late, PATCH:] = jnp.zeros((VIS, PATCH_PAD - PATCH), bf16)
        grad = nn(b_pred, w_head[...])
        have[K_GRAD][rows] = norm_back(grad, hat, spread, vec_d[4:5])
        sums[4:5] += column_sum(grad * hat)
        sums[5:6] += column_sum(grad)

    loop(SEQ // VIS - 1, head)
    have[K_GRAD][:VIS] = jnp.zeros((VIS, DD), f32)
    give(K_FINAL, K_B_PRED)

    keys = [K_GRAD, K_SLOPE, K_MIDDLE, K_B_DOWN, K_B_UP, K_B_PROJ, K_ATT]
    over_blocks(
        SEQ, blk, lambda *refs: back_up_stage(*refs, total, vec_d, wo, w1, w2, sums, bias_sum), *[have[name] for name in keys]
    )
    give(K_B_DOWN, K_B_UP, K_B_PROJ)
    attend_back_stage(
        have[K_JOINED], have[K_ATT], have[K_OUT], have[K_LSE], have[K_B_QKV], have[K_DK], have[K_DV], DD // HEADS_DEC
    )
    give(K_B_QKV)
    over_blocks(
        SEQ, blk, lambda *refs: back_in_stage(*refs, vec_d, w_qkv, sums), *[have[name] for name in (K_B_QKV, K_GRAD, K_TOKENS)]
    )
    first = have[K_GRAD][:VIS].astype(bf16)
    have[K_FIRST][...] = first
    give(K_FIRST)
    sums[10:11] = column_sum(have[K_GRAD][VIS:])
    back = nt(first, w_emb[...]).astype(bf16).astype(f32)
    grad_coded[...] = norm_back(back, hat_e, spread_e, vec_e[4:5])
    sums_e[...] = jnp.zeros_like(sums_e)
    sums_e[0:1] = column_sum(back * hat_e)
    sums_e[1:2] = column_sum(back)
    for line in range(11):
        put_vec(part_ref, tail_row, line * DD, sums[line : line + 1])
    put_vec(part_ref, tail_row, 11 * DD, bias_sum[...])
    put_vec(part_ref, tail_row, 11 * DD + FFD, column_sum(first))
    pairs = [(K_NORMED, K_B_QKV), (K_ATTENDED, K_B_PROJ), (K_SECOND, K_B_UP), (K_ACTIVE, K_B_DOWN), (K_B_PRED, K_FINAL), (K_SENT, K_FIRST)]
    for index, (a, b) in enumerate(pairs):
        put_left(part_ref, 1, index, factor, have[b], have[a], gain)
    for copy in copies.made:
        copy.wait()


def decode(flat, coded, place, table, vecs, target, mask, count, factor, tail_row, gain, rows):
    mats = section_shapes(1)
    dma = pltpu.SemaphoreType.DMA
    outs = pl.pallas_call(
        functools.partial(decode_body, tail_row=tail_row, gain=gain),
        in_specs=[ANYWHERE] + [WHOLE] * 8,
        out_specs=[ANYWHERE] * len(DEC_GIVEN) + [WHOLE] * 3,
        out_shape=[jax.ShapeDtypeStruct(shape, kind) for name, shape, kind in DEC_GIVEN]
        + [shape_of(VIS, DE), shape_of(8, DE), shape_of(rows, LANES)],
        scratch_shapes=[pltpu.VMEM(shape, kind) for name, shape, kind in DEC_GIVEN + DEC_HELD]
        + [pltpu.VMEM(shape, bf16) for shape in mats]
        + [
            pltpu.VMEM((2, flat_count(1), LANES), bf16), pltpu.VMEM((64 * FFD // LANES, LANES), f32),
            pltpu.VMEM((DEC_ROWS, DD), f32), pltpu.VMEM((16, DE), f32), pltpu.VMEM((1, FFE), f32), pltpu.VMEM((16, DD), f32),
            pltpu.VMEM((1, FFD), f32), pltpu.VMEM((1, DD), f32), dma((len(mats),)), dma((len(DEC_GIVEN),)),
        ],
        compiler_params=pltpu.CompilerParams(vmem_limit_bytes=BIG),
        name="decode",
    )(flat, coded, place, table, vecs, target, mask, count, factor)
    given = dict(zip([name for name, shape, kind in DEC_GIVEN], outs))
    return given, outs[-3], outs[-2], outs[-1]


ENC_GIVEN = [
    (K_B_QKV, (VIS, 3 * DE), bf16), (K_B_PROJ, (VIS, DE), bf16), (K_B_UP, (VIS, FFE), bf16), (K_B_DOWN, (VIS, DE), bf16),
    (K_START, (VIS, DE), bf16),
]
ENC_HELD = [
    (K_ATT, (VIS, DE), bf16), (K_DK, (VIS, LANES), f32), (K_DV, (VIS, LANES), f32), (K_SUMS, (16, DE), f32), (K_BIAS, (1, FFE), f32),
]
ENC_USED = [K_SLOPE, K_MIDDLE, K_JOINED, K_OUT, K_LSE, K_TOKENS, K_SECOND, K_ACTIVE, K_ATTENDED, K_NORMED]


def encode_back_body(*refs, tail_row, gain):
    used_n, given_n, held_n = len(ENC_USED), len(ENC_GIVEN), len(ENC_HELD)
    kept_in, mats_in, refs = refs[:used_n], refs[used_n : used_n + 4], refs[used_n + 4 :]
    grad_in, sums_e, vec_ref, pix, factor = refs[:5]
    given_out, part_ref, refs = refs[5 : 5 + given_n], refs[5 + given_n], refs[6 + given_n :]
    have = dict(zip(ENC_USED, refs[:used_n]))
    refs = refs[used_n:]
    have.update(zip([name for name, shape, kind in ENC_GIVEN + ENC_HELD], refs[: given_n + held_n]))
    mats = refs[given_n + held_n : given_n + held_n + 4]
    grad, total, vecs, bias_e, in_sems, out_sems = refs[given_n + held_n + 4 :]
    reads, copies = Copies(in_sems), Copies(out_sems)
    w2 = reads.start(mats_in[3], mats[3])
    take_rows(vec_ref, 0, DE, vecs, bias_e)
    waits = {name: reads.start(src, have[name]) for name, src in list(zip(ENC_USED, kept_in))[:2]}
    w1 = reads.start(mats_in[2], mats[2])
    wo = reads.start(mats_in[1], mats[1])
    waits.update({name: reads.start(src, have[name]) for name, src in list(zip(ENC_USED, kept_in))[2:]})
    w_qkv = reads.start(mats_in[0], mats[0])
    sums, bias_sum = have[K_SUMS], have[K_BIAS]

    def give(*names):
        for name in names:
            which = [entry[0] for entry in ENC_GIVEN].index(name)
            copies.start(have[name], given_out[which])

    part_ref[...] = jnp.zeros_like(part_ref)
    sums[...] = jnp.zeros_like(sums)
    bias_sum[...] = jnp.zeros_like(bias_sum)
    sums[4:5] = sums_e[0:1]
    sums[5:6] = sums_e[1:2]
    grad[...] = grad_in[...]
    for wait in (w2, waits[K_SLOPE], waits[K_MIDDLE], w1, wo):
        wait.wait()
    back_up_stage(
        grad, have[K_SLOPE], have[K_MIDDLE], have[K_B_DOWN], have[K_B_UP], have[K_B_PROJ], have[K_ATT], total,
        vecs, mats[1], mats[2], mats[3], sums, bias_sum,
    )
    give(K_B_DOWN, K_B_UP, K_B_PROJ)
    for name in (K_JOINED, K_OUT, K_LSE, K_TOKENS):
        waits[name].wait()
    attend_back_stage(
        have[K_JOINED], have[K_ATT], have[K_OUT], have[K_LSE], have[K_B_QKV], have[K_DK], have[K_DV], DE // HEADS_ENC
    )
    give(K_B_QKV)
    w_qkv.wait()
    back_in_stage(have[K_B_QKV], grad, have[K_TOKENS], vecs, mats[0], sums)
    start = grad[...].astype(bf16)
    have[K_START][...] = start
    give(K_START)
    sums[10:11] = column_sum(start)
    for line in range(11):
        put_vec(part_ref, tail_row, line * DE, sums[line : line + 1])
    put_vec(part_ref, tail_row, 11 * DE, bias_sum[...])
    for name in (K_SECOND, K_ACTIVE, K_ATTENDED, K_NORMED):
        waits[name].wait()
    pairs = [(K_NORMED, K_B_QKV), (K_ATTENDED, K_B_PROJ), (K_SECOND, K_B_UP), (K_ACTIVE, K_B_DOWN)]
    for index, (a, b) in enumerate(pairs):
        put_left(part_ref, 0, index, factor, have[b], have[a], gain)
    put_left(part_ref, 0, 4, factor, have[K_START], pix, gain)
    for copy in copies.made:
        copy.wait()


def encode_back(kept, mats, grad_coded, sums_e, vecs, pix, factor, tail_row, gain, rows):
    shapes = {name: (shape, kind) for name, shape, kind in ENC_KEPT}
    dma = pltpu.SemaphoreType.DMA
    outs = pl.pallas_call(
        functools.partial(encode_back_body, tail_row=tail_row, gain=gain),
        in_specs=[ANYWHERE] * (len(ENC_USED) + 4) + [WHOLE] * 5,
        out_specs=[ANYWHERE] * len(ENC_GIVEN) + [WHOLE],
        out_shape=[jax.ShapeDtypeStruct(shape, kind) for name, shape, kind in ENC_GIVEN] + [shape_of(rows, LANES)],
        scratch_shapes=[pltpu.VMEM(*shapes[name]) for name in ENC_USED]
        + [pltpu.VMEM(shape, kind) for name, shape, kind in ENC_GIVEN + ENC_HELD]
        + [pltpu.VMEM(shape, bf16) for shape in section_shapes(0)[:4]]
        + [
            pltpu.VMEM((VIS, DE), f32), pltpu.VMEM((VIS, DE), f32), pltpu.VMEM((16, DE), f32), pltpu.VMEM((1, FFE), f32),
            dma((len(ENC_USED) + 4,)), dma((len(ENC_GIVEN),)),
        ],
        compiler_params=pltpu.CompilerParams(vmem_limit_bytes=BIG),
        name="encode_back",
    )(*[kept[name] for name in ENC_USED], *mats[:4], grad_coded, sums_e, vecs, pix, factor)
    return dict(zip([name for name, shape, kind in ENC_GIVEN], outs)), outs[-1]


def tiles_of(width):
    return -(-width // LANES)


def spans(which):
    at, found = [], []
    for section in range(2):
        start = 0
        for shape in section_shapes(section):
            found.append((section, start, shape[which]))
            start += tiles_of(shape[which]) * LANES
        at.append(start)
    return found, at


ROW_SPANS, ROW_WIDTHS = spans(0)
COL_SPANS, COL_WIDTHS = spans(1)
ROW_PAD = max(ROW_WIDTHS)
VEC_TILES = -(-VLEN // (RANK * LANES))


def sum_rows(replicas, tiles):
    return -(-tiles // replicas) * replicas * RANK


def put_tiles(out_ref, section, start, value):
    width = value.shape[1]
    for tile in range(tiles_of(width)):
        here = min(LANES, width - tile * LANES)
        row = (start // LANES + tile) * RANK
        out_ref[section, row : row + RANK, :here] = value[:, tile * LANES : tile * LANES + here]


def chunk_rows(rows_n, cols_n):
    if rows_n == PATCH:
        return PATCH
    return 256


TAIL_STEPS = 12
MOST = max(chunk_rows(*shape) * shape[1] for which in range(2) for shape in section_shapes(which)) // LANES


def used_length(section):
    return sum(rows_n * cols_n for rows_n, cols_n in section_shapes(section))


class Prep:
    def __init__(self, errors, factor, stack, left, whole, raw, wide, made, pieces, total, tail, raw_sem, out_sem):
        self.errors, self.factor, self.stack, self.left, self.whole = errors, factor, stack, left, whole
        self.raw, self.wide, self.made, self.pieces, self.total, self.tail = raw, wide, made, pieces, total, tail
        self.raw_sem, self.out_sem = raw_sem, out_sem

    def fetch(self, start, step, chunk):
        slot = lax.rem(chunk, 2)
        at = pl.multiple_of(start + chunk * step * LANES, 1024)
        return pltpu.make_async_copy(
            self.errors.at[:, :, pl.ds(at, step * LANES)], self.raw.at[slot, :, :, pl.ds(0, step * LANES)], self.raw_sem.at[slot]
        )

    def run(self, count, start, step, store, work):
        self.fetch(start, step, jnp.int32(0)).start()

        def one(chunk):
            slot = lax.rem(chunk, 2)

            @pl.when(chunk + 1 < count)
            def _():
                self.fetch(start, step, chunk + 1).start()

            self.fetch(start, step, chunk).wait()

            @pl.when(chunk >= 2)
            def _():
                store(chunk - 2, slot).wait()

            work(chunk, slot)
            store(chunk, slot).start()

        loop(count, one)
        for chunk in range(max(count - 2, 0), count):
            store(jnp.int32(chunk), chunk % 2).wait()

    def matrix(self, section, index):
        shapes = section_shapes(section)
        start = sum(rows_n * cols_n for rows_n, cols_n in shapes[:index])
        rows_n, cols_n = shapes[index]
        base = len(section_shapes(0)) * section + index
        blocks, rows = cols_n // LANES, chunk_rows(rows_n, cols_n)
        step, tiles = rows * blocks, tiles_of(rows)
        col_at, row_tile = COL_SPANS[base][1], ROW_SPANS[base][1] // LANES
        self.pieces[:, :cols_n] = split3(self.factor[:, col_at : col_at + cols_n])

        def store(chunk, slot):
            at = pl.multiple_of(start // LANES + chunk * step, 16)
            return pltpu.make_async_copy(
                self.made.at[slot, pl.ds(0, step)], self.stack.at[pl.ds(at, step)], self.out_sem.at[slot]
            )

        def work(chunk, slot):
            def widen_one(part):
                here = pl.ds(pl.multiple_of(part * LANES * LANES, 1024), LANES * LANES)
                self.wide[rows_at(part, LANES)] = self.raw[slot, 0, :, here].reshape(LANES, LANES).astype(f32)

            loop(step // LANES, widen_one)
            self.total[...] = jnp.zeros_like(self.total)

            def block_one(block):
                part = self.wide[pl.ds(block, rows, stride=blocks), :].astype(bf16)
                self.made[slot, rows_at(block, rows)] = part
                self.total[:rows] += nt(part, self.pieces[:, cols_at(block)])

            loop(blocks, block_one)
            value = join3(self.total[:rows].T)
            for tile in range(tiles):
                here = min(LANES, rows - tile * LANES)
                at = pl.multiple_of((row_tile + chunk * tiles + tile) * RANK, RANK)
                self.left[pl.ds(at, RANK), :here] = value[:, tile * LANES : tile * LANES + here]

        self.run(rows_n // rows, start, step, store, work)

    def rest(self, section):
        start = used_length(section)
        step = (FLAT - start) // TAIL_STEPS // LANES

        def store(chunk, slot):
            at = pl.multiple_of(start + chunk * step * LANES, 1024)
            return pltpu.make_async_copy(self.tail.at[slot], self.whole.at[:, :, pl.ds(at, step * LANES)], self.out_sem.at[slot])

        def work(chunk, slot):
            def one(part):
                here = pl.ds(pl.multiple_of(part * 4096, 1024), 4096)
                self.tail[slot, 0, :, here] = self.raw[slot, 0, :, here].astype(f32)

            loop(step * LANES // 4096, one)

        self.run(TAIL_STEPS, start, step, store, work)


def prep_scratch():
    tail = (FLAT - used_length(1)) // TAIL_STEPS
    dma = pltpu.SemaphoreType.DMA
    return [
        pltpu.VMEM((2, 1, 1, MOST * LANES), bf16), pltpu.VMEM((MOST, LANES), f32), pltpu.VMEM((2, MOST, LANES), bf16),
        pltpu.VMEM((3 * RANK, FFE), bf16), pltpu.VMEM((256, 3 * RANK), f32), pltpu.VMEM((2, 1, 1, tail), f32), dma((2,)), dma((2,)),
    ]


def ortho_stage(sum_ref, out_ref, wide, scale):
    rank_id = lax.broadcasted_iota(jnp.int32, (RANK, 1), 0)
    for section, start, width in ROW_SPANS:
        padded = tiles_of(width) * LANES
        for tile in range(padded // LANES):
            row = (start // LANES + tile) * RANK
            wide[:, tile * LANES : (tile + 1) * LANES] = sum_ref[section, row : row + RANK] * scale
        basis = wide[:, :padded]
        for column in range(RANK):
            current = basis[column : column + 1]
            current = current * lax.rsqrt(jnp.sum(current * current, axis=1, keepdims=True) + 1e-12)
            dots = jnp.sum(basis * current, axis=1, keepdims=True)
            basis = jnp.where(
                rank_id > column, basis - dots * current, jnp.where(rank_id == column, current, basis)
            )
        out_ref[section, :, start : start + padded] = basis


def err_plan(section):
    plan = []
    start = 0
    spans = [(row, col) for row, col in zip(ROW_SPANS, COL_SPANS) if row[0] == section]
    for (rows_n, cols_n), (row_span, col_span) in zip(section_shapes(section), spans):
        rows = chunk_rows(rows_n, cols_n)
        blocks = cols_n // LANES
        for chunk in range(rows_n // rows):
            plan.append((start // LANES + chunk * rows * blocks, rows, blocks, row_span[1] + chunk * rows, col_span[1], chunk))
        start += rows_n * cols_n
    return plan


def put_tiles(out_ref, row, value):
    for tile in range(value.shape[1] // LANES):
        out_ref[row + tile * RANK : row + (tile + 1) * RANK] = value[:, tile * LANES : (tile + 1) * LANES]


def rights_body(*refs, n, scale, gain):
    sum_ref, err_ref, u_in, v_in = refs[0], refs[1], refs[2 : 2 + n], refs[2 + n : 2 + 2 * n]
    ortho_ref, part_ref, extra_ref = refs[2 + 2 * n : 5 + 2 * n]
    refs = refs[5 + 2 * n :]
    u_refs, v_refs = refs[:n], refs[n : 2 * n]
    wide, ring, ring_sems, in_sems = refs[2 * n :]
    section = lax.axis_index(SEC)
    depth = ring.shape[0]
    plans = [err_plan(which) for which in range(2)]

    def fetch(plan, index):
        at, rows, blocks = plan[index][:3]
        slot = index % depth
        return pltpu.make_async_copy(
            err_ref.at[pl.ds(at, rows * blocks)], ring.at[slot, pl.ds(0, rows * blocks)], ring_sems.at[slot]
        )

    for which, plan in enumerate(plans):

        @pl.when(section == which)
        def _():
            for index in range(depth - 1):
                fetch(plan, index).start()

    reads = Copies(in_sems)
    waits = [(reads.start(u_in[i], u_refs[i]), reads.start(v_in[i], v_refs[i])) for i in range(n)]
    ortho_stage(sum_ref, ortho_ref, wide, scale)
    extra_ref[...] = jnp.zeros_like(extra_ref)
    part_ref[...] = jnp.zeros_like(part_ref)
    for which, plan in enumerate(plans):

        @pl.when(section == which)
        def _():
            for index, (at, rows, blocks, row_at, col_at, chunk) in enumerate(plan):
                if index + depth - 1 < len(plan):
                    fetch(plan, index + depth - 1).start()
                fetch(plan, index).wait()
                pieces = split3(ortho_ref[which, :, row_at : row_at + rows])
                for block in range(0, blocks, 2):
                    pair = [ring[index % depth, (block + side) * rows : (block + side + 1) * rows] for side in range(2)]
                    part = join3(nn(pieces, jnp.concatenate(pair, axis=1)))
                    row = (col_at // LANES + block) * RANK
                    if chunk == 0:
                        put_tiles(extra_ref, row, part)
                    else:
                        for side in range(2):
                            extra_ref[row + side * RANK : row + (side + 1) * RANK] += part[:, side * LANES : (side + 1) * LANES]

    for (wait_u, wait_v), u_ref, v_ref, (which, row_at, rows), (unused, col_at, cols) in zip(waits, u_refs, v_refs, ROW_SPANS, COL_SPANS):
        wait_u.wait()
        wait_v.wait()
        padded = tiles_of(rows) * LANES
        part = join3(nt(split3(ortho_ref[which, :, row_at : row_at + padded]), u_ref[...]))
        put_tiles(part_ref.at[which], col_at // LANES * RANK, gain * join3(nn(split3(part), v_ref[...])))


def rights(sums, err, us, vs, scale, gain, rows):
    n = len(us)
    most = max(chunk_rows(*shape) * shape[1] // LANES for which in range(2) for shape in section_shapes(which))
    dma = pltpu.SemaphoreType.DMA
    return pl.pallas_call(
        functools.partial(rights_body, n=n, scale=scale, gain=gain),
        in_specs=[WHOLE] + [ANYWHERE] * (2 * n + 1),
        out_specs=[WHOLE] * 3,
        out_shape=[
            jax.ShapeDtypeStruct((2, RANK, ROW_PAD), f32), jax.ShapeDtypeStruct((2, rows, LANES), f32), shape_of(rows, LANES)
        ],
        scratch_shapes=[pltpu.VMEM(x.shape, bf16) for x in [*us, *vs]]
        + [pltpu.VMEM((RANK, FFE), f32), pltpu.VMEM((4, most, LANES), bf16), dma((4,)), dma((2 * n,))],
        compiler_params=pltpu.CompilerParams(vmem_limit_bytes=BIG),
        name="rights",
    )(sums, err, *us, *vs)


def final_right_body(sum_ref, ortho_ref, vec_ref, right_ref, norm_ref, *, scale):
    squares = jnp.sum(vec_ref[...] * vec_ref[...], keepdims=True)[0]
    for (section, start, width), (unused, row_at, row_width) in zip(COL_SPANS, ROW_SPANS):
        for tile in range(width // LANES):
            row = (start // LANES + tile) * RANK
            right_ref[section, :, start + tile * LANES : start + (tile + 1) * LANES] = sum_ref[section, row : row + RANK] * scale
        o_part = ortho_ref[section, :, row_at : row_at + tiles_of(row_width) * LANES]
        r_part = right_ref[section, :, start : start + width]
        for line in range(RANK):
            gram_o = jnp.sum(o_part * o_part[line : line + 1], axis=1, keepdims=True)
            gram_r = jnp.sum(r_part * r_part[line : line + 1], axis=1, keepdims=True)
            squares = squares + jnp.sum(gram_o * gram_r, keepdims=True)
    for section in range(2):
        used = COL_WIDTHS[section]
        if used < right_ref.shape[2]:
            right_ref[section, :, used:] = jnp.zeros((RANK, right_ref.shape[2] - used), f32)
    norm_ref[...] = jnp.broadcast_to(jnp.sqrt(squares), norm_ref.shape)


def final_right(sums, ortho, vecs, cols, scale):
    full = pl.BlockSpec(memory_space=pltpu.VMEM)
    return pl.pallas_call(
        functools.partial(final_right_body, scale=scale),
        in_specs=[full] * 3,
        out_specs=[full] * 2,
        out_shape=[jax.ShapeDtypeStruct((2, RANK, cols), f32), jax.ShapeDtypeStruct((1, LANES), f32)],
        name="final_right",
    )(sums, ortho, vecs)


def overlaps(first, count, me, shard):
    return (first < (me + 1) * shard) & (first + count > me * shard)


def finish_plan(section, heights):
    plan, start = [], 0
    for index, ((rows_n, cols_n), height) in enumerate(zip(section_shapes(section), heights)):
        base = len(section_shapes(0)) * section + index
        rows = chunk_rows(rows_n, cols_n)
        plan.append((start, rows_n // rows, rows, cols_n // LANES, rows_n, height, ROW_SPANS[base][1], COL_SPANS[base][1]))
        start += rows_n * cols_n
    return plan


def finish_section(
    section, heights, pairs, err, ortho, right, err_out, app_out, a_slots, b_slots, lhs, left, ring, made, kept,
    pair_sems, ring_sem, made_sem, kept_sem, *, gain, shard,
):
    plan = finish_plan(section, heights)
    offsets = [sum(entry[1] for entry in plan[:index]) for index in range(len(plan) + 1)]
    flat_plan = [(index, chunk) for index, entry in enumerate(plan) for chunk in range(entry[1])]
    me = lax.axis_index(DP)

    def load(index):
        height, rows_n, cols_n = plan[index][5], tiles_of(plan[index][4]) * LANES, plan[index][3] * LANES
        slot, copies = index % 2, []
        for sample in range(2):
            for side, (slots, width) in enumerate(((a_slots, rows_n), (b_slots, cols_n))):
                copies.append(pltpu.make_async_copy(
                    pairs[sample][2 * index + side],
                    slots.at[slot, pl.ds(sample * height, height), pl.ds(0, width)], pair_sems.at[slot, 2 * sample + side],
                ))
        return copies

    def fetch(index, chunk):
        start, unused, rows, blocks = plan[index][:4]
        slot = lax.rem(offsets[index] + chunk, 2)
        at = pl.multiple_of(start // LANES + chunk * rows * blocks, 16)
        return pltpu.make_async_copy(
            err.at[pl.ds(at, rows * blocks)], ring.at[slot, pl.ds(0, rows * blocks)], ring_sem.at[slot]
        )

    def store(index, chunk):
        start, unused, rows, blocks = plan[index][:4]
        slot, count = lax.rem(offsets[index] + chunk, 2), rows * blocks * LANES
        at = pl.multiple_of(start + chunk * count, 1024)
        return pltpu.make_async_copy(
            made.at[slot, :, :, pl.ds(0, count)], err_out.at[:, :, pl.ds(at, count)], made_sem.at[slot]
        )

    for copy in load(0):
        copy.start()
    fetch(0, jnp.int32(0)).start()
    for index, (start, count, rows, blocks, rows_n, height, row_at, col_at) in enumerate(plan):
        for copy in load(index):
            copy.wait()
        if index + 1 < len(plan):
            for copy in load(index + 1):
                copy.start()
        pair_slot, step, wide_rows = index % 2, rows * blocks, tiles_of(rows) * LANES

        def one(chunk):
            slot = lax.rem(offsets[index] + chunk, 2)

            @pl.when(chunk + 1 < count)
            def _():
                fetch(index, chunk + 1).start()

            if index + 1 < len(plan):

                @pl.when(chunk + 1 == count)
                def _():
                    fetch(index + 1, jnp.int32(0)).start()

            o_part = ortho[section, :, pl.ds(pl.multiple_of(row_at + chunk * wide_rows, LANES), wide_rows)]
            o_high = o_part.astype(bf16)
            o_low = (o_part - o_high.astype(f32)).astype(bf16)
            left[:wide_rows] = jnp.concatenate([o_high, o_low, o_high], axis=0).T

            def turn(part):
                lhs[:, cols_at(part, 256)] = a_slots[pair_slot, rows_at(part, 256), cols_at(chunk, 256)].T

            loop(2 * height // 256, turn)
            fetch(index, chunk).wait()
            for back in range(2):
                before = offsets[index] + back - 2
                if before >= 0 and back < count:
                    old_index, old_chunk = flat_plan[before]

                    @pl.when(chunk == back)
                    def _():
                        store(old_index, jnp.int32(old_chunk)).wait()

            @pl.when(chunk >= 2)
            def _():
                store(index, chunk - 2).wait()

            first = start + chunk * step * LANES
            keep = overlaps(first, step * LANES, me, shard)
            lines = made.at[slot, 0, :, pl.ds(0, step * LANES)].reshape(step, LANES)

            def pair_one(pair):
                cols = cols_at(pair, 2 * LANES)
                r_part = right[section, :, pl.ds(pl.multiple_of(col_at + pair * 2 * LANES, LANES), 2 * LANES)]
                r_high = r_part.astype(bf16)
                r_low = (r_part - r_high.astype(f32)).astype(bf16)
                approx = nn(left[:rows], jnp.concatenate([r_high, r_high, r_low], axis=0))
                grad = nn(lhs[:rows, : 2 * height], b_slots[pair_slot, : 2 * height, cols])
                for side in range(2):
                    half = slice(side * LANES, (side + 1) * LANES)
                    block = 2 * pair + side
                    given = ring[slot, pl.ds(pl.multiple_of(block * rows, 16), rows)].astype(f32)
                    lines[pl.ds(block, rows, stride=blocks), :] = (gain * grad[:, half] + given) - approx[:, half]

                    @pl.when(keep)
                    def _():
                        kept[pl.ds(block, rows, stride=blocks), :] = approx[:, half]

            loop(blocks // 2, pair_one)
            store(index, chunk).start()

            @pl.when(keep)
            def _():
                at = pl.multiple_of(start // LANES + chunk * step, 16)
                copy = pltpu.make_async_copy(kept.at[pl.ds(0, step)], app_out.at[pl.ds(at, step)], kept_sem)
                copy.start()
                copy.wait()

        loop(count, one)
    for old_index, old_chunk in flat_plan[-2:]:
        store(old_index, jnp.int32(old_chunk)).wait()


def finish_body(*refs, n_enc, n_dec, gain, shard, heights):
    mine, refs = refs[: n_enc + n_dec], refs[n_enc + n_dec :]
    theirs, refs = refs[: n_enc + n_dec], refs[n_enc + n_dec :]
    err, ortho, right, unused, err_out, app_out = refs[:6]
    a_enc, b_enc, a_dec, b_dec = refs[6:10]
    section = lax.axis_index(SEC)
    for which, (a_slots, b_slots, lo, hi) in enumerate(((a_enc, b_enc, 0, n_enc), (a_dec, b_dec, n_enc, n_enc + n_dec))):

        @pl.when(section == which)
        def _():
            finish_section(
                which, heights[which], (mine[lo:hi], theirs[lo:hi]), err, ortho, right, err_out, app_out, a_slots, b_slots,
                *refs[10:], gain=gain, shard=shard,
            )


def finish(mine_e, mine_d, theirs_e, theirs_d, err, ortho, right, whole, gain, shard):
    n_enc, n_dec = len(mine_e), len(mine_d)
    heights = [[x.shape[0] for x in mine[::2]] for mine in (mine_e, mine_d)]
    dma = pltpu.SemaphoreType.DMA
    slots = []
    for which in range(2):
        for side in range(2):
            slots.append(pltpu.VMEM((2, 2 * max(heights[which]), max(shape[side] for shape in section_shapes(which))), bf16))
    total = 2 * (n_enc + n_dec)
    return pl.pallas_call(
        functools.partial(finish_body, n_enc=n_enc, n_dec=n_dec, gain=gain, shard=shard, heights=heights),
        in_specs=[ANYWHERE] * (total + 1) + [WHOLE] * 2 + [ANYWHERE],
        out_specs=[ANYWHERE] * 2,
        out_shape=[jax.ShapeDtypeStruct((1, 1, FLAT), f32), jax.ShapeDtypeStruct((FLAT // LANES, LANES), f32)],
        input_output_aliases={total + 3: 0},
        scratch_shapes=slots
        + [
            pltpu.VMEM((256, 2 * SEQ), bf16), pltpu.VMEM((256, 3 * RANK), bf16), pltpu.VMEM((2, MOST, LANES), bf16),
            pltpu.VMEM((2, 1, 1, MOST * LANES), f32), pltpu.VMEM((MOST, LANES), f32),
            dma((2, 4)), dma((2,)), dma((2,)), dma(()),
        ],
        compiler_params=pltpu.CompilerParams(vmem_limit_bytes=BIG),
        name="finish",
    )(*mine_e, *mine_d, *theirs_e, *theirs_d, err, ortho, right, whole)


MESH = pl.DeviceIdType.MESH


def grid_of(replicas):
    side = 2 if replicas < 64 else 4
    return replicas // (side * side), side, side


def used_rows(section):
    counts = [sum(rows * cols for rows, cols in section_shapes(s)) // LANES for s in range(2)]
    return jnp.where(section == 0, counts[0], counts[1])


def meet(replicas):
    section, me = lax.axis_index(SEC), lax.axis_index(DP)
    barrier = pltpu.get_barrier_semaphore()
    pl.semaphore_signal(barrier, inc=1, device_id={SEC: 1 - section}, device_id_type=MESH)
    for step in range(1, replicas):
        pl.semaphore_signal(
            barrier, inc=1, device_id={DP: lax.rem(me + step, replicas)}, device_id_type=MESH
        )
    pl.semaphore_wait(barrier, replicas)


def gather_body(
    low_ref, cnt_ref, vec_ref, fac_ref, err_ref, flat_ref, cnts_ref, vec2_ref, fac2_ref, stack_ref, left_ref, whole_ref,
    send_sem, recv_sem, swap_sem, cnt_send, cnt_recv, side_send, side_recv, own_sem, *scratch, replicas, size,
):
    section, me = lax.axis_index(SEC), lax.axis_index(DP)
    other = 1 - section
    nz, ny, nx = grid_of(replicas)
    x, y, z = lax.rem(me, nx), lax.rem(me // nx, ny), me // (nx * ny)
    cut = size // 2 // 8 * 8 if size % 8 == 0 else size
    halves = [(0, cut), (cut, size - cut)] if cut < size else [(0, cut)]
    used = used_rows(section)
    used_other = used_rows(other)

    def block_id(at_z, at_y, at_x):
        return (at_z * ny + at_y) * nx + at_x

    meet(replicas)

    def side(src, dst, slot):
        return pltpu.make_async_remote_copy(
            src_ref=src, dst_ref=dst.at[section], send_sem=side_send.at[slot], recv_sem=side_recv.at[slot],
            device_id={SEC: other}, device_id_type=MESH,
        )

    def count_copy(step):
        return pltpu.make_async_remote_copy(
            src_ref=cnt_ref, dst_ref=cnts_ref.at[me], send_sem=cnt_send.at[step],
            recv_sem=cnt_recv.at[step], device_id={DP: lax.rem(me + step, replicas)}, device_id_type=MESH,
        )

    for step in range(1, replicas):
        count_copy(step).start()
    side(vec_ref, vec2_ref, 0).start()
    side(fac_ref, fac2_ref, 1).start()
    own = pltpu.make_async_copy(low_ref, flat_ref.at[section * replicas + me], own_sem)
    own.start()

    def copy(block, half, target, way, mine=False, swap=False):
        start, rows = halves[half]
        at = flat_ref.at[section * replicas + block, pl.ds(start, rows)]
        src = low_ref.at[pl.ds(start, rows)] if mine else at
        return pltpu.make_async_remote_copy(
            src_ref=src, dst_ref=at, send_sem=send_sem.at[block, half, way],
            recv_sem=(swap_sem if swap else recv_sem).at[block, half], device_id=target, device_id_type=MESH,
        )

    def needed(block, half, limit):
        return block * size + halves[half][0] < limit

    def at_z(value):
        return {DP: block_id(value, y, x)}

    def along_x(block, half, mine=False):
        for step in range(1, nx):
            copy(block, half, {DP: block_id(z, y, lax.rem(x + step, nx))}, 1 + step, mine).start()

    def along_y(block, half, mine=False):
        for step in range(1, ny):
            copy(block, half, {DP: block_id(z, lax.rem(y + step, ny), x)}, nx + step, mine).start()

    def across(block, half, mine=False):
        copy(block, half, {SEC: other}, nx + ny, mine, True).start()

    def arrived(block, half):
        copy(block, half, {SEC: other}, 0).wait_recv()

    def layers(k):
        return [z] if k == 0 else [z - k, z + k]

    def valid(at):
        return (at >= 0) & (at < nz)

    def first(k):
        for which, layer in enumerate(layers(k)):
            block = block_id(layer, y, x)
            for half in range(len(halves)):

                @pl.when(valid(layer) & needed(block, half, used))
                def _():
                    if k > 0:
                        arrived(block, half)
                    mine = k == 0
                    if k == 0 or which == 0:

                        @pl.when(z + 1 < nz)
                        def _():
                            copy(block, half, at_z(z + 1), 0, mine).start()

                    if k == 0 or which == 1:

                        @pl.when(z > 0)
                        def _():
                            copy(block, half, at_z(z - 1), 1, mine).start()

                    if half == 0:
                        along_x(block, half, mine)
                        along_y(block, half, mine)
                    else:
                        along_y(block, half, mine)
                        along_x(block, half, mine)
                    across(block, half, mine)

    def second(k):
        for layer in layers(k):
            for half in range(len(halves)):
                for step in range(1, nx if half == 0 else ny):
                    if half == 0:
                        block = block_id(layer, y, lax.rem(x + step, nx))
                    else:
                        block = block_id(layer, lax.rem(y + step, ny), x)

                    @pl.when(valid(layer) & needed(block, half, used))
                    def _():
                        arrived(block, half)
                        if half == 0:
                            along_y(block, half)
                        else:
                            along_x(block, half)
                        across(block, half)

    def third(k):
        for layer in layers(k):
            for half in range(len(halves)):
                for far in range(1, ny if half == 0 else nx):
                    for near in range(nx if half == 0 else ny):
                        if half == 0:
                            block = block_id(layer, lax.rem(y + far, ny), lax.rem(x + near, nx))
                        else:
                            block = block_id(layer, lax.rem(y + near, ny), lax.rem(x + far, nx))

                        @pl.when(valid(layer) & needed(block, half, used))
                        def _():
                            arrived(block, half)
                            across(block, half)

    prep = Prep(err_ref, fac_ref, stack_ref, left_ref, whole_ref, *scratch)
    left_ref[...] = jnp.zeros_like(left_ref)
    shares = [[[0], [2], [3], [1], [4]], [[0, 1], [2], [3], [4, 5], [None]]]
    for k in range(nz + 2):
        if k < nz:
            first(k)
        if 0 <= k - 1 < nz:
            second(k - 1)
        if 0 <= k - 2 < nz:
            third(k - 2)
        for which in range(2):
            if k < len(shares[which]):

                @pl.when(section == which)
                def _():
                    for index in shares[which][k]:
                        if index is None:
                            prep.rest(which)
                        else:
                            prep.matrix(which, index)

    def drain(block, carry):
        at_x_, at_y_, at_z_ = lax.rem(block, nx), lax.rem(block // nx, ny), block // (nx * ny)
        for half in range(len(halves)):
            column = (at_x_ == x) & (at_y_ == y)

            @pl.when(needed(block, half, used))
            def _():
                @pl.when(column & (at_z_ <= z) & (z + 1 < nz))
                def _():
                    copy(block, half, {SEC: other}, 0).wait_send()

                @pl.when(column & (at_z_ >= z) & (z > 0))
                def _():
                    copy(block, half, {SEC: other}, 1).wait_send()

                single = len(halves) == 1
                sent_x = (column if half == 0 else at_x_ == x)
                sent_y = (at_y_ == y) if half == 0 else column

                @pl.when(sent_x)
                def _():
                    for step in range(1, nx):
                        copy(block, half, {SEC: other}, 1 + step).wait_send()

                @pl.when(sent_y)
                def _():
                    for step in range(1, ny):
                        copy(block, half, {SEC: other}, nx + step).wait_send()

                copy(block, half, {SEC: other}, nx + ny).wait_send()

            @pl.when(needed(block, half, used_other))
            def _():
                copy(block, half, {SEC: other}, 0, False, True).wait_recv()

        return carry

    lax.fori_loop(0, replicas, drain, 0)
    own.wait()
    for step in range(1, replicas):
        count_copy(step).wait()
    cnts_ref[me] = cnt_ref[...]
    vec2_ref[section] = vec_ref[...]
    fac2_ref[section] = fac_ref[...]
    side(vec_ref, vec2_ref, 0).wait()
    side(fac_ref, fac2_ref, 1).wait()


def update_body(master_ref, moment_ref, approx_ref, scale_ref, master_out, low_out, moment_out):
    moment = moment_decay * moment_ref[...] + scale_ref[...] * approx_ref[...].reshape(moment_ref.shape)
    moment_out[...] = moment
    master = master_ref[...] - learning_rate() * moment
    master_out[...] = master
    low_out[...] = master.astype(bf16)


def update(master, moment, approx, scale):
    size = approx.shape[0]
    steps = 7 if size % 56 == 0 else 1
    line = pl.BlockSpec((1, master.shape[1] // steps), lambda i: (0, i))
    return pl.pallas_call(
        update_body,
        grid=(steps,),
        in_specs=[line, line, pl.BlockSpec((size // steps, LANES), lambda i: (i, 0)), pl.BlockSpec((1, 1), lambda i: (0, 0))],
        out_specs=[line] * 3,
        out_shape=[
            jax.ShapeDtypeStruct(master.shape, f32), jax.ShapeDtypeStruct(master.shape, bf16),
            jax.ShapeDtypeStruct(master.shape, f32),
        ],
        name="update",
    )(master, moment, approx, scale)


def cast_body(src_ref, out_ref):
    out_ref[...] = src_ref[...].reshape(out_ref.shape).astype(bf16)


def cast_shard(master, size):
    full = pl.BlockSpec(memory_space=pltpu.VMEM)
    return pl.pallas_call(
        cast_body, in_specs=[full], out_specs=full, out_shape=jax.ShapeDtypeStruct((size, LANES), bf16), name="cast"
    )(master)


def gather(low, cnt, vec, fac, errors, replicas, left_rows):
    size = low.shape[0]
    vmem = pl.BlockSpec(memory_space=pltpu.VMEM)
    nz, ny, nx = grid_of(replicas)
    dma = pltpu.SemaphoreType.DMA
    return pl.pallas_call(
        functools.partial(gather_body, replicas=replicas, size=size),
        in_specs=[vmem] * 4 + [ANYWHERE],
        out_specs=[ANYWHERE, vmem, vmem, vmem, ANYWHERE, vmem, ANYWHERE],
        out_shape=[
            jax.ShapeDtypeStruct((2 * replicas, size, LANES), bf16),
            jax.ShapeDtypeStruct((replicas,) + cnt.shape, f32),
            jax.ShapeDtypeStruct((2,) + vec.shape, f32),
            jax.ShapeDtypeStruct((2,) + fac.shape, f32),
            jax.ShapeDtypeStruct((FLAT // LANES, LANES), bf16),
            jax.ShapeDtypeStruct((left_rows, LANES), f32),
            jax.ShapeDtypeStruct((1, 1, FLAT), f32),
        ],
        scratch_shapes=[
            dma((replicas, 2, nx + ny + 1)), dma((replicas, 2)), dma((replicas, 2)),
            dma((replicas,)), dma((replicas,)), dma((2,)), dma((2,)), dma(()),
        ]
        + prep_scratch(),
        compiler_params=pltpu.CompilerParams(collective_id=2, has_side_effects=True, vmem_limit_bytes=BIG),
        name="gather",
    )(low, cnt, vec, fac, errors)


def sum_body(*refs, replicas, n_enc, n_dec):
    n = n_enc + n_dec
    sum_run(*refs[:2], refs[2 : 2 + n], refs[2 + n], refs[3 + n : 3 + 2 * n], *refs[3 + 2 * n :], replicas=replicas, n_enc=n_enc)


def sum_run(
    part_ref, extra_ref, given, total_ref, taken, mine, came, slots, seg, swap_send, swap_recv, send_a, recv_a, send_b, recv_b,
    give_sem, take_sem, *, replicas, n_enc,
):
    section, me = lax.axis_index(SEC), lax.axis_index(DP)
    other = 1 - section
    rows = part_ref.shape[1]
    size = rows // replicas
    meet(replicas)

    def rows_of(index):
        return pl.ds(pl.multiple_of(index * size, 8), size)

    swap = pltpu.make_async_remote_copy(
        src_ref=part_ref.at[other], dst_ref=came, send_sem=swap_send.at[0], recv_sem=swap_recv.at[0],
        device_id={SEC: other}, device_id_type=MESH,
    )
    swap.start()
    mine[...] = part_ref[section] + extra_ref[...]
    swap.wait()

    def give(i):
        return pltpu.make_async_remote_copy(
            src_ref=given[i], dst_ref=taken[i], send_sem=give_sem.at[i], recv_sem=take_sem.at[i],
            device_id={SEC: other}, device_id_type=MESH,
        )

    n = len(given)
    for i in range(n):

        @pl.when(section == (1 if i < n_enc else 0))
        def _():
            give(i).start()

    mine[...] = mine[...] + came[...]

    def scatter(step):
        peer = lax.rem(me + step, replicas)
        return pltpu.make_async_remote_copy(
            src_ref=mine.at[rows_of(peer)], dst_ref=slots.at[step], send_sem=send_a.at[step],
            recv_sem=recv_a.at[step], device_id={DP: peer}, device_id_type=MESH,
        )

    def spread(step):
        peer = lax.rem(me + step, replicas)
        return pltpu.make_async_remote_copy(
            src_ref=seg, dst_ref=total_ref.at[section, rows_of(me)], send_sem=send_b.at[step],
            recv_sem=recv_b.at[step], device_id={DP: peer}, device_id_type=MESH,
        )

    for step in range(1, replicas):
        scatter(step).start()
    total = mine[rows_of(me), :]
    for step in range(1, replicas):
        scatter(step).wait_recv()
        total = total + slots[step]
    seg[...] = total
    for step in range(1, replicas):
        spread(step).start()
    total_ref[section, rows_of(me)] = total
    for step in range(1, replicas):
        scatter(step).wait_send()
        spread(step).wait()
    back = pltpu.make_async_remote_copy(
        src_ref=total_ref.at[section], dst_ref=total_ref.at[section], send_sem=swap_send.at[1],
        recv_sem=swap_recv.at[1], device_id={SEC: other}, device_id_type=MESH,
    )
    back.start()
    back.wait()
    for i in range(n):

        @pl.when(section == (1 if i < n_enc else 0))
        def _():
            give(i).wait_send()

        @pl.when(section == (0 if i < n_enc else 1))
        def _():
            give(i).wait_recv()


def all_sum(part, extra, replicas, collective_id, enc=(), dec=()):
    rows = part.shape[1]
    vmem = pl.BlockSpec(memory_space=pltpu.VMEM)
    dma = pltpu.SemaphoreType.DMA
    size = rows // replicas
    given = list(enc) + list(dec)
    n = len(given)
    anywhere = pl.BlockSpec(memory_space=pl.ANY)
    outs = pl.pallas_call(
        functools.partial(sum_body, replicas=replicas, n_enc=len(enc), n_dec=len(dec)),
        in_specs=[vmem, vmem] + [anywhere] * n,
        out_specs=[vmem] + [anywhere] * n,
        out_shape=[jax.ShapeDtypeStruct(part.shape, f32)] + [jax.ShapeDtypeStruct(x.shape, x.dtype) for x in given],
        scratch_shapes=[
            pltpu.VMEM((rows, LANES), f32), pltpu.VMEM((rows, LANES), f32),
            pltpu.VMEM((replicas, size, LANES), f32), pltpu.VMEM((size, LANES), f32),
            dma((2,)), dma((2,)), dma((replicas,)), dma((replicas,)), dma((replicas,)), dma((replicas,)),
            dma((max(n, 1),)), dma((max(n, 1),)),
        ],
        compiler_params=pltpu.CompilerParams(collective_id=collective_id, has_side_effects=True),
        name="all_sum",
    )(part, extra, *given)
    return outs[0], outs[1 : 1 + len(enc)], outs[1 + len(enc) :]


def local(pixels, visible, masked, loss_mask, master, momentum, vectors, vec_moment, factors, errors):
    sec = lax.axis_index(SEC)
    replicas = lax.axis_size(DP)
    replica_id = lax.axis_index(DP)

    replicas_n = replicas
    shard_len = master.shape[1]
    size = shard_len // LANES
    gain = float(replicas)

    count_tile = jnp.full((RANK, LANES), jnp.sum(loss_mask).astype(f32))
    vec_tile = jnp.pad(vectors[0], (0, VEC_TILES * RANK * LANES - VLEN)).reshape(-1, LANES)
    left_rows = sum_rows(replicas, ROW_PAD // LANES + VEC_TILES + 1)
    flat_both, counts, vec_both, fac_both, err_stack, err_lefts, whole = gather(
        cast_shard(master, size), count_tile, vec_tile, factors[0], errors, replicas, left_rows
    )
    low_both = flat_both.reshape(-1, LANES)
    count = jnp.sum(counts[:, 0, 0])

    vis = lax.dynamic_index_in_dim(visible, sec, 0, keepdims=False)
    mas = lax.dynamic_index_in_dim(masked, sec, 0, keepdims=False)
    mask_row = lax.dynamic_index_in_dim(loss_mask, sec, 0, keepdims=False).astype(f32)
    order = jnp.concatenate([vis, mas])
    pix = lax.dynamic_index_in_dim(pixels, sec, 0, keepdims=False)
    pick = (order[:, None] == jnp.arange(SEQ, dtype=jnp.int32)[None, :]).astype(bf16)
    pix_order = nn(pick, pix).astype(bf16)
    pix_vis = jnp.pad(pix_order[:VIS], ((0, 0), (0, PATCH_PAD - PATCH)))
    target = pix_order[VIS:]
    place = order[:, None]
    mask_col = mask_row[:, None]
    tail_row = ROW_PAD // LANES * RANK
    right_rows = sum_rows(replicas, max(COL_WIDTHS) // LANES)

    kept, enc = encode(low_both, pix_vis, place[:VIS], angle_tables(DE), vec_both)
    given, grad_coded, sums_e, part_d = decode(
        low_both, kept[K_CODED], place, angle_tables(DD), vec_both, target, mask_col, count.reshape(1, 1), fac_both, tail_row, gain, left_rows,
    )
    back, part_e = encode_back(kept, enc, grad_coded, sums_e, vec_both, pix_vis, fac_both, tail_row, gain, left_rows)
    pairs_e = [
        (kept[K_NORMED], back[K_B_QKV]), (kept[K_ATTENDED], back[K_B_PROJ]), (kept[K_SECOND], back[K_B_UP]),
        (kept[K_ACTIVE], back[K_B_DOWN]), (pix_vis, back[K_START]),
    ]
    pairs_d = [
        (given[K_NORMED], given[K_B_QKV]), (given[K_ATTENDED], given[K_B_PROJ]), (given[K_SECOND], given[K_B_UP]),
        (given[K_ACTIVE], given[K_B_DOWN]), (given[K_B_PRED], given[K_FINAL]), (given[K_SENT], given[K_FIRST]),
    ]
    pairs = pairs_e + pairs_d
    n_enc = len(pairs_e)
    flat_e = [x for pair in pairs_e for x in pair]
    flat_d = [x for pair in pairs_d for x in pair]
    left_part = jnp.stack([part_e, part_d])
    early_e = [5, 6]
    late_e = [i for i in range(len(flat_e)) if i not in early_e]
    early_d = [5, 6]
    late_d = [i for i in range(len(flat_d)) if i not in early_d]
    left_sum, first_e, first_d = all_sum(
        left_part, err_lefts, replicas, 3, [flat_e[i] for i in early_e], [flat_d[i] for i in early_d]
    )
    vec_sum = left_sum[:, tail_row : tail_row + VEC_TILES * RANK]
    loss_sum = left_sum[1, tail_row + VEC_TILES * RANK, 0]

    ortho, right_part, err_rights = rights(
        left_sum, err_stack, [a for a, b in pairs], [b for a, b in pairs], 1.0 / replicas, gain, right_rows
    )
    sums, second_e, second_d = all_sum(
        right_part, err_rights, replicas, 4, [flat_e[i] for i in late_e], [flat_d[i] for i in late_d]
    )
    other_e = [x for i, x in sorted([*zip(early_e, first_e), *zip(late_e, second_e)], key=lambda entry: entry[0])]
    other_d = [x for i, x in sorted([*zip(early_d, first_d), *zip(late_d, second_d)], key=lambda entry: entry[0])]
    right_both, norm_row = final_right(sums, ortho, vec_sum, factors.shape[2], 1.0 / replicas)
    norm = norm_row[0, 0]
    scale = jnp.minimum(1.0, clip_limit / (norm + 1e-06))

    new_errors, approx = finish(
        flat_e, flat_d, other_e, other_d, err_stack, ortho, right_both, whole, gain, shard_len
    )
    own_part = lax.dynamic_slice_in_dim(approx, replica_id * size, size)
    used = jnp.where(sec == 0, *[sum(rows_n * cols_n for rows_n, cols_n in section_shapes(s)) // LANES for s in range(2)])
    inside = replica_id * size + lax.broadcasted_iota(jnp.int32, (size, 1), 0) < used
    own_part = jnp.where(inside, own_part, 0.0)
    rate = learning_rate()
    new_master, new_low, new_moment = update(master, momentum, own_part, scale.reshape(1, 1))
    vec_own = lax.dynamic_index_in_dim(vec_sum, sec, 0, keepdims=False).reshape(-1)[:VLEN]
    new_vm = moment_decay * vec_moment[0] + scale * vec_own
    new_vectors = vectors[0] - rate * new_vm
    new_factors = lax.dynamic_index_in_dim(right_both, sec, 0, keepdims=False)
    return (
        new_master,
        new_low,
        new_moment,
        new_vectors[None],
        new_vm[None],
        new_factors[None],
        new_errors,
        loss_sum.reshape(1),
        norm.reshape(1),
    )


def solution(mesh):
    return jax.shard_map(
        local,
        mesh=mesh,
        in_specs=(
            P(DP, None, None),
            P(DP, None),
            P(DP, None),
            P(DP, None),
            P(SEC, DP),
            P(SEC, DP),
            P(SEC, None),
            P(SEC, None),
            P(SEC, None, None),
            P(SEC, DP, None),
        ),
        out_specs=(
            P(SEC, DP),
            P(SEC, DP),
            P(SEC, DP),
            P(SEC, None),
            P(SEC, None),
            P(SEC, None, None),
            P(SEC, DP, None),
            P(),
            P(),
        ),
        check_vma=False,
    )
```

```python
import functools
import math

import jax
import jax.numpy as jnp
import numpy as np
from jax import lax
from jax.experimental import pallas as pl
from jax.experimental.pallas import tpu as pltpu
from jax.sharding import PartitionSpec as P

DE = 768
FFE = 3072
HEADS_ENC = 12
DD = 512
FFD = 2048
HEADS_DEC = 16
PATCH = 192
PATCH_PAD = 256
RANK = 8
SEQ = 1024
VIS = 256
FLAT = 7225344
VLEN = 11520

(K_TOKENS, K_NORMED, K_JOINED, K_OUT, K_LSE, K_ATTENDED, K_MIDDLE, K_SECOND, K_ACTIVE, K_SLOPE, K_CODED, K_B_QKV, K_B_PROJ, K_B_UP, K_B_DOWN, K_B_PRED, K_FINAL, K_SENT, K_FIRST, K_GRAD, K_ATT, K_DK, K_DV, K_SUMS, K_BIAS, K_START) = range(26)

f32 = jnp.float32
bf16 = jnp.bfloat16
clip_limit = 0.0001
moment_decay = 0.9
rate_base = 0.5
LANES = 128
SEC, DP = "section", "dp"
STEP = 32
DEC_ROWS = 512
CHUNK = 256
BIG = 66000000


def nn(left, right):
    return lax.dot_general(left, right, (((1,), (0,)), ((), ())), preferred_element_type=f32)


def nt(left, right):
    return lax.dot_general(left, right, (((1,), (1,)), ((), ())), preferred_element_type=f32)


def tn(left, right):
    return lax.dot_general(left, right, (((0,), (0,)), ((), ())), preferred_element_type=f32)


def split3(value):
    high = value.astype(bf16)
    rest = value - high.astype(f32)
    middle = rest.astype(bf16)
    return jnp.concatenate([high, middle, (rest - middle.astype(f32)).astype(bf16)], axis=0)


def join3(value):
    return value[:RANK] + value[RANK : 2 * RANK] + value[2 * RANK :]


def norm_parts(tokens):
    centred = tokens - jnp.mean(tokens, axis=-1, keepdims=True)
    spread = lax.rsqrt(jnp.mean(centred * centred, axis=-1, keepdims=True) + 1e-06)
    return centred * spread, spread


def norm_back(grad, hat, spread, gain):
    inner = grad * gain
    return spread * (
        inner - jnp.mean(inner, axis=-1, keepdims=True) - hat * jnp.mean(inner * hat, axis=-1, keepdims=True)
    )


def column_sum(value):
    return jnp.sum(value.astype(f32), axis=0, keepdims=True)


def angle_tables(width):
    column = np.arange(width)
    freqs = np.exp(-(column // 2 * 2) / width * math.log(10000.0))
    coarse = (np.arange(0, SEQ, STEP)[:, None] * freqs).astype(np.float64)
    fine = np.arange(STEP)[:, None] * freqs + (column % 2) * (math.pi / 2)
    return jnp.asarray(np.stack([np.sin(coarse), np.cos(coarse), np.cos(fine), np.sin(fine)]), f32)


def positions_of(place, tables):
    column = lax.broadcasted_iota(jnp.int32, (1, STEP), 1)
    coarse = (place // STEP == column).astype(bf16)
    fine = (place % STEP == column).astype(bf16)

    def take(pick, table):
        high = table.astype(bf16)
        rest = table - high.astype(f32)
        middle = rest.astype(bf16)
        low = (rest - middle.astype(f32)).astype(bf16)
        return nn(pick, high) + nn(pick, middle) + nn(pick, low)

    return take(coarse, tables[0]) * take(fine, tables[2]) + take(coarse, tables[1]) * take(fine, tables[3])


def section_shapes(section):
    if section == 0:
        return [(DE, 3 * DE), (DE, DE), (DE, FFE), (FFE, DE), (PATCH, DE)]
    return [(DD, 3 * DD), (DD, DD), (DD, FFD), (FFD, DD), (PATCH, DD), (DE, DD)]


def learning_rate():
    return rate_base * math.sqrt(2.0 * (FLAT + VLEN) / DD) / clip_limit


def head_mask(head, size):
    lane = lax.broadcasted_iota(jnp.int32, (1, LANES), 1)
    return (lane // size == head).astype(bf16)


def attend_body(q_ref, k_ref, v_ref, o_ref, lse_ref, *, size, rows_q):
    seq = k_ref.shape[0]
    scale = size ** (-0.5)
    fold = scale * math.log2(math.e)
    turned = v_ref[...].T

    def one(step, carry):
        at = pl.ds(pl.multiple_of(step * rows_q, rows_q), rows_q)
        queries = q_ref[at, :]
        parts = []
        for head in range(LANES // size):
            scores = nt(k_ref[...], queries * head_mask(head, size))
            peak = jnp.max(scores, axis=0, keepdims=True) * fold
            power = jnp.exp2(scores * fold - peak)
            mass = jnp.sum(power, axis=0, keepdims=True)
            parts.append(nn(turned[head * size : (head + 1) * size], power.astype(bf16)) * (1.0 / mass))
            lse_ref[0, head : head + 1, at] = peak + jnp.log2(mass)
        o_ref[at, :] = jnp.concatenate(parts, axis=0).T
        return carry

    lax.fori_loop(0, seq // rows_q, one, 0)


def attend_back_body(q_ref, k_ref, v_ref, do_ref, o_ref, lse_ref, dq_ref, dk_ref, dv_ref, dk_sum, dv_sum, *, size, rows_q):
    seq = k_ref.shape[0]
    scale = size ** (-0.5)
    fold = scale * math.log2(math.e)
    turned = k_ref[...].T
    dk_sum[...] = jnp.zeros_like(dk_sum)
    dv_sum[...] = jnp.zeros_like(dv_sum)

    def one(step, carry):
        at = pl.ds(pl.multiple_of(step * rows_q, rows_q), rows_q)
        queries = q_ref[at, :]
        grads = do_ref[at, :]
        prod = grads.astype(f32) * o_ref[at, :]
        parts = []
        high = prod.astype(bf16)
        rest = prod - high.astype(f32)
        middle = rest.astype(bf16)
        for head in range(LANES // size):
            mask = head_mask(head, size)
            wide = jnp.broadcast_to(mask, (16, LANES))
            delta = (nt(wide, high) + nt(wide, middle))[0:1]
            q_one = queries * mask
            g_one = grads * mask
            scores = nt(k_ref[...], q_one)
            probs = jnp.exp2(scores * fold - lse_ref[0, head : head + 1, at])
            slope = nt(v_ref[...], g_one)
            grad_s = (probs * (slope - delta)).astype(bf16)
            dv_sum[...] += nn(probs.astype(bf16), g_one)
            dk_sum[...] += nn(grad_s, q_one)
            parts.append(nn(turned[head * size : (head + 1) * size], grad_s))
        dq_ref[at, :] = (jnp.concatenate(parts, axis=0).T * scale).astype(bf16)
        return carry

    lax.fori_loop(0, seq // rows_q, one, 0)
    dk_ref[...] = (dk_sum[...] * scale).astype(bf16)
    dv_ref[...] = dv_sum[...].astype(bf16)


def rows_at(step, count):
    return pl.ds(pl.multiple_of(step * count, count), count)


def cols_at(step, count=LANES):
    return pl.ds(pl.multiple_of(step * count, count), count)


def shape_of(rows, cols, dtype=f32):
    return jax.ShapeDtypeStruct((rows, cols), dtype)


def loop(count, body):
    def one(step, carry):
        body(step)
        return carry

    lax.fori_loop(0, count, one, 0)


def over_blocks(seq, rows, body, *refs):
    loop(seq // rows, lambda step: body(*[ref.at[rows_at(step, rows)] for ref in refs]))


def open_stage(tok_ref, normed_ref, joined_ref, vec_ref, w_ref):
    width = tok_ref.shape[1]
    hat, unused = norm_parts(tok_ref[...])
    normed = (hat * vec_ref[0:1] + vec_ref[1:2]).astype(bf16)
    normed_ref[...] = normed
    for part, bias in ((0, vec_ref[6:7]), (1, None), (2, vec_ref[7:8])):
        cols = slice(part * width, (part + 1) * width)
        value = nn(normed, w_ref[:, cols])
        joined_ref[:, cols] = (value if bias is None else value + bias).astype(bf16)


def attend_stage(joined, out, lse, size):
    seq, width = out.shape
    groups = width // LANES

    def one(group):
        attend_body(
            joined.at[:, cols_at(group)], joined.at[:, cols_at(groups + group)],
            joined.at[:, cols_at(2 * groups + group)], out.at[:, cols_at(group)], lse.at[pl.ds(group, 1)],
            size=size, rows_q=min(512, seq),
        )

    loop(groups, one)


def attend_back_stage(joined, grad_att, out, lse, b_qkv, dk_sum, dv_sum, size):
    seq, width = out.shape
    groups = width // LANES

    def one(group):
        here = [cols_at(part * groups + group) for part in range(3)]
        attend_back_body(
            *[joined.at[:, cols] for cols in here], grad_att.at[:, here[0]], out.at[:, here[0]],
            lse.at[pl.ds(group, 1)], *[b_qkv.at[:, cols] for cols in here], dk_sum, dv_sum,
            size=size, rows_q=min(512, seq),
        )

    loop(groups, one)


def close_stage(
    tok_ref, o_ref, att_ref, mid_ref, sec_ref, act_ref, slope_ref, out_ref, vec_ref, bias_ref, wo_ref, w1_ref, w2_ref
):
    attended = o_ref[...].astype(bf16)
    att_ref[...] = attended
    middle = tok_ref[...] + nn(attended, wo_ref[...]) + vec_ref[8:9]
    mid_ref[...] = middle
    hat, unused = norm_parts(middle)
    sec_ref[...] = (hat * vec_ref[2:3] + vec_ref[3:4]).astype(bf16)
    out_ref[...] = middle + vec_ref[9:10]

    def one(step):
        cols = cols_at(step, CHUNK)
        hidden = nn(sec_ref[...], w1_ref[:, cols]) + bias_ref[:, cols]
        share = 0.5 * (1.0 + lax.erf(hidden * math.sqrt(0.5)))
        active = (hidden * share).astype(bf16)
        act_ref[:, cols] = active
        slope_ref[:, cols] = share + hidden * (jnp.exp(-0.5 * hidden * hidden) * (1.0 / math.sqrt(2.0 * math.pi)))
        out_ref[...] += nn(active, w2_ref[cols, :])

    loop(w1_ref.shape[1] // CHUNK, one)


def back_up_stage(
    grad_ref, slope_ref, mid_ref, down_ref, up_ref, proj_ref, att_ref, total, vec_ref, wo_ref, w1_ref, w2_ref, sums_ref, bias_ref
):
    down = grad_ref[...].astype(bf16)
    down_ref[...] = down
    total[...] = jnp.zeros_like(total)

    def one(step):
        cols = cols_at(step, CHUNK)
        part = (nt(down_ref[...], w2_ref[cols, :]) * slope_ref[:, cols]).astype(bf16)
        up_ref[:, cols] = part
        bias_ref[:, cols] += column_sum(part)
        total[...] += nt(part, w1_ref[:, cols])

    loop(w1_ref.shape[1] // CHUNK, one)
    grad = total[...]
    hat, spread = norm_parts(mid_ref[...])
    middle = grad_ref[...] + norm_back(grad, hat, spread, vec_ref[2:3])
    grad_ref[...] = middle
    proj = middle.astype(bf16)
    proj_ref[...] = proj
    att_ref[...] = nt(proj, wo_ref[...]).astype(bf16)
    sums_ref[2:3] += column_sum(grad * hat)
    sums_ref[3:4] += column_sum(grad)
    sums_ref[8:9] += column_sum(proj)
    sums_ref[9:10] += column_sum(down)


def back_in_stage(join_ref, grad_ref, tok_ref, vec_ref, w_ref, sums_ref):
    width = tok_ref.shape[1]
    grad = nt(join_ref[...], w_ref[...])
    sums_ref[6:7] += column_sum(join_ref[:, :width])
    sums_ref[7:8] += column_sum(join_ref[:, 2 * width :])
    hat, spread = norm_parts(tok_ref[...])
    grad_ref[...] += norm_back(grad, hat, spread, vec_ref[0:1])
    sums_ref[0:1] += column_sum(grad * hat)
    sums_ref[1:2] += column_sum(grad)


def widen(flat_ref, wide, w_ref):
    rows_n, cols_n = w_ref.shape
    blocks = cols_n // LANES
    count = 64 * blocks

    def one(step):
        wide[:count] = flat_ref[rows_at(step, count), :].astype(f32)
        for block in range(blocks):
            w_ref[rows_at(step, 64), block * LANES : (block + 1) * LANES] = wide[
                pl.ds(block, 64, stride=blocks), :
            ].astype(bf16)

    loop(rows_n // 64, one)


class Weights:
    def __init__(self, flat, section, order, slots, wide, mats, sems):
        self.flat, self.slots, self.wide, self.mats, self.sems = flat, slots, wide, mats, sems
        self.order, self.shapes, self.next = order, section_shapes(section), 0
        self.base = section * (FLAT // LANES)
        for position in range(2):
            self.fetch(position).start()

    def fetch(self, position):
        index = self.order[position]
        start = self.base + sum(rows * cols for rows, cols in self.shapes[:index]) // LANES
        count = self.shapes[index][0] * self.shapes[index][1] // LANES
        return pltpu.make_async_copy(
            self.flat.at[pl.ds(start, count)], self.slots.at[position % 2, pl.ds(0, count)], self.sems.at[position]
        )

    def take(self):
        position = self.next
        self.fetch(position).wait()
        mat = self.mats[self.order[position]]
        widen(self.slots.at[position % 2], self.wide, mat)
        if position + 2 < len(self.order):
            self.fetch(position + 2).start()
        self.next += 1
        return mat


def take_rows(vec_ref, section, width, rows_ref, bias_ref, extra_ref=None):
    places = [(rows_ref, line, line * width, width) for line in range(11)]
    places.append((bias_ref, 0, 11 * width, bias_ref.shape[1]))
    if extra_ref is not None:
        places.append((extra_ref, 0, 11 * width + bias_ref.shape[1], width))
    for ref, line, offset, count in places:
        for tile in range(count // LANES):
            row = offset // LANES + tile
            ref[line : line + 1, tile * LANES : (tile + 1) * LANES] = vec_ref[section, row : row + 1]


class Copies:
    def __init__(self, sems):
        self.sems, self.made = sems, []

    def start(self, src, dst):
        copy = pltpu.make_async_copy(src, dst, self.sems.at[len(self.made)])
        copy.start()
        self.made.append(copy)
        return copy


def flat_count(section):
    return max(rows * cols for rows, cols in section_shapes(section)) // LANES


ANYWHERE = pl.BlockSpec(memory_space=pl.ANY)
WHOLE = pl.BlockSpec(memory_space=pltpu.VMEM)
ENC_KEPT = [
    (K_TOKENS, (VIS, DE), f32), (K_NORMED, (VIS, DE), bf16), (K_JOINED, (VIS, 3 * DE), bf16), (K_OUT, (VIS, DE), f32),
    (K_LSE, (DE // LANES, 2, VIS), f32), (K_ATTENDED, (VIS, DE), bf16), (K_MIDDLE, (VIS, DE), f32),
    (K_SECOND, (VIS, DE), bf16), (K_ACTIVE, (VIS, FFE), bf16), (K_SLOPE, (VIS, FFE), f32), (K_CODED, (VIS, DE), f32),
]


def encode_body(flat, pix, place, table, vec_ref, *rest):
    kept_n, mats_n = len(ENC_KEPT), len(section_shapes(0))
    kept_out, mats_out = rest[:kept_n], rest[kept_n : kept_n + mats_n]
    rest = rest[kept_n + mats_n :]
    kept = dict(zip([name for name, shape, kind in ENC_KEPT], rest[:kept_n]))
    mats = rest[kept_n : kept_n + mats_n]
    slots, wide, vecs, bias, in_sems, out_sems = rest[kept_n + mats_n :]
    take_rows(vec_ref, 0, DE, vecs, bias)
    weights = Weights(flat, 0, [4, 0, 1, 2, 3], slots, wide, mats, in_sems)
    copies = Copies(out_sems)

    def give(*names):
        for name in names:
            which = [entry[0] for entry in ENC_KEPT].index(name)
            copies.start(kept[name], kept_out[which])

    def take(index):
        mat = weights.take()
        copies.start(mat, mats_out[index])
        return mat

    kept[K_TOKENS][...] = positions_of(place[...], table) + vecs[10:11] + nn(pix[:, :PATCH], take(4)[...])
    open_stage(kept[K_TOKENS], kept[K_NORMED], kept[K_JOINED], vecs, take(0))
    give(K_TOKENS, K_NORMED, K_JOINED)
    attend_stage(kept[K_JOINED], kept[K_OUT], kept[K_LSE], DE // HEADS_ENC)
    give(K_OUT, K_LSE)
    wo, w1, w2 = take(1), take(2), take(3)
    keys = [K_TOKENS, K_OUT, K_ATTENDED, K_MIDDLE, K_SECOND, K_ACTIVE, K_SLOPE, K_CODED]
    close_stage(*[kept[name] for name in keys], vecs, bias, wo, w1, w2)
    give(K_ATTENDED, K_MIDDLE, K_SECOND, K_ACTIVE, K_SLOPE, K_CODED)
    for copy in copies.made:
        copy.wait()


def encode(flat, pix, place, table, vecs):
    mats = section_shapes(0)
    dma = pltpu.SemaphoreType.DMA
    outs = pl.pallas_call(
        encode_body,
        in_specs=[ANYWHERE] + [WHOLE] * 4,
        out_specs=[ANYWHERE] * (len(ENC_KEPT) + len(mats)),
        out_shape=[jax.ShapeDtypeStruct(shape, kind) for name, shape, kind in ENC_KEPT] + [shape_of(*shape, bf16) for shape in mats],
        scratch_shapes=[pltpu.VMEM(shape, kind) for name, shape, kind in ENC_KEPT]
        + [pltpu.VMEM(shape, bf16) for shape in mats]
        + [
            pltpu.VMEM((2, flat_count(0), LANES), bf16), pltpu.VMEM((64 * FFE // LANES, LANES), f32),
            pltpu.VMEM((16, DE), f32), pltpu.VMEM((1, FFE), f32), dma((len(mats),)), dma((len(ENC_KEPT) + len(mats),)),
        ],
        compiler_params=pltpu.CompilerParams(vmem_limit_bytes=BIG),
        name="encode",
    )(flat, pix, place, table, vecs)
    return dict(zip([name for name, shape, kind in ENC_KEPT], outs)), outs[len(ENC_KEPT) :]


def put_vec(part_ref, tail_row, offset, value):
    for tile in range(value.shape[1] // LANES):
        row = tail_row + offset // LANES + tile
        part_ref[row : row + 1] = value[:, tile * LANES : (tile + 1) * LANES]


def put_left(part_ref, section, index, factor_ref, u_ref, v_ref, gain):
    base = len(section_shapes(0)) * section + index
    unused, start, width = COL_SPANS[base]
    part = join3(nt(split3(factor_ref[section, :, start : start + width]), u_ref[...]))
    value = gain * join3(nn(split3(part), v_ref[...]))
    unused, start, width = ROW_SPANS[base]
    for tile in range(tiles_of(width)):
        here = min(LANES, width - tile * LANES)
        row = (start // LANES + tile) * RANK
        part_ref[row : row + RANK, :here] = value[:, tile * LANES : tile * LANES + here]


DEC_GIVEN = [
    (K_NORMED, (SEQ, DD), bf16), (K_B_QKV, (SEQ, 3 * DD), bf16), (K_ATTENDED, (SEQ, DD), bf16), (K_B_PROJ, (SEQ, DD), bf16),
    (K_SECOND, (SEQ, DD), bf16), (K_B_UP, (SEQ, FFD), bf16), (K_ACTIVE, (SEQ, FFD), bf16), (K_B_DOWN, (SEQ, DD), bf16),
    (K_B_PRED, (SEQ - VIS, PATCH_PAD), bf16), (K_FINAL, (SEQ - VIS, DD), bf16), (K_SENT, (VIS, DE), bf16), (K_FIRST, (VIS, DD), bf16),
]
DEC_HELD = [
    (K_TOKENS, (SEQ, DD), f32), (K_JOINED, (SEQ, 3 * DD), bf16), (K_OUT, (SEQ, DD), f32), (K_LSE, (DD // LANES, 4, SEQ), f32),
    (K_MIDDLE, (SEQ, DD), f32), (K_SLOPE, (SEQ, FFD), f32), (K_GRAD, (SEQ, DD), f32), (K_ATT, (SEQ, DD), bf16),
    (K_DK, (SEQ, LANES), f32), (K_DV, (SEQ, LANES), f32), (K_SUMS, (16, DD), f32), (K_BIAS, (1, FFD), f32),
]


def decode_body(
    flat, coded, place, table, vec_ref, target, mask, count_ref, factor, *rest, tail_row, gain
):
    given_n, held_n, mats_n = len(DEC_GIVEN), len(DEC_HELD), len(section_shapes(1))
    given_out, grad_coded, sums_e, part_ref = rest[:given_n], rest[given_n], rest[given_n + 1], rest[given_n + 2]
    rest = rest[given_n + 3 :]
    have = dict(zip([name for name, shape, kind in DEC_GIVEN + DEC_HELD], rest[: given_n + held_n]))
    mats = rest[given_n + held_n : given_n + held_n + mats_n]
    slots, wide, total, vec_e, bias_e, vec_d, bias, extra, in_sems, out_sems = rest[given_n + held_n + mats_n :]
    take_rows(vec_ref, 0, DE, vec_e, bias_e)
    take_rows(vec_ref, 1, DD, vec_d, bias, extra)
    weights = Weights(flat, 1, [5, 0, 1, 2, 3, 4], slots, wide, mats, in_sems)
    copies = Copies(out_sems)
    blk = total.shape[0]
    sums, bias_sum = have[K_SUMS], have[K_BIAS]

    def give(*names):
        for name in names:
            which = [entry[0] for entry in DEC_GIVEN].index(name)
            copies.start(have[name], given_out[which])

    part_ref[...] = jnp.zeros_like(part_ref)
    sums[...] = jnp.zeros_like(sums)
    bias_sum[...] = jnp.zeros_like(bias_sum)

    w_emb = weights.take()
    hat_e, spread_e = norm_parts(coded[...])
    have[K_SENT][...] = (hat_e * vec_e[4:5] + vec_e[5:6]).astype(bf16)
    give(K_SENT)
    have[K_TOKENS][:VIS] = nn(have[K_SENT][...], w_emb[...]) + extra[...] + positions_of(place[:VIS], table)

    def fill(step):
        rows = pl.ds(pl.multiple_of(VIS + step * VIS, VIS), VIS)
        have[K_TOKENS][rows] = vec_d[10:11] + positions_of(place[rows], table)

    loop(SEQ // VIS - 1, fill)
    w_qkv = weights.take()
    over_blocks(
        SEQ, blk, lambda *refs: open_stage(*refs, vec_d, w_qkv), *[have[name] for name in (K_TOKENS, K_NORMED, K_JOINED)]
    )
    give(K_NORMED)
    attend_stage(have[K_JOINED], have[K_OUT], have[K_LSE], DD // HEADS_DEC)
    wo, w1, w2 = weights.take(), weights.take(), weights.take()
    keys = [K_TOKENS, K_OUT, K_ATTENDED, K_MIDDLE, K_SECOND, K_ACTIVE, K_SLOPE, K_GRAD]
    over_blocks(SEQ, blk, lambda *refs: close_stage(*refs, vec_d, bias, wo, w1, w2), *[have[name] for name in keys])
    give(K_ATTENDED, K_SECOND, K_ACTIVE)

    w_head = weights.take()
    count = count_ref[...]

    def head(step):
        rows = pl.ds(pl.multiple_of(VIS + step * VIS, VIS), VIS)
        late = rows_at(step, VIS)
        hat, spread = norm_parts(have[K_GRAD][rows])
        final = (hat * vec_d[4:5] + vec_d[5:6]).astype(bf16)
        have[K_FINAL][late] = final
        residual = nt(final, w_head[...]) - target[late].astype(f32)
        weight = mask[late]
        loss = jnp.sum(weight * jnp.mean(residual * residual, axis=1, keepdims=True), axis=0, keepdims=True) / count
        row = tail_row + VEC_TILES * RANK
        part_ref[row : row + RANK] += jnp.broadcast_to(loss, (RANK, LANES))
        b_pred = (weight * (2.0 * residual / PATCH) / count).astype(bf16)
        have[K_B_PRED][late, :PATCH] = b_pred
        have[K_B_PRED][late, PATCH:] = jnp.zeros((VIS, PATCH_PAD - PATCH), bf16)
        grad = nn(b_pred, w_head[...])
        have[K_GRAD][rows] = norm_back(grad, hat, spread, vec_d[4:5])
        sums[4:5] += column_sum(grad * hat)
        sums[5:6] += column_sum(grad)

    loop(SEQ // VIS - 1, head)
    have[K_GRAD][:VIS] = jnp.zeros((VIS, DD), f32)
    give(K_FINAL, K_B_PRED)

    keys = [K_GRAD, K_SLOPE, K_MIDDLE, K_B_DOWN, K_B_UP, K_B_PROJ, K_ATT]
    over_blocks(
        SEQ, blk, lambda *refs: back_up_stage(*refs, total, vec_d, wo, w1, w2, sums, bias_sum), *[have[name] for name in keys]
    )
    give(K_B_DOWN, K_B_UP, K_B_PROJ)
    attend_back_stage(
        have[K_JOINED], have[K_ATT], have[K_OUT], have[K_LSE], have[K_B_QKV], have[K_DK], have[K_DV], DD // HEADS_DEC
    )
    give(K_B_QKV)
    over_blocks(
        SEQ, blk, lambda *refs: back_in_stage(*refs, vec_d, w_qkv, sums), *[have[name] for name in (K_B_QKV, K_GRAD, K_TOKENS)]
    )
    first = have[K_GRAD][:VIS].astype(bf16)
    have[K_FIRST][...] = first
    give(K_FIRST)
    sums[10:11] = column_sum(have[K_GRAD][VIS:])
    back = nt(first, w_emb[...]).astype(bf16).astype(f32)
    grad_coded[...] = norm_back(back, hat_e, spread_e, vec_e[4:5])
    sums_e[...] = jnp.zeros_like(sums_e)
    sums_e[0:1] = column_sum(back * hat_e)
    sums_e[1:2] = column_sum(back)
    for line in range(11):
        put_vec(part_ref, tail_row, line * DD, sums[line : line + 1])
    put_vec(part_ref, tail_row, 11 * DD, bias_sum[...])
    put_vec(part_ref, tail_row, 11 * DD + FFD, column_sum(first))
    pairs = [(K_NORMED, K_B_QKV), (K_ATTENDED, K_B_PROJ), (K_SECOND, K_B_UP), (K_ACTIVE, K_B_DOWN), (K_B_PRED, K_FINAL), (K_SENT, K_FIRST)]
    for index, (a, b) in enumerate(pairs):
        put_left(part_ref, 1, index, factor, have[b], have[a], gain)
    for copy in copies.made:
        copy.wait()


def decode(flat, coded, place, table, vecs, target, mask, count, factor, tail_row, gain, rows):
    mats = section_shapes(1)
    dma = pltpu.SemaphoreType.DMA
    outs = pl.pallas_call(
        functools.partial(decode_body, tail_row=tail_row, gain=gain),
        in_specs=[ANYWHERE] + [WHOLE] * 8,
        out_specs=[ANYWHERE] * len(DEC_GIVEN) + [WHOLE] * 3,
        out_shape=[jax.ShapeDtypeStruct(shape, kind) for name, shape, kind in DEC_GIVEN]
        + [shape_of(VIS, DE), shape_of(8, DE), shape_of(rows, LANES)],
        scratch_shapes=[pltpu.VMEM(shape, kind) for name, shape, kind in DEC_GIVEN + DEC_HELD]
        + [pltpu.VMEM(shape, bf16) for shape in mats]
        + [
            pltpu.VMEM((2, flat_count(1), LANES), bf16), pltpu.VMEM((64 * FFD // LANES, LANES), f32),
            pltpu.VMEM((DEC_ROWS, DD), f32), pltpu.VMEM((16, DE), f32), pltpu.VMEM((1, FFE), f32), pltpu.VMEM((16, DD), f32),
            pltpu.VMEM((1, FFD), f32), pltpu.VMEM((1, DD), f32), dma((len(mats),)), dma((len(DEC_GIVEN),)),
        ],
        compiler_params=pltpu.CompilerParams(vmem_limit_bytes=BIG),
        name="decode",
    )(flat, coded, place, table, vecs, target, mask, count, factor)
    given = dict(zip([name for name, shape, kind in DEC_GIVEN], outs))
    return given, outs[-3], outs[-2], outs[-1]


ENC_GIVEN = [
    (K_B_QKV, (VIS, 3 * DE), bf16), (K_B_PROJ, (VIS, DE), bf16), (K_B_UP, (VIS, FFE), bf16), (K_B_DOWN, (VIS, DE), bf16),
    (K_START, (VIS, DE), bf16),
]
ENC_HELD = [
    (K_ATT, (VIS, DE), bf16), (K_DK, (VIS, LANES), f32), (K_DV, (VIS, LANES), f32), (K_SUMS, (16, DE), f32), (K_BIAS, (1, FFE), f32),
]
ENC_USED = [K_SLOPE, K_MIDDLE, K_JOINED, K_OUT, K_LSE, K_TOKENS, K_SECOND, K_ACTIVE, K_ATTENDED, K_NORMED]


def encode_back_body(*refs, tail_row, gain):
    used_n, given_n, held_n = len(ENC_USED), len(ENC_GIVEN), len(ENC_HELD)
    kept_in, mats_in, refs = refs[:used_n], refs[used_n : used_n + 4], refs[used_n + 4 :]
    grad_in, sums_e, vec_ref, pix, factor = refs[:5]
    given_out, part_ref, refs = refs[5 : 5 + given_n], refs[5 + given_n], refs[6 + given_n :]
    have = dict(zip(ENC_USED, refs[:used_n]))
    refs = refs[used_n:]
    have.update(zip([name for name, shape, kind in ENC_GIVEN + ENC_HELD], refs[: given_n + held_n]))
    mats = refs[given_n + held_n : given_n + held_n + 4]
    grad, total, vecs, bias_e, in_sems, out_sems = refs[given_n + held_n + 4 :]
    reads, copies = Copies(in_sems), Copies(out_sems)
    w2 = reads.start(mats_in[3], mats[3])
    take_rows(vec_ref, 0, DE, vecs, bias_e)
    waits = {name: reads.start(src, have[name]) for name, src in list(zip(ENC_USED, kept_in))[:2]}
    w1 = reads.start(mats_in[2], mats[2])
    wo = reads.start(mats_in[1], mats[1])
    waits.update({name: reads.start(src, have[name]) for name, src in list(zip(ENC_USED, kept_in))[2:]})
    w_qkv = reads.start(mats_in[0], mats[0])
    sums, bias_sum = have[K_SUMS], have[K_BIAS]

    def give(*names):
        for name in names:
            which = [entry[0] for entry in ENC_GIVEN].index(name)
            copies.start(have[name], given_out[which])

    part_ref[...] = jnp.zeros_like(part_ref)
    sums[...] = jnp.zeros_like(sums)
    bias_sum[...] = jnp.zeros_like(bias_sum)
    sums[4:5] = sums_e[0:1]
    sums[5:6] = sums_e[1:2]
    grad[...] = grad_in[...]
    for wait in (w2, waits[K_SLOPE], waits[K_MIDDLE], w1, wo):
        wait.wait()
    back_up_stage(
        grad, have[K_SLOPE], have[K_MIDDLE], have[K_B_DOWN], have[K_B_UP], have[K_B_PROJ], have[K_ATT], total,
        vecs, mats[1], mats[2], mats[3], sums, bias_sum,
    )
    give(K_B_DOWN, K_B_UP, K_B_PROJ)
    for name in (K_JOINED, K_OUT, K_LSE, K_TOKENS):
        waits[name].wait()
    attend_back_stage(
        have[K_JOINED], have[K_ATT], have[K_OUT], have[K_LSE], have[K_B_QKV], have[K_DK], have[K_DV], DE // HEADS_ENC
    )
    give(K_B_QKV)
    w_qkv.wait()
    back_in_stage(have[K_B_QKV], grad, have[K_TOKENS], vecs, mats[0], sums)
    start = grad[...].astype(bf16)
    have[K_START][...] = start
    give(K_START)
    sums[10:11] = column_sum(start)
    for line in range(11):
        put_vec(part_ref, tail_row, line * DE, sums[line : line + 1])
    put_vec(part_ref, tail_row, 11 * DE, bias_sum[...])
    for name in (K_SECOND, K_ACTIVE, K_ATTENDED, K_NORMED):
        waits[name].wait()
    pairs = [(K_NORMED, K_B_QKV), (K_ATTENDED, K_B_PROJ), (K_SECOND, K_B_UP), (K_ACTIVE, K_B_DOWN)]
    for index, (a, b) in enumerate(pairs):
        put_left(part_ref, 0, index, factor, have[b], have[a], gain)
    put_left(part_ref, 0, 4, factor, have[K_START], pix, gain)
    for copy in copies.made:
        copy.wait()


def encode_back(kept, mats, grad_coded, sums_e, vecs, pix, factor, tail_row, gain, rows):
    shapes = {name: (shape, kind) for name, shape, kind in ENC_KEPT}
    dma = pltpu.SemaphoreType.DMA
    outs = pl.pallas_call(
        functools.partial(encode_back_body, tail_row=tail_row, gain=gain),
        in_specs=[ANYWHERE] * (len(ENC_USED) + 4) + [WHOLE] * 5,
        out_specs=[ANYWHERE] * len(ENC_GIVEN) + [WHOLE],
        out_shape=[jax.ShapeDtypeStruct(shape, kind) for name, shape, kind in ENC_GIVEN] + [shape_of(rows, LANES)],
        scratch_shapes=[pltpu.VMEM(*shapes[name]) for name in ENC_USED]
        + [pltpu.VMEM(shape, kind) for name, shape, kind in ENC_GIVEN + ENC_HELD]
        + [pltpu.VMEM(shape, bf16) for shape in section_shapes(0)[:4]]
        + [
            pltpu.VMEM((VIS, DE), f32), pltpu.VMEM((VIS, DE), f32), pltpu.VMEM((16, DE), f32), pltpu.VMEM((1, FFE), f32),
            dma((len(ENC_USED) + 4,)), dma((len(ENC_GIVEN),)),
        ],
        compiler_params=pltpu.CompilerParams(vmem_limit_bytes=BIG),
        name="encode_back",
    )(*[kept[name] for name in ENC_USED], *mats[:4], grad_coded, sums_e, vecs, pix, factor)
    return dict(zip([name for name, shape, kind in ENC_GIVEN], outs)), outs[-1]


def tiles_of(width):
    return -(-width // LANES)


def spans(which):
    at, found = [], []
    for section in range(2):
        start = 0
        for shape in section_shapes(section):
            found.append((section, start, shape[which]))
            start += tiles_of(shape[which]) * LANES
        at.append(start)
    return found, at


ROW_SPANS, ROW_WIDTHS = spans(0)
COL_SPANS, COL_WIDTHS = spans(1)
ROW_PAD = max(ROW_WIDTHS)
VEC_TILES = -(-VLEN // (RANK * LANES))


def sum_rows(replicas, tiles):
    return -(-tiles // replicas) * replicas * RANK


def put_tiles(out_ref, section, start, value):
    width = value.shape[1]
    for tile in range(tiles_of(width)):
        here = min(LANES, width - tile * LANES)
        row = (start // LANES + tile) * RANK
        out_ref[section, row : row + RANK, :here] = value[:, tile * LANES : tile * LANES + here]


def chunk_rows(rows_n, cols_n):
    if rows_n == PATCH:
        return PATCH
    return 256


TAIL_STEPS = 24
MOST = max(chunk_rows(*shape) * shape[1] for which in range(2) for shape in section_shapes(which)) // LANES


def used_length(section):
    return sum(rows_n * cols_n for rows_n, cols_n in section_shapes(section))


TAIL_LENGTH = (FLAT - used_length(1)) // TAIL_STEPS


class Prep:
    def __init__(self, errors, factor, stack, left, raw, wide, made, pieces, total, raw_sem, out_sem):
        self.errors, self.factor, self.stack, self.left = errors, factor, stack, left
        self.raw, self.wide, self.made, self.pieces, self.total = raw, wide, made, pieces, total
        self.raw_sem, self.out_sem = raw_sem, out_sem

    def fetch(self, start, step, chunk):
        slot = lax.rem(chunk, 2)
        at = pl.multiple_of(start + chunk * step * LANES, 1024)
        return pltpu.make_async_copy(
            self.errors.at[:, :, pl.ds(at, step * LANES)], self.raw.at[slot, :, :, pl.ds(0, step * LANES)], self.raw_sem.at[slot]
        )

    def run(self, count, start, step, store, work):
        self.fetch(start, step, jnp.int32(0)).start()

        def one(chunk):
            slot = lax.rem(chunk, 2)

            @pl.when(chunk + 1 < count)
            def _():
                self.fetch(start, step, chunk + 1).start()

            self.fetch(start, step, chunk).wait()

            @pl.when(chunk >= 2)
            def _():
                store(chunk - 2, slot).wait()

            work(chunk, slot)
            store(chunk, slot).start()

        loop(count, one)
        for chunk in range(max(count - 2, 0), count):
            store(jnp.int32(chunk), chunk % 2).wait()

    def matrix(self, section, index):
        shapes = section_shapes(section)
        start = sum(rows_n * cols_n for rows_n, cols_n in shapes[:index])
        rows_n, cols_n = shapes[index]
        base = len(section_shapes(0)) * section + index
        blocks, rows = cols_n // LANES, chunk_rows(rows_n, cols_n)
        step, tiles = rows * blocks, tiles_of(rows)
        col_at, row_tile = COL_SPANS[base][1], ROW_SPANS[base][1] // LANES
        self.pieces[:, :cols_n] = split3(self.factor[:, col_at : col_at + cols_n])

        def store(chunk, slot):
            at = pl.multiple_of(start // LANES + chunk * step, 16)
            return pltpu.make_async_copy(
                self.made.at[slot, pl.ds(0, step)], self.stack.at[pl.ds(at, step)], self.out_sem.at[slot]
            )

        def work(chunk, slot):
            def widen_one(part):
                here = pl.ds(pl.multiple_of(part * LANES * LANES, 1024), LANES * LANES)
                self.wide[rows_at(part, LANES)] = self.raw[slot, 0, :, here].reshape(LANES, LANES).astype(f32)

            loop(step // LANES, widen_one)
            self.total[...] = jnp.zeros_like(self.total)

            def block_one(block):
                part = self.wide[pl.ds(block, rows, stride=blocks), :].astype(bf16)
                self.made[slot, rows_at(block, rows)] = part
                self.total[:rows] += nt(part, self.pieces[:, cols_at(block)])

            loop(blocks, block_one)
            value = join3(self.total[:rows].T)
            for tile in range(tiles):
                here = min(LANES, rows - tile * LANES)
                at = pl.multiple_of((row_tile + chunk * tiles + tile) * RANK, RANK)
                self.left[pl.ds(at, RANK), :here] = value[:, tile * LANES : tile * LANES + here]

        self.run(rows_n // rows, start, step, store, work)

def prep_scratch():
    dma = pltpu.SemaphoreType.DMA
    return [
        pltpu.VMEM((2, 1, 1, MOST * LANES), bf16), pltpu.VMEM((MOST, LANES), f32), pltpu.VMEM((2, MOST, LANES), bf16),
        pltpu.VMEM((3 * RANK, FFE), bf16), pltpu.VMEM((256, 3 * RANK), f32), dma((2,)), dma((2,)),
    ]


def ortho_stage(sum_ref, out_ref, wide, scale):
    rank_id = lax.broadcasted_iota(jnp.int32, (RANK, 1), 0)
    for section, start, width in ROW_SPANS:
        padded = tiles_of(width) * LANES
        for tile in range(padded // LANES):
            row = (start // LANES + tile) * RANK
            wide[:, tile * LANES : (tile + 1) * LANES] = sum_ref[section, row : row + RANK] * scale
        basis = wide[:, :padded]
        for column in range(RANK):
            current = basis[column : column + 1]
            current = current * lax.rsqrt(jnp.sum(current * current, axis=1, keepdims=True) + 1e-12)
            dots = jnp.sum(basis * current, axis=1, keepdims=True)
            basis = jnp.where(
                rank_id > column, basis - dots * current, jnp.where(rank_id == column, current, basis)
            )
        out_ref[section, :, start : start + padded] = basis


def err_plan(section):
    plan = []
    start = 0
    spans = [(row, col) for row, col in zip(ROW_SPANS, COL_SPANS) if row[0] == section]
    for (rows_n, cols_n), (row_span, col_span) in zip(section_shapes(section), spans):
        rows = chunk_rows(rows_n, cols_n)
        blocks = cols_n // LANES
        for chunk in range(rows_n // rows):
            plan.append((start // LANES + chunk * rows * blocks, rows, blocks, row_span[1] + chunk * rows, col_span[1], chunk))
        start += rows_n * cols_n
    return plan


def put_tiles(out_ref, row, value):
    for tile in range(value.shape[1] // LANES):
        out_ref[row + tile * RANK : row + (tile + 1) * RANK] = value[:, tile * LANES : (tile + 1) * LANES]


def rights_body(*refs, n, scale, gain):
    sum_ref, err_ref, u_in, v_in = refs[0], refs[1], refs[2 : 2 + n], refs[2 + n : 2 + 2 * n]
    ortho_ref, *part_refs, extra_ref = refs[2 + 2 * n : 6 + 2 * n]
    refs = refs[6 + 2 * n :]
    u_refs, v_refs = refs[:n], refs[n : 2 * n]
    wide, ring, ring_sems, in_sems = refs[2 * n :]
    section = lax.axis_index(SEC)
    depth = ring.shape[0]
    plans = [err_plan(which) for which in range(2)]

    def fetch(plan, index):
        at, rows, blocks = plan[index][:3]
        slot = index % depth
        return pltpu.make_async_copy(
            err_ref.at[pl.ds(at, rows * blocks)], ring.at[slot, pl.ds(0, rows * blocks)], ring_sems.at[slot]
        )

    for which, plan in enumerate(plans):

        @pl.when(section == which)
        def _():
            for index in range(depth - 1):
                fetch(plan, index).start()

    reads = Copies(in_sems)
    waits = [(reads.start(u_in[i], u_refs[i]), reads.start(v_in[i], v_refs[i])) for i in range(n)]
    ortho_stage(sum_ref, ortho_ref, wide, scale)
    extra_ref[...] = jnp.zeros_like(extra_ref)
    for part_ref in part_refs:
        part_ref[...] = jnp.zeros_like(part_ref)
    for which, plan in enumerate(plans):

        @pl.when(section == which)
        def _():
            for index, (at, rows, blocks, row_at, col_at, chunk) in enumerate(plan):
                if index + depth - 1 < len(plan):
                    fetch(plan, index + depth - 1).start()
                fetch(plan, index).wait()
                pieces = split3(ortho_ref[which, :, row_at : row_at + rows])
                for block in range(0, blocks, 2):
                    pair = [ring[index % depth, (block + side) * rows : (block + side + 1) * rows] for side in range(2)]
                    part = join3(nn(pieces, jnp.concatenate(pair, axis=1)))
                    row = (col_at // LANES + block) * RANK
                    for side in range(2):
                        extra_ref[row + side * RANK : row + (side + 1) * RANK] += part[:, side * LANES : (side + 1) * LANES]

    for (wait_u, wait_v), u_ref, v_ref, (which, row_at, rows), (unused, col_at, cols) in zip(waits, u_refs, v_refs, ROW_SPANS, COL_SPANS):
        wait_u.wait()
        wait_v.wait()
        padded = tiles_of(rows) * LANES
        part = join3(nt(split3(ortho_ref[which, :, row_at : row_at + padded]), u_ref[...]))
        put_tiles(part_refs[which], col_at // LANES * RANK, gain * join3(nn(split3(part), v_ref[...])))


def rights(sums, err, us, vs, scale, gain, rows):
    n = len(us)
    most = max(chunk_rows(*shape) * shape[1] // LANES for which in range(2) for shape in section_shapes(which))
    dma = pltpu.SemaphoreType.DMA
    return pl.pallas_call(
        functools.partial(rights_body, n=n, scale=scale, gain=gain),
        in_specs=[WHOLE] + [ANYWHERE] * (2 * n + 1),
        out_specs=[WHOLE] * 4,
        out_shape=[jax.ShapeDtypeStruct((2, RANK, ROW_PAD), f32)] + [shape_of(rows, LANES)] * 3,
        scratch_shapes=[pltpu.VMEM(x.shape, bf16) for x in [*us, *vs]]
        + [pltpu.VMEM((RANK, FFE), f32), pltpu.VMEM((4, most, LANES), bf16), dma((4,)), dma((2 * n,))],
        compiler_params=pltpu.CompilerParams(vmem_limit_bytes=BIG),
        name="rights",
    )(sums, err, *us, *vs)


def final_right_body(sum_ref, ortho_ref, left_ref, right_ref, norm_ref, *, scale, tail_row):
    vecs = left_ref[:, tail_row : tail_row + VEC_TILES * RANK]
    squares = jnp.sum(vecs * vecs, keepdims=True)[0]
    for (section, start, width), (unused, row_at, row_width) in zip(COL_SPANS, ROW_SPANS):
        for tile in range(width // LANES):
            row = (start // LANES + tile) * RANK
            right_ref[section, :, start + tile * LANES : start + (tile + 1) * LANES] = sum_ref[section, row : row + RANK] * scale
        o_part = ortho_ref[section, :, row_at : row_at + tiles_of(row_width) * LANES]
        r_part = right_ref[section, :, start : start + width]
        for line in range(RANK):
            gram_o = jnp.sum(o_part * o_part[line : line + 1], axis=1, keepdims=True)
            gram_r = jnp.sum(r_part * r_part[line : line + 1], axis=1, keepdims=True)
            squares = squares + jnp.sum(gram_o * gram_r, keepdims=True)
    for section in range(2):
        used = COL_WIDTHS[section]
        if used < right_ref.shape[2]:
            right_ref[section, :, used:] = jnp.zeros((RANK, right_ref.shape[2] - used), f32)
    norm_ref[...] = jnp.broadcast_to(jnp.sqrt(squares), norm_ref.shape)


def final_right(sums, ortho, lefts, cols, scale, tail_row):
    full = pl.BlockSpec(memory_space=pltpu.VMEM)
    return pl.pallas_call(
        functools.partial(final_right_body, scale=scale, tail_row=tail_row),
        in_specs=[full] * 3,
        out_specs=[full] * 2,
        out_shape=[jax.ShapeDtypeStruct((2, RANK, cols), f32), jax.ShapeDtypeStruct((1, LANES), f32)],
        name="final_right",
    )(sums, ortho, lefts)


def overlaps(first, count, me, shard):
    return (first < (me + 1) * shard) & (first + count > me * shard)


def finish_plan(section, heights):
    plan, start = [], 0
    for index, ((rows_n, cols_n), height) in enumerate(zip(section_shapes(section), heights)):
        base = len(section_shapes(0)) * section + index
        rows = chunk_rows(rows_n, cols_n)
        plan.append((start, rows_n // rows, rows, cols_n // LANES, rows_n, height, ROW_SPANS[base][1], COL_SPANS[base][1]))
        start += rows_n * cols_n
    return plan


def finish_section(
    section, heights, pairs, err, ortho, right, raw, err_out, app_out, a_slots, b_slots, lhs, left, ring, made, kept,
    raw_in, raw_out, pair_sems, ring_sem, made_sem, kept_sem, raw_sem, tail_sem, *, gain, shard,
):
    plan = finish_plan(section, heights)
    offsets = [sum(entry[1] for entry in plan[:index]) for index in range(len(plan) + 1)]
    flat_plan = [(index, chunk) for index, entry in enumerate(plan) for chunk in range(entry[1])]
    me = lax.axis_index(DP)

    def load(index):
        height, rows_n, cols_n = plan[index][5], tiles_of(plan[index][4]) * LANES, plan[index][3] * LANES
        slot, copies = index % 2, []
        for sample in range(2):
            for side, (slots, width) in enumerate(((a_slots, rows_n), (b_slots, cols_n))):
                copies.append(pltpu.make_async_copy(
                    pairs[sample][2 * index + side],
                    slots.at[slot, pl.ds(sample * height, height), pl.ds(0, width)], pair_sems.at[slot, 2 * sample + side],
                ))
        return copies

    def fetch(index, chunk):
        start, unused, rows, blocks = plan[index][:4]
        slot = lax.rem(offsets[index] + chunk, 2)
        at = pl.multiple_of(start // LANES + chunk * rows * blocks, 16)
        return pltpu.make_async_copy(
            err.at[pl.ds(at, rows * blocks)], ring.at[slot, pl.ds(0, rows * blocks)], ring_sem.at[slot]
        )

    def store(index, chunk):
        start, unused, rows, blocks = plan[index][:4]
        slot, count = lax.rem(offsets[index] + chunk, 2), rows * blocks * LANES
        at = pl.multiple_of(start + chunk * count, 1024)
        return pltpu.make_async_copy(
            made.at[slot, :, :, pl.ds(0, count)], err_out.at[:, :, pl.ds(at, count)], made_sem.at[slot]
        )

    steps = (FLAT - used_length(section)) // TAIL_LENGTH

    def tail_at(step):
        return pl.ds(pl.multiple_of(used_length(section) + step * TAIL_LENGTH, 1024), TAIL_LENGTH)

    def tail_in(step):
        slot = lax.rem(step, 2)
        return pltpu.make_async_copy(raw.at[:, :, tail_at(step)], raw_in.at[slot], raw_sem.at[slot])

    def tail_out(step):
        slot = lax.rem(step, 2)
        return pltpu.make_async_copy(raw_out.at[slot], err_out.at[:, :, tail_at(step)], tail_sem.at[slot])

    def tail_step(step):
        @pl.when(step < steps)
        def _():
            slot = lax.rem(step, 2)

            @pl.when(step + 1 < steps)
            def _():
                tail_in(step + 1).start()

            tail_in(step).wait()

            @pl.when(step >= 2)
            def _():
                tail_out(step - 2).wait()

            def one(part):
                here = pl.ds(pl.multiple_of(part * 2048, 1024), 2048)
                raw_out[slot, 0, :, here] = raw_in[slot, 0, :, here].astype(f32)

            loop(TAIL_LENGTH // 2048, one)
            tail_out(step).start()

    per_chunk = -(-steps // len(flat_plan))
    for copy in load(0):
        copy.start()
    fetch(0, jnp.int32(0)).start()
    if steps:
        tail_in(jnp.int32(0)).start()
    for index, (start, count, rows, blocks, rows_n, height, row_at, col_at) in enumerate(plan):
        for copy in load(index):
            copy.wait()
        if index + 1 < len(plan):
            for copy in load(index + 1):
                copy.start()
        pair_slot, step, wide_rows = index % 2, rows * blocks, tiles_of(rows) * LANES

        def one(chunk):
            slot = lax.rem(offsets[index] + chunk, 2)

            @pl.when(chunk + 1 < count)
            def _():
                fetch(index, chunk + 1).start()

            if index + 1 < len(plan):

                @pl.when(chunk + 1 == count)
                def _():
                    fetch(index + 1, jnp.int32(0)).start()

            o_part = ortho[section, :, pl.ds(pl.multiple_of(row_at + chunk * wide_rows, LANES), wide_rows)]
            o_high = o_part.astype(bf16)
            o_low = (o_part - o_high.astype(f32)).astype(bf16)
            left[:wide_rows] = jnp.concatenate([o_high, o_low, o_high], axis=0).T

            def turn(part):
                lhs[:, cols_at(part, 256)] = a_slots[pair_slot, rows_at(part, 256), cols_at(chunk, 256)].T

            loop(2 * height // 256, turn)
            fetch(index, chunk).wait()
            for back in range(2):
                before = offsets[index] + back - 2
                if before >= 0 and back < count:
                    old_index, old_chunk = flat_plan[before]

                    @pl.when(chunk == back)
                    def _():
                        store(old_index, jnp.int32(old_chunk)).wait()

            @pl.when(chunk >= 2)
            def _():
                store(index, chunk - 2).wait()

            first = start + chunk * step * LANES
            keep = overlaps(first, step * LANES, me, shard)
            lines = made.at[slot, 0, :, pl.ds(0, step * LANES)].reshape(step, LANES)

            def pair_one(pair):
                cols = cols_at(pair, 2 * LANES)
                r_part = right[section, :, pl.ds(pl.multiple_of(col_at + pair * 2 * LANES, LANES), 2 * LANES)]
                r_high = r_part.astype(bf16)
                r_low = (r_part - r_high.astype(f32)).astype(bf16)
                approx = nn(left[:rows], jnp.concatenate([r_high, r_high, r_low], axis=0))
                grad = nn(lhs[:rows, : 2 * height], b_slots[pair_slot, : 2 * height, cols])
                for side in range(2):
                    half = slice(side * LANES, (side + 1) * LANES)
                    block = 2 * pair + side
                    given = ring[slot, pl.ds(pl.multiple_of(block * rows, 16), rows)].astype(f32)
                    lines[pl.ds(block, rows, stride=blocks), :] = (gain * grad[:, half] + given) - approx[:, half]

                    @pl.when(keep)
                    def _():
                        kept[pl.ds(block, rows, stride=blocks), :] = approx[:, half]

            loop(blocks // 2, pair_one)
            store(index, chunk).start()
            for extra in range(per_chunk):
                tail_step((offsets[index] + chunk) * per_chunk + extra)

            @pl.when(keep)
            def _():
                at = pl.multiple_of(start // LANES + chunk * step, 16)
                copy = pltpu.make_async_copy(kept.at[pl.ds(0, step)], app_out.at[pl.ds(at, step)], kept_sem)
                copy.start()
                copy.wait()

        loop(count, one)
    for old_index, old_chunk in flat_plan[-2:]:
        store(old_index, jnp.int32(old_chunk)).wait()
    for step in range(max(steps - 2, 0), steps):
        tail_out(jnp.int32(step)).wait()


def finish_body(*refs, n_enc, n_dec, gain, shard, heights):
    mine, refs = refs[: n_enc + n_dec], refs[n_enc + n_dec :]
    theirs, refs = refs[: n_enc + n_dec], refs[n_enc + n_dec :]
    err, ortho, right, raw, err_out, app_out = refs[:6]
    a_enc, b_enc, a_dec, b_dec = refs[6:10]
    section = lax.axis_index(SEC)
    for which, (a_slots, b_slots, lo, hi) in enumerate(((a_enc, b_enc, 0, n_enc), (a_dec, b_dec, n_enc, n_enc + n_dec))):

        @pl.when(section == which)
        def _():
            finish_section(
                which, heights[which], (mine[lo:hi], theirs[lo:hi]), err, ortho, right, raw, err_out, app_out, a_slots, b_slots,
                *refs[10:], gain=gain, shard=shard,
            )


def finish(mine_e, mine_d, theirs_e, theirs_d, err, ortho, right, errors, gain, shard):
    n_enc, n_dec = len(mine_e), len(mine_d)
    heights = [[x.shape[0] for x in mine[::2]] for mine in (mine_e, mine_d)]
    dma = pltpu.SemaphoreType.DMA
    slots = []
    for which in range(2):
        for side in range(2):
            slots.append(pltpu.VMEM((2, 2 * max(heights[which]), max(shape[side] for shape in section_shapes(which))), bf16))
    total = 2 * (n_enc + n_dec)
    return pl.pallas_call(
        functools.partial(finish_body, n_enc=n_enc, n_dec=n_dec, gain=gain, shard=shard, heights=heights),
        in_specs=[ANYWHERE] * (total + 1) + [WHOLE] * 2 + [ANYWHERE],
        out_specs=[ANYWHERE] * 2,
        out_shape=[jax.ShapeDtypeStruct((1, 1, FLAT), f32), jax.ShapeDtypeStruct((FLAT // LANES, LANES), f32)],
        scratch_shapes=slots
        + [
            pltpu.VMEM((256, 2 * SEQ), bf16), pltpu.VMEM((256, 3 * RANK), bf16), pltpu.VMEM((2, MOST, LANES), bf16),
            pltpu.VMEM((2, 1, 1, MOST * LANES), f32), pltpu.VMEM((MOST, LANES), f32),
            pltpu.VMEM((2, 1, 1, TAIL_LENGTH), bf16), pltpu.VMEM((2, 1, 1, TAIL_LENGTH), f32),
            dma((2, 4)), dma((2,)), dma((2,)), dma(()), dma((2,)), dma((2,)),
        ],
        compiler_params=pltpu.CompilerParams(vmem_limit_bytes=BIG),
        name="finish",
    )(*mine_e, *mine_d, *theirs_e, *theirs_d, err, ortho, right, errors)


MESH = pl.DeviceIdType.MESH


def grid_of(replicas):
    side = 2 if replicas < 64 else 4
    return replicas // (side * side), side, side


def used_rows(section):
    counts = [sum(rows * cols for rows, cols in section_shapes(s)) // LANES for s in range(2)]
    return jnp.where(section == 0, counts[0], counts[1])


def meet(replicas):
    section, me = lax.axis_index(SEC), lax.axis_index(DP)
    barrier = pltpu.get_barrier_semaphore()
    pl.semaphore_signal(barrier, inc=1, device_id={SEC: 1 - section}, device_id_type=MESH)
    for step in range(1, replicas):
        pl.semaphore_signal(
            barrier, inc=1, device_id={DP: lax.rem(me + step, replicas)}, device_id_type=MESH
        )
    pl.semaphore_wait(barrier, replicas)


def gather_body(
    low_ref, cnt_ref, vec_ref, fac_ref, err_ref, flat_ref, cnts_ref, vec2_ref, fac2_ref, stack_ref, left_ref,
    send_sem, recv_sem, swap_sem, cnt_send, cnt_recv, side_send, side_recv, own_sem, *scratch, replicas, size,
):
    section, me = lax.axis_index(SEC), lax.axis_index(DP)
    other = 1 - section
    nz, ny, nx = grid_of(replicas)
    x, y, z = lax.rem(me, nx), lax.rem(me // nx, ny), me // (nx * ny)
    cut = size // 2 // 8 * 8 if size % 8 == 0 else size
    halves = [(0, cut), (cut, size - cut)] if cut < size else [(0, cut)]
    used = used_rows(section)
    used_other = used_rows(other)

    def block_id(at_z, at_y, at_x):
        return (at_z * ny + at_y) * nx + at_x

    meet(replicas)

    def side(src, dst, slot):
        return pltpu.make_async_remote_copy(
            src_ref=src, dst_ref=dst.at[section], send_sem=side_send.at[slot], recv_sem=side_recv.at[slot],
            device_id={SEC: other}, device_id_type=MESH,
        )

    def count_copy(step):
        return pltpu.make_async_remote_copy(
            src_ref=cnt_ref, dst_ref=cnts_ref.at[me], send_sem=cnt_send.at[step],
            recv_sem=cnt_recv.at[step], device_id={DP: lax.rem(me + step, replicas)}, device_id_type=MESH,
        )

    for step in range(1, replicas):
        count_copy(step).start()
    side(vec_ref, vec2_ref, 0).start()
    side(fac_ref, fac2_ref, 1).start()
    own = pltpu.make_async_copy(low_ref, flat_ref.at[section * replicas + me], own_sem)
    own.start()

    def copy(block, half, target, way, mine=False, swap=False):
        start, rows = halves[half]
        at = flat_ref.at[section * replicas + block, pl.ds(start, rows)]
        src = low_ref.at[pl.ds(start, rows)] if mine else at
        return pltpu.make_async_remote_copy(
            src_ref=src, dst_ref=at, send_sem=send_sem.at[block, half, way],
            recv_sem=(swap_sem if swap else recv_sem).at[block, half], device_id=target, device_id_type=MESH,
        )

    def needed(block, half, limit):
        return block * size + halves[half][0] < limit

    def at_z(value):
        return {DP: block_id(value, y, x)}

    def along_x(block, half, mine=False):
        for step in range(1, nx):
            copy(block, half, {DP: block_id(z, y, lax.rem(x + step, nx))}, 1 + step, mine).start()

    def along_y(block, half, mine=False):
        for step in range(1, ny):
            copy(block, half, {DP: block_id(z, lax.rem(y + step, ny), x)}, nx + step, mine).start()

    def across(block, half, mine=False):
        copy(block, half, {SEC: other}, nx + ny, mine, True).start()

    def arrived(block, half):
        copy(block, half, {SEC: other}, 0).wait_recv()

    def layers(k):
        return [z] if k == 0 else [z - k, z + k]

    def valid(at):
        return (at >= 0) & (at < nz)

    def first(k):
        for which, layer in enumerate(layers(k)):
            block = block_id(layer, y, x)
            for half in range(len(halves)):

                @pl.when(valid(layer) & needed(block, half, used))
                def _():
                    if k > 0:
                        arrived(block, half)
                    mine = k == 0
                    if k == 0 or which == 0:

                        @pl.when(z + 1 < nz)
                        def _():
                            copy(block, half, at_z(z + 1), 0, mine).start()

                    if k == 0 or which == 1:

                        @pl.when(z > 0)
                        def _():
                            copy(block, half, at_z(z - 1), 1, mine).start()

                    if half == 0:
                        along_x(block, half, mine)
                        along_y(block, half, mine)
                    else:
                        along_y(block, half, mine)
                        along_x(block, half, mine)
                    across(block, half, mine)

    def second(k):
        for layer in layers(k):
            for half in range(len(halves)):
                for step in range(1, nx if half == 0 else ny):
                    if half == 0:
                        block = block_id(layer, y, lax.rem(x + step, nx))
                    else:
                        block = block_id(layer, lax.rem(y + step, ny), x)

                    @pl.when(valid(layer) & needed(block, half, used))
                    def _():
                        arrived(block, half)
                        if half == 0:
                            along_y(block, half)
                        else:
                            along_x(block, half)
                        across(block, half)

    def third(k):
        for layer in layers(k):
            for half in range(len(halves)):
                for far in range(1, ny if half == 0 else nx):
                    for near in range(nx if half == 0 else ny):
                        if half == 0:
                            block = block_id(layer, lax.rem(y + far, ny), lax.rem(x + near, nx))
                        else:
                            block = block_id(layer, lax.rem(y + near, ny), lax.rem(x + far, nx))

                        @pl.when(valid(layer) & needed(block, half, used))
                        def _():
                            arrived(block, half)
                            across(block, half)

    prep = Prep(err_ref, fac_ref, stack_ref, left_ref, *scratch)
    left_ref[...] = jnp.zeros_like(left_ref)
    shares = [[[0], [2], [3], [1], [4]], [[0, 1], [2], [3], [4], [5]]]
    for k in range(nz + 2):
        if k < nz:
            first(k)
        if 0 <= k - 1 < nz:
            second(k - 1)
        if 0 <= k - 2 < nz:
            third(k - 2)
        for which in range(2):
            if k < len(shares[which]):

                @pl.when(section == which)
                def _():
                    for index in shares[which][k]:
                        prep.matrix(which, index)

    def drain(block, carry):
        at_x_, at_y_, at_z_ = lax.rem(block, nx), lax.rem(block // nx, ny), block // (nx * ny)
        for half in range(len(halves)):
            column = (at_x_ == x) & (at_y_ == y)

            @pl.when(needed(block, half, used))
            def _():
                @pl.when(column & (at_z_ <= z) & (z + 1 < nz))
                def _():
                    copy(block, half, {SEC: other}, 0).wait_send()

                @pl.when(column & (at_z_ >= z) & (z > 0))
                def _():
                    copy(block, half, {SEC: other}, 1).wait_send()

                single = len(halves) == 1
                sent_x = (column if half == 0 else at_x_ == x)
                sent_y = (at_y_ == y) if half == 0 else column

                @pl.when(sent_x)
                def _():
                    for step in range(1, nx):
                        copy(block, half, {SEC: other}, 1 + step).wait_send()

                @pl.when(sent_y)
                def _():
                    for step in range(1, ny):
                        copy(block, half, {SEC: other}, nx + step).wait_send()

                copy(block, half, {SEC: other}, nx + ny).wait_send()

            @pl.when(needed(block, half, used_other))
            def _():
                copy(block, half, {SEC: other}, 0, False, True).wait_recv()

        return carry

    lax.fori_loop(0, replicas, drain, 0)
    own.wait()
    for step in range(1, replicas):
        count_copy(step).wait()
    cnts_ref[me] = cnt_ref[...]
    vec2_ref[section] = vec_ref[...]
    fac2_ref[section] = fac_ref[...]
    side(vec_ref, vec2_ref, 0).wait()
    side(fac_ref, fac2_ref, 1).wait()


def update_body(master_ref, moment_ref, approx_ref, scale_ref, master_out, low_out, moment_out, own, sem):
    size = own.shape[0]
    first = lax.axis_index(DP) * size
    at = pl.multiple_of(first, RANK) if approx_ref.shape[0] > size else 0
    copy = pltpu.make_async_copy(approx_ref.at[pl.ds(at, size)], own, sem)
    copy.start()
    copy.wait()
    used = used_rows(lax.axis_index(SEC))
    inside = first + lax.broadcasted_iota(jnp.int32, (size, LANES), 0) < used
    approx = jnp.where(inside, own[...], 0.0)
    moment = moment_decay * moment_ref[...] + scale_ref[...] * approx.reshape(moment_ref.shape)
    moment_out[...] = moment
    master = master_ref[...] - learning_rate() * moment
    master_out[...] = master
    low_out[...] = master.astype(bf16)


def update(master, moment, approx, scale, size):
    return pl.pallas_call(
        update_body,
        in_specs=[WHOLE] * 2 + [ANYWHERE, WHOLE],
        out_specs=[WHOLE] * 3,
        out_shape=[
            jax.ShapeDtypeStruct(master.shape, f32), jax.ShapeDtypeStruct(master.shape, bf16),
            jax.ShapeDtypeStruct(master.shape, f32),
        ],
        scratch_shapes=[pltpu.VMEM((size, LANES), f32), pltpu.SemaphoreType.DMA(())],
        name="update",
    )(master, moment, approx, scale)


def cast_body(src_ref, out_ref):
    out_ref[...] = src_ref[...].reshape(out_ref.shape).astype(bf16)


def cast_shard(master, size):
    full = pl.BlockSpec(memory_space=pltpu.VMEM)
    return pl.pallas_call(
        cast_body, in_specs=[full], out_specs=full, out_shape=jax.ShapeDtypeStruct((size, LANES), bf16), name="cast"
    )(master)


def gather(low, cnt, vec, fac, errors, replicas, left_rows):
    size = low.shape[0]
    vmem = pl.BlockSpec(memory_space=pltpu.VMEM)
    nz, ny, nx = grid_of(replicas)
    dma = pltpu.SemaphoreType.DMA
    return pl.pallas_call(
        functools.partial(gather_body, replicas=replicas, size=size),
        in_specs=[vmem] * 4 + [ANYWHERE],
        out_specs=[ANYWHERE, vmem, vmem, vmem, ANYWHERE, vmem],
        out_shape=[
            jax.ShapeDtypeStruct((2 * replicas, size, LANES), bf16),
            jax.ShapeDtypeStruct((replicas,) + cnt.shape, f32),
            jax.ShapeDtypeStruct((2,) + vec.shape, f32),
            jax.ShapeDtypeStruct((2,) + fac.shape, f32),
            jax.ShapeDtypeStruct((FLAT // LANES, LANES), bf16),
            jax.ShapeDtypeStruct((left_rows, LANES), f32),
        ],
        scratch_shapes=[
            dma((replicas, 2, nx + ny + 1)), dma((replicas, 2)), dma((replicas, 2)),
            dma((replicas,)), dma((replicas,)), dma((2,)), dma((2,)), dma(()),
        ]
        + prep_scratch(),
        compiler_params=pltpu.CompilerParams(collective_id=2, has_side_effects=True, vmem_limit_bytes=BIG),
        name="gather",
    )(low, cnt, vec, fac, errors)


def sum_body(*refs, replicas, n_enc, n_dec):
    n = n_enc + n_dec
    sum_run(refs[:2], refs[2], refs[3 : 3 + n], refs[3 + n], refs[4 + n : 4 + 2 * n], *refs[4 + 2 * n :], replicas=replicas, n_enc=n_enc)


def sum_run(
    parts, extra_ref, given, total_ref, taken, mine, came, slots, seg, swap_send, swap_recv, send_a, recv_a, send_b, recv_b,
    give_sem, take_sem, *, replicas, n_enc,
):
    section, me = lax.axis_index(SEC), lax.axis_index(DP)
    other = 1 - section
    rows = extra_ref.shape[0]
    size = rows // replicas
    meet(replicas)

    def rows_of(index):
        return pl.ds(pl.multiple_of(index * size, 8), size)

    for which in range(2):

        @pl.when(section == which)
        def _():
            swap = pltpu.make_async_remote_copy(
                src_ref=parts[1 - which], dst_ref=came, send_sem=swap_send.at[0], recv_sem=swap_recv.at[0],
                device_id={SEC: other}, device_id_type=MESH,
            )
            swap.start()
            mine[...] = parts[which][...] + extra_ref[...]
            swap.wait()


    def give(i):
        return pltpu.make_async_remote_copy(
            src_ref=given[i], dst_ref=taken[i], send_sem=give_sem.at[i], recv_sem=take_sem.at[i],
            device_id={SEC: other}, device_id_type=MESH,
        )

    n = len(given)
    for i in range(n):

        @pl.when(section == (1 if i < n_enc else 0))
        def _():
            give(i).start()

    mine[...] = mine[...] + came[...]

    def scatter(step):
        peer = lax.rem(me + step, replicas)
        return pltpu.make_async_remote_copy(
            src_ref=mine.at[rows_of(peer)], dst_ref=slots.at[step], send_sem=send_a.at[step],
            recv_sem=recv_a.at[step], device_id={DP: peer}, device_id_type=MESH,
        )

    def spread(step):
        peer = lax.rem(me + step, replicas)
        return pltpu.make_async_remote_copy(
            src_ref=seg, dst_ref=total_ref.at[section, rows_of(me)], send_sem=send_b.at[step],
            recv_sem=recv_b.at[step], device_id={DP: peer}, device_id_type=MESH,
        )

    for step in range(1, replicas):
        scatter(step).start()
    total = mine[rows_of(me), :]
    for step in range(1, replicas):
        scatter(step).wait_recv()
        total = total + slots[step]
    seg[...] = total
    for step in range(1, replicas):
        spread(step).start()
    total_ref[section, rows_of(me)] = total
    for step in range(1, replicas):
        scatter(step).wait_send()
        spread(step).wait()
    back = pltpu.make_async_remote_copy(
        src_ref=total_ref.at[section], dst_ref=total_ref.at[section], send_sem=swap_send.at[1],
        recv_sem=swap_recv.at[1], device_id={SEC: other}, device_id_type=MESH,
    )
    back.start()
    back.wait()
    for i in range(n):

        @pl.when(section == (1 if i < n_enc else 0))
        def _():
            give(i).wait_send()

        @pl.when(section == (0 if i < n_enc else 1))
        def _():
            give(i).wait_recv()


def all_sum(parts, extra, replicas, collective_id, enc=(), dec=()):
    rows = extra.shape[0]
    vmem = pl.BlockSpec(memory_space=pltpu.VMEM)
    dma = pltpu.SemaphoreType.DMA
    size = rows // replicas
    given = list(enc) + list(dec)
    n = len(given)
    anywhere = pl.BlockSpec(memory_space=pl.ANY)
    outs = pl.pallas_call(
        functools.partial(sum_body, replicas=replicas, n_enc=len(enc), n_dec=len(dec)),
        in_specs=[vmem] * 3 + [anywhere] * n,
        out_specs=[vmem] + [anywhere] * n,
        out_shape=[jax.ShapeDtypeStruct((2, rows, LANES), f32)] + [jax.ShapeDtypeStruct(x.shape, x.dtype) for x in given],
        scratch_shapes=[
            pltpu.VMEM((rows, LANES), f32), pltpu.VMEM((rows, LANES), f32),
            pltpu.VMEM((replicas, size, LANES), f32), pltpu.VMEM((size, LANES), f32),
            dma((2,)), dma((2,)), dma((replicas,)), dma((replicas,)), dma((replicas,)), dma((replicas,)),
            dma((max(n, 1),)), dma((max(n, 1),)),
        ],
        compiler_params=pltpu.CompilerParams(collective_id=collective_id, has_side_effects=True),
        name="all_sum",
    )(*parts, extra, *given)
    return outs[0], outs[1 : 1 + len(enc)], outs[1 + len(enc) :]


def local(pixels, visible, masked, loss_mask, master, momentum, vectors, vec_moment, factors, errors):
    sec = lax.axis_index(SEC)
    replicas = lax.axis_size(DP)
    replica_id = lax.axis_index(DP)

    replicas_n = replicas
    shard_len = master.shape[1]
    size = shard_len // LANES
    gain = float(replicas)

    count_tile = jnp.full((RANK, LANES), jnp.sum(loss_mask).astype(f32))
    vec_tile = jnp.pad(vectors[0], (0, VEC_TILES * RANK * LANES - VLEN)).reshape(-1, LANES)
    left_rows = sum_rows(replicas, ROW_PAD // LANES + VEC_TILES + 1)
    flat_both, counts, vec_both, fac_both, err_stack, err_lefts = gather(
        cast_shard(master, size), count_tile, vec_tile, factors[0], errors, replicas, left_rows
    )
    low_both = flat_both.reshape(-1, LANES)
    count = jnp.sum(counts[:, 0, 0])

    vis = lax.dynamic_index_in_dim(visible, sec, 0, keepdims=False)
    mas = lax.dynamic_index_in_dim(masked, sec, 0, keepdims=False)
    mask_row = lax.dynamic_index_in_dim(loss_mask, sec, 0, keepdims=False).astype(f32)
    order = jnp.concatenate([vis, mas])
    pix = lax.dynamic_index_in_dim(pixels, sec, 0, keepdims=False)
    pick = (order[:, None] == jnp.arange(SEQ, dtype=jnp.int32)[None, :]).astype(bf16)
    pix_order = nn(pick, pix).astype(bf16)
    pix_vis = jnp.pad(pix_order[:VIS], ((0, 0), (0, PATCH_PAD - PATCH)))
    target = pix_order[VIS:]
    place = order[:, None]
    mask_col = mask_row[:, None]
    tail_row = ROW_PAD // LANES * RANK
    right_rows = sum_rows(replicas, max(COL_WIDTHS) // LANES)

    kept, enc = encode(low_both, pix_vis, place[:VIS], angle_tables(DE), vec_both)
    given, grad_coded, sums_e, part_d = decode(
        low_both, kept[K_CODED], place, angle_tables(DD), vec_both, target, mask_col, count.reshape(1, 1), fac_both, tail_row, gain, left_rows,
    )
    back, part_e = encode_back(kept, enc, grad_coded, sums_e, vec_both, pix_vis, fac_both, tail_row, gain, left_rows)
    pairs_e = [
        (kept[K_NORMED], back[K_B_QKV]), (kept[K_ATTENDED], back[K_B_PROJ]), (kept[K_SECOND], back[K_B_UP]),
        (kept[K_ACTIVE], back[K_B_DOWN]), (pix_vis, back[K_START]),
    ]
    pairs_d = [
        (given[K_NORMED], given[K_B_QKV]), (given[K_ATTENDED], given[K_B_PROJ]), (given[K_SECOND], given[K_B_UP]),
        (given[K_ACTIVE], given[K_B_DOWN]), (given[K_B_PRED], given[K_FINAL]), (given[K_SENT], given[K_FIRST]),
    ]
    pairs = pairs_e + pairs_d
    n_enc = len(pairs_e)
    flat_e = [x for pair in pairs_e for x in pair]
    flat_d = [x for pair in pairs_d for x in pair]
    early_e = [5, 6]
    late_e = [i for i in range(len(flat_e)) if i not in early_e]
    early_d = [5, 6]
    late_d = [i for i in range(len(flat_d)) if i not in early_d]
    left_sum, first_e, first_d = all_sum(
        (part_e, part_d), err_lefts, replicas, 3, [flat_e[i] for i in early_e], [flat_d[i] for i in early_d]
    )
    vec_sum = left_sum[:, tail_row : tail_row + VEC_TILES * RANK]
    loss_sum = left_sum[1, tail_row + VEC_TILES * RANK, 0]

    ortho, *right_parts, err_rights = rights(
        left_sum, err_stack, [a for a, b in pairs], [b for a, b in pairs], 1.0 / replicas, gain, right_rows
    )
    sums, second_e, second_d = all_sum(
        right_parts, err_rights, replicas, 4, [flat_e[i] for i in late_e], [flat_d[i] for i in late_d]
    )
    other_e = [x for i, x in sorted([*zip(early_e, first_e), *zip(late_e, second_e)], key=lambda entry: entry[0])]
    other_d = [x for i, x in sorted([*zip(early_d, first_d), *zip(late_d, second_d)], key=lambda entry: entry[0])]
    right_both, norm_row = final_right(sums, ortho, left_sum, factors.shape[2], 1.0 / replicas, tail_row)
    norm = norm_row[0, 0]
    scale = jnp.minimum(1.0, clip_limit / (norm + 1e-06))

    new_errors, approx = finish(
        flat_e, flat_d, other_e, other_d, err_stack, ortho, right_both, errors, gain, shard_len
    )
    if size % RANK:
        approx = lax.dynamic_slice_in_dim(approx, replica_id * size, size)
    rate = learning_rate()
    new_master, new_low, new_moment = update(master, momentum, approx, scale.reshape(1, 1), size)
    vec_own = lax.dynamic_index_in_dim(vec_sum, sec, 0, keepdims=False).reshape(-1)[:VLEN]
    new_vm = moment_decay * vec_moment[0] + scale * vec_own
    new_vectors = vectors[0] - rate * new_vm
    new_factors = lax.dynamic_index_in_dim(right_both, sec, 0, keepdims=False)
    return (
        new_master,
        new_low,
        new_moment,
        new_vectors[None],
        new_vm[None],
        new_factors[None],
        new_errors,
        loss_sum.reshape(1),
        norm.reshape(1),
    )


def solution(mesh):
    return jax.shard_map(
        local,
        mesh=mesh,
        in_specs=(
            P(DP, None, None),
            P(DP, None),
            P(DP, None),
            P(DP, None),
            P(SEC, DP),
            P(SEC, DP),
            P(SEC, None),
            P(SEC, None),
            P(SEC, None, None),
            P(SEC, DP, None),
        ),
        out_specs=(
            P(SEC, DP),
            P(SEC, DP),
            P(SEC, DP),
            P(SEC, None),
            P(SEC, None),
            P(SEC, None, None),
            P(SEC, DP, None),
            P(),
            P(),
        ),
        check_vma=False,
    )
```

```python
import functools
import math

import jax
import jax.numpy as jnp
import numpy as np
from jax import lax
from jax.experimental import pallas as pl
from jax.experimental.pallas import tpu as pltpu
from jax.sharding import PartitionSpec as P

DE = 768
FFE = 3072
HEADS_ENC = 12
DD = 512
FFD = 2048
HEADS_DEC = 16
PATCH = 192
PATCH_PAD = 256
RANK = 8
SEQ = 1024
VIS = 256
FLAT = 7225344
VLEN = 11520

(K_TOKENS, K_NORMED, K_JOINED, K_OUT, K_LSE, K_ATTENDED, K_MIDDLE, K_SECOND, K_ACTIVE, K_SLOPE, K_CODED, K_B_QKV, K_B_PROJ, K_B_UP, K_B_DOWN, K_B_PRED, K_FINAL, K_SENT, K_FIRST, K_GRAD, K_ATT, K_DK, K_DV, K_SUMS, K_BIAS, K_START) = range(26)

f32 = jnp.float32
bf16 = jnp.bfloat16
clip_limit = 0.0001
moment_decay = 0.9
rate_base = 0.5
LANES = 128
SEC, DP = "section", "dp"
STEP = 32
DEC_ROWS = 512
CHUNK = 256
BIG = 66000000


def nn(left, right):
    return lax.dot_general(left, right, (((1,), (0,)), ((), ())), preferred_element_type=f32)


def nt(left, right):
    return lax.dot_general(left, right, (((1,), (1,)), ((), ())), preferred_element_type=f32)


def tn(left, right):
    return lax.dot_general(left, right, (((0,), (0,)), ((), ())), preferred_element_type=f32)


def split3(value):
    high = value.astype(bf16)
    rest = value - high.astype(f32)
    middle = rest.astype(bf16)
    return jnp.concatenate([high, middle, (rest - middle.astype(f32)).astype(bf16)], axis=0)


def join3(value):
    return value[:RANK] + value[RANK : 2 * RANK] + value[2 * RANK :]


def norm_parts(tokens):
    centred = tokens - jnp.mean(tokens, axis=-1, keepdims=True)
    spread = lax.rsqrt(jnp.mean(centred * centred, axis=-1, keepdims=True) + 1e-06)
    return centred * spread, spread


def norm_back(grad, hat, spread, gain):
    inner = grad * gain
    return spread * (
        inner - jnp.mean(inner, axis=-1, keepdims=True) - hat * jnp.mean(inner * hat, axis=-1, keepdims=True)
    )


def column_sum(value):
    return jnp.sum(value.astype(f32), axis=0, keepdims=True)


def angle_tables(width):
    column = np.arange(width)
    freqs = np.exp(-(column // 2 * 2) / width * math.log(10000.0))
    coarse = (np.arange(0, SEQ, STEP)[:, None] * freqs).astype(np.float64)
    fine = np.arange(STEP)[:, None] * freqs + (column % 2) * (math.pi / 2)
    return jnp.asarray(np.stack([np.sin(coarse), np.cos(coarse), np.cos(fine), np.sin(fine)]), f32)


def positions_of(place, tables):
    column = lax.broadcasted_iota(jnp.int32, (1, STEP), 1)
    coarse = (place // STEP == column).astype(bf16)
    fine = (place % STEP == column).astype(bf16)

    def take(pick, table):
        high = table.astype(bf16)
        rest = table - high.astype(f32)
        middle = rest.astype(bf16)
        low = (rest - middle.astype(f32)).astype(bf16)
        return nn(pick, high) + nn(pick, middle) + nn(pick, low)

    return take(coarse, tables[0]) * take(fine, tables[2]) + take(coarse, tables[1]) * take(fine, tables[3])


def section_shapes(section):
    if section == 0:
        return [(DE, 3 * DE), (DE, DE), (DE, FFE), (FFE, DE), (PATCH, DE)]
    return [(DD, 3 * DD), (DD, DD), (DD, FFD), (FFD, DD), (PATCH, DD), (DE, DD)]


def learning_rate():
    return rate_base * math.sqrt(2.0 * (FLAT + VLEN) / DD) / clip_limit


def head_mask(head, size):
    lane = lax.broadcasted_iota(jnp.int32, (1, LANES), 1)
    return (lane // size == head).astype(bf16)


def attend_body(q_ref, k_ref, v_ref, o_ref, lse_ref, *, size, rows_q):
    seq = k_ref.shape[0]
    scale = size ** (-0.5)
    fold = scale * math.log2(math.e)
    turned = v_ref[...].T

    def one(step, carry):
        at = pl.ds(pl.multiple_of(step * rows_q, rows_q), rows_q)
        queries = q_ref[at, :]
        parts = []
        for head in range(LANES // size):
            scores = nt(k_ref[...], queries * head_mask(head, size))
            peak = jnp.max(scores, axis=0, keepdims=True) * fold
            power = jnp.exp2(scores * fold - peak)
            mass = jnp.sum(power, axis=0, keepdims=True)
            parts.append(nn(turned[head * size : (head + 1) * size], power.astype(bf16)) * (1.0 / mass))
            lse_ref[0, head : head + 1, at] = peak + jnp.log2(mass)
        o_ref[at, :] = jnp.concatenate(parts, axis=0).T
        return carry

    lax.fori_loop(0, seq // rows_q, one, 0)


def attend_back_body(q_ref, k_ref, v_ref, do_ref, o_ref, lse_ref, dq_ref, dk_ref, dv_ref, dk_sum, dv_sum, *, size, rows_q):
    seq = k_ref.shape[0]
    scale = size ** (-0.5)
    fold = scale * math.log2(math.e)
    turned = k_ref[...].T
    dk_sum[...] = jnp.zeros_like(dk_sum)
    dv_sum[...] = jnp.zeros_like(dv_sum)

    def one(step, carry):
        at = pl.ds(pl.multiple_of(step * rows_q, rows_q), rows_q)
        queries = q_ref[at, :]
        grads = do_ref[at, :]
        prod = grads.astype(f32) * o_ref[at, :]
        parts = []
        high = prod.astype(bf16)
        rest = prod - high.astype(f32)
        middle = rest.astype(bf16)
        for head in range(LANES // size):
            mask = head_mask(head, size)
            wide = jnp.broadcast_to(mask, (16, LANES))
            delta = (nt(wide, high) + nt(wide, middle))[0:1]
            q_one = queries * mask
            g_one = grads * mask
            scores = nt(k_ref[...], q_one)
            probs = jnp.exp2(scores * fold - lse_ref[0, head : head + 1, at])
            slope = nt(v_ref[...], g_one)
            grad_s = (probs * (slope - delta)).astype(bf16)
            dv_sum[...] += nn(probs.astype(bf16), g_one)
            dk_sum[...] += nn(grad_s, q_one)
            parts.append(nn(turned[head * size : (head + 1) * size], grad_s))
        dq_ref[at, :] = (jnp.concatenate(parts, axis=0).T * scale).astype(bf16)
        return carry

    lax.fori_loop(0, seq // rows_q, one, 0)
    dk_ref[...] = (dk_sum[...] * scale).astype(bf16)
    dv_ref[...] = dv_sum[...].astype(bf16)


def rows_at(step, count):
    return pl.ds(pl.multiple_of(step * count, count), count)


def cols_at(step, count=LANES):
    return pl.ds(pl.multiple_of(step * count, count), count)


def shape_of(rows, cols, dtype=f32):
    return jax.ShapeDtypeStruct((rows, cols), dtype)


def loop(count, body):
    def one(step, carry):
        body(step)
        return carry

    lax.fori_loop(0, count, one, 0)


def over_blocks(seq, rows, body, *refs):
    loop(seq // rows, lambda step: body(*[ref.at[rows_at(step, rows)] for ref in refs]))


def open_stage(tok_ref, normed_ref, joined_ref, vec_ref, w_ref):
    width = tok_ref.shape[1]
    hat, unused = norm_parts(tok_ref[...])
    normed = (hat * vec_ref[0:1] + vec_ref[1:2]).astype(bf16)
    normed_ref[...] = normed
    for part, bias in ((0, vec_ref[6:7]), (1, None), (2, vec_ref[7:8])):
        cols = slice(part * width, (part + 1) * width)
        value = nn(normed, w_ref[:, cols])
        joined_ref[:, cols] = (value if bias is None else value + bias).astype(bf16)


def attend_stage(joined, out, lse, size):
    seq, width = out.shape
    groups = width // LANES

    def one(group):
        attend_body(
            joined.at[:, cols_at(group)], joined.at[:, cols_at(groups + group)],
            joined.at[:, cols_at(2 * groups + group)], out.at[:, cols_at(group)], lse.at[pl.ds(group, 1)],
            size=size, rows_q=min(512, seq),
        )

    loop(groups, one)


def attend_back_stage(joined, grad_att, out, lse, b_qkv, dk_sum, dv_sum, size):
    seq, width = out.shape
    groups = width // LANES

    def one(group):
        here = [cols_at(part * groups + group) for part in range(3)]
        attend_back_body(
            *[joined.at[:, cols] for cols in here], grad_att.at[:, here[0]], out.at[:, here[0]],
            lse.at[pl.ds(group, 1)], *[b_qkv.at[:, cols] for cols in here], dk_sum, dv_sum,
            size=size, rows_q=min(512, seq),
        )

    loop(groups, one)


def close_stage(
    tok_ref, o_ref, att_ref, mid_ref, sec_ref, act_ref, slope_ref, out_ref, vec_ref, bias_ref, wo_ref, w1_ref, w2_ref
):
    attended = o_ref[...].astype(bf16)
    att_ref[...] = attended
    middle = tok_ref[...] + nn(attended, wo_ref[...]) + vec_ref[8:9]
    mid_ref[...] = middle
    hat, unused = norm_parts(middle)
    sec_ref[...] = (hat * vec_ref[2:3] + vec_ref[3:4]).astype(bf16)
    out_ref[...] = middle + vec_ref[9:10]

    def one(step):
        cols = cols_at(step, CHUNK)
        hidden = nn(sec_ref[...], w1_ref[:, cols]) + bias_ref[:, cols]
        share = 0.5 * (1.0 + lax.erf(hidden * math.sqrt(0.5)))
        active = (hidden * share).astype(bf16)
        act_ref[:, cols] = active
        slope_ref[:, cols] = share + hidden * (jnp.exp(-0.5 * hidden * hidden) * (1.0 / math.sqrt(2.0 * math.pi)))
        out_ref[...] += nn(active, w2_ref[cols, :])

    loop(w1_ref.shape[1] // CHUNK, one)


def back_up_stage(
    grad_ref, slope_ref, mid_ref, down_ref, up_ref, proj_ref, att_ref, total, vec_ref, wo_ref, w1_ref, w2_ref, sums_ref, bias_ref
):
    down = grad_ref[...].astype(bf16)
    down_ref[...] = down
    total[...] = jnp.zeros_like(total)

    def one(step):
        cols = cols_at(step, CHUNK)
        part = (nt(down_ref[...], w2_ref[cols, :]) * slope_ref[:, cols]).astype(bf16)
        up_ref[:, cols] = part
        bias_ref[:, cols] += column_sum(part)
        total[...] += nt(part, w1_ref[:, cols])

    loop(w1_ref.shape[1] // CHUNK, one)
    grad = total[...]
    hat, spread = norm_parts(mid_ref[...])
    middle = grad_ref[...] + norm_back(grad, hat, spread, vec_ref[2:3])
    grad_ref[...] = middle
    proj = middle.astype(bf16)
    proj_ref[...] = proj
    att_ref[...] = nt(proj, wo_ref[...]).astype(bf16)
    sums_ref[2:3] += column_sum(grad * hat)
    sums_ref[3:4] += column_sum(grad)
    sums_ref[8:9] += column_sum(proj)
    sums_ref[9:10] += column_sum(down)


def back_in_stage(join_ref, grad_ref, tok_ref, vec_ref, w_ref, sums_ref):
    width = tok_ref.shape[1]
    grad = nt(join_ref[...], w_ref[...])
    sums_ref[6:7] += column_sum(join_ref[:, :width])
    sums_ref[7:8] += column_sum(join_ref[:, 2 * width :])
    hat, spread = norm_parts(tok_ref[...])
    grad_ref[...] += norm_back(grad, hat, spread, vec_ref[0:1])
    sums_ref[0:1] += column_sum(grad * hat)
    sums_ref[1:2] += column_sum(grad)


def widen(flat_ref, wide, w_ref):
    rows_n, cols_n = w_ref.shape
    blocks = cols_n // LANES
    count = 64 * blocks

    def one(step):
        wide[:count] = flat_ref[rows_at(step, count), :].astype(f32)
        for block in range(blocks):
            w_ref[rows_at(step, 64), block * LANES : (block + 1) * LANES] = wide[
                pl.ds(block, 64, stride=blocks), :
            ].astype(bf16)

    loop(rows_n // 64, one)


class Weights:
    def __init__(self, flat, section, order, slots, wide, mats, sems):
        self.flat, self.slots, self.wide, self.mats, self.sems = flat, slots, wide, mats, sems
        self.order, self.shapes, self.next = order, section_shapes(section), 0
        self.base = section * (FLAT // LANES)
        for position in range(2):
            self.fetch(position).start()

    def fetch(self, position):
        index = self.order[position]
        start = self.base + sum(rows * cols for rows, cols in self.shapes[:index]) // LANES
        count = self.shapes[index][0] * self.shapes[index][1] // LANES
        return pltpu.make_async_copy(
            self.flat.at[pl.ds(start, count)], self.slots.at[position % 2, pl.ds(0, count)], self.sems.at[position]
        )

    def take(self):
        position = self.next
        self.fetch(position).wait()
        mat = self.mats[self.order[position]]
        widen(self.slots.at[position % 2], self.wide, mat)
        if position + 2 < len(self.order):
            self.fetch(position + 2).start()
        self.next += 1
        return mat


def take_rows(vec_ref, section, width, rows_ref, bias_ref, extra_ref=None):
    places = [(rows_ref, line, line * width, width) for line in range(11)]
    places.append((bias_ref, 0, 11 * width, bias_ref.shape[1]))
    if extra_ref is not None:
        places.append((extra_ref, 0, 11 * width + bias_ref.shape[1], width))
    for ref, line, offset, count in places:
        for tile in range(count // LANES):
            row = offset // LANES + tile
            ref[line : line + 1, tile * LANES : (tile + 1) * LANES] = vec_ref[section, row : row + 1]


class Copies:
    def __init__(self, sems):
        self.sems, self.made = sems, []

    def start(self, src, dst):
        copy = pltpu.make_async_copy(src, dst, self.sems.at[len(self.made)])
        copy.start()
        self.made.append(copy)
        return copy


def flat_count(section):
    return max(rows * cols for rows, cols in section_shapes(section)) // LANES


ANYWHERE = pl.BlockSpec(memory_space=pl.ANY)
WHOLE = pl.BlockSpec(memory_space=pltpu.VMEM)
ENC_KEPT = [
    (K_TOKENS, (VIS, DE), f32), (K_NORMED, (VIS, DE), bf16), (K_JOINED, (VIS, 3 * DE), bf16), (K_OUT, (VIS, DE), f32),
    (K_LSE, (DE // LANES, 2, VIS), f32), (K_ATTENDED, (VIS, DE), bf16), (K_MIDDLE, (VIS, DE), f32),
    (K_SECOND, (VIS, DE), bf16), (K_ACTIVE, (VIS, FFE), bf16), (K_SLOPE, (VIS, FFE), f32), (K_CODED, (VIS, DE), f32),
]


def encode_body(flat, pix, place, table, vec_ref, *rest):
    kept_n, mats_n = len(ENC_KEPT), len(section_shapes(0))
    kept_out, mats_out = rest[:kept_n], rest[kept_n : kept_n + mats_n]
    rest = rest[kept_n + mats_n :]
    kept = dict(zip([name for name, shape, kind in ENC_KEPT], rest[:kept_n]))
    mats = rest[kept_n : kept_n + mats_n]
    slots, wide, vecs, bias, in_sems, out_sems = rest[kept_n + mats_n :]
    take_rows(vec_ref, 0, DE, vecs, bias)
    weights = Weights(flat, 0, [4, 0, 1, 2, 3], slots, wide, mats, in_sems)
    copies = Copies(out_sems)

    def give(*names):
        for name in names:
            which = [entry[0] for entry in ENC_KEPT].index(name)
            copies.start(kept[name], kept_out[which])

    def take(index):
        mat = weights.take()
        copies.start(mat, mats_out[index])
        return mat

    kept[K_TOKENS][...] = positions_of(place[...], table) + vecs[10:11] + nn(pix[:, :PATCH], take(4)[...])
    open_stage(kept[K_TOKENS], kept[K_NORMED], kept[K_JOINED], vecs, take(0))
    give(K_TOKENS, K_NORMED, K_JOINED)
    attend_stage(kept[K_JOINED], kept[K_OUT], kept[K_LSE], DE // HEADS_ENC)
    give(K_OUT, K_LSE)
    wo, w1, w2 = take(1), take(2), take(3)
    keys = [K_TOKENS, K_OUT, K_ATTENDED, K_MIDDLE, K_SECOND, K_ACTIVE, K_SLOPE, K_CODED]
    close_stage(*[kept[name] for name in keys], vecs, bias, wo, w1, w2)
    give(K_ATTENDED, K_MIDDLE, K_SECOND, K_ACTIVE, K_SLOPE, K_CODED)
    for copy in copies.made:
        copy.wait()


def encode(flat, pix, place, table, vecs):
    mats = section_shapes(0)
    dma = pltpu.SemaphoreType.DMA
    outs = pl.pallas_call(
        encode_body,
        in_specs=[ANYWHERE] + [WHOLE] * 4,
        out_specs=[ANYWHERE] * (len(ENC_KEPT) + len(mats)),
        out_shape=[jax.ShapeDtypeStruct(shape, kind) for name, shape, kind in ENC_KEPT] + [shape_of(*shape, bf16) for shape in mats],
        scratch_shapes=[pltpu.VMEM(shape, kind) for name, shape, kind in ENC_KEPT]
        + [pltpu.VMEM(shape, bf16) for shape in mats]
        + [
            pltpu.VMEM((2, flat_count(0), LANES), bf16), pltpu.VMEM((64 * FFE // LANES, LANES), f32),
            pltpu.VMEM((16, DE), f32), pltpu.VMEM((1, FFE), f32), dma((len(mats),)), dma((len(ENC_KEPT) + len(mats),)),
        ],
        compiler_params=pltpu.CompilerParams(vmem_limit_bytes=BIG),
        name="encode",
    )(flat, pix, place, table, vecs)
    return dict(zip([name for name, shape, kind in ENC_KEPT], outs)), outs[len(ENC_KEPT) :]


def put_vec(part_ref, tail_row, offset, value):
    for tile in range(value.shape[1] // LANES):
        row = tail_row + offset // LANES + tile
        part_ref[row : row + 1] = value[:, tile * LANES : (tile + 1) * LANES]


def put_left(part_ref, section, index, factor_ref, u_ref, v_ref, gain):
    base = len(section_shapes(0)) * section + index
    unused, start, width = COL_SPANS[base]
    part = join3(nt(split3(factor_ref[section, :, start : start + width]), u_ref[...]))
    value = gain * join3(nn(split3(part), v_ref[...]))
    unused, start, width = ROW_SPANS[base]
    for tile in range(tiles_of(width)):
        here = min(LANES, width - tile * LANES)
        row = (start // LANES + tile) * RANK
        part_ref[row : row + RANK, :here] = value[:, tile * LANES : tile * LANES + here]


DEC_GIVEN = [
    (K_NORMED, (SEQ, DD), bf16), (K_B_QKV, (SEQ, 3 * DD), bf16), (K_ATTENDED, (SEQ, DD), bf16), (K_B_PROJ, (SEQ, DD), bf16),
    (K_SECOND, (SEQ, DD), bf16), (K_B_UP, (SEQ, FFD), bf16), (K_ACTIVE, (SEQ, FFD), bf16), (K_B_DOWN, (SEQ, DD), bf16),
    (K_B_PRED, (SEQ - VIS, PATCH_PAD), bf16), (K_FINAL, (SEQ - VIS, DD), bf16), (K_SENT, (VIS, DE), bf16), (K_FIRST, (VIS, DD), bf16),
]
DEC_HELD = [
    (K_TOKENS, (SEQ, DD), f32), (K_JOINED, (SEQ, 3 * DD), bf16), (K_OUT, (SEQ, DD), f32), (K_LSE, (DD // LANES, 4, SEQ), f32),
    (K_MIDDLE, (SEQ, DD), f32), (K_SLOPE, (SEQ, FFD), f32), (K_GRAD, (SEQ, DD), f32), (K_ATT, (SEQ, DD), bf16),
    (K_DK, (SEQ, LANES), f32), (K_DV, (SEQ, LANES), f32), (K_SUMS, (16, DD), f32), (K_BIAS, (1, FFD), f32),
]


def decode_body(
    flat, coded, place, table, vec_ref, target, mask, count_ref, factor, *rest, tail_row, gain
):
    given_n, held_n, mats_n = len(DEC_GIVEN), len(DEC_HELD), len(section_shapes(1))
    given_out, grad_coded, sums_e, part_ref = rest[:given_n], rest[given_n], rest[given_n + 1], rest[given_n + 2]
    rest = rest[given_n + 3 :]
    have = dict(zip([name for name, shape, kind in DEC_GIVEN + DEC_HELD], rest[: given_n + held_n]))
    mats = rest[given_n + held_n : given_n + held_n + mats_n]
    slots, wide, total, vec_e, bias_e, vec_d, bias, extra, in_sems, out_sems = rest[given_n + held_n + mats_n :]
    take_rows(vec_ref, 0, DE, vec_e, bias_e)
    take_rows(vec_ref, 1, DD, vec_d, bias, extra)
    weights = Weights(flat, 1, [5, 0, 1, 2, 3, 4], slots, wide, mats, in_sems)
    copies = Copies(out_sems)
    blk = total.shape[0]
    sums, bias_sum = have[K_SUMS], have[K_BIAS]

    def give(*names):
        for name in names:
            which = [entry[0] for entry in DEC_GIVEN].index(name)
            copies.start(have[name], given_out[which])

    part_ref[...] = jnp.zeros_like(part_ref)
    sums[...] = jnp.zeros_like(sums)
    bias_sum[...] = jnp.zeros_like(bias_sum)

    w_emb = weights.take()
    hat_e, spread_e = norm_parts(coded[...])
    have[K_SENT][...] = (hat_e * vec_e[4:5] + vec_e[5:6]).astype(bf16)
    give(K_SENT)
    have[K_TOKENS][:VIS] = nn(have[K_SENT][...], w_emb[...]) + extra[...] + positions_of(place[:VIS], table)

    def fill(step):
        rows = pl.ds(pl.multiple_of(VIS + step * VIS, VIS), VIS)
        have[K_TOKENS][rows] = vec_d[10:11] + positions_of(place[rows], table)

    loop(SEQ // VIS - 1, fill)
    w_qkv = weights.take()
    over_blocks(
        SEQ, blk, lambda *refs: open_stage(*refs, vec_d, w_qkv), *[have[name] for name in (K_TOKENS, K_NORMED, K_JOINED)]
    )
    give(K_NORMED)
    attend_stage(have[K_JOINED], have[K_OUT], have[K_LSE], DD // HEADS_DEC)
    wo, w1, w2 = weights.take(), weights.take(), weights.take()
    keys = [K_TOKENS, K_OUT, K_ATTENDED, K_MIDDLE, K_SECOND, K_ACTIVE, K_SLOPE, K_GRAD]
    over_blocks(SEQ, blk, lambda *refs: close_stage(*refs, vec_d, bias, wo, w1, w2), *[have[name] for name in keys])
    give(K_ATTENDED, K_SECOND, K_ACTIVE)

    w_head = weights.take()
    count = count_ref[...]

    def head(step):
        rows = pl.ds(pl.multiple_of(VIS + step * VIS, VIS), VIS)
        late = rows_at(step, VIS)
        hat, spread = norm_parts(have[K_GRAD][rows])
        final = (hat * vec_d[4:5] + vec_d[5:6]).astype(bf16)
        have[K_FINAL][late] = final
        residual = nt(final, w_head[...]) - target[late].astype(f32)
        weight = mask[late]
        loss = jnp.sum(weight * jnp.mean(residual * residual, axis=1, keepdims=True), axis=0, keepdims=True) / count
        row = tail_row + VEC_TILES * RANK
        part_ref[row : row + RANK] += jnp.broadcast_to(loss, (RANK, LANES))
        b_pred = (weight * (2.0 * residual / PATCH) / count).astype(bf16)
        have[K_B_PRED][late, :PATCH] = b_pred
        have[K_B_PRED][late, PATCH:] = jnp.zeros((VIS, PATCH_PAD - PATCH), bf16)
        grad = nn(b_pred, w_head[...])
        have[K_GRAD][rows] = norm_back(grad, hat, spread, vec_d[4:5])
        sums[4:5] += column_sum(grad * hat)
        sums[5:6] += column_sum(grad)

    loop(SEQ // VIS - 1, head)
    have[K_GRAD][:VIS] = jnp.zeros((VIS, DD), f32)
    give(K_FINAL, K_B_PRED)

    keys = [K_GRAD, K_SLOPE, K_MIDDLE, K_B_DOWN, K_B_UP, K_B_PROJ, K_ATT]
    over_blocks(
        SEQ, blk, lambda *refs: back_up_stage(*refs, total, vec_d, wo, w1, w2, sums, bias_sum), *[have[name] for name in keys]
    )
    give(K_B_DOWN, K_B_UP, K_B_PROJ)
    attend_back_stage(
        have[K_JOINED], have[K_ATT], have[K_OUT], have[K_LSE], have[K_B_QKV], have[K_DK], have[K_DV], DD // HEADS_DEC
    )
    give(K_B_QKV)
    over_blocks(
        SEQ, blk, lambda *refs: back_in_stage(*refs, vec_d, w_qkv, sums), *[have[name] for name in (K_B_QKV, K_GRAD, K_TOKENS)]
    )
    first = have[K_GRAD][:VIS].astype(bf16)
    have[K_FIRST][...] = first
    give(K_FIRST)
    sums[10:11] = column_sum(have[K_GRAD][VIS:])
    back = nt(first, w_emb[...]).astype(bf16).astype(f32)
    grad_coded[...] = norm_back(back, hat_e, spread_e, vec_e[4:5])
    sums_e[...] = jnp.zeros_like(sums_e)
    sums_e[0:1] = column_sum(back * hat_e)
    sums_e[1:2] = column_sum(back)
    for line in range(11):
        put_vec(part_ref, tail_row, line * DD, sums[line : line + 1])
    put_vec(part_ref, tail_row, 11 * DD, bias_sum[...])
    put_vec(part_ref, tail_row, 11 * DD + FFD, column_sum(first))
    pairs = [(K_NORMED, K_B_QKV), (K_ATTENDED, K_B_PROJ), (K_SECOND, K_B_UP), (K_ACTIVE, K_B_DOWN), (K_B_PRED, K_FINAL), (K_SENT, K_FIRST)]
    for index, (a, b) in enumerate(pairs):
        put_left(part_ref, 1, index, factor, have[b], have[a], gain)
    for copy in copies.made:
        copy.wait()


def decode(flat, coded, place, table, vecs, target, mask, count, factor, tail_row, gain, rows):
    mats = section_shapes(1)
    dma = pltpu.SemaphoreType.DMA
    outs = pl.pallas_call(
        functools.partial(decode_body, tail_row=tail_row, gain=gain),
        in_specs=[ANYWHERE] + [WHOLE] * 8,
        out_specs=[ANYWHERE] * len(DEC_GIVEN) + [WHOLE] * 3,
        out_shape=[jax.ShapeDtypeStruct(shape, kind) for name, shape, kind in DEC_GIVEN]
        + [shape_of(VIS, DE), shape_of(8, DE), shape_of(rows, LANES)],
        scratch_shapes=[pltpu.VMEM(shape, kind) for name, shape, kind in DEC_GIVEN + DEC_HELD]
        + [pltpu.VMEM(shape, bf16) for shape in mats]
        + [
            pltpu.VMEM((2, flat_count(1), LANES), bf16), pltpu.VMEM((64 * FFD // LANES, LANES), f32),
            pltpu.VMEM((DEC_ROWS, DD), f32), pltpu.VMEM((16, DE), f32), pltpu.VMEM((1, FFE), f32), pltpu.VMEM((16, DD), f32),
            pltpu.VMEM((1, FFD), f32), pltpu.VMEM((1, DD), f32), dma((len(mats),)), dma((len(DEC_GIVEN),)),
        ],
        compiler_params=pltpu.CompilerParams(vmem_limit_bytes=BIG),
        name="decode",
    )(flat, coded, place, table, vecs, target, mask, count, factor)
    given = dict(zip([name for name, shape, kind in DEC_GIVEN], outs))
    return given, outs[-3], outs[-2], outs[-1]


ENC_GIVEN = [
    (K_B_QKV, (VIS, 3 * DE), bf16), (K_B_PROJ, (VIS, DE), bf16), (K_B_UP, (VIS, FFE), bf16), (K_B_DOWN, (VIS, DE), bf16),
    (K_START, (VIS, DE), bf16),
]
ENC_HELD = [
    (K_ATT, (VIS, DE), bf16), (K_DK, (VIS, LANES), f32), (K_DV, (VIS, LANES), f32), (K_SUMS, (16, DE), f32), (K_BIAS, (1, FFE), f32),
]
ENC_USED = [K_SLOPE, K_MIDDLE, K_JOINED, K_OUT, K_LSE, K_TOKENS, K_SECOND, K_ACTIVE, K_ATTENDED, K_NORMED]


def encode_back_body(*refs, tail_row, gain):
    used_n, given_n, held_n = len(ENC_USED), len(ENC_GIVEN), len(ENC_HELD)
    kept_in, mats_in, refs = refs[:used_n], refs[used_n : used_n + 4], refs[used_n + 4 :]
    grad_in, sums_e, vec_ref, pix, factor = refs[:5]
    given_out, part_ref, refs = refs[5 : 5 + given_n], refs[5 + given_n], refs[6 + given_n :]
    have = dict(zip(ENC_USED, refs[:used_n]))
    refs = refs[used_n:]
    have.update(zip([name for name, shape, kind in ENC_GIVEN + ENC_HELD], refs[: given_n + held_n]))
    mats = refs[given_n + held_n : given_n + held_n + 4]
    grad, total, vecs, bias_e, in_sems, out_sems = refs[given_n + held_n + 4 :]
    reads, copies = Copies(in_sems), Copies(out_sems)
    w2 = reads.start(mats_in[3], mats[3])
    take_rows(vec_ref, 0, DE, vecs, bias_e)
    waits = {name: reads.start(src, have[name]) for name, src in list(zip(ENC_USED, kept_in))[:2]}
    w1 = reads.start(mats_in[2], mats[2])
    wo = reads.start(mats_in[1], mats[1])
    waits.update({name: reads.start(src, have[name]) for name, src in list(zip(ENC_USED, kept_in))[2:]})
    w_qkv = reads.start(mats_in[0], mats[0])
    sums, bias_sum = have[K_SUMS], have[K_BIAS]

    def give(*names):
        for name in names:
            which = [entry[0] for entry in ENC_GIVEN].index(name)
            copies.start(have[name], given_out[which])

    part_ref[...] = jnp.zeros_like(part_ref)
    sums[...] = jnp.zeros_like(sums)
    bias_sum[...] = jnp.zeros_like(bias_sum)
    sums[4:5] = sums_e[0:1]
    sums[5:6] = sums_e[1:2]
    grad[...] = grad_in[...]
    for wait in (w2, waits[K_SLOPE], waits[K_MIDDLE], w1, wo):
        wait.wait()
    back_up_stage(
        grad, have[K_SLOPE], have[K_MIDDLE], have[K_B_DOWN], have[K_B_UP], have[K_B_PROJ], have[K_ATT], total,
        vecs, mats[1], mats[2], mats[3], sums, bias_sum,
    )
    give(K_B_DOWN, K_B_UP, K_B_PROJ)
    for name in (K_JOINED, K_OUT, K_LSE, K_TOKENS):
        waits[name].wait()
    attend_back_stage(
        have[K_JOINED], have[K_ATT], have[K_OUT], have[K_LSE], have[K_B_QKV], have[K_DK], have[K_DV], DE // HEADS_ENC
    )
    give(K_B_QKV)
    w_qkv.wait()
    back_in_stage(have[K_B_QKV], grad, have[K_TOKENS], vecs, mats[0], sums)
    start = grad[...].astype(bf16)
    have[K_START][...] = start
    give(K_START)
    sums[10:11] = column_sum(start)
    for line in range(11):
        put_vec(part_ref, tail_row, line * DE, sums[line : line + 1])
    put_vec(part_ref, tail_row, 11 * DE, bias_sum[...])
    for name in (K_SECOND, K_ACTIVE, K_ATTENDED, K_NORMED):
        waits[name].wait()
    pairs = [(K_NORMED, K_B_QKV), (K_ATTENDED, K_B_PROJ), (K_SECOND, K_B_UP), (K_ACTIVE, K_B_DOWN)]
    for index, (a, b) in enumerate(pairs):
        put_left(part_ref, 0, index, factor, have[b], have[a], gain)
    put_left(part_ref, 0, 4, factor, have[K_START], pix, gain)
    for copy in copies.made:
        copy.wait()


def encode_back(kept, mats, grad_coded, sums_e, vecs, pix, factor, tail_row, gain, rows):
    shapes = {name: (shape, kind) for name, shape, kind in ENC_KEPT}
    dma = pltpu.SemaphoreType.DMA
    outs = pl.pallas_call(
        functools.partial(encode_back_body, tail_row=tail_row, gain=gain),
        in_specs=[ANYWHERE] * (len(ENC_USED) + 4) + [WHOLE] * 5,
        out_specs=[ANYWHERE] * len(ENC_GIVEN) + [WHOLE],
        out_shape=[jax.ShapeDtypeStruct(shape, kind) for name, shape, kind in ENC_GIVEN] + [shape_of(rows, LANES)],
        scratch_shapes=[pltpu.VMEM(*shapes[name]) for name in ENC_USED]
        + [pltpu.VMEM(shape, kind) for name, shape, kind in ENC_GIVEN + ENC_HELD]
        + [pltpu.VMEM(shape, bf16) for shape in section_shapes(0)[:4]]
        + [
            pltpu.VMEM((VIS, DE), f32), pltpu.VMEM((VIS, DE), f32), pltpu.VMEM((16, DE), f32), pltpu.VMEM((1, FFE), f32),
            dma((len(ENC_USED) + 4,)), dma((len(ENC_GIVEN),)),
        ],
        compiler_params=pltpu.CompilerParams(vmem_limit_bytes=BIG),
        name="encode_back",
    )(*[kept[name] for name in ENC_USED], *mats[:4], grad_coded, sums_e, vecs, pix, factor)
    return dict(zip([name for name, shape, kind in ENC_GIVEN], outs)), outs[-1]


def tiles_of(width):
    return -(-width // LANES)


def spans(which):
    at, found = [], []
    for section in range(2):
        start = 0
        for shape in section_shapes(section):
            found.append((section, start, shape[which]))
            start += tiles_of(shape[which]) * LANES
        at.append(start)
    return found, at


ROW_SPANS, ROW_WIDTHS = spans(0)
COL_SPANS, COL_WIDTHS = spans(1)
ROW_PAD = max(ROW_WIDTHS)
VEC_TILES = -(-VLEN // (RANK * LANES))


def sum_rows(replicas, tiles):
    return -(-tiles // replicas) * replicas * RANK


def put_tiles(out_ref, section, start, value):
    width = value.shape[1]
    for tile in range(tiles_of(width)):
        here = min(LANES, width - tile * LANES)
        row = (start // LANES + tile) * RANK
        out_ref[section, row : row + RANK, :here] = value[:, tile * LANES : tile * LANES + here]


def chunk_rows(rows_n, cols_n):
    if rows_n == PATCH:
        return PATCH
    return 256


TAIL_STEPS = 24
MOST = max(chunk_rows(*shape) * shape[1] for which in range(2) for shape in section_shapes(which)) // LANES


def used_length(section):
    return sum(rows_n * cols_n for rows_n, cols_n in section_shapes(section))


TAIL_LENGTH = (FLAT - used_length(1)) // TAIL_STEPS


class Prep:
    def __init__(self, errors, factor, stack, left, raw, wide, made, pieces, total, raw_sem, out_sem):
        self.errors, self.factor, self.stack, self.left = errors, factor, stack, left
        self.raw, self.wide, self.made, self.pieces, self.total = raw, wide, made, pieces, total
        self.raw_sem, self.out_sem = raw_sem, out_sem

    def fetch(self, start, step, chunk):
        slot = lax.rem(chunk, 2)
        at = pl.multiple_of(start + chunk * step * LANES, 1024)
        return pltpu.make_async_copy(
            self.errors.at[:, :, pl.ds(at, step * LANES)], self.raw.at[slot, :, :, pl.ds(0, step * LANES)], self.raw_sem.at[slot]
        )

    def run(self, count, start, step, store, work):
        self.fetch(start, step, jnp.int32(0)).start()

        def one(chunk):
            slot = lax.rem(chunk, 2)

            @pl.when(chunk + 1 < count)
            def _():
                self.fetch(start, step, chunk + 1).start()

            self.fetch(start, step, chunk).wait()

            @pl.when(chunk >= 2)
            def _():
                store(chunk - 2, slot).wait()

            work(chunk, slot)
            store(chunk, slot).start()

        loop(count, one)
        for chunk in range(max(count - 2, 0), count):
            store(jnp.int32(chunk), chunk % 2).wait()

    def matrix(self, section, index):
        shapes = section_shapes(section)
        start = sum(rows_n * cols_n for rows_n, cols_n in shapes[:index])
        rows_n, cols_n = shapes[index]
        base = len(section_shapes(0)) * section + index
        blocks, rows = cols_n // LANES, chunk_rows(rows_n, cols_n)
        step, tiles = rows * blocks, tiles_of(rows)
        col_at, row_tile = COL_SPANS[base][1], ROW_SPANS[base][1] // LANES
        self.pieces[:, :cols_n] = split3(self.factor[:, col_at : col_at + cols_n])

        def store(chunk, slot):
            at = pl.multiple_of(start // LANES + chunk * step, 16)
            return pltpu.make_async_copy(
                self.made.at[slot, pl.ds(0, step)], self.stack.at[pl.ds(at, step)], self.out_sem.at[slot]
            )

        def work(chunk, slot):
            def widen_one(part):
                here = pl.ds(pl.multiple_of(part * LANES * LANES, 1024), LANES * LANES)
                self.wide[rows_at(part, LANES)] = self.raw[slot, 0, :, here].reshape(LANES, LANES).astype(f32)

            loop(step // LANES, widen_one)
            self.total[...] = jnp.zeros_like(self.total)

            def block_one(block):
                part = self.wide[pl.ds(block, rows, stride=blocks), :].astype(bf16)
                self.made[slot, rows_at(block, rows)] = part
                self.total[:rows] += nt(part, self.pieces[:, cols_at(block)])

            loop(blocks, block_one)
            value = join3(self.total[:rows].T)
            for tile in range(tiles):
                here = min(LANES, rows - tile * LANES)
                at = pl.multiple_of((row_tile + chunk * tiles + tile) * RANK, RANK)
                self.left[pl.ds(at, RANK), :here] = value[:, tile * LANES : tile * LANES + here]

        self.run(rows_n // rows, start, step, store, work)

def prep_scratch():
    dma = pltpu.SemaphoreType.DMA
    return [
        pltpu.VMEM((2, 1, 1, MOST * LANES), bf16), pltpu.VMEM((MOST, LANES), f32), pltpu.VMEM((2, MOST, LANES), bf16),
        pltpu.VMEM((3 * RANK, FFE), bf16), pltpu.VMEM((256, 3 * RANK), f32), dma((2,)), dma((2,)),
    ]


def ortho_stage(sum_ref, out_ref, wide, scale):
    rank_id = lax.broadcasted_iota(jnp.int32, (RANK, 1), 0)
    for section, start, width in ROW_SPANS:
        padded = tiles_of(width) * LANES
        for tile in range(padded // LANES):
            row = (start // LANES + tile) * RANK
            wide[:, tile * LANES : (tile + 1) * LANES] = sum_ref[section, row : row + RANK] * scale
        basis = wide[:, :padded]
        for column in range(RANK):
            current = basis[column : column + 1]
            current = current * lax.rsqrt(jnp.sum(current * current, axis=1, keepdims=True) + 1e-12)
            dots = jnp.sum(basis * current, axis=1, keepdims=True)
            basis = jnp.where(
                rank_id > column, basis - dots * current, jnp.where(rank_id == column, current, basis)
            )
        out_ref[section, :, start : start + padded] = basis


def err_plan(section):
    plan = []
    start = 0
    spans = [(row, col) for row, col in zip(ROW_SPANS, COL_SPANS) if row[0] == section]
    for (rows_n, cols_n), (row_span, col_span) in zip(section_shapes(section), spans):
        rows = chunk_rows(rows_n, cols_n)
        blocks = cols_n // LANES
        for chunk in range(rows_n // rows):
            plan.append((start // LANES + chunk * rows * blocks, rows, blocks, row_span[1] + chunk * rows, col_span[1], chunk))
        start += rows_n * cols_n
    return plan


def put_tiles(out_ref, row, value):
    for tile in range(value.shape[1] // LANES):
        out_ref[row + tile * RANK : row + (tile + 1) * RANK] = value[:, tile * LANES : (tile + 1) * LANES]


def rights_body(*refs, n, scale, gain):
    sum_ref, err_ref, u_in, v_in = refs[0], refs[1], refs[2 : 2 + n], refs[2 + n : 2 + 2 * n]
    ortho_ref, *part_refs, extra_ref = refs[2 + 2 * n : 6 + 2 * n]
    refs = refs[6 + 2 * n :]
    u_refs, v_refs = refs[:n], refs[n : 2 * n]
    wide, ring, ring_sems, in_sems = refs[2 * n :]
    section = lax.axis_index(SEC)
    depth = ring.shape[0]
    plans = [err_plan(which) for which in range(2)]

    def fetch(plan, index):
        at, rows, blocks = plan[index][:3]
        slot = index % depth
        return pltpu.make_async_copy(
            err_ref.at[pl.ds(at, rows * blocks)], ring.at[slot, pl.ds(0, rows * blocks)], ring_sems.at[slot]
        )

    for which, plan in enumerate(plans):

        @pl.when(section == which)
        def _():
            for index in range(depth - 1):
                fetch(plan, index).start()

    reads = Copies(in_sems)
    waits = [(reads.start(u_in[i], u_refs[i]), reads.start(v_in[i], v_refs[i])) for i in range(n)]
    ortho_stage(sum_ref, ortho_ref, wide, scale)
    extra_ref[...] = jnp.zeros_like(extra_ref)
    for part_ref in part_refs:
        part_ref[...] = jnp.zeros_like(part_ref)
    for which, plan in enumerate(plans):

        @pl.when(section == which)
        def _():
            for index, (at, rows, blocks, row_at, col_at, chunk) in enumerate(plan):
                if index + depth - 1 < len(plan):
                    fetch(plan, index + depth - 1).start()
                fetch(plan, index).wait()
                pieces = split3(ortho_ref[which, :, row_at : row_at + rows])
                for block in range(0, blocks, 2):
                    pair = [ring[index % depth, (block + side) * rows : (block + side + 1) * rows] for side in range(2)]
                    part = join3(nn(pieces, jnp.concatenate(pair, axis=1)))
                    row = (col_at // LANES + block) * RANK
                    for side in range(2):
                        extra_ref[row + side * RANK : row + (side + 1) * RANK] += part[:, side * LANES : (side + 1) * LANES]

    for (wait_u, wait_v), u_ref, v_ref, (which, row_at, rows), (unused, col_at, cols) in zip(waits, u_refs, v_refs, ROW_SPANS, COL_SPANS):
        wait_u.wait()
        wait_v.wait()
        padded = tiles_of(rows) * LANES
        part = join3(nt(split3(ortho_ref[which, :, row_at : row_at + padded]), u_ref[...]))
        put_tiles(part_refs[which], col_at // LANES * RANK, gain * join3(nn(split3(part), v_ref[...])))


def rights(sums, err, us, vs, scale, gain, rows):
    n = len(us)
    most = max(chunk_rows(*shape) * shape[1] // LANES for which in range(2) for shape in section_shapes(which))
    dma = pltpu.SemaphoreType.DMA
    return pl.pallas_call(
        functools.partial(rights_body, n=n, scale=scale, gain=gain),
        in_specs=[WHOLE] + [ANYWHERE] * (2 * n + 1),
        out_specs=[WHOLE] * 4,
        out_shape=[jax.ShapeDtypeStruct((2, RANK, ROW_PAD), f32)] + [shape_of(rows, LANES)] * 3,
        scratch_shapes=[pltpu.VMEM(x.shape, bf16) for x in [*us, *vs]]
        + [pltpu.VMEM((RANK, FFE), f32), pltpu.VMEM((4, most, LANES), bf16), dma((4,)), dma((2 * n,))],
        compiler_params=pltpu.CompilerParams(vmem_limit_bytes=BIG),
        name="rights",
    )(sums, err, *us, *vs)


def final_right_body(sum_ref, ortho_ref, left_ref, right_ref, norm_ref, *, scale, tail_row):
    vecs = left_ref[:, tail_row : tail_row + VEC_TILES * RANK]
    squares = jnp.sum(vecs * vecs, keepdims=True)[0]
    for (section, start, width), (unused, row_at, row_width) in zip(COL_SPANS, ROW_SPANS):
        for tile in range(width // LANES):
            row = (start // LANES + tile) * RANK
            right_ref[section, :, start + tile * LANES : start + (tile + 1) * LANES] = sum_ref[section, row : row + RANK] * scale
        o_part = ortho_ref[section, :, row_at : row_at + tiles_of(row_width) * LANES]
        r_part = right_ref[section, :, start : start + width]
        for line in range(RANK):
            gram_o = jnp.sum(o_part * o_part[line : line + 1], axis=1, keepdims=True)
            gram_r = jnp.sum(r_part * r_part[line : line + 1], axis=1, keepdims=True)
            squares = squares + jnp.sum(gram_o * gram_r, keepdims=True)
    for section in range(2):
        used = COL_WIDTHS[section]
        if used < right_ref.shape[2]:
            right_ref[section, :, used:] = jnp.zeros((RANK, right_ref.shape[2] - used), f32)
    norm_ref[...] = jnp.broadcast_to(jnp.sqrt(squares), norm_ref.shape)


def final_right(sums, ortho, lefts, cols, scale, tail_row):
    full = pl.BlockSpec(memory_space=pltpu.VMEM)
    return pl.pallas_call(
        functools.partial(final_right_body, scale=scale, tail_row=tail_row),
        in_specs=[full] * 3,
        out_specs=[full] * 2,
        out_shape=[jax.ShapeDtypeStruct((2, RANK, cols), f32), jax.ShapeDtypeStruct((1, LANES), f32)],
        name="final_right",
    )(sums, ortho, lefts)


def overlaps(first, count, me, shard):
    return (first < (me + 1) * shard) & (first + count > me * shard)


def finish_plan(section, heights):
    plan, start = [], 0
    for index, ((rows_n, cols_n), height) in enumerate(zip(section_shapes(section), heights)):
        base = len(section_shapes(0)) * section + index
        rows = chunk_rows(rows_n, cols_n)
        plan.append((start, rows_n // rows, rows, cols_n // LANES, rows_n, height, ROW_SPANS[base][1], COL_SPANS[base][1]))
        start += rows_n * cols_n
    return plan


def finish_section(
    section, heights, pairs, err, ortho, right, raw, err_out, app_out, a_slots, b_slots, lhs, left, ring, made, kept,
    raw_in, raw_out, pair_sems, ring_sem, made_sem, kept_sem, raw_sem, tail_sem, *, gain, shard,
):
    plan = finish_plan(section, heights)
    offsets = [sum(entry[1] for entry in plan[:index]) for index in range(len(plan) + 1)]
    flat_plan = [(index, chunk) for index, entry in enumerate(plan) for chunk in range(entry[1])]
    me = lax.axis_index(DP)

    def load(index):
        height, rows_n, cols_n = plan[index][5], tiles_of(plan[index][4]) * LANES, plan[index][3] * LANES
        slot, copies = index % 2, []
        for sample in range(2):
            for side, (slots, width) in enumerate(((a_slots, rows_n), (b_slots, cols_n))):
                copies.append(pltpu.make_async_copy(
                    pairs[sample][2 * index + side],
                    slots.at[slot, pl.ds(sample * height, height), pl.ds(0, width)], pair_sems.at[slot, 2 * sample + side],
                ))
        return copies

    def fetch(index, chunk):
        start, unused, rows, blocks = plan[index][:4]
        slot = lax.rem(offsets[index] + chunk, 2)
        at = pl.multiple_of(start // LANES + chunk * rows * blocks, 16)
        return pltpu.make_async_copy(
            err.at[pl.ds(at, rows * blocks)], ring.at[slot, pl.ds(0, rows * blocks)], ring_sem.at[slot]
        )

    def store(index, chunk):
        start, unused, rows, blocks = plan[index][:4]
        slot, count = lax.rem(offsets[index] + chunk, 2), rows * blocks * LANES
        at = pl.multiple_of(start + chunk * count, 1024)
        return pltpu.make_async_copy(
            made.at[slot, :, :, pl.ds(0, count)], err_out.at[:, :, pl.ds(at, count)], made_sem.at[slot]
        )

    steps = (FLAT - used_length(section)) // TAIL_LENGTH

    def tail_at(step):
        return pl.ds(pl.multiple_of(used_length(section) + step * TAIL_LENGTH, 1024), TAIL_LENGTH)

    def tail_in(step):
        slot = lax.rem(step, 2)
        return pltpu.make_async_copy(raw.at[:, :, tail_at(step)], raw_in.at[slot], raw_sem.at[slot])

    def tail_out(step):
        slot = lax.rem(step, 2)
        return pltpu.make_async_copy(raw_out.at[slot], err_out.at[:, :, tail_at(step)], tail_sem.at[slot])

    def tail_step(step):
        @pl.when(step < steps)
        def _():
            slot = lax.rem(step, 2)

            @pl.when(step + 1 < steps)
            def _():
                tail_in(step + 1).start()

            tail_in(step).wait()

            @pl.when(step >= 2)
            def _():
                tail_out(step - 2).wait()

            raw_out[slot] = raw_in[slot].astype(f32)
            tail_out(step).start()

    per_chunk = -(-steps // len(flat_plan))
    for copy in load(0):
        copy.start()
    fetch(0, jnp.int32(0)).start()
    if steps:
        tail_in(jnp.int32(0)).start()
    for index, (start, count, rows, blocks, rows_n, height, row_at, col_at) in enumerate(plan):
        for copy in load(index):
            copy.wait()
        if index + 1 < len(plan):
            for copy in load(index + 1):
                copy.start()
        pair_slot, step, wide_rows = index % 2, rows * blocks, tiles_of(rows) * LANES

        def one(chunk):
            slot = lax.rem(offsets[index] + chunk, 2)

            @pl.when(chunk + 1 < count)
            def _():
                fetch(index, chunk + 1).start()

            if index + 1 < len(plan):

                @pl.when(chunk + 1 == count)
                def _():
                    fetch(index + 1, jnp.int32(0)).start()

            o_part = ortho[section, :, pl.ds(pl.multiple_of(row_at + chunk * wide_rows, LANES), wide_rows)]
            o_high = o_part.astype(bf16)
            o_low = (o_part - o_high.astype(f32)).astype(bf16)
            left[:wide_rows] = jnp.concatenate([o_high, o_low, o_high], axis=0).T

            def turn(part):
                lhs[:, cols_at(part, 256)] = a_slots[pair_slot, rows_at(part, 256), cols_at(chunk, 256)].T

            loop(2 * height // 256, turn)
            fetch(index, chunk).wait()
            for back in range(2):
                before = offsets[index] + back - 2
                if before >= 0 and back < count:
                    old_index, old_chunk = flat_plan[before]

                    @pl.when(chunk == back)
                    def _():
                        store(old_index, jnp.int32(old_chunk)).wait()

            @pl.when(chunk >= 2)
            def _():
                store(index, chunk - 2).wait()

            first = start + chunk * step * LANES
            keep = overlaps(first, step * LANES, me, shard)
            lines = made.at[slot, 0, :, pl.ds(0, step * LANES)].reshape(step, LANES)

            def pair_one(pair):
                cols = cols_at(pair, 2 * LANES)
                r_part = right[section, :, pl.ds(pl.multiple_of(col_at + pair * 2 * LANES, LANES), 2 * LANES)]
                r_high = r_part.astype(bf16)
                r_low = (r_part - r_high.astype(f32)).astype(bf16)
                approx = nn(left[:rows], jnp.concatenate([r_high, r_high, r_low], axis=0))
                grad = nn(lhs[:rows, : 2 * height], b_slots[pair_slot, : 2 * height, cols])
                for side in range(2):
                    half = slice(side * LANES, (side + 1) * LANES)
                    block = 2 * pair + side
                    given = ring[slot, pl.ds(pl.multiple_of(block * rows, 16), rows)].astype(f32)
                    lines[pl.ds(block, rows, stride=blocks), :] = (gain * grad[:, half] + given) - approx[:, half]

                    @pl.when(keep)
                    def _():
                        kept[pl.ds(block, rows, stride=blocks), :] = approx[:, half]

            loop(blocks // 2, pair_one)
            store(index, chunk).start()
            for extra in range(per_chunk):
                tail_step((offsets[index] + chunk) * per_chunk + extra)

            @pl.when(keep)
            def _():
                at = pl.multiple_of(start // LANES + chunk * step, 16)
                copy = pltpu.make_async_copy(kept.at[pl.ds(0, step)], app_out.at[pl.ds(at, step)], kept_sem)
                copy.start()
                copy.wait()

        loop(count, one)
    for old_index, old_chunk in flat_plan[-2:]:
        store(old_index, jnp.int32(old_chunk)).wait()
    for step in range(max(steps - 2, 0), steps):
        tail_out(jnp.int32(step)).wait()


def finish_body(*refs, n_enc, n_dec, gain, shard, heights):
    mine, refs = refs[: n_enc + n_dec], refs[n_enc + n_dec :]
    theirs, refs = refs[: n_enc + n_dec], refs[n_enc + n_dec :]
    err, ortho, right, raw, err_out, app_out = refs[:6]
    a_enc, b_enc, a_dec, b_dec = refs[6:10]
    section = lax.axis_index(SEC)
    for which, (a_slots, b_slots, lo, hi) in enumerate(((a_enc, b_enc, 0, n_enc), (a_dec, b_dec, n_enc, n_enc + n_dec))):

        @pl.when(section == which)
        def _():
            finish_section(
                which, heights[which], (mine[lo:hi], theirs[lo:hi]), err, ortho, right, raw, err_out, app_out, a_slots, b_slots,
                *refs[10:], gain=gain, shard=shard,
            )


def finish(mine_e, mine_d, theirs_e, theirs_d, err, ortho, right, errors, gain, shard):
    n_enc, n_dec = len(mine_e), len(mine_d)
    heights = [[x.shape[0] for x in mine[::2]] for mine in (mine_e, mine_d)]
    dma = pltpu.SemaphoreType.DMA
    slots = []
    for which in range(2):
        for side in range(2):
            slots.append(pltpu.VMEM((2, 2 * max(heights[which]), max(shape[side] for shape in section_shapes(which))), bf16))
    total = 2 * (n_enc + n_dec)
    return pl.pallas_call(
        functools.partial(finish_body, n_enc=n_enc, n_dec=n_dec, gain=gain, shard=shard, heights=heights),
        in_specs=[ANYWHERE] * (total + 1) + [WHOLE] * 2 + [ANYWHERE],
        out_specs=[ANYWHERE] * 2,
        out_shape=[jax.ShapeDtypeStruct((1, 1, FLAT), f32), jax.ShapeDtypeStruct((FLAT // LANES, LANES), f32)],
        scratch_shapes=slots
        + [
            pltpu.VMEM((256, 2 * SEQ), bf16), pltpu.VMEM((256, 3 * RANK), bf16), pltpu.VMEM((2, MOST, LANES), bf16),
            pltpu.VMEM((2, 1, 1, MOST * LANES), f32), pltpu.VMEM((MOST, LANES), f32),
            pltpu.VMEM((2, 1, 1, TAIL_LENGTH), bf16), pltpu.VMEM((2, 1, 1, TAIL_LENGTH), f32),
            dma((2, 4)), dma((2,)), dma((2,)), dma(()), dma((2,)), dma((2,)),
        ],
        compiler_params=pltpu.CompilerParams(vmem_limit_bytes=BIG),
        name="finish",
    )(*mine_e, *mine_d, *theirs_e, *theirs_d, err, ortho, right, errors)


MESH = pl.DeviceIdType.MESH


def grid_of(replicas):
    side = 2 if replicas < 64 else 4
    return replicas // (side * side), side, side


def routes(size, replicas):
    if size % 8:
        return [(0, size)], [(0, 2, 1)]
    if replicas >= 64:
        cut = size // 16 * 8
        return [(0, cut), (cut, size - cut)], [(0, 2, 1), (0, 1, 2)]
    short, long = size // 48 * 8, size // 24 * 8
    starts = [0, short, 2 * short, 2 * short + long, size]
    return [(start, end - start) for start, end in zip(starts, starts[1:])], [(0, 2, 1), (0, 1, 2), (2, 0, 1), (1, 0, 2)]


def used_rows(section):
    counts = [sum(rows * cols for rows, cols in section_shapes(s)) // LANES for s in range(2)]
    return jnp.where(section == 0, counts[0], counts[1])


def meet(replicas):
    section, me = lax.axis_index(SEC), lax.axis_index(DP)
    barrier = pltpu.get_barrier_semaphore()
    pl.semaphore_signal(barrier, inc=1, device_id={SEC: 1 - section}, device_id_type=MESH)
    for step in range(1, replicas):
        pl.semaphore_signal(
            barrier, inc=1, device_id={DP: lax.rem(me + step, replicas)}, device_id_type=MESH
        )
    pl.semaphore_wait(barrier, replicas)


def gather_body(
    low_ref, cnt_ref, vec_ref, fac_ref, err_ref, flat_ref, cnts_ref, vec2_ref, fac2_ref, stack_ref, left_ref,
    send_sem, recv_sem, swap_sem, cnt_send, cnt_recv, side_send, side_recv, own_sem, *scratch, replicas, size,
):
    section, me = lax.axis_index(SEC), lax.axis_index(DP)
    other = 1 - section
    nz, ny, nx = grid_of(replicas)
    x, y, z = lax.rem(me, nx), lax.rem(me // nx, ny), me // (nx * ny)
    parts, orders = routes(size, replicas)
    used = used_rows(section)
    used_other = used_rows(other)

    def block_id(at_z, at_y, at_x):
        return (at_z * ny + at_y) * nx + at_x

    meet(replicas)

    def side(src, dst, slot):
        return pltpu.make_async_remote_copy(
            src_ref=src, dst_ref=dst.at[section], send_sem=side_send.at[slot], recv_sem=side_recv.at[slot],
            device_id={SEC: other}, device_id_type=MESH,
        )

    def count_copy(step):
        return pltpu.make_async_remote_copy(
            src_ref=cnt_ref, dst_ref=cnts_ref.at[me], send_sem=cnt_send.at[step],
            recv_sem=cnt_recv.at[step], device_id={DP: lax.rem(me + step, replicas)}, device_id_type=MESH,
        )

    for step in range(1, replicas):
        count_copy(step).start()
    side(vec_ref, vec2_ref, 0).start()
    side(fac_ref, fac2_ref, 1).start()
    own = pltpu.make_async_copy(low_ref, flat_ref.at[section * replicas + me], own_sem)
    own.start()

    def copy(block, part, target, way, mine=False, swap=False):
        start, rows = parts[part]
        at = flat_ref.at[section * replicas + block, pl.ds(start, rows)]
        src = low_ref.at[pl.ds(start, rows)] if mine else at
        return pltpu.make_async_remote_copy(
            src_ref=src, dst_ref=at, send_sem=send_sem.at[block, part, way],
            recv_sem=(swap_sem if swap else recv_sem).at[block, part], device_id=target, device_id_type=MESH,
        )

    def needed(block, part, limit):
        return block * size + parts[part][0] < limit

    def ways(part, at_z, at_y, at_x):
        same = (at_z == z, at_y == y, at_x == x)
        order = orders[part]
        later = [functools.reduce(jnp.logical_and, [same[axis] for axis in order[order.index(axis) :]]) for axis in range(3)]
        rest = [same[axis] for axis in order[order.index(0) + 1 :]]
        moving = functools.reduce(jnp.logical_and, rest, at_z != z)
        found = [
            ((later[0] | (moving & (at_z < z))) & (z + 1 < nz), 0, {DP: block_id(z + 1, y, x)}),
            ((later[0] | (moving & (at_z > z))) & (z > 0), 1, {DP: block_id(z - 1, y, x)}),
        ]
        for step in range(1, nx):
            found.append((later[2], 1 + step, {DP: block_id(z, y, lax.rem(x + step, nx))}))
        for step in range(1, ny):
            found.append((later[1], nx + step, {DP: block_id(z, lax.rem(y + step, ny), x)}))
        return found

    everywhere = nx + ny
    for part in range(len(parts)):

        @pl.when(needed(me, part, used))
        def _():
            for go, way, target in ways(part, z, y, x):

                @pl.when(go)
                def _():
                    copy(me, part, target, way, True).start()

            copy(me, part, {SEC: other}, everywhere, True, True).start()

    def arrive(part, at_z, at_y, at_x, there):
        block = block_id(at_z, at_y, at_x)

        @pl.when(there & (at_z >= 0) & (at_z < nz) & needed(block, part, used))
        def _():
            copy(block, part, {SEC: other}, 0).wait_recv()
            for go, way, target in ways(part, at_z, at_y, at_x):

                @pl.when(go)
                def _():
                    copy(block, part, target, way).start()

            copy(block, part, {SEC: other}, everywhere, False, True).start()

    prep = Prep(err_ref, fac_ref, stack_ref, left_ref, *scratch)
    left_ref[...] = jnp.zeros_like(left_ref)
    shares = [[[0], [2], [3], [1], [4]], [[0, 1], [2], [3], [4], [5]]]
    sides = [(step_y, step_x) for step_y in range(ny) for step_x in range(nx)]

    def hop(step):
        for turns in range(3):
            far = step - turns
            for step_y, step_x in sides:
                if (step_y > 0) + (step_x > 0) != turns:
                    continue
                for sign in (-1, 1):
                    there = (far > 0) if turns == 0 or sign > 0 else (far >= 0)
                    for part in range(len(parts)):
                        arrive(
                            part, z + sign * far, lax.rem(y + step_y, ny), lax.rem(x + step_x, nx), there & (far < nz)
                        )
        for which in range(2):
            for late, indices in enumerate(shares[which]):

                @pl.when((section == which) & (step == late))
                def _():
                    for index in indices:
                        prep.matrix(which, index)

    loop(nz + 2, hop)

    def drain(block):
        at_x, at_y, at_z = lax.rem(block, nx), lax.rem(block // nx, ny), block // (nx * ny)
        for part in range(len(parts)):

            @pl.when(needed(block, part, used))
            def _():
                for go, way, target in ways(part, at_z, at_y, at_x):

                    @pl.when(go)
                    def _():
                        copy(block, part, {SEC: other}, way).wait_send()

                copy(block, part, {SEC: other}, everywhere).wait_send()

            @pl.when(needed(block, part, used_other))
            def _():
                copy(block, part, {SEC: other}, 0, False, True).wait_recv()

    loop(replicas, drain)
    own.wait()
    for step in range(1, replicas):
        count_copy(step).wait()
    cnts_ref[me] = cnt_ref[...]
    vec2_ref[section] = vec_ref[...]
    fac2_ref[section] = fac_ref[...]
    side(vec_ref, vec2_ref, 0).wait()
    side(fac_ref, fac2_ref, 1).wait()


def update_body(master_ref, moment_ref, approx_ref, scale_ref, master_out, low_out, moment_out, own, sem):
    size = own.shape[0]
    first = lax.axis_index(DP) * size
    at = pl.multiple_of(first, RANK) if approx_ref.shape[0] > size else 0
    copy = pltpu.make_async_copy(approx_ref.at[pl.ds(at, size)], own, sem)
    copy.start()
    copy.wait()
    used = used_rows(lax.axis_index(SEC))
    inside = first + lax.broadcasted_iota(jnp.int32, (size, LANES), 0) < used
    approx = jnp.where(inside, own[...], 0.0)
    moment = moment_decay * moment_ref[...] + scale_ref[...] * approx.reshape(moment_ref.shape)
    moment_out[...] = moment
    master = master_ref[...] - learning_rate() * moment
    master_out[...] = master
    low_out[...] = master.astype(bf16)


def update(master, moment, approx, scale, size):
    return pl.pallas_call(
        update_body,
        in_specs=[WHOLE] * 2 + [ANYWHERE, WHOLE],
        out_specs=[WHOLE] * 3,
        out_shape=[
            jax.ShapeDtypeStruct(master.shape, f32), jax.ShapeDtypeStruct(master.shape, bf16),
            jax.ShapeDtypeStruct(master.shape, f32),
        ],
        scratch_shapes=[pltpu.VMEM((size, LANES), f32), pltpu.SemaphoreType.DMA(())],
        name="update",
    )(master, moment, approx, scale)


def cast_body(src_ref, out_ref):
    out_ref[...] = src_ref[...].reshape(out_ref.shape).astype(bf16)


def cast_shard(master, size):
    full = pl.BlockSpec(memory_space=pltpu.VMEM)
    return pl.pallas_call(
        cast_body, in_specs=[full], out_specs=full, out_shape=jax.ShapeDtypeStruct((size, LANES), bf16), name="cast"
    )(master)


def gather(low, cnt, vec, fac, errors, replicas, left_rows):
    size = low.shape[0]
    vmem = pl.BlockSpec(memory_space=pltpu.VMEM)
    nz, ny, nx = grid_of(replicas)
    count = len(routes(size, replicas)[0])
    dma = pltpu.SemaphoreType.DMA
    return pl.pallas_call(
        functools.partial(gather_body, replicas=replicas, size=size),
        in_specs=[vmem] * 4 + [ANYWHERE],
        out_specs=[ANYWHERE, vmem, vmem, vmem, ANYWHERE, vmem],
        out_shape=[
            jax.ShapeDtypeStruct((2 * replicas, size, LANES), bf16),
            jax.ShapeDtypeStruct((replicas,) + cnt.shape, f32),
            jax.ShapeDtypeStruct((2,) + vec.shape, f32),
            jax.ShapeDtypeStruct((2,) + fac.shape, f32),
            jax.ShapeDtypeStruct((FLAT // LANES, LANES), bf16),
            jax.ShapeDtypeStruct((left_rows, LANES), f32),
        ],
        scratch_shapes=[
            dma((replicas, count, nx + ny + 1)), dma((replicas, count)), dma((replicas, count)),
            dma((replicas,)), dma((replicas,)), dma((2,)), dma((2,)), dma(()),
        ]
        + prep_scratch(),
        compiler_params=pltpu.CompilerParams(collective_id=2, has_side_effects=True, vmem_limit_bytes=BIG),
        name="gather",
    )(low, cnt, vec, fac, errors)


def sum_body(*refs, replicas, n_enc, n_dec):
    n = n_enc + n_dec
    sum_run(refs[:2], refs[2], refs[3 : 3 + n], refs[3 + n], refs[4 + n : 4 + 2 * n], *refs[4 + 2 * n :], replicas=replicas, n_enc=n_enc)


def sum_run(
    parts, extra_ref, given, total_ref, taken, mine, came, slots, seg, swap_send, swap_recv, send_a, recv_a, send_b, recv_b,
    give_sem, take_sem, *, replicas, n_enc,
):
    section, me = lax.axis_index(SEC), lax.axis_index(DP)
    other = 1 - section
    rows = extra_ref.shape[0]
    size = rows // replicas
    meet(replicas)

    def rows_of(index):
        return pl.ds(pl.multiple_of(index * size, 8), size)

    for which in range(2):

        @pl.when(section == which)
        def _():
            swap = pltpu.make_async_remote_copy(
                src_ref=parts[1 - which], dst_ref=came, send_sem=swap_send.at[0], recv_sem=swap_recv.at[0],
                device_id={SEC: other}, device_id_type=MESH,
            )
            swap.start()
            mine[...] = parts[which][...] + extra_ref[...]
            swap.wait()


    def give(i):
        return pltpu.make_async_remote_copy(
            src_ref=given[i], dst_ref=taken[i], send_sem=give_sem.at[i], recv_sem=take_sem.at[i],
            device_id={SEC: other}, device_id_type=MESH,
        )

    n = len(given)
    for i in range(n):

        @pl.when(section == (1 if i < n_enc else 0))
        def _():
            give(i).start()

    mine[...] = mine[...] + came[...]

    def scatter(step):
        peer = lax.rem(me + step, replicas)
        return pltpu.make_async_remote_copy(
            src_ref=mine.at[rows_of(peer)], dst_ref=slots.at[step], send_sem=send_a.at[step],
            recv_sem=recv_a.at[step], device_id={DP: peer}, device_id_type=MESH,
        )

    def spread(step):
        peer = lax.rem(me + step, replicas)
        return pltpu.make_async_remote_copy(
            src_ref=seg, dst_ref=total_ref.at[section, rows_of(me)], send_sem=send_b.at[step],
            recv_sem=recv_b.at[step], device_id={DP: peer}, device_id_type=MESH,
        )

    for step in range(1, replicas):
        scatter(step).start()
    total = mine[rows_of(me), :]
    for step in range(1, replicas):
        scatter(step).wait_recv()
        total = total + slots[step]
    seg[...] = total
    for step in range(1, replicas):
        spread(step).start()
    total_ref[section, rows_of(me)] = total
    for step in range(1, replicas):
        scatter(step).wait_send()
        spread(step).wait()
    back = pltpu.make_async_remote_copy(
        src_ref=total_ref.at[section], dst_ref=total_ref.at[section], send_sem=swap_send.at[1],
        recv_sem=swap_recv.at[1], device_id={SEC: other}, device_id_type=MESH,
    )
    back.start()
    back.wait()
    for i in range(n):

        @pl.when(section == (1 if i < n_enc else 0))
        def _():
            give(i).wait_send()

        @pl.when(section == (0 if i < n_enc else 1))
        def _():
            give(i).wait_recv()


def all_sum(parts, extra, replicas, collective_id, enc=(), dec=()):
    rows = extra.shape[0]
    vmem = pl.BlockSpec(memory_space=pltpu.VMEM)
    dma = pltpu.SemaphoreType.DMA
    size = rows // replicas
    given = list(enc) + list(dec)
    n = len(given)
    anywhere = pl.BlockSpec(memory_space=pl.ANY)
    outs = pl.pallas_call(
        functools.partial(sum_body, replicas=replicas, n_enc=len(enc), n_dec=len(dec)),
        in_specs=[vmem] * 3 + [anywhere] * n,
        out_specs=[vmem] + [anywhere] * n,
        out_shape=[jax.ShapeDtypeStruct((2, rows, LANES), f32)] + [jax.ShapeDtypeStruct(x.shape, x.dtype) for x in given],
        scratch_shapes=[
            pltpu.VMEM((rows, LANES), f32), pltpu.VMEM((rows, LANES), f32),
            pltpu.VMEM((replicas, size, LANES), f32), pltpu.VMEM((size, LANES), f32),
            dma((2,)), dma((2,)), dma((replicas,)), dma((replicas,)), dma((replicas,)), dma((replicas,)),
            dma((max(n, 1),)), dma((max(n, 1),)),
        ],
        compiler_params=pltpu.CompilerParams(collective_id=collective_id, has_side_effects=True),
        name="all_sum",
    )(*parts, extra, *given)
    return outs[0], outs[1 : 1 + len(enc)], outs[1 + len(enc) :]


def local(pixels, visible, masked, loss_mask, master, momentum, vectors, vec_moment, factors, errors):
    sec = lax.axis_index(SEC)
    replicas = lax.axis_size(DP)
    replica_id = lax.axis_index(DP)

    replicas_n = replicas
    shard_len = master.shape[1]
    size = shard_len // LANES
    gain = float(replicas)

    count_tile = jnp.full((RANK, LANES), jnp.sum(loss_mask).astype(f32))
    vec_tile = jnp.pad(vectors[0], (0, VEC_TILES * RANK * LANES - VLEN)).reshape(-1, LANES)
    left_rows = sum_rows(replicas, ROW_PAD // LANES + VEC_TILES + 1)
    flat_both, counts, vec_both, fac_both, err_stack, err_lefts = gather(
        cast_shard(master, size), count_tile, vec_tile, factors[0], errors, replicas, left_rows
    )
    low_both = flat_both.reshape(-1, LANES)
    count = jnp.sum(counts[:, 0, 0])

    vis = lax.dynamic_index_in_dim(visible, sec, 0, keepdims=False)
    mas = lax.dynamic_index_in_dim(masked, sec, 0, keepdims=False)
    mask_row = lax.dynamic_index_in_dim(loss_mask, sec, 0, keepdims=False).astype(f32)
    order = jnp.concatenate([vis, mas])
    pix = lax.dynamic_index_in_dim(pixels, sec, 0, keepdims=False)
    pick = (order[:, None] == jnp.arange(SEQ, dtype=jnp.int32)[None, :]).astype(bf16)
    pix_order = nn(pick, pix).astype(bf16)
    pix_vis = jnp.pad(pix_order[:VIS], ((0, 0), (0, PATCH_PAD - PATCH)))
    target = pix_order[VIS:]
    place = order[:, None]
    mask_col = mask_row[:, None]
    tail_row = ROW_PAD // LANES * RANK
    right_rows = sum_rows(replicas, max(COL_WIDTHS) // LANES)

    kept, enc = encode(low_both, pix_vis, place[:VIS], angle_tables(DE), vec_both)
    given, grad_coded, sums_e, part_d = decode(
        low_both, kept[K_CODED], place, angle_tables(DD), vec_both, target, mask_col, count.reshape(1, 1), fac_both, tail_row, gain, left_rows,
    )
    back, part_e = encode_back(kept, enc, grad_coded, sums_e, vec_both, pix_vis, fac_both, tail_row, gain, left_rows)
    pairs_e = [
        (kept[K_NORMED], back[K_B_QKV]), (kept[K_ATTENDED], back[K_B_PROJ]), (kept[K_SECOND], back[K_B_UP]),
        (kept[K_ACTIVE], back[K_B_DOWN]), (pix_vis, back[K_START]),
    ]
    pairs_d = [
        (given[K_NORMED], given[K_B_QKV]), (given[K_ATTENDED], given[K_B_PROJ]), (given[K_SECOND], given[K_B_UP]),
        (given[K_ACTIVE], given[K_B_DOWN]), (given[K_B_PRED], given[K_FINAL]), (given[K_SENT], given[K_FIRST]),
    ]
    pairs = pairs_e + pairs_d
    n_enc = len(pairs_e)
    flat_e = [x for pair in pairs_e for x in pair]
    flat_d = [x for pair in pairs_d for x in pair]
    early_e = [5, 6]
    late_e = [i for i in range(len(flat_e)) if i not in early_e]
    early_d = [5, 6]
    late_d = [i for i in range(len(flat_d)) if i not in early_d]
    left_sum, first_e, first_d = all_sum(
        (part_e, part_d), err_lefts, replicas, 3, [flat_e[i] for i in early_e], [flat_d[i] for i in early_d]
    )
    vec_sum = left_sum[:, tail_row : tail_row + VEC_TILES * RANK]
    loss_sum = left_sum[1, tail_row + VEC_TILES * RANK, 0]

    ortho, *right_parts, err_rights = rights(
        left_sum, err_stack, [a for a, b in pairs], [b for a, b in pairs], 1.0 / replicas, gain, right_rows
    )
    sums, second_e, second_d = all_sum(
        right_parts, err_rights, replicas, 4, [flat_e[i] for i in late_e], [flat_d[i] for i in late_d]
    )
    other_e = [x for i, x in sorted([*zip(early_e, first_e), *zip(late_e, second_e)], key=lambda entry: entry[0])]
    other_d = [x for i, x in sorted([*zip(early_d, first_d), *zip(late_d, second_d)], key=lambda entry: entry[0])]
    right_both, norm_row = final_right(sums, ortho, left_sum, factors.shape[2], 1.0 / replicas, tail_row)
    norm = norm_row[0, 0]
    scale = jnp.minimum(1.0, clip_limit / (norm + 1e-06))

    new_errors, approx = finish(
        flat_e, flat_d, other_e, other_d, err_stack, ortho, right_both, errors, gain, shard_len
    )
    if size % RANK:
        approx = lax.dynamic_slice_in_dim(approx, replica_id * size, size)
    rate = learning_rate()
    new_master, new_low, new_moment = update(master, momentum, approx, scale.reshape(1, 1), size)
    vec_own = lax.dynamic_index_in_dim(vec_sum, sec, 0, keepdims=False).reshape(-1)[:VLEN]
    new_vm = moment_decay * vec_moment[0] + scale * vec_own
    new_vectors = vectors[0] - rate * new_vm
    new_factors = lax.dynamic_index_in_dim(right_both, sec, 0, keepdims=False)
    return (
        new_master,
        new_low,
        new_moment,
        new_vectors[None],
        new_vm[None],
        new_factors[None],
        new_errors,
        loss_sum.reshape(1),
        norm.reshape(1),
    )


def solution(mesh):
    return jax.shard_map(
        local,
        mesh=mesh,
        in_specs=(
            P(DP, None, None),
            P(DP, None),
            P(DP, None),
            P(DP, None),
            P(SEC, DP),
            P(SEC, DP),
            P(SEC, None),
            P(SEC, None),
            P(SEC, None, None),
            P(SEC, DP, None),
        ),
        out_specs=(
            P(SEC, DP),
            P(SEC, DP),
            P(SEC, DP),
            P(SEC, None),
            P(SEC, None),
            P(SEC, None, None),
            P(SEC, DP, None),
            P(),
            P(),
        ),
        check_vma=False,
    )
```
